32 devices in a mesh: dp: 4 (over y, z), cp: 8 (over x, core).
Axes of the slice: x: 4, y: 2, z: 2, core: 2. Of those that a mesh axis runs over, the one named last changes fastest.
The devices are a block of a 4x4x8 slice.
Arguments:
- x_act: bfloat16 [12288, 2048], P(('dp', 'cp')), parts along dimension 0
- seg_ids: int32 [12288], P(('dp', 'cp')), parts along dimension 0
- w_q: bfloat16 [2048, 32, 64], replicated
- w_k: bfloat16 [2048, 8, 64], replicated
- w_v: bfloat16 [2048, 8, 64], replicated
- w_o: bfloat16 [2048, 32, 64], replicated
- dy_act: bfloat16 [12288, 2048], P(('dp', 'cp')), parts along dimension 0
Outputs:
- output 1: bfloat16 [12288, 2048], P(('dp', 'cp')), parts along dimension 0
- output 2: bfloat16 [12288, 2048], P(('dp', 'cp')), parts along dimension 0
- output 3: float32 [8192, 32, 64], P(('dp', 'cp')), parts along dimension 0
- output 4: float32 [8192, 8, 64], P(('dp', 'cp')), parts along dimension 0
- output 5: float32 [8192, 8, 64], P(('dp', 'cp')), parts along dimension 0
- output 6: float32 [8192, 32, 64], P(('dp', 'cp')), parts along dimension 0
There are 4 independent parts. The reference program is written for one: setup_inputs(seed, part) draws one part's arguments, and reference() takes and returns one part's arrays. A program takes and returns all parts, laid end to end along the dimension named above; an argument that names none is the same for every part.
All inputs are finite; a program needn't handle non-finite values.
Results may differ from the reference program's by a relative error of at most 0.02.
Values are sent between devices in bfloat16 or wider.
A program may use at most 768 MiB of HBM per device.

```python
import jax
import jax.numpy as jnp
from jax import lax

CP_SIZE = 8
TOK_DEV = 384
MODEL_DIM = 2048
Q_HEADS = 32
KV_HEADS = 8
HEAD_DIM = 64

SEQ_LEN = CP_SIZE * TOK_DEV
GROUP_SIZE = Q_HEADS // KV_HEADS
Q_BLOCK = min(TOK_DEV, 128)
N_BLOCKS = SEQ_LEN // Q_BLOCK


def draw_segments(seg_key):
    key_zone, key_kind, key_short = jax.random.split(seg_key, 3)
    positions = jnp.arange(SEQ_LEN)
    zone_start = (jax.random.randint(key_zone, (SEQ_LEN,), 0, 2 * TOK_DEV) == 0) | (positions == 0)
    zone_index = jnp.cumsum(zone_start.astype(jnp.int32))
    parity = jax.random.randint(key_kind, (), 0, 2)
    short_zone = (zone_index + parity) % 2 == 0
    short_start = jax.random.randint(key_short, (SEQ_LEN,), 0, max(TOK_DEV // 8, 2)) == 0
    starts = zone_start | (short_zone & short_start)
    return (jnp.cumsum(starts.astype(jnp.int32)) - 1).astype(jnp.int32)


def setup_inputs(seed: int = 0, part: int = 0) -> dict:
    base_key = jax.random.key(seed)
    part_key = jax.random.fold_in(base_key, part)
    weight_key = jax.random.fold_in(base_key, 1000003)
    key_seg, key_x, key_dy = jax.random.split(part_key, 3)
    key_q, key_k, key_v, key_o = jax.random.split(weight_key, 4)
    in_scale = MODEL_DIM ** -0.5
    out_scale = (Q_HEADS * HEAD_DIM) ** -0.5
    q_shape = (MODEL_DIM, Q_HEADS, HEAD_DIM)
    kv_shape = (MODEL_DIM, KV_HEADS, HEAD_DIM)
    return {
        'x_act': jax.random.normal(key_x, (SEQ_LEN, MODEL_DIM), jnp.float32).astype(jnp.bfloat16),
        'seg_ids': draw_segments(key_seg),
        'w_q': (1.5 * in_scale * jax.random.normal(key_q, q_shape, jnp.float32)).astype(jnp.bfloat16),
        'w_k': (in_scale * jax.random.normal(key_k, kv_shape, jnp.float32)).astype(jnp.bfloat16),
        'w_v': (in_scale * jax.random.normal(key_v, kv_shape, jnp.float32)).astype(jnp.bfloat16),
        'w_o': (out_scale * jax.random.normal(key_o, q_shape, jnp.float32)).astype(jnp.bfloat16),
        'dy_act': jax.random.normal(key_dy, (SEQ_LEN, MODEL_DIM), jnp.float32).astype(jnp.bfloat16),
    }


def product32(einsum_form, left_arg, right_arg):
    return jnp.einsum(einsum_form, left_arg.astype(jnp.float32), right_arg.astype(jnp.float32))


def reference(x_act, seg_ids, w_q, w_k, w_v, w_o, dy_act):
    score_scale = HEAD_DIM ** -0.5
    w_q4 = w_q.reshape(MODEL_DIM, KV_HEADS, GROUP_SIZE, HEAD_DIM)
    w_o4 = w_o.reshape(MODEL_DIM, KV_HEADS, GROUP_SIZE, HEAD_DIM)
    q_all = product32('sm,mkgd->skgd', x_act, w_q4).astype(jnp.bfloat16)
    k_all = product32('sm,mkd->skd', x_act, w_k).astype(jnp.bfloat16)
    v_all = product32('sm,mkd->skd', x_act, w_v).astype(jnp.bfloat16)
    do_all = product32('qm,mkgd->qkgd', dy_act, w_o4).astype(jnp.bfloat16)
    k_wide = k_all.astype(jnp.float32)
    v_wide = v_all.astype(jnp.float32)
    key_pos = jnp.arange(SEQ_LEN)

    def block_step(carry_in, block_in):
        dk_acc, dv_acc = carry_in
        q_blk, do_blk, seg_blk, first_pos = block_in
        q_wide = q_blk.astype(jnp.float32)
        do_wide = do_blk.astype(jnp.float32)
        query_pos = first_pos + jnp.arange(Q_BLOCK)
        allowed = (seg_blk[:, None] == seg_ids[None, :]) & (key_pos[None, :] <= query_pos[:, None])
        scores = jnp.einsum('qkgd,skd->kqgs', q_wide, k_wide) * score_scale
        scores = jnp.where(allowed[None, :, None, :], scores, -jnp.inf)
        attn_prob = jax.nn.softmax(scores, axis=-1)
        prob_half = attn_prob.astype(jnp.bfloat16).astype(jnp.float32)
        out_blk = jnp.einsum('kqgs,skd->kqgd', prob_half, v_wide).astype(jnp.bfloat16)
        row_delta = jnp.einsum('qkgd,kqgd->kqg', do_wide, out_blk.astype(jnp.float32))
        dprobs = jnp.einsum('qkgd,skd->kqgs', do_wide, v_wide)
        dscores = (attn_prob * (dprobs - row_delta[..., None])).astype(jnp.bfloat16).astype(jnp.float32)
        dq_blk = (jnp.einsum('kqgs,skd->kqgd', dscores, k_wide) * score_scale).astype(jnp.bfloat16)
        dk_acc = dk_acc + jnp.einsum('kqgs,qkgd->skd', dscores, q_wide)
        dv_acc = dv_acc + jnp.einsum('kqgs,qkgd->skd', prob_half, do_wide)
        return (dk_acc, dv_acc), (out_blk, dq_blk)

    zeros_kv = jnp.zeros((SEQ_LEN, KV_HEADS, HEAD_DIM), jnp.float32)
    block_inputs = (
        q_all.reshape(N_BLOCKS, Q_BLOCK, KV_HEADS, GROUP_SIZE, HEAD_DIM),
        do_all.reshape(N_BLOCKS, Q_BLOCK, KV_HEADS, GROUP_SIZE, HEAD_DIM),
        seg_ids.reshape(N_BLOCKS, Q_BLOCK),
        jnp.arange(N_BLOCKS) * Q_BLOCK,
    )
    (dk_acc, dv_acc), (out_blocks, dq_blocks) = lax.scan(block_step, (zeros_kv, zeros_kv), block_inputs)
    grad_k = (dk_acc * score_scale).astype(jnp.bfloat16)
    grad_v = dv_acc.astype(jnp.bfloat16)
    x_blocks = x_act.reshape(N_BLOCKS, Q_BLOCK, MODEL_DIM)
    dy_blocks = dy_act.reshape(N_BLOCKS, Q_BLOCK, MODEL_DIM)
    y_out = product32('nkqgd,mkgd->nqm', out_blocks, w_o4).reshape(SEQ_LEN, MODEL_DIM).astype(jnp.bfloat16)
    dx_wide = (product32('nkqgd,mkgd->nqm', dq_blocks, w_q4).reshape(SEQ_LEN, MODEL_DIM)
               + product32('skd,mkd->sm', grad_k, w_k) + product32('skd,mkd->sm', grad_v, w_v))
    dx_out = dx_wide.astype(jnp.bfloat16)
    dw_q = product32('nqm,nkqgd->mkgd', x_blocks, dq_blocks).reshape(MODEL_DIM, Q_HEADS, HEAD_DIM)
    dw_k = product32('sm,skd->mkd', x_act, grad_k)
    dw_v = product32('sm,skd->mkd', x_act, grad_v)
    dw_o = product32('nqm,nkqgd->mkgd', dy_blocks, out_blocks).reshape(MODEL_DIM, Q_HEADS, HEAD_DIM)
    return (y_out, dx_out, dw_q, dw_k, dw_v, dw_o)
```

```python
import functools

import jax
import jax.numpy as jnp
from jax import lax
from jax.experimental import pallas as pl
from jax.experimental.pallas import tpu as pltpu
from jax.sharding import PartitionSpec as P

BF = jnp.bfloat16
F32 = jnp.float32
LANES = 128
LOG2E = 1.4426950408889634
VMEM_MAX = 62 * 1024 * 1024


def rdma(src, dst, send_sem, recv_sem, peer):
    return pltpu.make_async_remote_copy(src_ref=src, dst_ref=dst, send_sem=send_sem, recv_sem=recv_sem,
                                        device_id={'cp': peer}, device_id_type=pl.DeviceIdType.MESH)


def dot_nt(left, right):
    return lax.dot_general(left, right, (((1,), (1,)), ((), ())), preferred_element_type=F32)


def dot_tn(left, right):
    return lax.dot_general(left, right, (((0,), (0,)), ((), ())), preferred_element_type=F32)


def dot_nn(left, right):
    return lax.dot_general(left, right, (((1,), (0,)), ((), ())), preferred_element_type=F32)


def project_kernel(dims, x_ref, dy_ref, seg_ref, wq_ref, wk_ref, wv_ref, wo_ref, out_ref, start_ref, first_ref,
                   wbuf, sbuf, rbuf, seg_mine, seg_all, wsem, ssem, rsem, fsem, fsend, gsend, grecv, lsem):
    n, qrows, krows, nblk = dims
    chips = n // 2
    me = lax.axis_index('cp')
    chip, core = me // 2, me % 2
    sgn = 1 - 2 * core
    rows = 2 * qrows + 2 * krows

    def device(chip_off, flip):
        return ((chip + sgn * chip_off + chips) % chips) * 2 + (core + flip) % 2

    dests = [device(2, 0), device(2, 1), device(-1, 0), device(-1, 1), device(1, 0), device(1, 1), device(0, 1), me]
    forward = dests[4]

    barrier = pltpu.get_barrier_semaphore()
    for t in range(n - 1):
        pl.semaphore_signal(barrier, inc=1, device_id={'cp': dests[t]}, device_id_type=pl.DeviceIdType.MESH)

    def dest_of(step):
        pair, flip = step // 2, (step + step // 6) % 2
        off = 2 - 3 * pair + 5 * (pair // 2) + 2 * (pair // 3)
        return ((chip + sgn * off + chips) % chips) * 2 + (core + flip) % 2

    def weight_copies(step, slot):
        dst = dest_of(step)
        return [
            pltpu.make_async_copy(wq_ref.at[pl.ds(dst * qrows, qrows)], wbuf.at[slot, pl.ds(0, qrows)], wsem.at[slot, 0]),
            pltpu.make_async_copy(wk_ref.at[pl.ds(dst * krows, krows)], wbuf.at[slot, pl.ds(qrows, krows)], wsem.at[slot, 1]),
            pltpu.make_async_copy(wv_ref.at[pl.ds(dst * krows, krows)], wbuf.at[slot, pl.ds(qrows + krows, krows)], wsem.at[slot, 2]),
            pltpu.make_async_copy(wo_ref.at[pl.ds(dst * qrows, qrows)], wbuf.at[slot, pl.ds(qrows + 2 * krows, qrows)], wsem.at[slot, 3]),
        ]

    for copy in weight_copies(0, 0):
        copy.start()
    seg_mine[...] = jnp.broadcast_to(seg_ref[...], seg_mine.shape)
    pl.semaphore_wait(barrier, n - 1)

    my_blocks = pl.ds(me * nblk, nblk)
    def first_leg(t):
        return rdma(sbuf.at[t], rbuf.at[t], ssem.at[t], fsem.at[t], forward)

    def direct(t):
        return rdma(sbuf.at[t], out_ref.at[my_blocks], ssem.at[t], rsem.at[t], dests[t])

    relay_from = ((chip - sgn + chips) % chips) * 2 + core

    def second_leg(t):
        return rdma(rbuf.at[t], out_ref.at[pl.ds(relay_from * nblk, nblk)], fsend.at[t], rsem.at[t], device(1, t))

    def seg_copy(t):
        return rdma(seg_mine, seg_all.at[me], gsend.at[t], grecv.at[t], dests[t])

    for t in range(n - 1):
        seg_copy(t).start()
    seg_all[me] = seg_mine[...]

    def compute_step(step, carry):
        slot = step % 2

        @pl.when(step < n - 1)
        def _():
            for copy in weight_copies(step + 1, 1 - slot):
                copy.start()

        for copy in weight_copies(step, slot):
            copy.wait()
        qkv = dot_nt(wbuf[slot, 0:qrows + 2 * krows], x_ref[...]).astype(BF)
        for b in range(nblk):
            sbuf[step, b, 0:qrows + 2 * krows] = qkv[:, b * LANES:(b + 1) * LANES]
        dout = dot_nt(wbuf[slot, qrows + 2 * krows:rows], dy_ref[...]).astype(BF)
        for b in range(nblk):
            sbuf[step, b, qrows + 2 * krows:rows] = dout[:, b * LANES:(b + 1) * LANES]
        for t in range(n):
            @pl.when(step == t)
            def _():
                if t < 2:
                    first_leg(t).start()
                elif t < n - 1:
                    direct(t).start()
                else:
                    pltpu.make_async_copy(sbuf.at[t], out_ref.at[my_blocks], lsem.at[0]).start()
        return carry

    lax.fori_loop(0, n, compute_step, 0)
    for t in range(2):
        first_leg(t).wait_recv()
        second_leg(t).start()

    for t in range(n - 1):
        seg_copy(t).wait_recv()
    tok = seg_all.shape[2]
    row_id = lax.broadcasted_iota(jnp.int32, (n, tok), 0)
    lane_id = lax.broadcasted_iota(jnp.int32, (n, tok), 1)
    seg = jnp.zeros((n, tok), jnp.int32)
    for d in range(n):
        seg = jnp.where(row_id == d, seg_all[d], seg)
    before = jnp.where(lane_id == 0, pltpu.roll(pltpu.roll(seg, 1, 1), 1, 0), pltpu.roll(seg, 1, 1))
    pos = row_id * tok + lane_id
    best = jnp.where((seg != before) & (pos > 0), pos, 0)
    shift = 1
    while shift < tok:
        best = jnp.maximum(best, jnp.where(lane_id >= shift, pltpu.roll(best, shift, 1), 0))
        shift *= 2
    last = jnp.broadcast_to(best[:, tok - 1:tok], (n, tok))
    carry_max = jnp.where(row_id >= 1, pltpu.roll(last, 1, 0), 0)
    shift = 1
    while shift < n:
        carry_max = jnp.maximum(carry_max, jnp.where(row_id >= shift, pltpu.roll(carry_max, shift, 0), 0))
        shift *= 2
    best = jnp.maximum(best, carry_max)
    start_ref[...] = best
    for d in range(n):
        for b in range(nblk):
            first_ref[d * nblk + b] = jnp.broadcast_to(best[d:d + 1, b * LANES:(b + 1) * LANES], (8, LANES))

    pltpu.make_async_copy(sbuf.at[n - 1], out_ref.at[my_blocks], lsem.at[0]).wait()
    for t in range(n - 1):
        direct(t).wait_recv()
    for t in range(2):
        first_leg(t).wait_send()
        second_leg(t).wait_send()
    for t in range(2, n - 1):
        direct(t).wait_send()
    for t in range(n - 1):
        seg_copy(t).wait_send()


def project(n, x_act, dy_act, seg, wq, wk, wv, wo):
    tok, model = x_act.shape
    qrows, krows = wq.shape[0] // n, wk.shape[0] // n
    rows = 2 * qrows + 2 * krows
    nblk = tok // LANES
    vmem = pl.BlockSpec(memory_space=pltpu.VMEM)
    anym = pl.BlockSpec(memory_space=pl.ANY)
    dma = pltpu.SemaphoreType.DMA
    return pl.pallas_call(
        functools.partial(project_kernel, (n, qrows, krows, nblk)),
        out_shape=(jax.ShapeDtypeStruct((n * nblk, rows, LANES), BF), jax.ShapeDtypeStruct((n, tok), jnp.int32),
                   jax.ShapeDtypeStruct((n * nblk, 8, LANES), jnp.int32)),
        in_specs=[vmem, vmem, vmem, anym, anym, anym, anym],
        out_specs=(anym, vmem, vmem),
        scratch_shapes=[
            pltpu.VMEM((2, rows, model), BF),
            pltpu.VMEM((n, nblk, rows, LANES), BF),
            pltpu.VMEM((2, nblk, rows, LANES), BF),
            pltpu.VMEM((n, tok), jnp.int32),
            pltpu.VMEM((n, n, tok), jnp.int32),
            dma((2, 4)), dma((n,)), dma((n,)), dma((2,)), dma((2,)), dma((n,)), dma((n,)), dma((1,)),
        ],
        compiler_params=pltpu.CompilerParams(collective_id=0, has_side_effects=True, vmem_limit_bytes=VMEM_MAX),
        name='project_exchange',
    )(x_act, dy_act, seg.reshape(1, tok), wq, wk, wv, wo)


def attention_kernel(dims, start_smem, qkv_ref, first_ref, g_ref, kvn, pbuf, oacc, dqacc, dkacc, dvacc):
    qrows, krows, blocks, tok_blocks, scale = dims
    heads = qrows // krows
    width = heads * LANES
    kb = 2 * LANES
    score_mul = scale * LOG2E
    kv0 = qrows
    do0 = qrows + 2 * krows

    def transpose_block(b, carry):
        kvn[pl.ds(pl.multiple_of(b * LANES, LANES), LANES), :] = qkv_ref[b, kv0:do0, :].T
        return carry

    lax.fori_loop(0, blocks, transpose_block, 0)
    dkacc[...] = jnp.zeros_like(dkacc)
    dvacc[...] = jnp.zeros_like(dvacc)
    zeros = jnp.zeros((krows, width), BF)

    def pair(c, row0, row1):
        return jnp.concatenate([qkv_ref[2 * c, row0:row1, :], qkv_ref[2 * c + 1, row0:row1, :]], axis=1)

    def query_block(i, carry):
        qs = jnp.concatenate([qkv_ref[i, krows * h:krows * (h + 1), :] for h in range(heads)], axis=1)
        dos = jnp.concatenate([qkv_ref[i, do0 + krows * h:do0 + krows * (h + 1), :] for h in range(heads)], axis=1)
        rhs_q = jnp.concatenate([qs, zeros], axis=0)
        rhs_d = jnp.concatenate([zeros, dos], axis=0)
        srow, soff = i // tok_blocks, (i % tok_blocks) * LANES
        first = first_ref[i][0:1]
        first = jnp.concatenate([first] * heads, axis=1)
        qpos = i * LANES + lax.broadcasted_iota(jnp.int32, (1, LANES), 1)
        qpos = jnp.concatenate([qpos] * heads, axis=1)
        c0 = start_smem[srow, soff] // kb
        c1 = i // 2 + 1
        key_iota = lax.broadcasted_iota(jnp.int32, (kb, width), 0)

        def score_step(c, top):
            k_blk = kvn[pl.ds(pl.multiple_of(c * kb, kb), kb), :]
            s = dot_nn(k_blk, rhs_q)
            kpos = key_iota + c * kb
            s = jnp.where((kpos >= first) & (kpos <= qpos), s, -jnp.inf)
            pbuf[c] = s
            return jnp.maximum(top, jnp.max(s.reshape(kb // 8, 8, width), axis=0))

        top = lax.fori_loop(c0, c1, score_step, jnp.full((8, width), -jnp.inf, F32))
        top = jnp.max(top, axis=0, keepdims=True) * score_mul
        oacc[...] = jnp.zeros_like(oacc)

        def value_step(c, total):
            p = jnp.exp2(pbuf[c] * score_mul - top)
            pbuf[c] = p
            oacc[...] += dot_nn(pair(c, kv0 + krows, do0), p.astype(BF))
            return total + jnp.sum(p.reshape(kb // 8, 8, width), axis=0)

        total = lax.fori_loop(c0, c1, value_step, jnp.zeros((8, width), F32))
        inv = 1.0 / jnp.sum(total, axis=0, keepdims=True)
        o_blk = (oacc[...] * inv).astype(BF)
        delta = jnp.sum(dos.astype(F32) * o_blk.astype(F32), axis=0, keepdims=True)
        here = pl.ds(pl.multiple_of(i * LANES, LANES), LANES)
        for h in range(heads):
            g_ref[krows * h:krows * (h + 1), here] = o_blk[:, LANES * h:LANES * (h + 1)]
        dqacc[...] = jnp.zeros_like(dqacc)

        def grad_step(c, carry):
            kv_blk = kvn[pl.ds(pl.multiple_of(c * kb, kb), kb), :]
            dp = dot_nn(kv_blk, rhs_d)
            p = pbuf[c] * inv
            ds = (p * (dp - delta)).astype(BF)
            dqacc[...] += dot_nn(pair(c, kv0, kv0 + krows), ds)
            dkacc[c] += dot_nt(qs, ds)
            dvacc[c] += dot_nt(dos, p.astype(BF))
            return carry

        lax.fori_loop(c0, c1, grad_step, 0)
        dq = (dqacc[...] * scale).astype(BF)
        for h in range(heads):
            g_ref[qrows + krows * h:qrows + krows * (h + 1), here] = dq[:, LANES * h:LANES * (h + 1)]
        return carry

    lax.fori_loop(0, blocks, query_block, 0)

    for c in range(blocks // 2):
        g_ref[2 * qrows:2 * qrows + krows, c * kb:(c + 1) * kb] = (dkacc[c] * scale).astype(BF)
        g_ref[2 * qrows + krows:2 * qrows + 2 * krows, c * kb:(c + 1) * kb] = dvacc[c].astype(BF)


def attention(n, qkv, start, first, krows):
    blocks, rows, _ = qkv.shape
    qrows = rows // 2 - krows
    heads = qrows // krows
    tok = start.shape[1]
    width = heads * LANES
    vmem = pl.BlockSpec(memory_space=pltpu.VMEM)
    total = blocks * LANES
    flops = 14 * heads * total * total // 2 * krows
    return pl.pallas_call(
        functools.partial(attention_kernel, (qrows, krows, blocks, tok // LANES, krows ** -0.5)),
        out_shape=jax.ShapeDtypeStruct((rows, total), BF),
        grid_spec=pltpu.PrefetchScalarGridSpec(
            num_scalar_prefetch=1, grid=(1,),
            in_specs=[vmem, vmem], out_specs=vmem,
            scratch_shapes=[
                pltpu.VMEM((total, 2 * krows), BF),
                pltpu.VMEM((blocks // 2, 2 * LANES, width), F32),
                pltpu.VMEM((krows, width), F32), pltpu.VMEM((krows, width), F32),
                pltpu.VMEM((blocks // 2, krows, 2 * LANES), F32), pltpu.VMEM((blocks // 2, krows, 2 * LANES), F32),
            ]),
        compiler_params=pltpu.CompilerParams(vmem_limit_bytes=VMEM_MAX),
        cost_estimate=pl.CostEstimate(flops=flops, bytes_accessed=4 * rows * total, transcendentals=heads * total * total // 2),
        name='head_attention',
    )(start, qkv, first)


PIECES = 10


def finish_kernel(dims, g_ref, xc_ref, dyc_ref, wq_ref, wk_ref, wv_ref, wo_ref,
                  y_ref, dx_ref, dwq_ref, dwk_ref, dwv_ref, dwo_ref,
                  gall, yacc, dxacc, woa, wob, sta, stb, wasem, wbsem, oasem, obsem,
                  osem, relsem, parsem, rsem, lsem):
    n, qrows, krows, tok = dims
    chips = n // 2
    me = lax.axis_index('cp')
    chip, core = me // 2, me % 2
    right = ((chip + 1) % chips) * 2 + core
    left = ((chip + chips - 1) % chips) * 2 + core
    partner = chip * 2 + (1 - core)
    rows = 2 * qrows + 2 * krows
    prow = rows // PIECES
    half = PIECES // 2
    brows = rows - qrows
    model = yacc.shape[1]
    ncol = 512
    own_tok = pl.ds(pl.multiple_of(me * tok, LANES), tok)

    barrier = pltpu.get_barrier_semaphore()
    for peer in (right, left, partner):
        pl.semaphore_signal(barrier, inc=1, device_id={'cp': peer}, device_id_type=pl.DeviceIdType.MESH)

    def piece(i):
        return pl.ds(i * prow, prow)

    def own_right(i):
        return rdma(g_ref.at[piece(i)], gall.at[1, piece(i)], osem.at[0, i], rsem.at[1, i], right)

    def own_left(i):
        return rdma(g_ref.at[piece(i)], gall.at[2, piece(i)], osem.at[1, i], rsem.at[2, i], left)

    def relay(i):
        if i < half:
            return rdma(gall.at[1, piece(i)], gall.at[3, piece(i)], relsem.at[i], rsem.at[3, i], right)
        return rdma(gall.at[2, piece(i)], gall.at[3, piece(i)], relsem.at[i], rsem.at[3, i], left)

    def to_partner(slot, i):
        src = g_ref if slot == 0 else gall.at[slot]
        return rdma(src.at[piece(i)], gall.at[4 + slot, piece(i)], parsem.at[slot, i], rsem.at[4 + slot, i], partner)

    def source_of(order):
        pair, flip = order // 2, order % 2
        off = 3 * (pair // 2) + 2 * (pair // 3) - pair
        return ((chip + off + chips) % chips) * 2 + (core + flip) % 2

    def slot_of(order):
        return order // 2 + 4 * (order % 2)

    def load_a(order, buf):
        src = source_of(order)
        return [pltpu.make_async_copy(wo_ref.at[pl.ds(src * qrows, qrows)], woa.at[buf], wasem.at[buf])]

    def load_b(order, buf):
        src = source_of(order)
        return [
            pltpu.make_async_copy(wq_ref.at[pl.ds(src * qrows, qrows)], wob.at[buf, pl.ds(0, qrows)], wbsem.at[buf, 0]),
            pltpu.make_async_copy(wk_ref.at[pl.ds(src * krows, krows)], wob.at[buf, pl.ds(qrows, krows)], wbsem.at[buf, 1]),
            pltpu.make_async_copy(wv_ref.at[pl.ds(src * krows, krows)], wob.at[buf, pl.ds(qrows + krows, krows)], wbsem.at[buf, 2]),
        ]

    def save_a(order, buf):
        src = source_of(order)
        return [pltpu.make_async_copy(sta.at[buf], dwo_ref.at[pl.ds(src * qrows, qrows)], oasem.at[buf])]

    def save_b(order, buf):
        src = source_of(order)
        return [
            pltpu.make_async_copy(stb.at[buf, pl.ds(0, qrows)], dwq_ref.at[pl.ds(src * qrows, qrows)], obsem.at[buf, 0]),
            pltpu.make_async_copy(stb.at[buf, pl.ds(qrows, krows)], dwk_ref.at[pl.ds(src * krows, krows)], obsem.at[buf, 1]),
            pltpu.make_async_copy(stb.at[buf, pl.ds(qrows + krows, krows)], dwv_ref.at[pl.ds(src * krows, krows)], obsem.at[buf, 2]),
        ]

    own_copy = pltpu.make_async_copy(g_ref, gall.at[0], lsem.at[0])
    own_copy.start()
    for copy in load_a(0, 0) + load_b(0, 0):
        copy.start()
    pl.semaphore_wait(barrier, 3)
    for i in range(PIECES):
        own_right(i).start()
        own_left((i + half) % PIECES).start()
    for i in range(PIECES):
        to_partner(0, i).start()
    yacc[...] = jnp.zeros_like(yacc)
    dxacc[...] = jnp.zeros_like(dxacc)

    def arrive_near():
        for i in range(half):
            own_right(i).wait_recv()
            relay(i).start()
            to_partner(1, i).start()
            own_left(i + half).wait_recv()
            relay(i + half).start()
            to_partner(2, i + half).start()
        for i in range(half):
            own_right(i + half).wait_recv()
            to_partner(1, i + half).start()
            own_left(i).wait_recv()
            to_partner(2, i).start()

    def arrive_far(pieces):
        for i in pieces:
            relay(i).wait_recv()
            to_partner(3, i).start()
            relay(i + half).wait_recv()
            to_partner(3, i + half).start()

    def arrive_partner(slot, pieces):
        for i in pieces:
            to_partner(slot, i).wait_recv()

    def part_a(order):
        buf = order % 2
        slot = slot_of(order)
        for copy in load_a(order, buf):
            copy.wait()

        @pl.when(order < n - 1)
        def _():
            for copy in load_a(order + 1, 1 - buf):
                copy.start()

        @pl.when(order >= 2)
        def _():
            for copy in save_a(order - 2, buf):
                copy.wait()
        sta[buf] = dot_nn(gall[slot, 0:qrows, :], dyc_ref[...])
        for copy in save_a(order, buf):
            copy.start()
        left_t = gall[slot, 0:qrows, own_tok]

        def col(j, carry):
            cols = pl.ds(pl.multiple_of(j * ncol, ncol), ncol)
            yacc[:, cols] += dot_tn(left_t, woa[buf, :, cols])
            return carry

        lax.fori_loop(0, model // ncol, col, 0)

    def part_b(order):
        buf = order % 2
        slot = slot_of(order)
        for copy in load_b(order, buf):
            copy.wait()

        @pl.when(order < n - 1)
        def _():
            for copy in load_b(order + 1, 1 - buf):
                copy.start()

        @pl.when(order >= 2)
        def _():
            for copy in save_b(order - 2, buf):
                copy.wait()
        stb[buf] = dot_nn(gall[slot, qrows:rows, :], xc_ref[...])
        for copy in save_b(order, buf):
            copy.start()
        left_t = gall[slot, qrows:rows, own_tok]

        def col(j, carry):
            cols = pl.ds(pl.multiple_of(j * ncol, ncol), ncol)
            dxacc[:, cols] += dot_tn(left_t, wob[buf, :, cols])
            return carry

        lax.fori_loop(0, model // ncol, col, 0)

    def round_step(r, carry):
        @pl.when(r == 0)
        def _():
            own_copy.wait()

        @pl.when(r == 1)
        def _():
            arrive_partner(0, range(PIECES))

        @pl.when(r == 2)
        def _():
            arrive_near()

        @pl.when(r == 3)
        def _():
            arrive_partner(1, range(PIECES))

        @pl.when(r == 5)
        def _():
            arrive_partner(2, range(PIECES))

        @pl.when(r == 6)
        def _():
            arrive_far(range(half - 1))

        @pl.when(r == 7)
        def _():
            arrive_partner(3, range(half - 1))

        @pl.when(r < n)
        def _():
            part_a(r)

        @pl.when(r == 7)
        def _():
            arrive_far(range(half - 1, half))

        @pl.when(r == 8)
        def _():
            arrive_partner(3, [half - 1] + list(range(half, PIECES)))

        @pl.when(r >= 1)
        def _():
            part_b(r - 1)
        return carry

    lax.fori_loop(0, n + 1, round_step, 0)
    y_ref[...] = yacc[...].astype(BF)
    dx_ref[...] = dxacc[...].astype(BF)
    for order in (n - 2, n - 1):
        for copy in save_a(order, order % 2) + save_b(order, order % 2):
            copy.wait()
    for i in range(PIECES):
        own_right(i).wait_send()
        own_left(i).wait_send()
        relay(i).wait_send()
        for slot in range(4):
            to_partner(slot, i).wait_send()


def finish(n, g_all, xc, dyc, wq, wk, wv, wo):
    rows, total = g_all.shape
    qrows, krows = wq.shape[0] // n, wk.shape[0] // n
    tok = total // n
    model = wq.shape[1]
    mcol = xc.shape[1]
    brows = rows - qrows
    vmem = pl.BlockSpec(memory_space=pltpu.VMEM)
    anym = pl.BlockSpec(memory_space=pl.ANY)
    dma = pltpu.SemaphoreType.DMA
    return pl.pallas_call(
        functools.partial(finish_kernel, (n, qrows, krows, tok)),
        out_shape=(jax.ShapeDtypeStruct((tok, model), BF), jax.ShapeDtypeStruct((tok, model), BF),
                   jax.ShapeDtypeStruct((wq.shape[0], mcol), F32), jax.ShapeDtypeStruct((wk.shape[0], mcol), F32),
                   jax.ShapeDtypeStruct((wv.shape[0], mcol), F32), jax.ShapeDtypeStruct((wo.shape[0], mcol), F32)),
        in_specs=[anym, vmem, vmem, anym, anym, anym, anym],
        out_specs=(vmem, vmem, anym, anym, anym, anym),
        scratch_shapes=[
            pltpu.VMEM((n, rows, total), BF),
            pltpu.VMEM((tok, model), F32), pltpu.VMEM((tok, model), F32),
            pltpu.VMEM((2, qrows, model), BF), pltpu.VMEM((2, brows, model), BF),
            pltpu.VMEM((2, qrows, mcol), F32), pltpu.VMEM((2, brows, mcol), F32),
            dma((2,)), dma((2, 3)), dma((2,)), dma((2, 3)),
            dma((2, PIECES)), dma((PIECES,)), dma((4, PIECES)), dma((8, PIECES)), dma((1,)),
        ],
        compiler_params=pltpu.CompilerParams(collective_id=1, has_side_effects=True, vmem_limit_bytes=VMEM_MAX),
        name='gather_finish',
    )(g_all, xc, dyc, wq, wk, wv, wo)


def solution(mesh):
    n = mesh.shape['cp']
    row_spec = P(('dp', 'cp'), None)
    tok_spec = P(('dp', 'cp'))
    weight_spec = P(None, None, None)
    grad_spec = P(('dp', 'cp'), None, None)

    def local_step(x_act, seg_ids, w_q, w_k, w_v, w_o, dy_act):
        model, q_heads, head_dim = w_q.shape
        kv_heads = w_k.shape[1]
        assert kv_heads == n and x_act.shape[0] % LANES == 0

        def flat(w):
            return w.transpose(1, 2, 0).reshape(w.shape[1] * head_dim, model)

        def unflat(g, heads):
            return g.reshape(heads, head_dim, g.shape[1]).transpose(2, 0, 1)

        wq, wk, wv, wo = flat(w_q), flat(w_k), flat(w_v), flat(w_o)
        xc = lax.all_to_all(x_act, 'cp', split_axis=1, concat_axis=0, tiled=True)
        dyc = lax.all_to_all(dy_act, 'cp', split_axis=1, concat_axis=0, tiled=True)
        qkv, start, first = project(n, x_act, dy_act, seg_ids, wq, wk, wv, wo)
        g_own = attention(n, qkv, start, first, head_dim)
        y_out, dx_out, dwq, dwk, dwv, dwo = finish(n, g_own, xc, dyc, wq, wk, wv, wo)
        return (y_out, dx_out, unflat(dwq, q_heads), unflat(dwk, kv_heads), unflat(dwv, kv_heads), unflat(dwo, q_heads))

    return jax.shard_map(local_step, mesh=mesh,
                         in_specs=(row_spec, tok_spec, weight_spec, weight_spec, weight_spec, weight_spec, row_spec),
                         out_specs=(row_spec, row_spec, grad_spec, grad_spec, grad_spec, grad_spec),
                         check_vma=False)
```

```python
import functools

import jax
import jax.numpy as jnp
from jax import lax
from jax.experimental import pallas as pl
from jax.experimental.pallas import tpu as pltpu
from jax.sharding import PartitionSpec as P

BF = jnp.bfloat16
F32 = jnp.float32
LANES = 128
LOG2E = 1.4426950408889634
VMEM_MAX = 48 * 1024 * 1024


def rdma(src, dst, send_sem, recv_sem, peer):
    return pltpu.make_async_remote_copy(src_ref=src, dst_ref=dst, send_sem=send_sem, recv_sem=recv_sem,
                                        device_id={'cp': peer}, device_id_type=pl.DeviceIdType.MESH)


def dot_nt(left, right):
    return lax.dot_general(left, right, (((1,), (1,)), ((), ())), preferred_element_type=F32)


def dot_tn(left, right):
    return lax.dot_general(left, right, (((0,), (0,)), ((), ())), preferred_element_type=F32)


def dot_nn(left, right):
    return lax.dot_general(left, right, (((1,), (0,)), ((), ())), preferred_element_type=F32)


def project_kernel(dims, x_ref, dy_ref, seg_ref, wq_ref, wk_ref, wv_ref, wo_ref, out_ref, first_ref,
                   wbuf, sbuf, rbuf, seg_mine, seg_all, wsem, ssem, rsem, fsem, fsend, gsend, grecv, lsem):
    n, qrows, krows, nblk = dims
    chips = n // 2
    me = lax.axis_index('cp')
    chip, core = me // 2, me % 2
    sgn = 1 - 2 * core
    rows = 2 * qrows + 2 * krows

    def device(chip_off, flip):
        return ((chip + sgn * chip_off + chips) % chips) * 2 + (core + flip) % 2

    dests = [device(2, 0), device(2, 1), device(-1, 0), device(-1, 1), device(1, 0), device(1, 1), device(0, 1), me]
    forward = dests[4]

    barrier = pltpu.get_barrier_semaphore()
    for t in range(n - 1):
        pl.semaphore_signal(barrier, inc=1, device_id={'cp': dests[t]}, device_id_type=pl.DeviceIdType.MESH)

    def dest_of(step):
        pair, flip = step // 2, (step + step // 6) % 2
        off = 2 - 3 * pair + 5 * (pair // 2) + 2 * (pair // 3)
        return ((chip + sgn * off + chips) % chips) * 2 + (core + flip) % 2

    def weight_copies(step, slot):
        dst = dest_of(step)
        return [
            pltpu.make_async_copy(wq_ref.at[pl.ds(dst * qrows, qrows)], wbuf.at[slot, pl.ds(0, qrows)], wsem.at[slot, 0]),
            pltpu.make_async_copy(wk_ref.at[pl.ds(dst * krows, krows)], wbuf.at[slot, pl.ds(qrows, krows)], wsem.at[slot, 1]),
            pltpu.make_async_copy(wv_ref.at[pl.ds(dst * krows, krows)], wbuf.at[slot, pl.ds(qrows + krows, krows)], wsem.at[slot, 2]),
            pltpu.make_async_copy(wo_ref.at[pl.ds(dst * qrows, qrows)], wbuf.at[slot, pl.ds(qrows + 2 * krows, qrows)], wsem.at[slot, 3]),
        ]

    for copy in weight_copies(0, 0):
        copy.start()
    seg_mine[...] = jnp.broadcast_to(seg_ref[...], seg_mine.shape)
    pl.semaphore_wait(barrier, n - 1)

    my_blocks = pl.ds(me * nblk, nblk)
    def first_leg(t):
        return rdma(sbuf.at[t], rbuf.at[t], ssem.at[t], fsem.at[t], forward)

    def direct(t):
        return rdma(sbuf.at[t], out_ref.at[my_blocks], ssem.at[t], rsem.at[t], dests[t])

    relay_from = ((chip - sgn + chips) % chips) * 2 + core

    def second_leg(t):
        return rdma(rbuf.at[t], out_ref.at[pl.ds(relay_from * nblk, nblk)], fsend.at[t], rsem.at[t], device(1, t))

    def seg_copy(t):
        return rdma(seg_mine, seg_all.at[me], gsend.at[t], grecv.at[t], dests[t])

    for t in range(n - 1):
        seg_copy(t).start()
    seg_all[me] = seg_mine[...]

    def compute_step(step, carry):
        slot = step % 2

        @pl.when(step < n - 1)
        def _():
            for copy in weight_copies(step + 1, 1 - slot):
                copy.start()

        for copy in weight_copies(step, slot):
            copy.wait()
        qkv = dot_nt(wbuf[slot, 0:qrows + 2 * krows], x_ref[...]).astype(BF)
        for b in range(nblk):
            sbuf[step, b, 0:qrows + 2 * krows] = qkv[:, b * LANES:(b + 1) * LANES]
        dout = dot_nt(wbuf[slot, qrows + 2 * krows:rows], dy_ref[...]).astype(BF)
        for b in range(nblk):
            sbuf[step, b, qrows + 2 * krows:rows] = dout[:, b * LANES:(b + 1) * LANES]
        for t in range(n):
            @pl.when(step == t)
            def _():
                if t < 2:
                    first_leg(t).start()
                elif t < n - 1:
                    direct(t).start()
                else:
                    pltpu.make_async_copy(sbuf.at[t], out_ref.at[my_blocks], lsem.at[0]).start()
        return carry

    lax.fori_loop(0, n, compute_step, 0)
    for t in range(2):
        first_leg(t).wait_recv()
        second_leg(t).start()

    for t in range(n - 1):
        seg_copy(t).wait_recv()
    tok = seg_all.shape[2]
    row_id = lax.broadcasted_iota(jnp.int32, (n, tok), 0)
    lane_id = lax.broadcasted_iota(jnp.int32, (n, tok), 1)
    seg = jnp.zeros((n, tok), jnp.int32)
    for d in range(n):
        seg = jnp.where(row_id == d, seg_all[d], seg)
    before = jnp.where(lane_id == 0, pltpu.roll(pltpu.roll(seg, 1, 1), 1, 0), pltpu.roll(seg, 1, 1))
    pos = row_id * tok + lane_id
    best = jnp.where((seg != before) & (pos > 0), pos, 0)
    shift = 1
    while shift < tok:
        best = jnp.maximum(best, jnp.where(lane_id >= shift, pltpu.roll(best, shift, 1), 0))
        shift *= 2
    last = jnp.broadcast_to(best[:, tok - 1:tok], (n, tok))
    carry_max = jnp.where(row_id >= 1, pltpu.roll(last, 1, 0), 0)
    shift = 1
    while shift < n:
        carry_max = jnp.maximum(carry_max, jnp.where(row_id >= shift, pltpu.roll(carry_max, shift, 0), 0))
        shift *= 2
    best = jnp.maximum(best, carry_max)
    for d in range(n):
        for b in range(nblk):
            first_ref[d * nblk + b] = jnp.broadcast_to(best[d:d + 1, b * LANES:(b + 1) * LANES], (8, LANES))

    pltpu.make_async_copy(sbuf.at[n - 1], out_ref.at[my_blocks], lsem.at[0]).wait()
    for t in range(n - 1):
        direct(t).wait_recv()
    for t in range(2):
        first_leg(t).wait_send()
        second_leg(t).wait_send()
    for t in range(2, n - 1):
        direct(t).wait_send()
    for t in range(n - 1):
        seg_copy(t).wait_send()


def project(n, x_act, dy_act, seg, wq, wk, wv, wo):
    tok, model = x_act.shape
    qrows, krows = wq.shape[0] // n, wk.shape[0] // n
    rows = 2 * qrows + 2 * krows
    nblk = tok // LANES
    vmem = pl.BlockSpec(memory_space=pltpu.VMEM)
    anym = pl.BlockSpec(memory_space=pl.ANY)
    dma = pltpu.SemaphoreType.DMA
    return pl.pallas_call(
        functools.partial(project_kernel, (n, qrows, krows, nblk)),
        out_shape=(jax.ShapeDtypeStruct((n * nblk, rows, LANES), BF),
                   jax.ShapeDtypeStruct((n * nblk, 8, LANES), jnp.int32)),
        in_specs=[vmem, vmem, vmem, anym, anym, anym, anym],
        out_specs=(anym, vmem),
        scratch_shapes=[
            pltpu.VMEM((2, rows, model), BF),
            pltpu.VMEM((n, nblk, rows, LANES), BF),
            pltpu.VMEM((2, nblk, rows, LANES), BF),
            pltpu.VMEM((n, tok), jnp.int32),
            pltpu.VMEM((n, n, tok), jnp.int32),
            dma((2, 4)), dma((n,)), dma((n,)), dma((2,)), dma((2,)), dma((n,)), dma((n,)), dma((1,)),
        ],
        compiler_params=pltpu.CompilerParams(collective_id=0, has_side_effects=True, vmem_limit_bytes=VMEM_MAX),
        name='project_exchange',
    )(x_act, dy_act, seg.reshape(1, tok), wq, wk, wv, wo)


def pick(index, values):
    out = values[0]
    for k in range(1, len(values)):
        out = jnp.where(index == k, values[k], out)
    return out


def main_kernel(dims, qkv_ref, first_ref, x_ref, dy_ref, wq_ref, wk_ref, wv_ref, wo_ref,
                y_ref, dx_ref, dwq_ref, dwk_ref, dwv_ref, dwo_ref,
                kvn, pbuf, oacc, dqacc, dkacc, dvacc, gall, xc, dyc, xrel, yacc, dxacc, woa, wob, sta, stb,
                wasem, wbsem, oasem, obsem, osem, relsem, parsem, rsem, xsend, xrecv, xfirst, xsecond, lsem):
    n, qrows, krows, tok, scale = dims
    chips = n // 2
    heads = qrows // krows
    me = lax.axis_index('cp')
    chip, core = me // 2, me % 2
    sgn = 1 - 2 * core
    rows = 2 * qrows + 2 * krows
    pieces = rows // krows
    brows = rows - qrows
    model = yacc.shape[1]
    mcol = xc.shape[1]
    ncol = 512
    tile = pbuf.shape[1]
    tblk = tile // LANES
    tiles = n * tok // tile
    kv0, do0 = qrows, qrows + 2 * krows
    own_tok = pl.ds(pl.multiple_of(me * tok, LANES), tok)

    def device(chip_off, flip):
        return ((chip + chip_off + chips) % chips) * 2 + (core + flip) % 2

    right, left, partner = device(1, 0), device(-1, 0), device(0, 1)
    dests = [device(2, 0), device(2, 1), device(-sgn, 0), device(-sgn, 1), device(sgn, 0), device(sgn, 1), partner]
    ahead = dests[4]
    relay_from = device(-sgn, 0)

    barrier = pltpu.get_barrier_semaphore()
    for peer in dests:
        pl.semaphore_signal(barrier, inc=1, device_id={'cp': peer}, device_id_type=pl.DeviceIdType.MESH)

    sides = ((x_ref, xc), (dy_ref, dyc))

    def columns(ref, dst):
        return ref.at[:, pl.ds(pl.multiple_of(dst * mcol, LANES), mcol)]

    def token_rows(ref, src):
        return ref.at[pl.ds(pl.multiple_of(src * tok, LANES), tok)]

    def x_first(a, t):
        return rdma(columns(sides[a][0], dests[t]), xrel.at[a, t], xsend.at[a, t], xfirst.at[a, t], ahead)

    def x_second(a, t):
        return rdma(xrel.at[a, t], token_rows(sides[a][1], relay_from), xsecond.at[a, t], xrecv.at[a, t], device(sgn, t))

    def x_direct(a, t):
        return rdma(columns(sides[a][0], dests[t]), token_rows(sides[a][1], me), xsend.at[a, t], xrecv.at[a, t], dests[t])

    def x_own(a):
        return pltpu.make_async_copy(columns(sides[a][0], me), token_rows(sides[a][1], me), lsem.at[a])

    def piece(i):
        return pl.ds(pl.multiple_of(i * krows, krows), krows)

    def own_right(i):
        return rdma(gall.at[0, piece(i)], gall.at[1, piece(i)], osem.at[0, i], rsem.at[1, i], right)

    def own_left(i):
        return rdma(gall.at[0, piece(i)], gall.at[2, piece(i)], osem.at[1, i], rsem.at[2, i], left)

    def relay_plus(i):
        return rdma(gall.at[1, piece(i)], gall.at[3, piece(i)], relsem.at[i], rsem.at[3, i], right)

    def relay_minus(i):
        return rdma(gall.at[2, piece(i)], gall.at[3, piece(i)], relsem.at[i], rsem.at[3, i], left)

    def to_partner(slot, i):
        return rdma(gall.at[slot, piece(i)], gall.at[4 + slot, piece(i)], parsem.at[slot, i], rsem.at[4 + slot, i], partner)

    def send_own(i, j):
        for k in (i, j):
            own_right(k).start()
            own_left(k).start()
            to_partner(0, k).start()

    def serve_near(i, j):
        own_right(i).wait_recv()
        relay_plus(i).start()
        to_partner(1, i).start()
        own_left(j).wait_recv()
        relay_minus(j).start()
        to_partner(2, j).start()
        own_right(j).wait_recv()
        to_partner(1, j).start()
        own_left(i).wait_recv()
        to_partner(2, i).start()

    def serve_far(i, j):
        relay_plus(i).wait_recv()
        to_partner(3, i).start()
        relay_minus(j).wait_recv()
        to_partner(3, j).start()

    def arrived(slot, which):
        for i in which:
            to_partner(slot - 4, i).wait_recv()

    slot_table = (0, 4, 1, 2, 5, 6, 3, 7)
    off_table = (0, 0, chips - 1, 1, chips - 1, 1, 2, 2)
    flip_table = (0, 1, 0, 0, 1, 1, 0, 1)

    def source_of(order):
        return ((chip + pick(order, off_table)) % chips) * 2 + (core + pick(order, flip_table)) % 2

    def load_a(order, buf):
        src = source_of(order)
        return [pltpu.make_async_copy(wo_ref.at[pl.ds(src * qrows, qrows)], woa.at[buf], wasem.at[buf])]

    def load_b(order, buf):
        src = source_of(order)
        return [
            pltpu.make_async_copy(wq_ref.at[pl.ds(src * qrows, qrows)], wob.at[buf, pl.ds(0, qrows)], wbsem.at[buf, 0]),
            pltpu.make_async_copy(wk_ref.at[pl.ds(src * krows, krows)], wob.at[buf, pl.ds(qrows, krows)], wbsem.at[buf, 1]),
            pltpu.make_async_copy(wv_ref.at[pl.ds(src * krows, krows)], wob.at[buf, pl.ds(qrows + krows, krows)], wbsem.at[buf, 2]),
        ]

    def save_a(order, buf):
        src = source_of(order)
        return [pltpu.make_async_copy(sta.at[buf], dwo_ref.at[pl.ds(src * qrows, qrows)], oasem.at[buf])]

    def save_b(order, buf):
        src = source_of(order)
        return [
            pltpu.make_async_copy(stb.at[buf, pl.ds(0, qrows)], dwq_ref.at[pl.ds(src * qrows, qrows)], obsem.at[buf, 0]),
            pltpu.make_async_copy(stb.at[buf, pl.ds(qrows, krows)], dwk_ref.at[pl.ds(src * krows, krows)], obsem.at[buf, 1]),
            pltpu.make_async_copy(stb.at[buf, pl.ds(qrows + krows, krows)], dwv_ref.at[pl.ds(src * krows, krows)], obsem.at[buf, 2]),
        ]

    def closing_part(order, load, save, wbuf, stage, row0, row1, other, acc):
        buf = order % 2
        slot = pick(order, slot_table)
        for copy in load(order, buf):
            copy.wait()

        @pl.when(order < n - 1)
        def _():
            for copy in load(order + 1, 1 - buf):
                copy.start()

        @pl.when(order >= 2)
        def _():
            for copy in save(order - 2, buf):
                copy.wait()
        stage[buf] = dot_nn(gall[slot, row0:row1, :], other[...])
        for copy in save(order, buf):
            copy.start()
        left_t = gall[slot, row0:row1, own_tok]

        def col(j, carry):
            cols = pl.ds(pl.multiple_of(j * ncol, ncol), ncol)
            acc[:, cols] += dot_tn(left_t, wbuf[buf, :, cols])
            return carry

        lax.fori_loop(0, model // ncol, col, 0)

    for a in range(2):
        x_own(a).start()
    for copy in load_a(0, 0) + load_b(0, 0):
        copy.start()
    pl.semaphore_wait(barrier, n - 1)
    for t in range(n - 1):
        for a in range(2):
            (x_first if t < 2 else x_direct)(a, t).start()

    def transpose_block(b, carry):
        kvn[pl.ds(pl.multiple_of(b * LANES, LANES), LANES), :] = qkv_ref[b, kv0:do0, :].T
        return carry

    lax.fori_loop(0, n * tok // LANES, transpose_block, 0)
    dkacc[...] = jnp.zeros_like(dkacc)
    dvacc[...] = jnp.zeros_like(dvacc)
    yacc[...] = jnp.zeros_like(yacc)
    dxacc[...] = jnp.zeros_like(dxacc)
    zeros = jnp.zeros((krows, tile), BF)
    score_mul = scale * LOG2E
    grp = tile // 8

    def lanes_of(c, row0):
        return jnp.concatenate([qkv_ref[c * tblk + b, pl.ds(row0, krows), :] for b in range(tblk)], axis=1)

    def head_step(h, carry):
        q0 = pl.multiple_of(h * krows, krows)

        def tile_step(i, carry):
            qs = lanes_of(i, q0)
            dos = lanes_of(i, do0 + q0)
            rhs_q = jnp.concatenate([qs, zeros], axis=0)
            rhs_d = jnp.concatenate([zeros, dos], axis=0)
            first = jnp.concatenate([first_ref[i * tblk + b][0:1] for b in range(tblk)], axis=1)
            qpos = i * tile + lax.broadcasted_iota(jnp.int32, (1, tile), 1)
            key_iota = lax.broadcasted_iota(jnp.int32, (tile, tile), 0)

            def score_step(c, top):
                k_blk = kvn[pl.ds(pl.multiple_of(c * tile, tile), tile), :]
                s = dot_nn(k_blk, rhs_q)
                kpos = key_iota + c * tile
                s = jnp.where((kpos >= first) & (kpos <= qpos), s, -jnp.inf)
                pbuf[c] = s
                return jnp.maximum(top, jnp.max(s.reshape(grp, 8, tile), axis=0))

            top = lax.fori_loop(0, i + 1, score_step, jnp.full((8, tile), -jnp.inf, F32))
            top = jnp.max(top, axis=0, keepdims=True) * score_mul
            oacc[...] = jnp.zeros_like(oacc)

            def value_step(c, total):
                p = jnp.exp2(pbuf[c] * score_mul - top)
                pbuf[c] = p
                oacc[...] += dot_nn(lanes_of(c, kv0 + krows), p.astype(BF))
                return total + jnp.sum(p.reshape(grp, 8, tile), axis=0)

            total = lax.fori_loop(0, i + 1, value_step, jnp.zeros((8, tile), F32))
            inv = 1.0 / jnp.sum(total, axis=0, keepdims=True)
            o_blk = (oacc[...] * inv).astype(BF)
            delta = jnp.sum(dos.astype(F32) * o_blk.astype(F32), axis=0, keepdims=True)
            here = pl.ds(pl.multiple_of(i * tile, tile), tile)
            gall[0, pl.ds(q0, krows), here] = o_blk
            dqacc[...] = jnp.zeros_like(dqacc)

            def grad_step(c, carry):
                kv_blk = kvn[pl.ds(pl.multiple_of(c * tile, tile), tile), :]
                dp = dot_nn(kv_blk, rhs_d)
                p = pbuf[c] * inv
                ds = (p * (dp - delta)).astype(BF)
                dqacc[...] += dot_nn(lanes_of(c, kv0), ds)
                dkacc[c] += dot_nt(qs, ds)
                dvacc[c] += dot_nt(dos, p.astype(BF))
                return carry

            lax.fori_loop(0, i + 1, grad_step, 0)
            gall[0, pl.ds(qrows + q0, krows), here] = (dqacc[...] * scale).astype(BF)
            return carry

        lax.fori_loop(0, tiles, tile_step, 0)
        send_own(h, heads + h)

        @pl.when(h == 0)
        def _():
            for t in range(2):
                for a in range(2):
                    x_first(a, t).wait_recv()
                    x_second(a, t).start()

        @pl.when(h >= 1)
        def _():
            serve_near(h - 1, heads + h - 1)

        @pl.when(h >= 2)
        def _():
            serve_far(h - 2, heads + h - 2)
        return carry

    lax.fori_loop(0, heads, head_step, 0)
    pk, pv = 2 * heads, 2 * heads + 1
    for c in range(tiles):
        gall[0, 2 * qrows:2 * qrows + krows, c * tile:(c + 1) * tile] = (dkacc[c] * scale).astype(BF)
        gall[0, 2 * qrows + krows:rows, c * tile:(c + 1) * tile] = dvacc[c].astype(BF)
    send_own(pk, pv)

    for a in range(2):
        x_own(a).wait()
        for t in range(n - 1):
            x_direct(a, t).wait_recv()

    lag = n // 2
    last = heads - 1
    a_pieces = list(range(heads))
    b_pieces = list(range(heads, pieces))

    def closing_step(r, carry):
        @pl.when(r == 1)
        def _():
            arrived(4, a_pieces + b_pieces)

        @pl.when(r == 2)
        def _():
            serve_near(last, heads + last)
            serve_far(last - 1, heads + last - 1)

        @pl.when(r == 4)
        def _():
            arrived(5, a_pieces)
            arrived(6, a_pieces)

        @pl.when(r == 6)
        def _():
            serve_near(pk, pv)
            serve_far(last, heads + last)

        @pl.when(r == 7)
        def _():
            arrived(7, a_pieces)

        @pl.when(r < n)
        def _():
            closing_part(r, load_a, save_a, woa, sta, 0, qrows, dyc, yacc)

        @pl.when(r == 8)
        def _():
            arrived(5, b_pieces)
            arrived(6, b_pieces)

        @pl.when(r == 10)
        def _():
            serve_far(pk, pv)

        @pl.when(r == 11)
        def _():
            arrived(7, b_pieces)

        @pl.when(r >= lag)
        def _():
            closing_part(r - lag, load_b, save_b, wob, stb, qrows, rows, xc, dxacc)
        return carry

    lax.fori_loop(0, n + lag, closing_step, 0)
    out_y = [
        pltpu.make_async_copy(woa.at[0], y_ref.at[pl.ds(0, qrows)], lsem.at[2]),
        pltpu.make_async_copy(woa.at[1, pl.ds(0, tok - qrows)], y_ref.at[pl.ds(qrows, tok - qrows)], lsem.at[3]),
        pltpu.make_async_copy(wob.at[0], dx_ref, lsem.at[4]),
    ]
    woa[0] = yacc[0:qrows].astype(BF)
    woa[1, 0:tok - qrows] = yacc[qrows:tok].astype(BF)
    wob[0] = dxacc[...].astype(BF)
    for copy in out_y:
        copy.start()
    for order in (n - 2, n - 1):
        for copy in save_a(order, order % 2) + save_b(order, order % 2):
            copy.wait()
    for copy in out_y:
        copy.wait()
    for a in range(2):
        for t in range(n - 1):
            x_direct(a, t).wait_send()
        for t in range(2):
            x_second(a, t).wait_send()
    for i in range(pieces):
        own_right(i).wait_send()
        own_left(i).wait_send()
        relay_plus(i).wait_send()
        for slot in range(4):
            to_partner(slot, i).wait_send()


def attend_finish(n, qkv, first, x_act, dy_act, wq, wk, wv, wo):
    blocks, rows, _ = qkv.shape
    tok, model = x_act.shape
    qrows, krows = wq.shape[0] // n, wk.shape[0] // n
    total = blocks * LANES
    mcol = model // n
    brows = rows - qrows
    tile = 512
    pieces = rows // krows
    vmem = pl.BlockSpec(memory_space=pltpu.VMEM)
    anym = pl.BlockSpec(memory_space=pl.ANY)
    dma = pltpu.SemaphoreType.DMA
    assert brows == tok
    return pl.pallas_call(
        functools.partial(main_kernel, (n, qrows, krows, tok, krows ** -0.5)),
        out_shape=(jax.ShapeDtypeStruct((tok, model), BF), jax.ShapeDtypeStruct((tok, model), BF),
                   jax.ShapeDtypeStruct((wq.shape[0], mcol), F32), jax.ShapeDtypeStruct((wk.shape[0], mcol), F32),
                   jax.ShapeDtypeStruct((wv.shape[0], mcol), F32), jax.ShapeDtypeStruct((wo.shape[0], mcol), F32)),
        in_specs=[vmem, vmem, anym, anym, anym, anym, anym, anym],
        out_specs=(anym,) * 6,
        scratch_shapes=[
            pltpu.VMEM((total, 2 * krows), BF),
            pltpu.VMEM((total // tile, tile, tile), F32),
            pltpu.VMEM((krows, tile), F32), pltpu.VMEM((krows, tile), F32),
            pltpu.VMEM((total // tile, krows, tile), F32), pltpu.VMEM((total // tile, krows, tile), F32),
            pltpu.VMEM((n, rows, total), BF),
            pltpu.VMEM((total, mcol), BF), pltpu.VMEM((total, mcol), BF),
            pltpu.VMEM((2, 2, tok, mcol), BF),
            pltpu.VMEM((tok, model), F32), pltpu.VMEM((tok, model), F32),
            pltpu.VMEM((2, qrows, model), BF), pltpu.VMEM((2, brows, model), BF),
            pltpu.VMEM((2, qrows, mcol), F32), pltpu.VMEM((2, brows, mcol), F32),
            dma((2,)), dma((2, 3)), dma((2,)), dma((2, 3)),
            dma((2, pieces)), dma((pieces,)), dma((4, pieces)), dma((8, pieces)),
            dma((2, n)), dma((2, n)), dma((2, 2)), dma((2, 2)), dma((5,)),
        ],
        compiler_params=pltpu.CompilerParams(collective_id=1, has_side_effects=True, vmem_limit_bytes=67043328),
        name='attend_finish',
    )(qkv, first, x_act, dy_act, wq, wk, wv, wo)


def solution(mesh):
    n = mesh.shape['cp']
    row_spec = P(('dp', 'cp'), None)
    tok_spec = P(('dp', 'cp'))
    weight_spec = P(None, None, None)
    grad_spec = P(('dp', 'cp'), None, None)

    def local_step(x_act, seg_ids, w_q, w_k, w_v, w_o, dy_act):
        model, q_heads, head_dim = w_q.shape
        kv_heads = w_k.shape[1]
        assert kv_heads == n and x_act.shape[0] % LANES == 0

        def flat(w):
            return w.transpose(1, 2, 0).reshape(w.shape[1] * head_dim, model)

        def unflat(g, heads):
            return g.reshape(heads, head_dim, g.shape[1]).transpose(2, 0, 1)

        wq, wk, wv, wo = flat(w_q), flat(w_k), flat(w_v), flat(w_o)
        qkv, first = project(n, x_act, dy_act, seg_ids, wq, wk, wv, wo)
        y_out, dx_out, dwq, dwk, dwv, dwo = attend_finish(n, qkv, first, x_act, dy_act, wq, wk, wv, wo)
        return (y_out, dx_out, unflat(dwq, q_heads), unflat(dwk, kv_heads), unflat(dwv, kv_heads), unflat(dwo, q_heads))

    return jax.shard_map(local_step, mesh=mesh,
                         in_specs=(row_spec, tok_spec, weight_spec, weight_spec, weight_spec, weight_spec, row_spec),
                         out_specs=(row_spec, row_spec, grad_spec, grad_spec, grad_spec, grad_spec),
                         check_vma=False)
```

```python
import functools

import jax
import jax.numpy as jnp
from jax import lax
from jax.experimental import pallas as pl
from jax.experimental.pallas import tpu as pltpu
from jax.sharding import PartitionSpec as P

BF = jnp.bfloat16
F32 = jnp.float32
LANES = 128
LOG2E = 1.4426950408889634
VMEM_MAX = 48 * 1024 * 1024


def rdma(src, dst, send_sem, recv_sem, peer):
    return pltpu.make_async_remote_copy(src_ref=src, dst_ref=dst, send_sem=send_sem, recv_sem=recv_sem,
                                        device_id={'cp': peer}, device_id_type=pl.DeviceIdType.MESH)


def dot_nt(left, right):
    return lax.dot_general(left, right, (((1,), (1,)), ((), ())), preferred_element_type=F32)


def dot_tn(left, right):
    return lax.dot_general(left, right, (((0,), (0,)), ((), ())), preferred_element_type=F32)


def dot_nn(left, right):
    return lax.dot_general(left, right, (((1,), (0,)), ((), ())), preferred_element_type=F32)


def project_kernel(dims, x_ref, dy_ref, seg_ref, wq_ref, wk_ref, wv_ref, wo_ref, out_ref, first_ref,
                   xbuf, dybuf, wbuf, sbuf, rbuf, seg_mine, seg_all, wsem, ssem, rsem, fsem, fsend, gsend, grecv, lsem):
    n, qrows, krows = dims
    chips = n // 2
    me = lax.axis_index('cp')
    chip, core = me // 2, me % 2
    sgn = 1 - 2 * core
    rows = 2 * qrows + 2 * krows
    srow = qrows + 2 * krows

    def device(chip_off, flip):
        return ((chip + chip_off + chips) % chips) * 2 + (core + flip) % 2

    dests = [device(2, 0), device(2, 1), device(-sgn, 0), device(-sgn, 1), device(sgn, 0), device(sgn, 1), device(0, 1)]
    ahead = dests[4]
    relay_from = device(-sgn, 0)

    barrier = pltpu.get_barrier_semaphore()
    for peer in dests:
        pl.semaphore_signal(barrier, inc=1, device_id={'cp': peer}, device_id_type=pl.DeviceIdType.MESH)

    def dest_of(step):
        pair, flip = step // 2, (step + step // 6) % 2
        off = 2 - 3 * pair + 5 * (pair // 2) + 2 * (pair // 3)
        return ((chip + sgn * off + chips) % chips) * 2 + (core + flip) % 2

    def weight_copies(step, slot):
        dst = dest_of(step)
        return [
            pltpu.make_async_copy(wq_ref.at[pl.ds(dst * qrows, qrows)], wbuf.at[slot, pl.ds(0, qrows)], wsem.at[slot, 0]),
            pltpu.make_async_copy(wk_ref.at[pl.ds(dst * krows, krows)], wbuf.at[slot, pl.ds(qrows, krows)], wsem.at[slot, 1]),
            pltpu.make_async_copy(wv_ref.at[pl.ds(dst * krows, krows)], wbuf.at[slot, pl.ds(qrows + krows, krows)], wsem.at[slot, 2]),
            pltpu.make_async_copy(wo_ref.at[pl.ds(dst * qrows, qrows)], wbuf.at[slot, pl.ds(srow, qrows)], wsem.at[slot, 3]),
        ]

    x_in = pltpu.make_async_copy(x_ref, xbuf, lsem.at[1])
    dy_in = pltpu.make_async_copy(dy_ref, dybuf, lsem.at[2])
    x_in.start()
    for copy in weight_copies(0, 0):
        copy.start()
    dy_in.start()
    seg_mine[...] = jnp.broadcast_to(seg_ref[...], seg_mine.shape)
    pl.semaphore_wait(barrier, n - 1)

    def first_leg(t):
        return rdma(sbuf.at[t], rbuf.at[t], ssem.at[t], fsem.at[t], ahead)

    def second_leg(t):
        return rdma(rbuf.at[t], out_ref.at[relay_from], fsend.at[t], rsem.at[t], device(sgn, t))

    def direct(t):
        return rdma(sbuf.at[t], out_ref.at[me], ssem.at[t], rsem.at[t], dests[t])

    def own_block():
        return pltpu.make_async_copy(sbuf.at[n - 1], out_ref.at[me], lsem.at[0])

    def seg_copy(t):
        return rdma(seg_mine, seg_all.at[me], gsend.at[t], grecv.at[t], dests[t])

    for t in range(n - 1):
        seg_copy(t).start()
    seg_all[me] = seg_mine[...]
    x_in.wait()
    dy_in.wait()

    def compute_step(step, carry):
        slot = step % 2

        @pl.when(step < n - 1)
        def _():
            for copy in weight_copies(step + 1, 1 - slot):
                copy.start()

        for copy in weight_copies(step, slot):
            copy.wait()
        sbuf[step, 0:srow] = dot_nt(wbuf[slot, 0:srow], xbuf[...]).astype(BF)
        sbuf[step, srow:rows] = dot_nt(wbuf[slot, srow:rows], dybuf[...]).astype(BF)
        for t in range(n):
            @pl.when(step == t)
            def _():
                if t < 2:
                    first_leg(t).start()
                elif t < n - 1:
                    direct(t).start()
                else:
                    own_block().start()
        return carry

    lax.fori_loop(0, n, compute_step, 0)
    for t in range(2):
        first_leg(t).wait_recv()
        second_leg(t).start()

    for t in range(n - 1):
        seg_copy(t).wait_recv()
    tok = seg_all.shape[2]
    row_id = lax.broadcasted_iota(jnp.int32, (n, tok), 0)
    lane_id = lax.broadcasted_iota(jnp.int32, (n, tok), 1)
    seg = jnp.zeros((n, tok), jnp.int32)
    for d in range(n):
        seg = jnp.where(row_id == d, seg_all[d], seg)
    before = jnp.where(lane_id == 0, pltpu.roll(pltpu.roll(seg, 1, 1), 1, 0), pltpu.roll(seg, 1, 1))
    pos = row_id * tok + lane_id
    best = jnp.where((seg != before) & (pos > 0), pos, 0)
    shift = 1
    while shift < tok:
        best = jnp.maximum(best, jnp.where(lane_id >= shift, pltpu.roll(best, shift, 1), 0))
        shift *= 2
    last = jnp.broadcast_to(best[:, tok - 1:tok], (n, tok))
    carry_max = jnp.where(row_id >= 1, pltpu.roll(last, 1, 0), 0)
    shift = 1
    while shift < n:
        carry_max = jnp.maximum(carry_max, jnp.where(row_id >= shift, pltpu.roll(carry_max, shift, 0), 0))
        shift *= 2
    best = jnp.maximum(best, carry_max)
    for d in range(n):
        first_ref[d] = jnp.broadcast_to(best[d:d + 1], (8, tok))

    own_block().wait()
    for t in range(n - 1):
        direct(t).wait_recv()
    for t in range(2):
        first_leg(t).wait_send()
        second_leg(t).wait_send()
    for t in range(2, n - 1):
        direct(t).wait_send()
    for t in range(n - 1):
        seg_copy(t).wait_send()


def project(n, x_act, dy_act, seg, wq, wk, wv, wo):
    tok, model = x_act.shape
    qrows, krows = wq.shape[0] // n, wk.shape[0] // n
    rows = 2 * qrows + 2 * krows
    vmem = pl.BlockSpec(memory_space=pltpu.VMEM)
    anym = pl.BlockSpec(memory_space=pl.ANY)
    dma = pltpu.SemaphoreType.DMA
    return pl.pallas_call(
        functools.partial(project_kernel, (n, qrows, krows)),
        out_shape=(jax.ShapeDtypeStruct((n, rows, tok), BF), jax.ShapeDtypeStruct((n, 8, tok), jnp.int32)),
        in_specs=[anym, anym, vmem, anym, anym, anym, anym],
        out_specs=(anym, vmem),
        scratch_shapes=[
            pltpu.VMEM((tok, model), BF), pltpu.VMEM((tok, model), BF),
            pltpu.VMEM((2, rows, model), BF),
            pltpu.VMEM((n, rows, tok), BF),
            pltpu.VMEM((2, rows, tok), BF),
            pltpu.VMEM((8, tok), jnp.int32),
            pltpu.VMEM((n, 8, tok), jnp.int32),
            dma((2, 4)), dma((n,)), dma((n,)), dma((2,)), dma((2,)), dma((n,)), dma((n,)), dma((3,)),
        ],
        compiler_params=pltpu.CompilerParams(collective_id=0, has_side_effects=True, vmem_limit_bytes=VMEM_MAX),
        name='project_exchange',
    )(x_act, dy_act, seg.reshape(1, tok), wq, wk, wv, wo)


def pick(index, values):
    out = values[0]
    for k in range(1, len(values)):
        out = jnp.where(index == k, values[k], out)
    return out


def main_kernel(dims, qkv_ref, first_ref, x_ref, dy_ref, wq_ref, wk_ref, wv_ref, wo_ref,
                y_ref, dx_ref, dwq_ref, dwk_ref, dwv_ref, dwo_ref,
                kvn, pbuf, rhsq, rhsd, oacc, dqacc, dkacc, dvacc, gall, xc, dyc, xrel, yacc, dxacc,
                woa, wob, woc, sta, stb, stc, wsem, outsem, osem, relsem, parsem, rsem, xsend, xrecv, xfirst, xsecond, lsem):
    n, qrows, krows, tok, scale = dims
    chips = n // 2
    heads = qrows // krows
    group = rhsq.shape[1] // tok
    me = lax.axis_index('cp')
    chip, core = me // 2, me % 2
    sgn = 1 - 2 * core
    rows = 2 * qrows + 2 * krows
    model = yacc.shape[1]
    mcol = xc.shape[1]
    ncol = 1024
    width = group * tok
    kv0, do0 = qrows, qrows + 2 * krows

    def device(chip_off, flip):
        return ((chip + chip_off + chips) % chips) * 2 + (core + flip) % 2

    right, left, partner = device(1, 0), device(-1, 0), device(0, 1)
    dests = [device(2, 0), device(2, 1), device(-sgn, 0), device(-sgn, 1), device(sgn, 0), device(sgn, 1), partner]
    ahead = dests[4]
    relay_from = device(-sgn, 0)

    barrier = pltpu.get_barrier_semaphore()
    for peer in dests:
        pl.semaphore_signal(barrier, inc=1, device_id={'cp': peer}, device_id_type=pl.DeviceIdType.MESH)

    sides = ((x_ref, xc), (dy_ref, dyc))

    def columns(ref, dst):
        return ref.at[:, pl.ds(pl.multiple_of(dst * mcol, LANES), mcol)]

    def token_rows(ref, src):
        return ref.at[pl.ds(pl.multiple_of(src * tok, LANES), tok)]

    def x_first(a, t):
        return rdma(columns(sides[a][0], dests[t]), xrel.at[a, t], xsend.at[a, t], xfirst.at[a, t], ahead)

    def x_second(a, t):
        return rdma(xrel.at[a, t], token_rows(sides[a][1], relay_from), xsecond.at[a, t], xrecv.at[a, t], device(sgn, t))

    def x_direct(a, t):
        return rdma(columns(sides[a][0], dests[t]), token_rows(sides[a][1], me), xsend.at[a, t], xrecv.at[a, t], dests[t])

    def x_own(a):
        return pltpu.make_async_copy(columns(sides[a][0], me), token_rows(sides[a][1], me), lsem.at[a])

    def view(slot, part, j):
        if part == 0:
            return gall.at[slot, j, pl.ds(0, qrows)]
        if part == 1:
            return gall.at[slot, j, pl.ds(do0, qrows)]
        return gall.at[slot, pl.ds(j * (n // 2), n // 2), pl.ds(kv0, 2 * krows)]

    def own_right(part, j):
        return rdma(view(0, part, j), view(1, part, j), osem.at[0, part, j], rsem.at[1, part, j], right)

    def own_left(part, j):
        return rdma(view(0, part, j), view(2, part, j), osem.at[1, part, j], rsem.at[2, part, j], left)

    def relay_plus(part, j):
        return rdma(view(1, part, j), view(3, part, j), relsem.at[part, j], rsem.at[3, part, j], right)

    def relay_minus(part, j):
        return rdma(view(2, part, j), view(3, part, j), relsem.at[part, j], rsem.at[3, part, j], left)

    def to_partner(slot, part, j):
        return rdma(view(slot, part, j), view(4 + slot, part, j), parsem.at[slot, part, j], rsem.at[4 + slot, part, j], partner)

    def send_own(first, second):
        for item in (first, second):
            own_right(*item).start()
            own_left(*item).start()
            to_partner(0, *item).start()

    def serve_near(first, second):
        own_right(*first).wait_recv()
        relay_plus(*first).start()
        to_partner(1, *first).start()
        own_left(*second).wait_recv()
        relay_minus(*second).start()
        to_partner(2, *second).start()
        own_right(*second).wait_recv()
        to_partner(1, *second).start()
        own_left(*first).wait_recv()
        to_partner(2, *first).start()

    def serve_far(first, second):
        relay_plus(*first).wait_recv()
        to_partner(3, *first).start()
        relay_minus(*second).wait_recv()
        to_partner(3, *second).start()

    def tile_items(j):
        return (0, j), (1, j)

    kv_items = ((2, 0), (2, 1))

    def arrived_tiles(slot):
        for j in range(n):
            for item in tile_items(j):
                to_partner(slot - 4, *item).wait_recv()

    def arrived_kv(slot):
        for item in kv_items:
            to_partner(slot - 4, *item).wait_recv()

    slot_table = (0, 4, 1, 2, 5, 6, 3, 7)
    off_table = (0, 0, chips - 1, 1, chips - 1, 1, 2, 2)
    flip_table = (0, 1, 0, 0, 1, 1, 0, 1)

    def source_of(order):
        return ((chip + pick(order, off_table)) % chips) * 2 + (core + pick(order, flip_table)) % 2

    def load(kind, order, buf):
        src = source_of(order)
        if kind == 0:
            return [pltpu.make_async_copy(wo_ref.at[pl.ds(src * qrows, qrows)], woa.at[buf], wsem.at[0, buf])]
        if kind == 1:
            return [pltpu.make_async_copy(wq_ref.at[pl.ds(src * qrows, qrows)], wob.at[buf], wsem.at[1, buf])]
        return [pltpu.make_async_copy(wk_ref.at[pl.ds(src * krows, krows)], woc.at[buf, pl.ds(0, krows)], wsem.at[2, buf]),
                pltpu.make_async_copy(wv_ref.at[pl.ds(src * krows, krows)], woc.at[buf, pl.ds(krows, krows)], wsem.at[3, buf])]

    def save(kind, order, buf):
        src = source_of(order)
        if kind == 0:
            return [pltpu.make_async_copy(sta.at[buf], dwo_ref.at[pl.ds(src * qrows, qrows)], outsem.at[0, buf])]
        if kind == 1:
            return [pltpu.make_async_copy(stb.at[buf], dwq_ref.at[pl.ds(src * qrows, qrows)], outsem.at[1, buf])]
        return [pltpu.make_async_copy(stc.at[buf, pl.ds(0, krows)], dwk_ref.at[pl.ds(src * krows, krows)], outsem.at[2, buf]),
                pltpu.make_async_copy(stc.at[buf, pl.ds(krows, krows)], dwv_ref.at[pl.ds(src * krows, krows)], outsem.at[3, buf])]

    kinds = ((0, qrows, woa, sta, dyc, yacc), (do0, rows, wob, stb, xc, dxacc), (kv0, do0, woc, stc, xc, dxacc))

    def closing_part(kind, order):
        row0, row1, wbuf, stage, other, acc = kinds[kind]
        buf = order % 2
        slot = pick(order, slot_table)
        for copy in load(kind, order, buf):
            copy.wait()

        @pl.when(order < n - 1)
        def _():
            for copy in load(kind, order + 1, 1 - buf):
                copy.start()

        @pl.when(order >= 2)
        def _():
            for copy in save(kind, order - 2, buf):
                copy.wait()
        wide = jnp.concatenate([gall[slot, j, row0:row1, :] for j in range(n)], axis=1)
        stage[buf] = dot_nn(wide, other[...])
        for copy in save(kind, order, buf):
            copy.start()
        left_t = gall[slot, me, row0:row1, :]

        def col(j, carry):
            cols = pl.ds(pl.multiple_of(j * ncol, ncol), ncol)
            acc[:, cols] += dot_tn(left_t, wbuf[buf, :, cols])
            return carry

        lax.fori_loop(0, model // ncol, col, 0)

    qkv_in = pltpu.make_async_copy(qkv_ref, gall.at[0], lsem.at[2])
    qkv_in.start()
    for a in range(2):
        x_own(a).start()
    for kind in range(3):
        for copy in load(kind, 0, 0):
            copy.start()
    pl.semaphore_wait(barrier, n - 1)
    for t in range(n - 1):
        for a in range(2):
            (x_first if t < 2 else x_direct)(a, t).start()
    dkacc[...] = jnp.zeros_like(dkacc)
    dvacc[...] = jnp.zeros_like(dvacc)
    yacc[...] = jnp.zeros_like(yacc)
    dxacc[...] = jnp.zeros_like(dxacc)
    rhsq[...] = jnp.zeros_like(rhsq)
    rhsd[...] = jnp.zeros_like(rhsd)
    qkv_in.wait()

    def transpose_tile(c, carry):
        kvn[pl.ds(pl.multiple_of(c * tok, LANES), tok), :] = gall[0, c, kv0:do0, :].T
        return carry

    lax.fori_loop(0, n, transpose_tile, 0)
    score_mul = scale * LOG2E
    grp = tok // 8

    def attend(i, pair):
        q0 = pl.multiple_of(pair * group * krows, krows)
        for g in range(group):
            lanes = slice(g * tok, (g + 1) * tok)
            rhsq[0:krows, lanes] = gall[0, i, pl.ds(q0 + g * krows, krows), :]
            rhsd[krows:2 * krows, lanes] = gall[0, i, pl.ds(do0 + q0 + g * krows, krows), :]
        first = jnp.concatenate([first_ref[i][0:1]] * group, axis=1)
        qpos = i * tok + lax.broadcasted_iota(jnp.int32, (1, tok), 1)
        qpos = jnp.concatenate([qpos] * group, axis=1)

        def score_step(c, top):
            s = dot_nn(kvn[pl.ds(pl.multiple_of(c * tok, LANES), tok), :], rhsq[...])
            kpos = lax.broadcasted_iota(jnp.int32, (tok, width), 0) + c * tok
            s = jnp.where((kpos >= first) & (kpos <= qpos), s, -jnp.inf)
            pbuf[c] = s
            return jnp.maximum(top, jnp.max(s.reshape(grp, 8, width), axis=0))

        top = lax.fori_loop(0, i + 1, score_step, jnp.full((8, width), -jnp.inf, F32))
        top = jnp.max(top, axis=0, keepdims=True) * score_mul
        oacc[...] = jnp.zeros_like(oacc)

        def value_step(c, total):
            p = jnp.exp2(pbuf[c] * score_mul - top)
            pbuf[c] = p
            oacc[...] += dot_nn(gall[0, c, kv0 + krows:do0, :], p.astype(BF))
            return total + jnp.sum(p.reshape(grp, 8, width), axis=0)

        total = lax.fori_loop(0, i + 1, value_step, jnp.zeros((8, width), F32))
        inv = 1.0 / jnp.sum(total, axis=0, keepdims=True)
        o_blk = (oacc[...] * inv).astype(BF)
        delta = jnp.sum(rhsd[krows:2 * krows, :].astype(F32) * o_blk.astype(F32), axis=0, keepdims=True)
        for g in range(group):
            gall[0, i, pl.ds(q0 + g * krows, krows), :] = o_blk[:, g * tok:(g + 1) * tok]
        dqacc[...] = jnp.zeros_like(dqacc)

        def grad_step(c, carry):
            dp = dot_nn(kvn[pl.ds(pl.multiple_of(c * tok, LANES), tok), :], rhsd[...])
            p = pbuf[c] * inv
            ds = (p * (dp - delta)).astype(BF)
            dqacc[...] += dot_nn(gall[0, c, kv0:kv0 + krows, :], ds)
            dkacc[c] += dot_nt(rhsq[0:krows, :], ds)
            dvacc[c] += dot_nt(rhsd[krows:2 * krows, :], p.astype(BF))
            return carry

        lax.fori_loop(0, i + 1, grad_step, 0)
        dq = (dqacc[...] * scale).astype(BF)
        for g in range(group):
            gall[0, i, pl.ds(do0 + q0 + g * krows, krows), :] = dq[:, g * tok:(g + 1) * tok]

    lag = n // 2

    def tile_step(i, carry):
        def pair_step(pair, inner):
            attend(i, pair)
            return inner

        lax.fori_loop(0, heads // group, pair_step, 0)
        send_own(*tile_items(i))

        @pl.when(i == 2)
        def _():
            for t in range(2):
                for a in range(2):
                    x_first(a, t).wait_recv()
                    x_second(a, t).start()

        @pl.when(i >= lag)
        def _():
            serve_near(*tile_items(i - lag))
        return carry

    lax.fori_loop(0, n, tile_step, 0)
    for c in range(n):
        gall[0, c, kv0:kv0 + krows, :] = (dkacc[c] * scale).astype(BF)
        gall[0, c, kv0 + krows:do0, :] = dvacc[c].astype(BF)
    send_own(*kv_items)

    for a in range(2):
        x_own(a).wait()
        for t in range(n - 1):
            x_direct(a, t).wait_recv()

    def closing_step(r, carry):
        @pl.when(r == 0)
        def _():
            serve_near(*tile_items(lag))

        @pl.when(r == 1)
        def _():
            serve_near(*tile_items(lag + 1))
            arrived_tiles(4)

        @pl.when(r == 2)
        def _():
            for j in range(lag + 2, n):
                serve_near(*tile_items(j))

        @pl.when(r == 4)
        def _():
            for j in range(lag):
                serve_far(*tile_items(j))
            arrived_tiles(5)

        @pl.when(r == 5)
        def _():
            arrived_tiles(6)

        @pl.when(r == 6)
        def _():
            serve_near(*kv_items)
            for j in range(lag, n):
                serve_far(*tile_items(j))

        @pl.when(r == 7)
        def _():
            arrived_tiles(7)

        @pl.when(r < n)
        def _():
            closing_part(0, r)
            closing_part(1, r)

        @pl.when(r == n + 1)
        def _():
            arrived_kv(4)

        @pl.when(r == n + 4)
        def _():
            arrived_kv(5)
            arrived_kv(6)

        @pl.when(r == n + 6)
        def _():
            serve_far(*kv_items)

        @pl.when(r == n + 7)
        def _():
            arrived_kv(7)

        @pl.when(r >= n)
        def _():
            closing_part(2, r - n)
        return carry

    lax.fori_loop(0, 2 * n, closing_step, 0)
    spare = tok - qrows
    outs = [
        pltpu.make_async_copy(woa.at[0], y_ref.at[pl.ds(0, qrows)], lsem.at[3]),
        pltpu.make_async_copy(woa.at[1, pl.ds(0, spare)], y_ref.at[pl.ds(qrows, spare)], lsem.at[4]),
        pltpu.make_async_copy(wob.at[0], dx_ref.at[pl.ds(0, qrows)], lsem.at[5]),
        pltpu.make_async_copy(wob.at[1, pl.ds(0, spare)], dx_ref.at[pl.ds(qrows, spare)], lsem.at[6]),
    ]
    woa[0] = yacc[0:qrows].astype(BF)
    woa[1, 0:spare] = yacc[qrows:tok].astype(BF)
    wob[0] = dxacc[0:qrows].astype(BF)
    wob[1, 0:spare] = dxacc[qrows:tok].astype(BF)
    for copy in outs:
        copy.start()
    for kind in range(3):
        for order in (n - 2, n - 1):
            for copy in save(kind, order, order % 2):
                copy.wait()
    for copy in outs:
        copy.wait()
    for a in range(2):
        for t in range(n - 1):
            x_direct(a, t).wait_send()
        for t in range(2):
            x_second(a, t).wait_send()

    def drain(items):
        for item in items:
            own_right(*item).wait_send()
            own_left(*item).wait_send()
            for slot in range(4):
                to_partner(slot, *item).wait_send()
        relay_plus(*items[0]).wait_send()
        relay_minus(*items[1]).wait_send()

    for j in range(n):
        drain(tile_items(j))
    drain(kv_items)


def attend_finish(n, qkv, first, x_act, dy_act, wq, wk, wv, wo):
    _, rows, tok = qkv.shape
    model = x_act.shape[1]
    qrows, krows = wq.shape[0] // n, wk.shape[0] // n
    total = n * tok
    mcol = model // n
    group = 2
    width = group * tok
    vmem = pl.BlockSpec(memory_space=pltpu.VMEM)
    anym = pl.BlockSpec(memory_space=pl.ANY)
    dma = pltpu.SemaphoreType.DMA
    return pl.pallas_call(
        functools.partial(main_kernel, (n, qrows, krows, tok, krows ** -0.5)),
        out_shape=(jax.ShapeDtypeStruct((tok, model), BF), jax.ShapeDtypeStruct((tok, model), BF),
                   jax.ShapeDtypeStruct((wq.shape[0], mcol), F32), jax.ShapeDtypeStruct((wk.shape[0], mcol), F32),
                   jax.ShapeDtypeStruct((wv.shape[0], mcol), F32), jax.ShapeDtypeStruct((wo.shape[0], mcol), F32)),
        in_specs=[anym, vmem, anym, anym, anym, anym, anym, anym],
        out_specs=(anym,) * 6,
        scratch_shapes=[
            pltpu.VMEM((total, 2 * krows), BF),
            pltpu.VMEM((n, tok, width), F32),
            pltpu.VMEM((2 * krows, width), BF), pltpu.VMEM((2 * krows, width), BF),
            pltpu.VMEM((krows, width), F32), pltpu.VMEM((krows, width), F32),
            pltpu.VMEM((n, krows, tok), F32), pltpu.VMEM((n, krows, tok), F32),
            pltpu.VMEM((n, n, rows, tok), BF),
            pltpu.VMEM((total, mcol), BF), pltpu.VMEM((total, mcol), BF),
            pltpu.VMEM((2, 2, tok, mcol), BF),
            pltpu.VMEM((tok, model), F32), pltpu.VMEM((tok, model), F32),
            pltpu.VMEM((2, qrows, model), BF), pltpu.VMEM((2, qrows, model), BF), pltpu.VMEM((2, 2 * krows, model), BF),
            pltpu.VMEM((2, qrows, mcol), F32), pltpu.VMEM((2, qrows, mcol), F32), pltpu.VMEM((2, 2 * krows, mcol), F32),
            dma((4, 2)), dma((4, 2)),
            dma((2, 3, n)), dma((3, n)), dma((4, 3, n)), dma((8, 3, n)),
            dma((2, n)), dma((2, n)), dma((2, 2)), dma((2, 2)), dma((7,)),
        ],
        compiler_params=pltpu.CompilerParams(collective_id=1, has_side_effects=True, vmem_limit_bytes=67043328),
        name='attend_finish',
    )(qkv, first, x_act, dy_act, wq, wk, wv, wo)


def solution(mesh):
    n = mesh.shape['cp']
    row_spec = P(('dp', 'cp'), None)
    tok_spec = P(('dp', 'cp'))
    weight_spec = P(None, None, None)
    grad_spec = P(('dp', 'cp'), None, None)

    def local_step(x_act, seg_ids, w_q, w_k, w_v, w_o, dy_act):
        model, q_heads, head_dim = w_q.shape
        kv_heads = w_k.shape[1]
        assert kv_heads == n and x_act.shape[0] % LANES == 0

        def flat(w):
            return w.transpose(1, 2, 0).reshape(w.shape[1] * head_dim, model)

        def unflat(g, heads):
            return g.reshape(heads, head_dim, g.shape[1]).transpose(2, 0, 1)

        wq, wk, wv, wo = flat(w_q), flat(w_k), flat(w_v), flat(w_o)
        qkv, first = project(n, x_act, dy_act, seg_ids, wq, wk, wv, wo)
        y_out, dx_out, dwq, dwk, dwv, dwo = attend_finish(n, qkv, first, x_act, dy_act, wq, wk, wv, wo)
        return (y_out, dx_out, unflat(dwq, q_heads), unflat(dwk, kv_heads), unflat(dwv, kv_heads), unflat(dwo, q_heads))

    return jax.shard_map(local_step, mesh=mesh,
                         in_specs=(row_spec, tok_spec, weight_spec, weight_spec, weight_spec, weight_spec, row_spec),
                         out_specs=(row_spec, row_spec, grad_spec, grad_spec, grad_spec, grad_spec),
                         check_vma=False)
```

```python
import functools

import jax
import jax.numpy as jnp
from jax import lax
from jax.experimental import pallas as pl
from jax.experimental.pallas import tpu as pltpu
from jax.sharding import PartitionSpec as P

BF = jnp.bfloat16
F32 = jnp.float32
LANES = 128
LOG2E = 1.4426950408889634
VMEM_MAX = 67043328


def rdma(src, dst, send_sem, recv_sem, peer):
    return pltpu.make_async_remote_copy(src_ref=src, dst_ref=dst, send_sem=send_sem, recv_sem=recv_sem,
                                        device_id={'cp': peer}, device_id_type=pl.DeviceIdType.MESH)


def dot_nt(left, right):
    return lax.dot_general(left, right, (((1,), (1,)), ((), ())), preferred_element_type=F32)


def dot_tn(left, right):
    return lax.dot_general(left, right, (((0,), (0,)), ((), ())), preferred_element_type=F32)


def dot_nn(left, right):
    return lax.dot_general(left, right, (((1,), (0,)), ((), ())), preferred_element_type=F32)


def pick(index, values):
    out = values[0]
    for k in range(1, len(values)):
        out = jnp.where(index == k, values[k], out)
    return out


def main_kernel(dims, x_ref, dy_ref, seg_ref, wq_ref, wk_ref, wv_ref, wo_ref,
                y_ref, dx_ref, dwq_ref, dwk_ref, dwv_ref, dwo_ref,
                xbuf, dybuf, seg_mine, seg_all, first_ref,
                kvn, pbuf, rhsq, rhsd, oacc, dqacc, dkacc, dvacc, gall, xc, dyc, xrel, yacc, dxacc,
                woa, wob, woc, sta, stb, stc, wsem, outsem, osem, relsem, parsem, rsem, xsend, xrecv, xfirst, xsecond, lsem,
                psend, precv, pfirst, psecond, gsend, grecv, free_far, free_par):
    n, qrows, krows, tok, scale = dims
    chips = n // 2
    heads = qrows // krows
    group = rhsq.shape[1] // tok
    me = lax.axis_index('cp')
    chip, core = me // 2, me % 2
    sgn = 1 - 2 * core
    rows = 2 * qrows + 2 * krows
    model = yacc.shape[1]
    mcol = xc.shape[1]
    ncol = 1024
    width = group * tok
    kv0, do0 = qrows, qrows + 2 * krows

    def device(chip_off, flip):
        return ((chip + chip_off + chips) % chips) * 2 + (core + flip) % 2

    right, left, partner = device(1, 0), device(-1, 0), device(0, 1)
    dests = [device(2, 0), device(2, 1), device(-sgn, 0), device(-sgn, 1), device(sgn, 0), device(sgn, 1), partner]
    ahead = dests[4]
    relay_from = device(-sgn, 0)

    barrier = pltpu.get_barrier_semaphore()
    for peer in dests:
        pl.semaphore_signal(barrier, inc=1, device_id={'cp': peer}, device_id_type=pl.DeviceIdType.MESH)

    sides = ((x_ref, xc), (dy_ref, dyc))

    def columns(ref, dst):
        return ref.at[:, pl.ds(pl.multiple_of(dst * mcol, LANES), mcol)]

    def token_rows(ref, src):
        return ref.at[pl.ds(pl.multiple_of(src * tok, LANES), tok)]

    def x_first(a, t):
        return rdma(columns(sides[a][0], dests[t]), xrel.at[a, t], xsend.at[a, t], xfirst.at[a, t], ahead)

    def x_second(a, t):
        return rdma(xrel.at[a, t], token_rows(sides[a][1], relay_from), xsecond.at[a, t], xrecv.at[a, t], device(sgn, t))

    def x_direct(a, t):
        return rdma(columns(sides[a][0], dests[t]), token_rows(sides[a][1], me), xsend.at[a, t], xrecv.at[a, t], dests[t])

    def x_own(a):
        return pltpu.make_async_copy(columns(sides[a][0], me), token_rows(sides[a][1], me), lsem.at[a])

    def view(slot, part, j):
        if part == 0:
            return gall.at[slot, j, pl.ds(0, qrows)]
        if part == 1:
            return gall.at[slot, j, pl.ds(do0, qrows)]
        return gall.at[slot, pl.ds(j * (n // 2), n // 2), pl.ds(kv0, 2 * krows)]

    def own_right(part, j):
        return rdma(view(0, part, j), view(1, part, j), osem.at[0, part, j], rsem.at[1, part, j], right)

    def own_left(part, j):
        return rdma(view(0, part, j), view(2, part, j), osem.at[1, part, j], rsem.at[2, part, j], left)

    def relay_plus(part, j):
        return rdma(view(1, part, j), view(3, part, j), relsem.at[part, j], rsem.at[3, part, j], right)

    def relay_minus(part, j):
        return rdma(view(2, part, j), view(3, part, j), relsem.at[part, j], rsem.at[3, part, j], left)

    def to_partner(slot, part, j):
        return rdma(view(slot, part, j), view(4 + slot, part, j), parsem.at[slot, part, j], rsem.at[4 + slot, part, j], partner)

    def send_own(first, second):
        for item in (first, second):
            own_right(*item).start()
            own_left(*item).start()
            to_partner(0, *item).start()

    def serve_near(first, second):
        own_right(*first).wait_recv()
        relay_plus(*first).start()
        to_partner(1, *first).start()
        own_left(*second).wait_recv()
        relay_minus(*second).start()
        to_partner(2, *second).start()
        own_right(*second).wait_recv()
        to_partner(1, *second).start()
        own_left(*first).wait_recv()
        to_partner(2, *first).start()

    def serve_far(first, second):
        relay_plus(*first).wait_recv()
        to_partner(3, *first).start()
        relay_minus(*second).wait_recv()
        to_partner(3, *second).start()

    def tile_items(j):
        return (0, j), (1, j)

    kv_items = ((2, 0), (2, 1))

    def arrived_tiles(slot):
        for j in range(n):
            for item in tile_items(j):
                to_partner(slot - 4, *item).wait_recv()

    def arrived_kv(slot):
        for item in kv_items:
            to_partner(slot - 4, *item).wait_recv()

    slot_table = (0, 4, 1, 2, 5, 6, 3, 7)
    off_table = (0, 0, chips - 1, 1, chips - 1, 1, 2, 2)
    flip_table = (0, 1, 0, 0, 1, 1, 0, 1)

    def source_of(order):
        return ((chip + pick(order, off_table)) % chips) * 2 + (core + pick(order, flip_table)) % 2

    def load(kind, order, buf):
        src = source_of(order)
        if kind == 0:
            return [pltpu.make_async_copy(wo_ref.at[pl.ds(src * qrows, qrows)], woa.at[buf], wsem.at[0, buf])]
        if kind == 1:
            return [pltpu.make_async_copy(wq_ref.at[pl.ds(src * qrows, qrows)], wob.at[buf], wsem.at[1, buf])]
        return [pltpu.make_async_copy(wk_ref.at[pl.ds(src * krows, krows)], woc.at[buf, pl.ds(0, krows)], wsem.at[2, buf]),
                pltpu.make_async_copy(wv_ref.at[pl.ds(src * krows, krows)], woc.at[buf, pl.ds(krows, krows)], wsem.at[3, buf])]

    def save(kind, order, buf):
        src = source_of(order)
        if kind == 0:
            return [pltpu.make_async_copy(sta.at[buf], dwo_ref.at[pl.ds(src * qrows, qrows)], outsem.at[0, buf])]
        if kind == 1:
            return [pltpu.make_async_copy(stb.at[buf], dwq_ref.at[pl.ds(src * qrows, qrows)], outsem.at[1, buf])]
        return [pltpu.make_async_copy(stc.at[buf, pl.ds(0, krows)], dwk_ref.at[pl.ds(src * krows, krows)], outsem.at[2, buf]),
                pltpu.make_async_copy(stc.at[buf, pl.ds(krows, krows)], dwv_ref.at[pl.ds(src * krows, krows)], outsem.at[3, buf])]

    kinds = ((0, qrows, woa, sta, dyc, yacc), (do0, rows, wob, stb, xc, dxacc), (kv0, do0, woc, stc, xc, dxacc))

    def closing_part(kind, order):
        row0, row1, wbuf, stage, other, acc = kinds[kind]
        buf = order % 2
        slot = pick(order, slot_table)
        for copy in load(kind, order, buf):
            copy.wait()

        @pl.when(order < n - 1)
        def _():
            for copy in load(kind, order + 1, 1 - buf):
                copy.start()

        @pl.when(order >= 2)
        def _():
            for copy in save(kind, order - 2, buf):
                copy.wait()
        wide = jnp.concatenate([gall[slot, j, row0:row1, :] for j in range(n)], axis=1)
        stage[buf] = dot_nn(wide, other[...])
        for copy in save(kind, order, buf):
            copy.start()
        left_t = gall[slot, me, row0:row1, :]

        def col(j, carry):
            cols = pl.ds(pl.multiple_of(j * ncol, ncol), ncol)
            acc[:, cols] += dot_tn(left_t, wbuf[buf, :, cols])
            return carry

        lax.fori_loop(0, model // ncol, col, 0)

    def block_copies(step, buf):
        pair, flip = step // 2, (step + step // 6) % 2
        off = 2 - 3 * pair + 5 * (pair // 2) + 2 * (pair // 3)
        dst = ((chip + sgn * off + chips) % chips) * 2 + (core + flip) % 2
        return [
            pltpu.make_async_copy(wo_ref.at[pl.ds(dst * qrows, qrows)], woa.at[buf], wsem.at[0, buf]),
            pltpu.make_async_copy(wq_ref.at[pl.ds(dst * qrows, qrows)], wob.at[buf], wsem.at[1, buf]),
            pltpu.make_async_copy(wk_ref.at[pl.ds(dst * krows, krows)], woc.at[buf, pl.ds(0, krows)], wsem.at[2, buf]),
            pltpu.make_async_copy(wv_ref.at[pl.ds(dst * krows, krows)], woc.at[buf, pl.ds(krows, krows)], wsem.at[3, buf]),
        ]

    def p_first(t):
        return rdma(gall.at[3, t], gall.at[7, t], psend.at[t], pfirst.at[t], ahead)

    def p_second(t):
        return rdma(gall.at[7, t], gall.at[0, relay_from], psecond.at[t], precv.at[t], device(sgn, t))

    def p_direct(t):
        return rdma(gall.at[3, t], gall.at[0, me], psend.at[t], precv.at[t], dests[t])

    def seg_copy(t):
        return rdma(seg_mine, seg_all.at[me], gsend.at[t], grecv.at[t], dests[t])

    x_in = pltpu.make_async_copy(x_ref, xbuf, lsem.at[2])
    dy_in = pltpu.make_async_copy(dy_ref, dybuf, lsem.at[3])
    x_in.start()
    for copy in block_copies(0, 0):
        copy.start()
    dy_in.start()
    for a in range(2):
        x_own(a).start()
    seg_mine[...] = jnp.broadcast_to(seg_ref[...], seg_mine.shape)
    pl.semaphore_wait(barrier, n - 1)
    for t in range(n - 1):
        seg_copy(t).start()
    seg_all[me] = seg_mine[...]
    x_in.wait()
    dy_in.wait()

    def project_step(step, carry):
        buf = step % 2

        @pl.when(step < n - 1)
        def _():
            for copy in block_copies(step + 1, 1 - buf):
                copy.start()

        for copy in block_copies(step, buf):
            copy.wait()
        slot = 3 - 3 * (step // (n - 1))
        place = step + (me - step) * (step // (n - 1))
        gall[slot, place, 0:qrows] = dot_nt(wob[buf], xbuf[...]).astype(BF)
        gall[slot, place, kv0:do0] = dot_nt(woc[buf], xbuf[...]).astype(BF)
        gall[slot, place, do0:rows] = dot_nt(woa[buf], dybuf[...]).astype(BF)
        for t in range(n - 1):
            @pl.when(step == t)
            def _():
                (p_first if t < 2 else p_direct)(t).start()
        return carry

    lax.fori_loop(0, n, project_step, 0)
    for t in range(n - 1):
        for a in range(2):
            (x_first if t < 2 else x_direct)(a, t).start()
    for kind in range(3):
        for copy in load(kind, 0, 0):
            copy.start()
    for t in range(2):
        p_first(t).wait_recv()
        p_second(t).start()

    for t in range(n - 1):
        seg_copy(t).wait_recv()
    row_id = lax.broadcasted_iota(jnp.int32, (n, tok), 0)
    lane_id = lax.broadcasted_iota(jnp.int32, (n, tok), 1)
    seg = jnp.zeros((n, tok), jnp.int32)
    for d in range(n):
        seg = jnp.where(row_id == d, seg_all[d], seg)
    before = jnp.where(lane_id == 0, pltpu.roll(pltpu.roll(seg, 1, 1), 1, 0), pltpu.roll(seg, 1, 1))
    pos = row_id * tok + lane_id
    best = jnp.where((seg != before) & (pos > 0), pos, 0)
    shift = 1
    while shift < tok:
        best = jnp.maximum(best, jnp.where(lane_id >= shift, pltpu.roll(best, shift, 1), 0))
        shift *= 2
    end = jnp.broadcast_to(best[:, tok - 1:tok], (n, tok))
    carry_max = jnp.where(row_id >= 1, pltpu.roll(end, 1, 0), 0)
    shift = 1
    while shift < n:
        carry_max = jnp.maximum(carry_max, jnp.where(row_id >= shift, pltpu.roll(carry_max, shift, 0), 0))
        shift *= 2
    best = jnp.maximum(best, carry_max)
    for d in range(n):
        first_ref[d] = jnp.broadcast_to(best[d:d + 1], (8, tok))
    dkacc[...] = jnp.zeros_like(dkacc)
    dvacc[...] = jnp.zeros_like(dvacc)
    yacc[...] = jnp.zeros_like(yacc)
    dxacc[...] = jnp.zeros_like(dxacc)
    rhsq[...] = jnp.zeros_like(rhsq)
    rhsd[...] = jnp.zeros_like(rhsd)
    for t in range(n - 1):
        p_direct(t).wait_recv()

    def transpose_tile(c, carry):
        kvn[pl.ds(pl.multiple_of(c * tok, LANES), tok), :] = gall[0, c, kv0:do0, :].T
        return carry

    lax.fori_loop(0, n, transpose_tile, 0)
    score_mul = scale * LOG2E
    grp = tok // 8

    def attend(i, pair):
        q0 = pl.multiple_of(pair * group * krows, krows)
        for g in range(group):
            lanes = slice(g * tok, (g + 1) * tok)
            rhsq[0:krows, lanes] = gall[0, i, pl.ds(q0 + g * krows, krows), :]
            rhsd[krows:2 * krows, lanes] = gall[0, i, pl.ds(do0 + q0 + g * krows, krows), :]
        first = jnp.concatenate([first_ref[i][0:1]] * group, axis=1)
        qpos = i * tok + lax.broadcasted_iota(jnp.int32, (1, tok), 1)
        qpos = jnp.concatenate([qpos] * group, axis=1)

        def score_step(c, top):
            s = dot_nn(kvn[pl.ds(pl.multiple_of(c * tok, LANES), tok), :], rhsq[...])
            kpos = lax.broadcasted_iota(jnp.int32, (tok, width), 0) + c * tok
            s = jnp.where((kpos >= first) & (kpos <= qpos), s, -jnp.inf)
            pbuf[c] = s
            return jnp.maximum(top, jnp.max(s.reshape(grp, 8, width), axis=0))

        top = lax.fori_loop(0, i + 1, score_step, jnp.full((8, width), -jnp.inf, F32))
        top = jnp.max(top, axis=0, keepdims=True) * score_mul
        oacc[...] = jnp.zeros_like(oacc)

        def value_step(c, total):
            p = jnp.exp2(pbuf[c] * score_mul - top)
            pbuf[c] = p
            oacc[...] += dot_nn(gall[0, c, kv0 + krows:do0, :], p.astype(BF))
            return total + jnp.sum(p.reshape(grp, 8, width), axis=0)

        total = lax.fori_loop(0, i + 1, value_step, jnp.zeros((8, width), F32))
        inv = 1.0 / jnp.sum(total, axis=0, keepdims=True)
        o_blk = (oacc[...] * inv).astype(BF)
        delta = jnp.sum(rhsd[krows:2 * krows, :].astype(F32) * o_blk.astype(F32), axis=0, keepdims=True)
        for g in range(group):
            gall[0, i, pl.ds(q0 + g * krows, krows), :] = o_blk[:, g * tok:(g + 1) * tok]
        dqacc[...] = jnp.zeros_like(dqacc)

        def grad_step(c, carry):
            dp = dot_nn(kvn[pl.ds(pl.multiple_of(c * tok, LANES), tok), :], rhsd[...])
            p = pbuf[c] * inv
            ds = (p * (dp - delta)).astype(BF)
            dqacc[...] += dot_nn(gall[0, c, kv0:kv0 + krows, :], ds)
            dkacc[c] += dot_nt(rhsq[0:krows, :], ds)
            dvacc[c] += dot_nt(rhsd[krows:2 * krows, :], p.astype(BF))
            return carry

        lax.fori_loop(0, i + 1, grad_step, 0)
        dq = (dqacc[...] * scale).astype(BF)
        for g in range(group):
            gall[0, i, pl.ds(do0 + q0 + g * krows, krows), :] = dq[:, g * tok:(g + 1) * tok]

    lag = n // 2

    def tile_step(i, carry):
        def pair_step(pair, inner):
            attend(i, pair)
            return inner

        lax.fori_loop(0, heads // group, pair_step, 0)
        send_own(*tile_items(i))

        @pl.when(i == 1)
        def _():
            for t in range(n - 1):
                p_direct(t).wait_send()
            for t in range(2):
                p_second(t).wait_send()
            for peer in (right, left):
                pl.semaphore_signal(free_far, inc=1, device_id={'cp': peer}, device_id_type=pl.DeviceIdType.MESH)
            pl.semaphore_signal(free_par, inc=1, device_id={'cp': partner}, device_id_type=pl.DeviceIdType.MESH)

        @pl.when(i == 2)
        def _():
            for t in range(2):
                for a in range(2):
                    x_first(a, t).wait_recv()
                    x_second(a, t).start()

        @pl.when(i == lag)
        def _():
            pl.semaphore_wait(free_far, 2)

        @pl.when(i >= lag)
        def _():
            serve_near(*tile_items(i - lag))
        return carry

    lax.fori_loop(0, n, tile_step, 0)
    for c in range(n):
        gall[0, c, kv0:kv0 + krows, :] = (dkacc[c] * scale).astype(BF)
        gall[0, c, kv0 + krows:do0, :] = dvacc[c].astype(BF)
    send_own(*kv_items)

    for a in range(2):
        x_own(a).wait()
        for t in range(n - 1):
            x_direct(a, t).wait_recv()

    near = n - 2
    spare = tok - qrows

    def rounded(acc, buf, out, sem):
        buf[0] = acc[0:qrows].astype(BF)
        buf[1, 0:spare] = acc[qrows:tok].astype(BF)
        return [pltpu.make_async_copy(buf.at[0], out.at[pl.ds(0, qrows)], lsem.at[sem]),
                pltpu.make_async_copy(buf.at[1, pl.ds(0, spare)], out.at[pl.ds(qrows, spare)], lsem.at[sem + 1])]

    def closing_step(r, carry):
        @pl.when(r == 0)
        def _():
            serve_near(*tile_items(lag))

        @pl.when(r == 1)
        def _():
            serve_near(*tile_items(lag + 1))
            arrived_tiles(4)

        @pl.when(r == 2)
        def _():
            for j in range(lag + 2, n):
                serve_near(*tile_items(j))

        @pl.when(r == 4)
        def _():
            pl.semaphore_wait(free_par, 1)
            for j in range(lag):
                serve_far(*tile_items(j))
            arrived_tiles(5)

        @pl.when(r == 5)
        def _():
            arrived_tiles(6)

        @pl.when(r == near)
        def _():
            serve_near(*kv_items)

        @pl.when(r == near + 1)
        def _():
            arrived_kv(4)

        @pl.when(r == near + 4)
        def _():
            arrived_kv(5)
            arrived_kv(6)

        @pl.when(r == 2 * near)
        def _():
            for j in range(lag, n):
                serve_far(*tile_items(j))

        @pl.when(r == 2 * near + 1)
        def _():
            arrived_tiles(7)

        @pl.when((r < near) | ((r >= 2 * near) & (r < 2 * near + 2)))
        def _():
            order = r - near * (r // (2 * near))
            closing_part(0, order)
            closing_part(1, order)

        @pl.when(r == 2 * near + 2)
        def _():
            for copy in rounded(yacc, woa, y_ref, 2):
                copy.start()
            serve_far(*kv_items)

        @pl.when(r == 2 * near + 3)
        def _():
            arrived_kv(7)

        @pl.when(((r >= near) & (r < 2 * near)) | (r >= 2 * near + 2))
        def _():
            closing_part(2, r - near - 2 * (r // (2 * near + 2)))
        return carry

    lax.fori_loop(0, 2 * n, closing_step, 0)
    outs = rounded(dxacc, wob, dx_ref, 4)
    for copy in outs:
        copy.start()
    for kind in range(3):
        for order in (n - 2, n - 1):
            for copy in save(kind, order, order % 2):
                copy.wait()
    for copy in [pltpu.make_async_copy(woa.at[0], y_ref.at[pl.ds(0, qrows)], lsem.at[2]),
                 pltpu.make_async_copy(woa.at[1, pl.ds(0, spare)], y_ref.at[pl.ds(qrows, spare)], lsem.at[3])] + outs:
        copy.wait()
    for a in range(2):
        for t in range(n - 1):
            x_direct(a, t).wait_send()
        for t in range(2):
            x_second(a, t).wait_send()
    for t in range(n - 1):
        seg_copy(t).wait_send()

    def drain(items):
        for item in items:
            own_right(*item).wait_send()
            own_left(*item).wait_send()
            for slot in range(4):
                to_partner(slot, *item).wait_send()
        relay_plus(*items[0]).wait_send()
        relay_minus(*items[1]).wait_send()

    for j in range(n):
        drain(tile_items(j))
    drain(kv_items)


def attention_layer(n, x_act, dy_act, seg, wq, wk, wv, wo):
    tok, model = x_act.shape
    qrows, krows = wq.shape[0] // n, wk.shape[0] // n
    rows = 2 * qrows + 2 * krows
    total = n * tok
    mcol = model // n
    group = 2
    width = group * tok
    vmem = pl.BlockSpec(memory_space=pltpu.VMEM)
    anym = pl.BlockSpec(memory_space=pl.ANY)
    dma = pltpu.SemaphoreType.DMA
    return pl.pallas_call(
        functools.partial(main_kernel, (n, qrows, krows, tok, krows ** -0.5)),
        out_shape=(jax.ShapeDtypeStruct((tok, model), BF), jax.ShapeDtypeStruct((tok, model), BF),
                   jax.ShapeDtypeStruct((wq.shape[0], mcol), F32), jax.ShapeDtypeStruct((wk.shape[0], mcol), F32),
                   jax.ShapeDtypeStruct((wv.shape[0], mcol), F32), jax.ShapeDtypeStruct((wo.shape[0], mcol), F32)),
        in_specs=[anym, anym, vmem, anym, anym, anym, anym],
        out_specs=(anym,) * 6,
        scratch_shapes=[
            pltpu.VMEM((tok, model), BF), pltpu.VMEM((tok, model), BF),
            pltpu.VMEM((8, tok), jnp.int32), pltpu.VMEM((n, 8, tok), jnp.int32), pltpu.VMEM((n, 8, tok), jnp.int32),
            pltpu.VMEM((total, 2 * krows), BF),
            pltpu.VMEM((n, tok, width), F32),
            pltpu.VMEM((2 * krows, width), BF), pltpu.VMEM((2 * krows, width), BF),
            pltpu.VMEM((krows, width), F32), pltpu.VMEM((krows, width), F32),
            pltpu.VMEM((n, krows, tok), F32), pltpu.VMEM((n, krows, tok), F32),
            pltpu.VMEM((n, n, rows, tok), BF),
            pltpu.VMEM((total, mcol), BF), pltpu.VMEM((total, mcol), BF),
            pltpu.VMEM((2, 2, tok, mcol), BF),
            pltpu.VMEM((tok, model), F32), pltpu.VMEM((tok, model), F32),
            pltpu.VMEM((2, qrows, model), BF), pltpu.VMEM((2, qrows, model), BF), pltpu.VMEM((2, 2 * krows, model), BF),
            pltpu.VMEM((2, qrows, mcol), F32), pltpu.VMEM((2, qrows, mcol), F32), pltpu.VMEM((2, 2 * krows, mcol), F32),
            dma((4, 2)), dma((4, 2)),
            dma((2, 3, n)), dma((3, n)), dma((4, 3, n)), dma((8, 3, n)),
            dma((2, n)), dma((2, n)), dma((2, 2)), dma((2, 2)), dma((6,)),
            dma((n,)), dma((n,)), dma((2,)), dma((2,)), dma((n,)), dma((n,)),
            pltpu.SemaphoreType.REGULAR, pltpu.SemaphoreType.REGULAR,
        ],
        compiler_params=pltpu.CompilerParams(collective_id=0, has_side_effects=True, vmem_limit_bytes=VMEM_MAX),
        name='attention_layer',
    )(x_act, dy_act, seg.reshape(1, tok), wq, wk, wv, wo)


def solution(mesh):
    n = mesh.shape['cp']
    row_spec = P(('dp', 'cp'), None)
    tok_spec = P(('dp', 'cp'))
    weight_spec = P(None, None, None)
    grad_spec = P(('dp', 'cp'), None, None)

    def local_step(x_act, seg_ids, w_q, w_k, w_v, w_o, dy_act):
        model, q_heads, head_dim = w_q.shape
        kv_heads = w_k.shape[1]
        assert kv_heads == n and x_act.shape[0] % LANES == 0

        def flat(w):
            return w.transpose(1, 2, 0).reshape(w.shape[1] * head_dim, model)

        def unflat(g, heads):
            return g.reshape(heads, head_dim, g.shape[1]).transpose(2, 0, 1)

        wq, wk, wv, wo = flat(w_q), flat(w_k), flat(w_v), flat(w_o)
        y_out, dx_out, dwq, dwk, dwv, dwo = attention_layer(n, x_act, dy_act, seg_ids, wq, wk, wv, wo)
        return (y_out, dx_out, unflat(dwq, q_heads), unflat(dwk, kv_heads), unflat(dwv, kv_heads), unflat(dwo, q_heads))

    return jax.shard_map(local_step, mesh=mesh,
                         in_specs=(row_spec, tok_spec, weight_spec, weight_spec, weight_spec, weight_spec, row_spec),
                         out_specs=(row_spec, row_spec, grad_spec, grad_spec, grad_spec, grad_spec),
                         check_vma=False)
```

```python
import functools

import jax
import jax.numpy as jnp
from jax import lax
from jax.experimental import pallas as pl
from jax.experimental.pallas import tpu as pltpu
from jax.sharding import PartitionSpec as P

BF = jnp.bfloat16
F32 = jnp.float32
LANES = 128
LOG2E = 1.4426950408889634
VMEM_MAX = 67043328


def rdma(src, dst, send_sem, recv_sem, peer):
    return pltpu.make_async_remote_copy(src_ref=src, dst_ref=dst, send_sem=send_sem, recv_sem=recv_sem,
                                        device_id={'cp': peer}, device_id_type=pl.DeviceIdType.MESH)


def dot_nt(left, right):
    return lax.dot_general(left, right, (((1,), (1,)), ((), ())), preferred_element_type=F32)


def dot_tn(left, right):
    return lax.dot_general(left, right, (((0,), (0,)), ((), ())), preferred_element_type=F32)


def dot_nn(left, right):
    return lax.dot_general(left, right, (((1,), (0,)), ((), ())), preferred_element_type=F32)


def pick(index, values):
    out = values[0]
    for k in range(1, len(values)):
        out = jnp.where(index == k, values[k], out)
    return out


def main_kernel(dims, x_ref, dy_ref, seg_ref, wq_ref, wk_ref, wv_ref, wo_ref,
                y_ref, dx_ref, dwq_ref, dwk_ref, dwv_ref, dwo_ref,
                xbuf, dybuf, seg_mine, seg_all, first_ref,
                kvn, pbuf, rhsq, rhsd, oacc, dqacc, dkacc, dvacc, gall, xc, dyc, xrel, yacc, dxacc,
                woa, wob, woc, sta, stb, stc, wsem, outsem, osem, relsem, parsem, rsem, xsend, xrecv, xfirst, xsecond, lsem,
                psend, precv, pfirst, psecond, gsend, grecv, free_far, free_par):
    n, qrows, krows, tok, scale = dims
    chips = n // 2
    heads = qrows // krows
    group = rhsq.shape[1] // tok
    me = lax.axis_index('cp')
    chip, core = me // 2, me % 2
    sgn = 1 - 2 * core
    rows = 2 * qrows + 2 * krows
    model = yacc.shape[1]
    mcol = xc.shape[1]
    ncol = 1024
    width = group * tok
    kv0, do0 = qrows, qrows + 2 * krows

    def device(chip_off, flip):
        return ((chip + chip_off + chips) % chips) * 2 + (core + flip) % 2

    right, left, partner = device(1, 0), device(-1, 0), device(0, 1)
    dests = [device(2, 0), device(2, 1), device(-sgn, 0), device(-sgn, 1), device(sgn, 0), device(sgn, 1), partner]
    ahead = dests[4]
    relay_from = device(-sgn, 0)

    barrier = pltpu.get_barrier_semaphore()
    for peer in dests:
        pl.semaphore_signal(barrier, inc=1, device_id={'cp': peer}, device_id_type=pl.DeviceIdType.MESH)

    sides = ((x_ref, xc), (dy_ref, dyc))

    def columns(ref, dst):
        return ref.at[:, pl.ds(pl.multiple_of(dst * mcol, LANES), mcol)]

    def token_rows(ref, src):
        return ref.at[pl.ds(pl.multiple_of(src * tok, LANES), tok)]

    def x_first(a, t):
        return rdma(columns(sides[a][0], dests[t]), xrel.at[a, t], xsend.at[a, t], xfirst.at[a, t], ahead)

    def x_second(a, t):
        return rdma(xrel.at[a, t], token_rows(sides[a][1], relay_from), xsecond.at[a, t], xrecv.at[a, t], device(sgn, t))

    def x_direct(a, t):
        return rdma(columns(sides[a][0], dests[t]), token_rows(sides[a][1], me), xsend.at[a, t], xrecv.at[a, t], dests[t])

    def x_own(a):
        return pltpu.make_async_copy(columns(sides[a][0], me), token_rows(sides[a][1], me), lsem.at[a])

    def view(slot, part, j):
        if part == 0:
            return gall.at[slot, j, pl.ds(0, qrows)]
        if part == 1:
            return gall.at[slot, j, pl.ds(do0, qrows)]
        return gall.at[slot, pl.ds(j * (n // 2), n // 2), pl.ds(kv0, 2 * krows)]

    def own_right(part, j):
        return rdma(view(0, part, j), view(1, part, j), osem.at[0, part, j], rsem.at[1, part, j], right)

    def own_left(part, j):
        return rdma(view(0, part, j), view(2, part, j), osem.at[1, part, j], rsem.at[2, part, j], left)

    def relay_plus(part, j):
        return rdma(view(1, part, j), view(3, part, j), relsem.at[part, j], rsem.at[3, part, j], right)

    def relay_minus(part, j):
        return rdma(view(2, part, j), view(3, part, j), relsem.at[part, j], rsem.at[3, part, j], left)

    def to_partner(slot, part, j):
        return rdma(view(slot, part, j), view(4 + slot, part, j), parsem.at[slot, part, j], rsem.at[4 + slot, part, j], partner)

    def send_own(first, second):
        for item in (first, second):
            own_right(*item).start()
            own_left(*item).start()
            to_partner(0, *item).start()

    def serve_near(first, second):
        own_right(*first).wait_recv()
        relay_plus(*first).start()
        to_partner(1, *first).start()
        own_left(*second).wait_recv()
        relay_minus(*second).start()
        to_partner(2, *second).start()
        own_right(*second).wait_recv()
        to_partner(1, *second).start()
        own_left(*first).wait_recv()
        to_partner(2, *first).start()

    def serve_far(first, second):
        relay_plus(*first).wait_recv()
        to_partner(3, *first).start()
        relay_minus(*second).wait_recv()
        to_partner(3, *second).start()

    def tile_items(j):
        return (0, j), (1, j)

    kv_items = ((2, 0), (2, 1))

    def arrived_tiles(slot):
        for j in range(n):
            for item in tile_items(j):
                to_partner(slot - 4, *item).wait_recv()

    def arrived_kv(slot):
        for item in kv_items:
            to_partner(slot - 4, *item).wait_recv()

    slot_table = (0, 4, 1, 2, 5, 6, 3, 7)
    off_table = (0, 0, chips - 1, 1, chips - 1, 1, 2, 2)
    flip_table = (0, 1, 0, 0, 1, 1, 0, 1)

    def source_of(order):
        return ((chip + pick(order, off_table)) % chips) * 2 + (core + pick(order, flip_table)) % 2

    def load(kind, order, buf):
        src = source_of(order)
        if kind == 0:
            return [pltpu.make_async_copy(wo_ref.at[pl.ds(src * qrows, qrows)], woa.at[buf], wsem.at[0, buf])]
        if kind == 1:
            return [pltpu.make_async_copy(wq_ref.at[pl.ds(src * qrows, qrows)], wob.at[buf], wsem.at[1, buf])]
        return [pltpu.make_async_copy(wk_ref.at[pl.ds(src * krows, krows)], woc.at[buf, pl.ds(0, krows)], wsem.at[2, buf]),
                pltpu.make_async_copy(wv_ref.at[pl.ds(src * krows, krows)], woc.at[buf, pl.ds(krows, krows)], wsem.at[3, buf])]

    def save(kind, order, buf):
        src = source_of(order)
        if kind == 0:
            return [pltpu.make_async_copy(sta.at[buf], dwo_ref.at[pl.ds(src * qrows, qrows)], outsem.at[0, buf])]
        if kind == 1:
            return [pltpu.make_async_copy(stb.at[buf], dwq_ref.at[pl.ds(src * qrows, qrows)], outsem.at[1, buf])]
        return [pltpu.make_async_copy(stc.at[buf, pl.ds(0, krows)], dwk_ref.at[pl.ds(src * krows, krows)], outsem.at[2, buf]),
                pltpu.make_async_copy(stc.at[buf, pl.ds(krows, krows)], dwv_ref.at[pl.ds(src * krows, krows)], outsem.at[3, buf])]

    kinds = ((0, qrows, woa, sta, dyc, yacc), (do0, rows, wob, stb, xc, dxacc), (kv0, do0, woc, stc, xc, dxacc))

    def closing_part(kind, order):
        row0, row1, wbuf, stage, other, acc = kinds[kind]
        buf = order % 2
        slot = pick(order, slot_table)
        for copy in load(kind, order, buf):
            copy.wait()

        @pl.when(order < n - 1)
        def _():
            for copy in load(kind, order + 1, 1 - buf):
                copy.start()

        @pl.when(order >= 2)
        def _():
            for copy in save(kind, order - 2, buf):
                copy.wait()
        wide = jnp.concatenate([gall[slot, j, row0:row1, :] for j in range(n)], axis=1)
        stage[buf] = dot_nn(wide, other[...])
        for copy in save(kind, order, buf):
            copy.start()
        left_t = gall[slot, me, row0:row1, :]

        def col(j, carry):
            cols = pl.ds(pl.multiple_of(j * ncol, ncol), ncol)
            acc[:, cols] += dot_tn(left_t, wbuf[buf, :, cols])
            return carry

        lax.fori_loop(0, model // ncol, col, 0)

    def block_copies(step, buf):
        pair, flip = step // 2, (step + step // 6) % 2
        off = 2 - 3 * pair + 5 * (pair // 2) + 2 * (pair // 3)
        dst = ((chip + sgn * off + chips) % chips) * 2 + (core + flip) % 2
        return [
            pltpu.make_async_copy(wo_ref.at[pl.ds(dst * qrows, qrows)], woa.at[buf], wsem.at[0, buf]),
            pltpu.make_async_copy(wq_ref.at[pl.ds(dst * qrows, qrows)], wob.at[buf], wsem.at[1, buf]),
            pltpu.make_async_copy(wk_ref.at[pl.ds(dst * krows, krows)], woc.at[buf, pl.ds(0, krows)], wsem.at[2, buf]),
            pltpu.make_async_copy(wv_ref.at[pl.ds(dst * krows, krows)], woc.at[buf, pl.ds(krows, krows)], wsem.at[3, buf]),
        ]

    def p_first(t):
        return rdma(gall.at[3, t], gall.at[7, t], psend.at[t], pfirst.at[t], ahead)

    def p_second(t):
        return rdma(gall.at[7, t], gall.at[0, relay_from], psecond.at[t], precv.at[t], device(sgn, t))

    def p_direct(t):
        return rdma(gall.at[3, t], gall.at[0, me], psend.at[t], precv.at[t], dests[t])

    def seg_copy(t):
        return rdma(seg_mine, seg_all.at[me], gsend.at[t], grecv.at[t], dests[t])

    x_in = pltpu.make_async_copy(x_ref, xbuf, lsem.at[2])
    dy_in = pltpu.make_async_copy(dy_ref, dybuf, lsem.at[3])
    x_in.start()
    for copy in block_copies(0, 0):
        copy.start()
    dy_in.start()
    for a in range(2):
        x_own(a).start()
    seg_mine[...] = jnp.broadcast_to(seg_ref[...], seg_mine.shape)
    pl.semaphore_wait(barrier, n - 1)
    for t in range(n - 1):
        seg_copy(t).start()
    seg_all[me] = seg_mine[...]
    x_in.wait()
    dy_in.wait()

    def project_step(step, carry):
        buf = step % 2

        @pl.when(step < n - 1)
        def _():
            for copy in block_copies(step + 1, 1 - buf):
                copy.start()

        for copy in block_copies(step, buf):
            copy.wait()
        slot = 3 - 3 * (step // (n - 1))
        place = step + (me - step) * (step // (n - 1))
        gall[slot, place, 0:qrows] = dot_nt(wob[buf], xbuf[...]).astype(BF)
        gall[slot, place, kv0:do0] = dot_nt(woc[buf], xbuf[...]).astype(BF)
        gall[slot, place, do0:rows] = dot_nt(woa[buf], dybuf[...]).astype(BF)
        for t in range(n - 1):
            @pl.when(step == t)
            def _():
                (p_first if t < 2 else p_direct)(t).start()
        return carry

    lax.fori_loop(0, n, project_step, 0)
    for kind in range(3):
        for copy in load(kind, 0, 0):
            copy.start()
    for t in range(2):
        p_first(t).wait_recv()
        p_second(t).start()
    for t in range(n - 1):
        for a in range(2):
            (x_first if t < 2 else x_direct)(a, t).start()

    for t in range(n - 1):
        seg_copy(t).wait_recv()
    row_id = lax.broadcasted_iota(jnp.int32, (n, tok), 0)
    lane_id = lax.broadcasted_iota(jnp.int32, (n, tok), 1)
    seg = jnp.zeros((n, tok), jnp.int32)
    for d in range(n):
        seg = jnp.where(row_id == d, seg_all[d], seg)
    before = jnp.where(lane_id == 0, pltpu.roll(pltpu.roll(seg, 1, 1), 1, 0), pltpu.roll(seg, 1, 1))
    pos = row_id * tok + lane_id
    best = jnp.where((seg != before) & (pos > 0), pos, 0)
    shift = 1
    while shift < tok:
        best = jnp.maximum(best, jnp.where(lane_id >= shift, pltpu.roll(best, shift, 1), 0))
        shift *= 2
    end = jnp.broadcast_to(best[:, tok - 1:tok], (n, tok))
    carry_max = jnp.where(row_id >= 1, pltpu.roll(end, 1, 0), 0)
    shift = 1
    while shift < n:
        carry_max = jnp.maximum(carry_max, jnp.where(row_id >= shift, pltpu.roll(carry_max, shift, 0), 0))
        shift *= 2
    best = jnp.maximum(best, carry_max)
    for d in range(n):
        first_ref[d] = jnp.broadcast_to(best[d:d + 1], (8, tok))
    dkacc[...] = jnp.zeros_like(dkacc)
    dvacc[...] = jnp.zeros_like(dvacc)
    yacc[...] = jnp.zeros_like(yacc)
    dxacc[...] = jnp.zeros_like(dxacc)
    rhsq[...] = jnp.zeros_like(rhsq)
    rhsd[...] = jnp.zeros_like(rhsd)
    for t in range(n - 1):
        p_direct(t).wait_recv()

    def transpose_tile(c, carry):
        kvn[pl.ds(pl.multiple_of(c * tok, LANES), tok), :] = gall[0, c, kv0:do0, :].T
        return carry

    lax.fori_loop(0, n, transpose_tile, 0)
    score_mul = scale * LOG2E
    grp = tok // 8

    def attend(i, pair):
        q0 = pl.multiple_of(pair * group * krows, krows)
        for g in range(group):
            lanes = slice(g * tok, (g + 1) * tok)
            rhsq[0:krows, lanes] = gall[0, i, pl.ds(q0 + g * krows, krows), :]
            rhsd[krows:2 * krows, lanes] = gall[0, i, pl.ds(do0 + q0 + g * krows, krows), :]
        first = jnp.concatenate([first_ref[i][0:1]] * group, axis=1)
        qpos = i * tok + lax.broadcasted_iota(jnp.int32, (1, tok), 1)
        qpos = jnp.concatenate([qpos] * group, axis=1)

        def score_step(c, top):
            s = dot_nn(kvn[pl.ds(pl.multiple_of(c * tok, LANES), tok), :], rhsq[...])
            kpos = lax.broadcasted_iota(jnp.int32, (tok, width), 0) + c * tok
            s = jnp.where((kpos >= first) & (kpos <= qpos), s, -jnp.inf)
            pbuf[c] = s
            return jnp.maximum(top, jnp.max(s.reshape(grp, 8, width), axis=0))

        top = lax.fori_loop(0, i + 1, score_step, jnp.full((8, width), -jnp.inf, F32))
        top = jnp.max(top, axis=0, keepdims=True) * score_mul
        oacc[...] = jnp.zeros_like(oacc)

        def value_step(c, total):
            p = jnp.exp2(pbuf[c] * score_mul - top)
            pbuf[c] = p
            oacc[...] += dot_nn(gall[0, c, kv0 + krows:do0, :], p.astype(BF))
            return total + jnp.sum(p.reshape(grp, 8, width), axis=0)

        total = lax.fori_loop(0, i + 1, value_step, jnp.zeros((8, width), F32))
        inv = 1.0 / jnp.sum(total, axis=0, keepdims=True)
        o_blk = (oacc[...] * inv).astype(BF)
        delta = jnp.sum(rhsd[krows:2 * krows, :].astype(F32) * o_blk.astype(F32), axis=0, keepdims=True)
        for g in range(group):
            gall[0, i, pl.ds(q0 + g * krows, krows), :] = o_blk[:, g * tok:(g + 1) * tok]
        dqacc[...] = jnp.zeros_like(dqacc)

        def grad_step(c, carry):
            dp = dot_nn(kvn[pl.ds(pl.multiple_of(c * tok, LANES), tok), :], rhsd[...])
            p = pbuf[c] * inv
            ds = (p * (dp - delta)).astype(BF)
            dqacc[...] += dot_nn(gall[0, c, kv0:kv0 + krows, :], ds)
            dkacc[c] += dot_nt(rhsq[0:krows, :], ds)
            dvacc[c] += dot_nt(rhsd[krows:2 * krows, :], p.astype(BF))
            return carry

        lax.fori_loop(0, i + 1, grad_step, 0)
        dq = (dqacc[...] * scale).astype(BF)
        for g in range(group):
            gall[0, i, pl.ds(do0 + q0 + g * krows, krows), :] = dq[:, g * tok:(g + 1) * tok]

    lag = n // 2

    def tile_step(i, carry):
        def pair_step(pair, inner):
            attend(i, pair)
            return inner

        lax.fori_loop(0, heads // group, pair_step, 0)
        send_own(*tile_items(i))

        @pl.when(i == 1)
        def _():
            for t in range(n - 1):
                p_direct(t).wait_send()
            for t in range(2):
                p_second(t).wait_send()
            for peer in (right, left):
                pl.semaphore_signal(free_far, inc=1, device_id={'cp': peer}, device_id_type=pl.DeviceIdType.MESH)
            pl.semaphore_signal(free_par, inc=1, device_id={'cp': partner}, device_id_type=pl.DeviceIdType.MESH)

        @pl.when(i == 2)
        def _():
            for t in range(2):
                for a in range(2):
                    x_first(a, t).wait_recv()
                    x_second(a, t).start()

        @pl.when(i == lag)
        def _():
            pl.semaphore_wait(free_far, 2)

        @pl.when(i >= lag)
        def _():
            serve_near(*tile_items(i - lag))
        return carry

    lax.fori_loop(0, n, tile_step, 0)
    for c in range(n):
        gall[0, c, kv0:kv0 + krows, :] = (dkacc[c] * scale).astype(BF)
        gall[0, c, kv0 + krows:do0, :] = dvacc[c].astype(BF)
    send_own(*kv_items)

    for a in range(2):
        x_own(a).wait()
        for t in range(n - 1):
            x_direct(a, t).wait_recv()

    near = n - 2
    spare = tok - qrows

    def rounded(acc, buf, out, sem):
        buf[0] = acc[0:qrows].astype(BF)
        buf[1, 0:spare] = acc[qrows:tok].astype(BF)
        return [pltpu.make_async_copy(buf.at[0], out.at[pl.ds(0, qrows)], lsem.at[sem]),
                pltpu.make_async_copy(buf.at[1, pl.ds(0, spare)], out.at[pl.ds(qrows, spare)], lsem.at[sem + 1])]

    def closing_step(r, carry):
        @pl.when(r == 0)
        def _():
            serve_near(*tile_items(lag))

        @pl.when(r == 1)
        def _():
            serve_near(*tile_items(lag + 1))
            arrived_tiles(4)

        @pl.when(r == 2)
        def _():
            for j in range(lag + 2, n):
                serve_near(*tile_items(j))

        @pl.when(r == 4)
        def _():
            pl.semaphore_wait(free_par, 1)
            for j in range(lag):
                serve_far(*tile_items(j))
            arrived_tiles(5)

        @pl.when(r == 5)
        def _():
            arrived_tiles(6)

        @pl.when(r == near)
        def _():
            serve_near(*kv_items)

        @pl.when(r == near + 1)
        def _():
            arrived_kv(4)

        @pl.when(r == near + 4)
        def _():
            arrived_kv(5)
            arrived_kv(6)

        @pl.when(r == 2 * near)
        def _():
            for j in range(lag, n):
                serve_far(*tile_items(j))

        @pl.when(r == 2 * near + 1)
        def _():
            arrived_tiles(7)

        @pl.when((r < near) | ((r >= 2 * near) & (r < 2 * near + 2)))
        def _():
            order = r - near * (r // (2 * near))
            closing_part(0, order)
            closing_part(1, order)

        @pl.when(r == 2 * near + 2)
        def _():
            for copy in rounded(yacc, woa, y_ref, 2):
                copy.start()
            serve_far(*kv_items)

        @pl.when(r == 2 * near + 3)
        def _():
            arrived_kv(7)

        @pl.when(((r >= near) & (r < 2 * near)) | (r >= 2 * near + 2))
        def _():
            closing_part(2, r - near - 2 * (r // (2 * near + 2)))
        return carry

    lax.fori_loop(0, 2 * n, closing_step, 0)
    outs = rounded(dxacc, wob, dx_ref, 4)
    for copy in outs:
        copy.start()
    for kind in range(3):
        for order in (n - 2, n - 1):
            for copy in save(kind, order, order % 2):
                copy.wait()
    for copy in [pltpu.make_async_copy(woa.at[0], y_ref.at[pl.ds(0, qrows)], lsem.at[2]),
                 pltpu.make_async_copy(woa.at[1, pl.ds(0, spare)], y_ref.at[pl.ds(qrows, spare)], lsem.at[3])] + outs:
        copy.wait()
    for a in range(2):
        for t in range(n - 1):
            x_direct(a, t).wait_send()
        for t in range(2):
            x_second(a, t).wait_send()
    for t in range(n - 1):
        seg_copy(t).wait_send()

    def drain(items):
        for item in items:
            own_right(*item).wait_send()
            own_left(*item).wait_send()
            for slot in range(4):
                to_partner(slot, *item).wait_send()
        relay_plus(*items[0]).wait_send()
        relay_minus(*items[1]).wait_send()

    for j in range(n):
        drain(tile_items(j))
    drain(kv_items)


def attention_layer(n, x_act, dy_act, seg, wq, wk, wv, wo):
    tok, model = x_act.shape
    qrows, krows = wq.shape[0] // n, wk.shape[0] // n
    rows = 2 * qrows + 2 * krows
    total = n * tok
    mcol = model // n
    group = 2
    width = group * tok
    vmem = pl.BlockSpec(memory_space=pltpu.VMEM)
    anym = pl.BlockSpec(memory_space=pl.ANY)
    dma = pltpu.SemaphoreType.DMA
    return pl.pallas_call(
        functools.partial(main_kernel, (n, qrows, krows, tok, krows ** -0.5)),
        out_shape=(jax.ShapeDtypeStruct((tok, model), BF), jax.ShapeDtypeStruct((tok, model), BF),
                   jax.ShapeDtypeStruct((wq.shape[0], mcol), F32), jax.ShapeDtypeStruct((wk.shape[0], mcol), F32),
                   jax.ShapeDtypeStruct((wv.shape[0], mcol), F32), jax.ShapeDtypeStruct((wo.shape[0], mcol), F32)),
        in_specs=[anym, anym, vmem, anym, anym, anym, anym],
        out_specs=(anym,) * 6,
        scratch_shapes=[
            pltpu.VMEM((tok, model), BF), pltpu.VMEM((tok, model), BF),
            pltpu.VMEM((8, tok), jnp.int32), pltpu.VMEM((n, 8, tok), jnp.int32), pltpu.VMEM((n, 8, tok), jnp.int32),
            pltpu.VMEM((total, 2 * krows), BF),
            pltpu.VMEM((n, tok, width), F32),
            pltpu.VMEM((2 * krows, width), BF), pltpu.VMEM((2 * krows, width), BF),
            pltpu.VMEM((krows, width), F32), pltpu.VMEM((krows, width), F32),
            pltpu.VMEM((n, krows, tok), F32), pltpu.VMEM((n, krows, tok), F32),
            pltpu.VMEM((n, n, rows, tok), BF),
            pltpu.VMEM((total, mcol), BF), pltpu.VMEM((total, mcol), BF),
            pltpu.VMEM((2, 2, tok, mcol), BF),
            pltpu.VMEM((tok, model), F32), pltpu.VMEM((tok, model), F32),
            pltpu.VMEM((2, qrows, model), BF), pltpu.VMEM((2, qrows, model), BF), pltpu.VMEM((2, 2 * krows, model), BF),
            pltpu.VMEM((2, qrows, mcol), F32), pltpu.VMEM((2, qrows, mcol), F32), pltpu.VMEM((2, 2 * krows, mcol), F32),
            dma((4, 2)), dma((4, 2)),
            dma((2, 3, n)), dma((3, n)), dma((4, 3, n)), dma((8, 3, n)),
            dma((2, n)), dma((2, n)), dma((2, 2)), dma((2, 2)), dma((6,)),
            dma((n,)), dma((n,)), dma((2,)), dma((2,)), dma((n,)), dma((n,)),
            pltpu.SemaphoreType.REGULAR, pltpu.SemaphoreType.REGULAR,
        ],
        compiler_params=pltpu.CompilerParams(collective_id=0, has_side_effects=True, vmem_limit_bytes=VMEM_MAX),
        name='attention_layer',
    )(x_act, dy_act, seg.reshape(1, tok), wq, wk, wv, wo)


def solution(mesh):
    n = mesh.shape['cp']
    row_spec = P(('dp', 'cp'), None)
    tok_spec = P(('dp', 'cp'))
    weight_spec = P(None, None, None)
    grad_spec = P(('dp', 'cp'), None, None)

    def local_step(x_act, seg_ids, w_q, w_k, w_v, w_o, dy_act):
        model, q_heads, head_dim = w_q.shape
        kv_heads = w_k.shape[1]
        assert kv_heads == n and x_act.shape[0] % LANES == 0

        def flat(w):
            return w.transpose(1, 2, 0).reshape(w.shape[1] * head_dim, model)

        def unflat(g, heads):
            return g.reshape(heads, head_dim, g.shape[1]).transpose(2, 0, 1)

        wq, wk, wv, wo = flat(w_q), flat(w_k), flat(w_v), flat(w_o)
        y_out, dx_out, dwq, dwk, dwv, dwo = attention_layer(n, x_act, dy_act, seg_ids, wq, wk, wv, wo)
        return (y_out, dx_out, unflat(dwq, q_heads), unflat(dwk, kv_heads), unflat(dwv, kv_heads), unflat(dwo, q_heads))

    return jax.shard_map(local_step, mesh=mesh,
                         in_specs=(row_spec, tok_spec, weight_spec, weight_spec, weight_spec, weight_spec, row_spec),
                         out_specs=(row_spec, row_spec, grad_spec, grad_spec, grad_spec, grad_spec),
                         check_vma=False)
```

```python
import functools

import jax
import jax.numpy as jnp
from jax import lax
from jax.experimental import pallas as pl
from jax.experimental.pallas import tpu as pltpu
from jax.sharding import PartitionSpec as P

BF = jnp.bfloat16
F32 = jnp.float32
LANES = 128
LOG2E = 1.4426950408889634
VMEM_MAX = 67043328


def rdma(src, dst, send_sem, recv_sem, peer):
    return pltpu.make_async_remote_copy(src_ref=src, dst_ref=dst, send_sem=send_sem, recv_sem=recv_sem,
                                        device_id={'cp': peer}, device_id_type=pl.DeviceIdType.MESH)


def dot_nt(left, right):
    return lax.dot_general(left, right, (((1,), (1,)), ((), ())), preferred_element_type=F32)


def dot_tn(left, right):
    return lax.dot_general(left, right, (((0,), (0,)), ((), ())), preferred_element_type=F32)


def dot_nn(left, right):
    return lax.dot_general(left, right, (((1,), (0,)), ((), ())), preferred_element_type=F32)


def pick(index, values):
    out = values[0]
    for k in range(1, len(values)):
        out = jnp.where(index == k, values[k], out)
    return out


def main_kernel(dims, x_ref, dy_ref, seg_ref, wq_ref, wk_ref, wv_ref, wo_ref,
                y_ref, dx_ref, dwq_ref, dwk_ref, dwv_ref, dwo_ref,
                seg_mine, seg_all, first_ref, kvn, pbuf, rhsq, rhsd, stats, oacc, dqacc, dkacc, dvacc, gall, xc, dyc, xrel,
                woa, wob, woc, wsem, outsem, osem, relsem, parsem, rsem, xsend, xrecv, xfirst, xsecond, lsem, xload,
                psend, precv, pfirst, psecond, gsend, grecv, free_near, free_far, free_par):
    n, qrows, krows, tok, scale = dims
    chips = n // 2
    heads = qrows // krows
    width = rhsq.shape[2]
    group = width // tok
    me = lax.axis_index('cp')
    chip, core = me // 2, me % 2
    sgn = 1 - 2 * core
    rows = 2 * qrows + 2 * krows
    model = x_ref.shape[1]
    mcol = xc.shape[1]
    kv0, do0 = qrows, qrows + 2 * krows

    def device(chip_off, flip):
        return ((chip + chip_off + chips) % chips) * 2 + (core + flip) % 2

    right, left, partner = device(1, 0), device(-1, 0), device(0, 1)
    dests = [device(2, 0), device(2, 1), device(-sgn, 0), device(-sgn, 1), device(sgn, 0), device(sgn, 1), partner]
    ahead = dests[4]
    relay_from = device(-sgn, 0)

    barrier = pltpu.get_barrier_semaphore()
    for peer in dests:
        pl.semaphore_signal(barrier, inc=1, device_id={'cp': peer}, device_id_type=pl.DeviceIdType.MESH)

    sides = ((x_ref, xc), (dy_ref, dyc))

    def columns(ref, dst):
        return ref.at[:, pl.ds(pl.multiple_of(dst * mcol, LANES), mcol)]

    def token_rows(ref, src):
        return ref.at[pl.ds(pl.multiple_of(src * tok, LANES), tok)]

    def x_first(a, t):
        return rdma(columns(sides[a][0], dests[t]), xrel.at[a, t], xsend.at[a, t], xfirst.at[a, t], ahead)

    def x_second(a, t):
        return rdma(xrel.at[a, t], token_rows(sides[a][1], relay_from), xsecond.at[a, t], xrecv.at[a, t], device(sgn, t))

    def x_direct(a, t):
        return rdma(columns(sides[a][0], dests[t]), token_rows(sides[a][1], me), xsend.at[a, t], xrecv.at[a, t], dests[t])

    def x_own(a):
        return pltpu.make_async_copy(columns(sides[a][0], me), token_rows(sides[a][1], me), lsem.at[a])

    def view(slot, part, j):
        if part == 0:
            return gall.at[slot, j, pl.ds(0, qrows)]
        if part == 1:
            return gall.at[slot, j, pl.ds(do0, qrows)]
        return gall.at[slot, pl.ds(j * (n // 2), n // 2), pl.ds(kv0, 2 * krows)]

    def own_right(part, j):
        return rdma(view(0, part, j), view(1, part, j), osem.at[0, part, j], rsem.at[1, part, j], right)

    def own_left(part, j):
        return rdma(view(0, part, j), view(2, part, j), osem.at[1, part, j], rsem.at[2, part, j], left)

    def relay_plus(part, j):
        return rdma(view(1, part, j), view(3, part, j), relsem.at[part, j], rsem.at[3, part, j], right)

    def relay_minus(part, j):
        return rdma(view(2, part, j), view(3, part, j), relsem.at[part, j], rsem.at[3, part, j], left)

    def to_partner(slot, part, j):
        return rdma(view(slot, part, j), view(4 + slot, part, j), parsem.at[slot, part, j], rsem.at[4 + slot, part, j], partner)

    def send_own(first, second):
        for item in (first, second):
            own_right(*item).start()
            own_left(*item).start()
            to_partner(0, *item).start()

    def serve_near(first, second):
        own_right(*first).wait_recv()
        relay_plus(*first).start()
        to_partner(1, *first).start()
        own_left(*second).wait_recv()
        relay_minus(*second).start()
        to_partner(2, *second).start()
        own_right(*second).wait_recv()
        to_partner(1, *second).start()
        own_left(*first).wait_recv()
        to_partner(2, *first).start()

    def serve_far(first, second):
        relay_plus(*first).wait_recv()
        to_partner(3, *first).start()
        relay_minus(*second).wait_recv()
        to_partner(3, *second).start()

    def tile_items(j):
        return (0, j), (1, j)

    kv_items = ((2, 0), (2, 1))

    def arrived_tiles(slot):
        for j in range(n):
            for item in tile_items(j):
                to_partner(slot - 4, *item).wait_recv()

    def arrived_kv(slot):
        for item in kv_items:
            to_partner(slot - 4, *item).wait_recv()

    slot_table = (0, 4, 1, 2, 5, 6, 3, 7)
    off_table = (0, 0, chips - 1, 1, chips - 1, 1, 2, 2)
    flip_table = (0, 1, 0, 0, 1, 1, 0, 1)

    def source_of(order):
        return ((chip + pick(order, off_table)) % chips) * 2 + (core + pick(order, flip_table)) % 2

    def load(kind, order, buf):
        src = source_of(order)
        if kind == 0:
            return [pltpu.make_async_copy(wo_ref.at[pl.ds(src * qrows, qrows)], woa.at[buf], wsem.at[0, buf])]
        if kind == 1:
            return [pltpu.make_async_copy(wq_ref.at[pl.ds(src * qrows, qrows)], wob.at[buf], wsem.at[1, buf])]
        return [pltpu.make_async_copy(wk_ref.at[pl.ds(src * krows, krows)], woc.at[buf, pl.ds(0, krows)], wsem.at[2, buf]),
                pltpu.make_async_copy(wv_ref.at[pl.ds(src * krows, krows)], woc.at[buf, pl.ds(krows, krows)], wsem.at[3, buf])]

    def stage(kind, buf):
        if kind < 2:
            return pbuf.at[0, 6 + kind, pl.ds(0, qrows), pl.ds(pl.multiple_of(buf * mcol, LANES), mcol)]
        return pbuf.at[0, 6, pl.ds(pl.multiple_of(buf * 2 * krows, 8), 2 * krows), pl.ds(2 * mcol, mcol)]

    def save(kind, order, buf):
        src = source_of(order)
        if kind == 0:
            return [pltpu.make_async_copy(stage(0, buf), dwo_ref.at[pl.ds(src * qrows, qrows)], outsem.at[0, buf])]
        if kind == 1:
            return [pltpu.make_async_copy(stage(1, buf), dwq_ref.at[pl.ds(src * qrows, qrows)], outsem.at[1, buf])]
        both = stage(2, buf)
        return [pltpu.make_async_copy(both.at[pl.ds(0, krows)], dwk_ref.at[pl.ds(src * krows, krows)], outsem.at[2, buf]),
                pltpu.make_async_copy(both.at[pl.ds(krows, krows)], dwv_ref.at[pl.ds(src * krows, krows)], outsem.at[3, buf])]

    parts = [(j, slice(j * width, min((j + 1) * width, model))) for j in range(-(-model // width))]
    kinds = ((0, qrows, woa, dyc, 0), (do0, rows, wob, xc, 3), (kv0, do0, woc, xc, 3))

    def closing_part(kind, order):
        row0, row1, wbuf, other, acc = kinds[kind]
        buf = order % 2
        slot = pick(order, slot_table)
        for copy in load(kind, order, buf):
            copy.wait()

        @pl.when(order < n - 1)
        def _():
            for copy in load(kind, order + 1, 1 - buf):
                copy.start()

        @pl.when(order >= 2)
        def _():
            for copy in save(kind, order - 2, buf):
                copy.wait()

        @pl.when(order >= 0)
        def _():
            wide = jnp.concatenate([gall[slot, j, row0:row1, :] for j in range(n)], axis=1)
            stage(kind, buf)[...] = dot_nn(wide, other[...])

        for copy in save(kind, order, buf):
            copy.start()
        for j, cols in parts:
            @pl.when(order >= 0)
            def _():
                pbuf[0, acc + j, :, 0:cols.stop - cols.start] += dot_tn(gall[slot, me, row0:row1, :], wbuf[buf, :, cols])

    def block_copies(step, buf):
        pair, flip = step // 2, (step + step // 6) % 2
        off = 2 - 3 * pair + 5 * (pair // 2) + 2 * (pair // 3)
        dst = ((chip + sgn * off + chips) % chips) * 2 + (core + flip) % 2
        return [
            pltpu.make_async_copy(wo_ref.at[pl.ds(dst * qrows, qrows)], woa.at[buf], wsem.at[0, buf]),
            pltpu.make_async_copy(wq_ref.at[pl.ds(dst * qrows, qrows)], wob.at[buf], wsem.at[1, buf]),
            pltpu.make_async_copy(wk_ref.at[pl.ds(dst * krows, krows)], woc.at[buf, pl.ds(0, krows)], wsem.at[2, buf]),
            pltpu.make_async_copy(wv_ref.at[pl.ds(dst * krows, krows)], woc.at[buf, pl.ds(krows, krows)], wsem.at[3, buf]),
        ]

    def p_first(t):
        return rdma(gall.at[3, t], gall.at[7, t], psend.at[t], pfirst.at[t], ahead)

    def p_second(t):
        return rdma(gall.at[7, t], gall.at[0, relay_from], psecond.at[t], precv.at[t], device(sgn, t))

    def p_direct(t):
        return rdma(gall.at[3, t], gall.at[0, me], psend.at[t], precv.at[t], dests[t])

    def seg_copy(t):
        return rdma(seg_mine, seg_all.at[me], gsend.at[t], grecv.at[t], dests[t])

    xcols = [(c, c * tok, min(tok, model - c * tok)) for c in range(-(-model // tok))]

    def x_loads(a):
        return [pltpu.make_async_copy(sides[a][0].at[:, pl.ds(lo, size)], gall.at[1 + a, c, pl.ds(0, tok), pl.ds(0, size)],
                                      xload.at[a, c]) for c, lo, size in xcols]

    def x_whole(a):
        return jnp.concatenate([gall[1 + a, c, 0:tok, 0:size] for c, lo, size in xcols], axis=1)

    for copy in x_loads(0):
        copy.start()
    for copy in block_copies(0, 0):
        copy.start()
    for copy in x_loads(1):
        copy.start()
    for a in range(2):
        x_own(a).start()
    seg_mine[...] = jnp.broadcast_to(seg_ref[...], seg_mine.shape)
    pl.semaphore_wait(barrier, n - 1)
    for t in range(n - 1):
        seg_copy(t).start()
    seg_all[me] = seg_mine[...]
    for copy in x_loads(0) + x_loads(1):
        copy.wait()

    def project_step(step, carry):
        buf = step % 2

        @pl.when(step < n - 1)
        def _():
            for copy in block_copies(step + 1, 1 - buf):
                copy.start()

        for copy in block_copies(step, buf):
            copy.wait()
        slot = 3 - 3 * (step // (n - 1))
        place = step + (me - step) * (step // (n - 1))
        gall[slot, place, 0:qrows] = dot_nt(wob[buf], x_whole(0)).astype(BF)
        gall[slot, place, kv0:do0] = dot_nt(woc[buf], x_whole(0)).astype(BF)
        gall[slot, place, do0:rows] = dot_nt(woa[buf], x_whole(1)).astype(BF)
        for t in range(n - 1):
            @pl.when(step == t)
            def _():
                (p_first if t < 2 else p_direct)(t).start()
        return carry

    lax.fori_loop(0, n, project_step, 0)
    for peer in (right, left):
        pl.semaphore_signal(free_near, inc=1, device_id={'cp': peer}, device_id_type=pl.DeviceIdType.MESH)
    for t in range(2):
        p_first(t).wait_recv()
        p_second(t).start()
    for t in range(n - 1):
        for a in range(2):
            (x_first if t < 2 else x_direct)(a, t).start()

    for t in range(n - 1):
        seg_copy(t).wait_recv()
    row_id = lax.broadcasted_iota(jnp.int32, (n, tok), 0)
    lane_id = lax.broadcasted_iota(jnp.int32, (n, tok), 1)
    seg = jnp.zeros((n, tok), jnp.int32)
    for d in range(n):
        seg = jnp.where(row_id == d, seg_all[d], seg)
    before = jnp.where(lane_id == 0, pltpu.roll(pltpu.roll(seg, 1, 1), 1, 0), pltpu.roll(seg, 1, 1))
    pos = row_id * tok + lane_id
    best = jnp.where((seg != before) & (pos > 0), pos, 0)
    shift = 1
    while shift < tok:
        best = jnp.maximum(best, jnp.where(lane_id >= shift, pltpu.roll(best, shift, 1), 0))
        shift *= 2
    end = jnp.broadcast_to(best[:, tok - 1:tok], (n, tok))
    carry_max = jnp.where(row_id >= 1, pltpu.roll(end, 1, 0), 0)
    shift = 1
    while shift < n:
        carry_max = jnp.maximum(carry_max, jnp.where(row_id >= shift, pltpu.roll(carry_max, shift, 0), 0))
        shift *= 2
    best = jnp.maximum(best, carry_max)
    for d in range(n):
        first_ref[d] = jnp.broadcast_to(best[d:d + 1], (8, tok))
    dkacc[...] = jnp.zeros_like(dkacc)
    dvacc[...] = jnp.zeros_like(dvacc)
    rhsq[...] = jnp.zeros_like(rhsq)
    rhsd[...] = jnp.zeros_like(rhsd)
    for t in range(n - 1):
        p_direct(t).wait_recv()

    def transpose_tile(c, carry):
        kvn[pl.ds(pl.multiple_of(c * tok, LANES), tok), :] = gall[0, c, kv0:do0, :].T
        return carry

    lax.fori_loop(0, n, transpose_tile, 0)
    score_mul = scale * LOG2E
    grp = tok // 8
    lag = 2

    def keys(c):
        return kvn[pl.ds(pl.multiple_of(c * tok, LANES), tok), :]

    def q_rows(pair, g):
        return pl.ds(pl.multiple_of((pair * group + g) * krows, krows), krows)

    def do_rows(pair, g):
        return pl.ds(pl.multiple_of(do0 + (pair * group + g) * krows, krows), krows)

    def doc_starts(i):
        return jnp.concatenate([first_ref[i][0:1]] * group, axis=1)

    def score(i, pair, c, top, diagonal):
        t = dot_nn(keys(c), rhsq[pair]) * score_mul
        kpos = lax.broadcasted_iota(jnp.int32, (tok, width), 0)
        keep = kpos >= doc_starts(i) - c * tok
        if diagonal:
            qpos = lax.broadcasted_iota(jnp.int32, (1, tok), 1)
            keep = keep & (kpos <= jnp.concatenate([qpos] * group, axis=1))
        t = jnp.where(keep, t, -jnp.inf)
        pbuf[pair, c] = t
        return jnp.maximum(top, jnp.max(t.reshape(grp, 8, width), axis=0))

    def value(pair, c, top, total):
        p = jnp.exp2(pbuf[pair, c] - top)
        oacc[...] += dot_nn(gall[0, c, kv0 + krows:do0, :], p.astype(BF))
        return total + jnp.sum(p.reshape(grp, 8, width), axis=0)

    def grad(pair, c):
        p = jnp.exp2(pbuf[pair, c] - stats[pair, 0:1])
        dp = dot_nn(keys(c), rhsd[pair])
        ds = (p * (dp - stats[pair, 8:9])).astype(BF)
        dqacc[...] += dot_nn(gall[0, c, kv0:kv0 + krows, :], ds)
        pb = p.astype(BF)
        spans = [(slice(j * mcol, (j + 1) * mcol), slice(j * tok, (j + 1) * tok)) for j in range(width // mcol)]
        for qs, place in spans:
            woa[0, :, place] = ds[:, qs].T
            wob[0, :, place] = pb[:, qs].T
        dkacc[c] += sum(dot_nn(rhsq[pair, 0:krows, qs], woa[0, :, place]) for qs, place in spans)
        dvacc[c] += sum(dot_nn(rhsd[pair, krows:2 * krows, qs], wob[0, :, place]) for qs, place in spans)

    def finish_dq(i, pair):
        dq = (dqacc[...] * scale).astype(BF)
        for g in range(group):
            gall[0, i, do_rows(pair, g), :] = dq[:, g * tok:(g + 1) * tok]

    def tile_done(i):
        @pl.when(i == 0)
        def _():
            for t in range(n - 1):
                p_direct(t).wait_send()
            for t in range(2):
                p_second(t).wait_send()
            for peer in (right, left):
                pl.semaphore_signal(free_far, inc=1, device_id={'cp': peer}, device_id_type=pl.DeviceIdType.MESH)
            pl.semaphore_signal(free_par, inc=1, device_id={'cp': partner}, device_id_type=pl.DeviceIdType.MESH)
            pl.semaphore_wait(free_near, 2)

        send_own(*tile_items(i))

        @pl.when(i == 1)
        def _():
            for t in range(2):
                for a in range(2):
                    x_first(a, t).wait_recv()
                    x_second(a, t).start()

        @pl.when(i == lag)
        def _():
            pl.semaphore_wait(free_far, 2)

        @pl.when(i >= lag)
        def _():
            serve_near(*tile_items(i - lag))

    def item_step(m, carry):
        i, pair = m // 2, m % 2
        last = 1 - pair
        top0 = jnp.full((8, width), -jnp.inf, F32)

        for g in range(group):
            lanes = slice(g * tok, (g + 1) * tok)
            rhsq[pair, 0:krows, lanes] = gall[0, i, q_rows(pair, g), :]
            rhsd[pair, krows:2 * krows, lanes] = gall[0, i, do_rows(pair, g), :]
        dqacc[...] = jnp.zeros_like(dqacc)

        def both_step(c, top):
            grad(last, c)
            return score(i, pair, c, top, False)

        top = lax.fori_loop(0, i, both_step, top0)
        stats[pair, 16:24] = top

        @pl.when(pair == 1)
        def _():
            grad(last, i)
            stats[pair, 16:24] = score(i, pair, i, stats[pair, 16:24], True)

        @pl.when(pair == 0)
        def _():
            stats[pair, 16:24] = score(i, pair, i, stats[pair, 16:24], True)

        @pl.when(m >= 1)
        def _():
            finish_dq((m - 1) // 2, last)

        top = jnp.max(stats[pair, 16:24], axis=0, keepdims=True)
        oacc[...] = jnp.zeros_like(oacc)
        total = lax.fori_loop(0, i + 1, lambda c, acc: value(pair, c, top, acc), jnp.zeros((8, width), F32))
        total = jnp.sum(total, axis=0, keepdims=True)
        o_blk = (oacc[...] * (1.0 / total)).astype(BF)
        stats[pair, 0:8] = jnp.broadcast_to(top + jnp.log2(total), (8, width))
        delta = jnp.sum(rhsd[pair, krows:2 * krows].astype(F32) * o_blk.astype(F32), axis=0, keepdims=True)
        stats[pair, 8:16] = jnp.broadcast_to(delta, (8, width))
        for g in range(group):
            gall[0, i, q_rows(pair, g), :] = o_blk[:, g * tok:(g + 1) * tok]

        @pl.when((pair == 0) & (i >= 1))
        def _():
            tile_done(i - 1)
        return carry

    lax.fori_loop(0, n * heads // group, item_step, 0)
    dqacc[...] = jnp.zeros_like(dqacc)

    def last_step(c, carry):
        grad(1, c)
        return carry

    lax.fori_loop(0, n, last_step, 0)
    finish_dq(n - 1, 1)
    tile_done(n - 1)
    for c in range(n):
        gall[0, c, kv0:kv0 + krows, :] = (dkacc[c] * scale).astype(BF)
        gall[0, c, kv0 + krows:do0, :] = dvacc[c].astype(BF)
    send_own(*kv_items)
    for kind in range(3):
        for copy in load(kind, 0, 0):
            copy.start()
    pbuf[0, 0:6] = jnp.zeros((6, tok, width), F32)

    for a in range(2):
        x_own(a).wait()
        for t in range(n - 1):
            x_direct(a, t).wait_recv()

    near = n - 2
    spare = tok - qrows

    def rounded(acc, buf, out, sem):
        for j, cols in parts:
            wide = pbuf[0, acc + j, :, 0:cols.stop - cols.start].astype(BF)
            buf[0, :, cols] = wide[0:qrows]
            buf[1, 0:spare, cols] = wide[qrows:tok]
        return [pltpu.make_async_copy(buf.at[0], out.at[pl.ds(0, qrows)], lsem.at[sem]),
                pltpu.make_async_copy(buf.at[1, pl.ds(0, spare)], out.at[pl.ds(qrows, spare)], lsem.at[sem + 1])]

    def closing_step(r, carry):
        @pl.when(r == 1)
        def _():
            arrived_tiles(4)

        @pl.when(r == 2)
        def _():
            for j in range(n - lag, n):
                serve_near(*tile_items(j))

        @pl.when(r == 4)
        def _():
            pl.semaphore_wait(free_par, 1)
            for j in range(n - 2 * lag):
                serve_far(*tile_items(j))
            arrived_tiles(5)

        @pl.when(r == 5)
        def _():
            arrived_tiles(6)

        @pl.when(r == near)
        def _():
            serve_near(*kv_items)

        @pl.when(r == near + 1)
        def _():
            arrived_kv(4)

        @pl.when(r == near + 4)
        def _():
            arrived_kv(5)
            arrived_kv(6)

        @pl.when(r == 2 * near)
        def _():
            for a in range(2):
                for t in range(n - 1):
                    x_direct(a, t).wait_send()
                for t in range(2):
                    x_second(a, t).wait_send()
            for t in range(n - 1):
                seg_copy(t).wait_send()
            for j in range(n):
                for item in tile_items(j):
                    own_right(*item).wait_send()
                    own_left(*item).wait_send()
                    for slot in range(3):
                        to_partner(slot, *item).wait_send()
            for j in range(n - 2 * lag):
                relay_plus(0, j).wait_send()
                relay_minus(1, j).wait_send()
            for j in range(n - 2 * lag, n):
                serve_far(*tile_items(j))

        @pl.when(r == 2 * near + 1)
        def _():
            arrived_tiles(7)

        @pl.when((r < near) | ((r >= 2 * near) & (r < 2 * near + 2)))
        def _():
            order = r - near * (r // (2 * near))
            closing_part(0, order)
            closing_part(1, order)

        @pl.when(r == 2 * near + 2)
        def _():
            for copy in rounded(0, woa, y_ref, 2):
                copy.start()
            serve_far(*kv_items)

        @pl.when(r == 2 * near + 3)
        def _():
            arrived_kv(7)

        @pl.when(((r >= near) & (r < 2 * near)) | (r >= 2 * near + 2))
        def _():
            closing_part(2, r - near - 2 * (r // (2 * near + 2)))
        return carry

    lax.fori_loop(0, 2 * n, closing_step, 0)
    outs = rounded(3, wob, dx_ref, 4)
    for copy in outs:
        copy.start()
    for kind in range(3):
        for order in (n - 2, n - 1):
            for copy in save(kind, order, order % 2):
                copy.wait()
    for copy in [pltpu.make_async_copy(woa.at[0], y_ref.at[pl.ds(0, qrows)], lsem.at[2]),
                 pltpu.make_async_copy(woa.at[1, pl.ds(0, spare)], y_ref.at[pl.ds(qrows, spare)], lsem.at[3])] + outs:
        copy.wait()
    for j in range(n):
        for item in tile_items(j):
            to_partner(3, *item).wait_send()
    for j in range(n - 2 * lag, n):
        relay_plus(0, j).wait_send()
        relay_minus(1, j).wait_send()
    for item in kv_items:
        for slot in range(4):
            to_partner(slot, *item).wait_send()
        own_right(*item).wait_send()
        own_left(*item).wait_send()
    relay_plus(*kv_items[0]).wait_send()
    relay_minus(*kv_items[1]).wait_send()


def attention_layer(n, x_act, dy_act, seg, wq, wk, wv, wo):
    tok, model = x_act.shape
    qrows, krows = wq.shape[0] // n, wk.shape[0] // n
    rows = 2 * qrows + 2 * krows
    total = n * tok
    mcol = model // n
    group = 2
    width = group * tok
    vmem = pl.BlockSpec(memory_space=pltpu.VMEM)
    anym = pl.BlockSpec(memory_space=pl.ANY)
    dma = pltpu.SemaphoreType.DMA
    return pl.pallas_call(
        functools.partial(main_kernel, (n, qrows, krows, tok, krows ** -0.5)),
        out_shape=(jax.ShapeDtypeStruct((tok, model), BF), jax.ShapeDtypeStruct((tok, model), BF),
                   jax.ShapeDtypeStruct((wq.shape[0], mcol), F32), jax.ShapeDtypeStruct((wk.shape[0], mcol), F32),
                   jax.ShapeDtypeStruct((wv.shape[0], mcol), F32), jax.ShapeDtypeStruct((wo.shape[0], mcol), F32)),
        in_specs=[anym, anym, vmem, anym, anym, anym, anym],
        out_specs=(anym,) * 6,
        scratch_shapes=[
            pltpu.VMEM((8, tok), jnp.int32), pltpu.VMEM((n, 8, tok), jnp.int32), pltpu.VMEM((n, 8, tok), jnp.int32),
            pltpu.VMEM((total, 2 * krows), BF),
            pltpu.VMEM((2, n, tok, width), F32),
            pltpu.VMEM((2, 2 * krows, width), BF), pltpu.VMEM((2, 2 * krows, width), BF),
            pltpu.VMEM((2, 24, width), F32),
            pltpu.VMEM((krows, width), F32), pltpu.VMEM((krows, width), F32),
            pltpu.VMEM((n, krows, tok), F32), pltpu.VMEM((n, krows, tok), F32),
            pltpu.VMEM((n, n, rows, tok), BF),
            pltpu.VMEM((total, mcol), BF), pltpu.VMEM((total, mcol), BF),
            pltpu.VMEM((2, 2, tok, mcol), BF),
            pltpu.VMEM((2, qrows, model), BF), pltpu.VMEM((2, qrows, model), BF), pltpu.VMEM((2, 2 * krows, model), BF),
            dma((4, 2)), dma((4, 2)),
            dma((2, 3, n)), dma((3, n)), dma((4, 3, n)), dma((8, 3, n)),
            dma((2, n)), dma((2, n)), dma((2, 2)), dma((2, 2)), dma((6,)), dma((2, n)),
            dma((n,)), dma((n,)), dma((2,)), dma((2,)), dma((n,)), dma((n,)),
            pltpu.SemaphoreType.REGULAR, pltpu.SemaphoreType.REGULAR, pltpu.SemaphoreType.REGULAR,
        ],
        compiler_params=pltpu.CompilerParams(collective_id=0, has_side_effects=True, vmem_limit_bytes=VMEM_MAX),
        name='attention_layer',
    )(x_act, dy_act, seg.reshape(1, tok), wq, wk, wv, wo)


def solution(mesh):
    n = mesh.shape['cp']
    row_spec = P(('dp', 'cp'), None)
    tok_spec = P(('dp', 'cp'))
    weight_spec = P(None, None, None)
    grad_spec = P(('dp', 'cp'), None, None)

    def local_step(x_act, seg_ids, w_q, w_k, w_v, w_o, dy_act):
        model, q_heads, head_dim = w_q.shape
        kv_heads = w_k.shape[1]
        assert kv_heads == n and x_act.shape[0] % LANES == 0

        def flat(w):
            return w.transpose(1, 2, 0).reshape(w.shape[1] * head_dim, model)

        def unflat(g, heads):
            return g.reshape(heads, head_dim, g.shape[1]).transpose(2, 0, 1)

        wq, wk, wv, wo = flat(w_q), flat(w_k), flat(w_v), flat(w_o)
        y_out, dx_out, dwq, dwk, dwv, dwo = attention_layer(n, x_act, dy_act, seg_ids, wq, wk, wv, wo)
        return (y_out, dx_out, unflat(dwq, q_heads), unflat(dwk, kv_heads), unflat(dwv, kv_heads), unflat(dwo, q_heads))

    return jax.shard_map(local_step, mesh=mesh,
                         in_specs=(row_spec, tok_spec, weight_spec, weight_spec, weight_spec, weight_spec, row_spec),
                         out_specs=(row_spec, row_spec, grad_spec, grad_spec, grad_spec, grad_spec),
                         check_vma=False)
```

```python
import functools

import jax
import jax.numpy as jnp
from jax import lax
from jax.experimental import pallas as pl
from jax.experimental.pallas import tpu as pltpu
from jax.sharding import PartitionSpec as P

BF = jnp.bfloat16
F32 = jnp.float32
LANES = 128
LOG2E = 1.4426950408889634
VMEM_MAX = 67043328


def rdma(src, dst, send_sem, recv_sem, peer):
    return pltpu.make_async_remote_copy(src_ref=src, dst_ref=dst, send_sem=send_sem, recv_sem=recv_sem,
                                        device_id={'cp': peer}, device_id_type=pl.DeviceIdType.MESH)


def dot_nt(left, right):
    return lax.dot_general(left, right, (((1,), (1,)), ((), ())), preferred_element_type=F32)


def dot_tn(left, right):
    return lax.dot_general(left, right, (((0,), (0,)), ((), ())), preferred_element_type=F32)


def dot_nn(left, right):
    return lax.dot_general(left, right, (((1,), (0,)), ((), ())), preferred_element_type=F32)


def pick(index, values):
    out = values[0]
    for k in range(1, len(values)):
        out = jnp.where(index == k, values[k], out)
    return out


def main_kernel(dims, x_ref, dy_ref, seg_ref, wq_ref, wk_ref, wv_ref, wo_ref,
                y_ref, dx_ref, dwq_ref, dwk_ref, dwv_ref, dwo_ref,
                seg_mine, seg_all, first_ref, kvn, pbuf, rhsq, rhsd, stats, oacc, dqacc, dkacc, dvacc, gall, xc, dyc, xrel,
                woa, wob, woc, wsem, outsem, osem, relsem, parsem, rsem, xsend, xrecv, xfirst, xsecond, lsem, xload,
                psend, precv, pfirst, psecond, gsend, grecv, free_near, free_far, free_par):
    n, qrows, krows, tok, scale = dims
    chips = n // 2
    heads = qrows // krows
    width = rhsq.shape[2]
    group = width // tok
    me = lax.axis_index('cp')
    chip, core = me // 2, me % 2
    sgn = 1 - 2 * core
    rows = 2 * qrows + 2 * krows
    model = x_ref.shape[1]
    mcol = xc.shape[1]
    do0, kv0 = qrows, 2 * qrows

    def device(chip_off, flip):
        return ((chip + chip_off + chips) % chips) * 2 + (core + flip) % 2

    right, left, partner = device(1, 0), device(-1, 0), device(0, 1)
    dests = [device(2, 0), device(2, 1), device(-sgn, 0), device(-sgn, 1), device(sgn, 0), device(sgn, 1), partner]
    ahead = dests[4]
    relay_from = device(-sgn, 0)

    barrier = pltpu.get_barrier_semaphore()
    for peer in dests:
        pl.semaphore_signal(barrier, inc=1, device_id={'cp': peer}, device_id_type=pl.DeviceIdType.MESH)

    sides = ((x_ref, xc), (dy_ref, dyc))

    def columns(ref, dst):
        return ref.at[:, pl.ds(pl.multiple_of(dst * mcol, LANES), mcol)]

    def token_rows(ref, src):
        return ref.at[pl.ds(pl.multiple_of(src * tok, LANES), tok)]

    def x_first(a, t):
        return rdma(columns(sides[a][0], dests[t]), xrel.at[a, t], xsend.at[a, t], xfirst.at[a, t], ahead)

    def x_second(a, t):
        return rdma(xrel.at[a, t], token_rows(sides[a][1], relay_from), xsecond.at[a, t], xrecv.at[a, t], device(sgn, t))

    def x_direct(a, t):
        return rdma(columns(sides[a][0], dests[t]), token_rows(sides[a][1], me), xsend.at[a, t], xrecv.at[a, t], dests[t])

    def x_own(a):
        return pltpu.make_async_copy(columns(sides[a][0], me), token_rows(sides[a][1], me), lsem.at[a])

    def view(slot, part, j):
        if part == 0:
            return gall.at[slot, j, pl.ds(0, kv0)]
        return gall.at[slot, pl.ds(j * (n // 2), n // 2), pl.ds(kv0, 2 * krows)]

    def own_right(part, j):
        return rdma(view(0, part, j), view(1, part, j), osem.at[0, part, j], rsem.at[1, part, j], right)

    def own_left(part, j):
        return rdma(view(0, part, j), view(2, part, j), osem.at[1, part, j], rsem.at[2, part, j], left)

    def relay_plus(part, j):
        src, dst = view(1, part, j), view(3, part, j)
        if part == 0:
            src, dst = src.at[pl.ds(0, do0)], dst.at[pl.ds(0, do0)]
        return rdma(src, dst, relsem.at[0, part, j], rsem.at[3, part, j], right)

    def relay_minus(part, j):
        src, dst = view(2, part, j), view(3, part, j)
        if part == 0:
            src, dst = src.at[pl.ds(do0, do0)], dst.at[pl.ds(do0, do0)]
        return rdma(src, dst, relsem.at[1, part, j], rsem.at[0, part, j], left)

    def to_partner(slot, part, j):
        return rdma(view(slot, part, j), view(4 + slot, part, j), parsem.at[slot, part, j], rsem.at[4 + slot, part, j], partner)

    def send_own(part, j):
        own_right(part, j).start()
        own_left(part, j).start()
        to_partner(0, part, j).start()

    def serve_near(j):
        own_right(0, j).wait_recv()
        relay_plus(0, j).start()
        to_partner(1, 0, j).start()
        own_left(0, j).wait_recv()
        relay_minus(0, j).start()
        to_partner(2, 0, j).start()

    def serve_near_kv():
        own_right(1, 0).wait_recv()
        relay_plus(1, 0).start()
        own_left(1, 1).wait_recv()
        relay_minus(1, 1).start()
        to_partner(1, 1, 0).start()
        to_partner(2, 1, 1).start()
        own_right(1, 1).wait_recv()
        to_partner(1, 1, 1).start()
        own_left(1, 0).wait_recv()
        to_partner(2, 1, 0).start()

    def serve_far(j):
        relay_plus(0, j).wait_recv()
        relay_minus(0, j).wait_recv()
        to_partner(3, 0, j).start()

    def serve_far_kv():
        relay_plus(1, 0).wait_recv()
        to_partner(3, 1, 0).start()
        relay_minus(1, 1).wait_recv()
        to_partner(3, 1, 1).start()

    def arrived_tiles(slot):
        for j in range(n):
            to_partner(slot - 4, 0, j).wait_recv()

    def arrived_kv(slot):
        for j in range(2):
            to_partner(slot - 4, 1, j).wait_recv()

    slot_table = (0, 4, 1, 2, 5, 6, 3, 7)
    off_table = (0, 0, chips - 1, 1, chips - 1, 1, 2, 2)
    flip_table = (0, 1, 0, 0, 1, 1, 0, 1)

    def source_of(order):
        return ((chip + pick(order, off_table)) % chips) * 2 + (core + pick(order, flip_table)) % 2

    def load(kind, order, buf):
        src = source_of(order)
        if kind == 0:
            return [pltpu.make_async_copy(wo_ref.at[pl.ds(src * qrows, qrows)], woa.at[buf], wsem.at[0, buf])]
        if kind == 1:
            return [pltpu.make_async_copy(wq_ref.at[pl.ds(src * qrows, qrows)], wob.at[buf], wsem.at[1, buf])]
        return [pltpu.make_async_copy(wk_ref.at[pl.ds(src * krows, krows)], woc.at[buf, pl.ds(0, krows)], wsem.at[2, buf]),
                pltpu.make_async_copy(wv_ref.at[pl.ds(src * krows, krows)], woc.at[buf, pl.ds(krows, krows)], wsem.at[3, buf])]

    def stage(kind, buf):
        if kind < 2:
            return pbuf.at[0, 6 + kind, pl.ds(0, qrows), pl.ds(pl.multiple_of(buf * mcol, LANES), mcol)]
        return pbuf.at[0, 6, pl.ds(pl.multiple_of(buf * 2 * krows, 8), 2 * krows), pl.ds(2 * mcol, mcol)]

    def save(kind, order, buf):
        src = source_of(order)
        if kind == 0:
            return [pltpu.make_async_copy(stage(0, buf), dwo_ref.at[pl.ds(src * qrows, qrows)], outsem.at[0, buf])]
        if kind == 1:
            return [pltpu.make_async_copy(stage(1, buf), dwq_ref.at[pl.ds(src * qrows, qrows)], outsem.at[1, buf])]
        both = stage(2, buf)
        return [pltpu.make_async_copy(both.at[pl.ds(0, krows)], dwk_ref.at[pl.ds(src * krows, krows)], outsem.at[2, buf]),
                pltpu.make_async_copy(both.at[pl.ds(krows, krows)], dwv_ref.at[pl.ds(src * krows, krows)], outsem.at[3, buf])]

    parts = [(j, slice(j * width, min((j + 1) * width, model))) for j in range(-(-model // width))]
    kinds = ((0, do0, woa, dyc, 0), (do0, kv0, wob, xc, 3), (kv0, rows, woc, xc, 3))

    def closing_part(kind, order):
        row0, row1, wbuf, other, acc = kinds[kind]
        buf = order % 2
        slot = pick(order, slot_table)
        for copy in load(kind, order, buf):
            copy.wait()

        @pl.when(order < n - 1)
        def _():
            for copy in load(kind, order + 1, 1 - buf):
                copy.start()

        @pl.when(order >= 2)
        def _():
            for copy in save(kind, order - 2, buf):
                copy.wait()

        @pl.when(order >= 0)
        def _():
            wide = jnp.concatenate([gall[slot, j, row0:row1, :] for j in range(n)], axis=1)
            stage(kind, buf)[...] = dot_nn(wide, other[...])

        for copy in save(kind, order, buf):
            copy.start()
        for j, cols in parts:
            @pl.when(order >= 0)
            def _():
                pbuf[0, acc + j, :, 0:cols.stop - cols.start] += dot_tn(gall[slot, me, row0:row1, :], wbuf[buf, :, cols])

    def block_copies(step, buf):
        pair, flip = step // 2, (step + step // 6) % 2
        off = 2 - 3 * pair + 5 * (pair // 2) + 2 * (pair // 3)
        dst = ((chip + sgn * off + chips) % chips) * 2 + (core + flip) % 2
        return [
            pltpu.make_async_copy(wo_ref.at[pl.ds(dst * qrows, qrows)], woa.at[buf], wsem.at[0, buf]),
            pltpu.make_async_copy(wq_ref.at[pl.ds(dst * qrows, qrows)], wob.at[buf], wsem.at[1, buf]),
            pltpu.make_async_copy(wk_ref.at[pl.ds(dst * krows, krows)], woc.at[buf, pl.ds(0, krows)], wsem.at[2, buf]),
            pltpu.make_async_copy(wv_ref.at[pl.ds(dst * krows, krows)], woc.at[buf, pl.ds(krows, krows)], wsem.at[3, buf]),
        ]

    def p_first(t):
        return rdma(gall.at[3, t], gall.at[7, t], psend.at[t], pfirst.at[t], ahead)

    def p_second(t):
        return rdma(gall.at[7, t], gall.at[0, relay_from], psecond.at[t], precv.at[t], device(sgn, t))

    def p_direct(t):
        return rdma(gall.at[3, t], gall.at[0, me], psend.at[t], precv.at[t], dests[t])

    def seg_copy(t):
        row = pl.ds(0, 1)
        return rdma(seg_mine.at[row], seg_all.at[me, row], gsend.at[t], grecv.at[t], dests[t])

    xcols = [(c, c * tok, min(tok, model - c * tok)) for c in range(-(-model // tok))]

    def x_loads(a):
        return [pltpu.make_async_copy(sides[a][0].at[:, pl.ds(lo, size)], gall.at[1 + a, c, pl.ds(0, tok), pl.ds(0, size)],
                                      xload.at[a, c]) for c, lo, size in xcols]

    def x_whole(a):
        return jnp.concatenate([gall[1 + a, c, 0:tok, 0:size] for c, lo, size in xcols], axis=1)

    for copy in x_loads(0):
        copy.start()
    for copy in block_copies(0, 0):
        copy.start()
    for copy in x_loads(1):
        copy.start()
    for a in range(2):
        x_own(a).start()
    seg_mine[...] = jnp.broadcast_to(seg_ref[...].reshape(1, tok), seg_mine.shape)
    pl.semaphore_wait(barrier, n - 1)
    for a in range(2):
        x_direct(a, 2).start()
    for t in range(n - 1):
        seg_copy(t).start()
    seg_all[me] = seg_mine[...]
    for copy in x_loads(0) + x_loads(1):
        copy.wait()

    def project_step(step, carry):
        buf = step % 2

        @pl.when(step < n - 1)
        def _():
            for copy in block_copies(step + 1, 1 - buf):
                copy.start()

        for copy in block_copies(step, buf):
            copy.wait()
        slot = 3 - 3 * (step // (n - 1))
        place = step + (me - step) * (step // (n - 1))
        gall[slot, place, 0:qrows] = dot_nt(wob[buf], x_whole(0)).astype(BF)
        gall[slot, place, kv0:rows] = dot_nt(woc[buf], x_whole(0)).astype(BF)
        gall[slot, place, do0:kv0] = dot_nt(woa[buf], x_whole(1)).astype(BF)
        for t in range(n - 1):
            @pl.when(step == t)
            def _():
                (p_first if t < 2 else p_direct)(t).start()
        return carry

    lax.fori_loop(0, n, project_step, 0)
    for peer in (right, left):
        pl.semaphore_signal(free_near, inc=1, device_id={'cp': peer}, device_id_type=pl.DeviceIdType.MESH)
    for t in range(2):
        p_first(t).wait_recv()
        p_second(t).start()
    for t in range(n - 1):
        for a in range(2):
            if t != 2:
                (x_first if t < 2 else x_direct)(a, t).start()

    for t in range(n - 1):
        seg_copy(t).wait_recv()
    row_id = lax.broadcasted_iota(jnp.int32, (n, tok), 0)
    lane_id = lax.broadcasted_iota(jnp.int32, (n, tok), 1)
    seg = jnp.zeros((n, tok), jnp.int32)
    for d in range(n):
        seg = jnp.where(row_id == d, seg_all[d, 0:1], seg)
    before = jnp.where(lane_id == 0, pltpu.roll(pltpu.roll(seg, 1, 1), 1, 0), pltpu.roll(seg, 1, 1))
    pos = row_id * tok + lane_id
    best = jnp.where((seg != before) & (pos > 0), pos, 0)
    shift = 1
    while shift < tok:
        best = jnp.maximum(best, jnp.where(lane_id >= shift, pltpu.roll(best, shift, 1), 0))
        shift *= 2
    end = jnp.broadcast_to(best[:, tok - 1:tok], (n, tok))
    carry_max = jnp.where(row_id >= 1, pltpu.roll(end, 1, 0), 0)
    shift = 1
    while shift < n:
        carry_max = jnp.maximum(carry_max, jnp.where(row_id >= shift, pltpu.roll(carry_max, shift, 0), 0))
        shift *= 2
    best = jnp.maximum(best, carry_max)
    for d in range(n):
        first_ref[d] = jnp.broadcast_to(best[d:d + 1], (8, tok))
    dkacc[...] = jnp.zeros_like(dkacc)
    dvacc[...] = jnp.zeros_like(dvacc)
    rhsq[...] = jnp.zeros_like(rhsq)
    rhsd[...] = jnp.zeros_like(rhsd)
    for t in range(n - 1):
        p_direct(t).wait_recv()

    def transpose_tile(c, carry):
        kvn[pl.ds(pl.multiple_of(c * tok, LANES), tok), :] = gall[0, c, kv0:rows, :].T
        return carry

    lax.fori_loop(0, n, transpose_tile, 0)
    score_mul = scale * LOG2E
    grp = tok // 8
    lag = 2

    def keys(c):
        return kvn[pl.ds(pl.multiple_of(c * tok, LANES), tok), :]

    def q_rows(pair, g):
        return pl.ds(pl.multiple_of((pair * group + g) * krows, krows), krows)

    def do_rows(pair, g):
        return pl.ds(pl.multiple_of(do0 + (pair * group + g) * krows, krows), krows)

    def doc_starts(i):
        return jnp.concatenate([first_ref[i][0:1]] * group, axis=1)

    def score(i, pair, c, top, diagonal):
        t = dot_nn(keys(c), rhsq[pair]) * score_mul
        kpos = lax.broadcasted_iota(jnp.int32, (tok, width), 0)
        keep = kpos >= doc_starts(i) - c * tok
        if diagonal:
            qpos = lax.broadcasted_iota(jnp.int32, (1, tok), 1)
            keep = keep & (kpos <= jnp.concatenate([qpos] * group, axis=1))
        t = jnp.where(keep, t, -jnp.inf)
        pbuf[pair, c] = t
        return jnp.maximum(top, jnp.max(t.reshape(grp, 8, width), axis=0))

    def value(pair, c, top, total):
        p = jnp.exp2(pbuf[pair, c] - top)
        oacc[...] += dot_nn(gall[0, c, kv0 + krows:rows, :], p.astype(BF))
        return total + jnp.sum(p.reshape(grp, 8, width), axis=0)

    def grad(pair, c):
        p = jnp.exp2(pbuf[pair, c] - stats[pair, 0:1])
        dp = dot_nn(keys(c), rhsd[pair])
        ds = (p * (dp - stats[pair, 8:9])).astype(BF)
        dqacc[...] += dot_nn(gall[0, c, kv0:kv0 + krows, :], ds)
        pb = p.astype(BF)
        spans = [(slice(j * mcol, (j + 1) * mcol), slice(j * tok, (j + 1) * tok)) for j in range(width // mcol)]
        for qs, place in spans:
            woa[0, :, place] = ds[:, qs].T
            wob[0, :, place] = pb[:, qs].T
        dkacc[c] += sum(dot_nn(rhsq[pair, 0:krows, qs], woa[0, :, place]) for qs, place in spans)
        dvacc[c] += sum(dot_nn(rhsd[pair, krows:2 * krows, qs], wob[0, :, place]) for qs, place in spans)

    def finish_dq(i, pair):
        dq = (dqacc[...] * scale).astype(BF)
        for g in range(group):
            gall[0, i, do_rows(pair, g), :] = dq[:, g * tok:(g + 1) * tok]

    def tile_done(i):
        @pl.when(i == 0)
        def _():
            for t in range(n - 1):
                p_direct(t).wait_send()
            for t in range(2):
                p_second(t).wait_send()
            for peer in (right, left):
                pl.semaphore_signal(free_far, inc=1, device_id={'cp': peer}, device_id_type=pl.DeviceIdType.MESH)
            pl.semaphore_signal(free_par, inc=1, device_id={'cp': partner}, device_id_type=pl.DeviceIdType.MESH)
            pl.semaphore_wait(free_near, 2)

        send_own(0, i)

        @pl.when(i == 1)
        def _():
            for t in range(2):
                for a in range(2):
                    x_first(a, t).wait_recv()
                    x_second(a, t).start()

        @pl.when(i == lag)
        def _():
            pl.semaphore_wait(free_far, 2)

        @pl.when(i >= lag)
        def _():
            serve_near(i - lag)

    def item_step(m, carry):
        i, pair = m // 2, m % 2
        last = 1 - pair
        top0 = jnp.full((8, width), -jnp.inf, F32)

        for g in range(group):
            lanes = slice(g * tok, (g + 1) * tok)
            rhsq[pair, 0:krows, lanes] = gall[0, i, q_rows(pair, g), :]
            rhsd[pair, krows:2 * krows, lanes] = gall[0, i, do_rows(pair, g), :]
        dqacc[...] = jnp.zeros_like(dqacc)

        def both_step(c, top):
            grad(last, c)
            return score(i, pair, c, top, False)

        top = lax.fori_loop(0, i, both_step, top0)
        stats[pair, 16:24] = top

        @pl.when(pair == 1)
        def _():
            grad(last, i)
            stats[pair, 16:24] = score(i, pair, i, stats[pair, 16:24], True)

        @pl.when(pair == 0)
        def _():
            stats[pair, 16:24] = score(i, pair, i, stats[pair, 16:24], True)

        @pl.when(m >= 1)
        def _():
            finish_dq((m - 1) // 2, last)

        top = jnp.max(stats[pair, 16:24], axis=0, keepdims=True)
        oacc[...] = jnp.zeros_like(oacc)
        total = lax.fori_loop(0, i + 1, lambda c, acc: value(pair, c, top, acc), jnp.zeros((8, width), F32))
        total = jnp.sum(total, axis=0, keepdims=True)
        o_blk = (oacc[...] * (1.0 / total)).astype(BF)
        stats[pair, 0:8] = jnp.broadcast_to(top + jnp.log2(total), (8, width))
        delta = jnp.sum(rhsd[pair, krows:2 * krows].astype(F32) * o_blk.astype(F32), axis=0, keepdims=True)
        stats[pair, 8:16] = jnp.broadcast_to(delta, (8, width))
        for g in range(group):
            gall[0, i, q_rows(pair, g), :] = o_blk[:, g * tok:(g + 1) * tok]

        @pl.when((pair == 0) & (i >= 1))
        def _():
            tile_done(i - 1)
        return carry

    lax.fori_loop(0, n * heads // group, item_step, 0)
    dqacc[...] = jnp.zeros_like(dqacc)

    def last_step(c, carry):
        grad(1, c)
        return carry

    lax.fori_loop(0, n, last_step, 0)
    finish_dq(n - 1, 1)
    tile_done(n - 1)
    for c in range(n):
        gall[0, c, kv0:kv0 + krows, :] = (dkacc[c] * scale).astype(BF)
        gall[0, c, kv0 + krows:rows, :] = dvacc[c].astype(BF)
    for j in range(2):
        send_own(1, j)
    for kind in range(3):
        for copy in load(kind, 0, 0):
            copy.start()
    pbuf[0, 0:6] = jnp.zeros((6, tok, width), F32)

    for a in range(2):
        x_own(a).wait()
        for t in range(n - 1):
            x_direct(a, t).wait_recv()

    near = n - 2
    spare = tok - qrows

    def rounded(acc, buf, out, sem):
        for j, cols in parts:
            wide = pbuf[0, acc + j, :, 0:cols.stop - cols.start].astype(BF)
            buf[0, :, cols] = wide[0:qrows]
            buf[1, 0:spare, cols] = wide[qrows:tok]
        return [pltpu.make_async_copy(buf.at[0], out.at[pl.ds(0, qrows)], lsem.at[sem]),
                pltpu.make_async_copy(buf.at[1, pl.ds(0, spare)], out.at[pl.ds(qrows, spare)], lsem.at[sem + 1])]

    def closing_step(r, carry):
        @pl.when(r == 1)
        def _():
            arrived_tiles(4)

        @pl.when(r == 2)
        def _():
            for j in range(n - lag, n):
                serve_near(j)

        @pl.when(r == 4)
        def _():
            pl.semaphore_wait(free_par, 1)
            for j in range(n - 2 * lag):
                serve_far(j)
            arrived_tiles(5)

        @pl.when(r == 5)
        def _():
            arrived_tiles(6)

        @pl.when(r == near)
        def _():
            serve_near_kv()

        @pl.when(r == near + 1)
        def _():
            arrived_kv(4)

        @pl.when(r == near + 4)
        def _():
            arrived_kv(5)
            arrived_kv(6)

        @pl.when(r == 2 * near)
        def _():
            for a in range(2):
                for t in range(n - 1):
                    x_direct(a, t).wait_send()
                for t in range(2):
                    x_second(a, t).wait_send()
            for t in range(n - 1):
                seg_copy(t).wait_send()
            for j in range(n):
                own_right(0, j).wait_send()
                own_left(0, j).wait_send()
                for slot in range(3):
                    to_partner(slot, 0, j).wait_send()
            for j in range(n - 2 * lag):
                relay_plus(0, j).wait_send()
                relay_minus(0, j).wait_send()
            for j in range(n - 2 * lag, n):
                serve_far(j)

        @pl.when(r == 2 * near + 1)
        def _():
            arrived_tiles(7)

        @pl.when((r < near) | ((r >= 2 * near) & (r < 2 * near + 2)))
        def _():
            order = r - near * (r // (2 * near))
            closing_part(0, order)
            closing_part(1, order)

        @pl.when(r == 2 * near + 2)
        def _():
            for copy in rounded(0, woa, y_ref, 2):
                copy.start()
            serve_far_kv()

        @pl.when(r == 2 * near + 3)
        def _():
            arrived_kv(7)

        @pl.when(((r >= near) & (r < 2 * near)) | (r >= 2 * near + 2))
        def _():
            closing_part(2, r - near - 2 * (r // (2 * near + 2)))
        return carry

    lax.fori_loop(0, 2 * n, closing_step, 0)
    outs = rounded(3, wob, dx_ref, 4)
    for copy in outs:
        copy.start()
    for kind in range(3):
        for order in (n - 2, n - 1):
            for copy in save(kind, order, order % 2):
                copy.wait()
    for copy in [pltpu.make_async_copy(woa.at[0], y_ref.at[pl.ds(0, qrows)], lsem.at[2]),
                 pltpu.make_async_copy(woa.at[1, pl.ds(0, spare)], y_ref.at[pl.ds(qrows, spare)], lsem.at[3])] + outs:
        copy.wait()
    for j in range(n):
        to_partner(3, 0, j).wait_send()
    for j in range(n - 2 * lag, n):
        relay_plus(0, j).wait_send()
        relay_minus(0, j).wait_send()
    for j in range(2):
        for slot in range(4):
            to_partner(slot, 1, j).wait_send()
        own_right(1, j).wait_send()
        own_left(1, j).wait_send()
    relay_plus(1, 0).wait_send()
    relay_minus(1, 1).wait_send()


def attention_layer(n, x_act, dy_act, seg, wq, wk, wv, wo):
    tok, model = x_act.shape
    qrows, krows = wq.shape[0] // n, wk.shape[0] // n
    rows = 2 * qrows + 2 * krows
    total = n * tok
    mcol = model // n
    group = 2
    width = group * tok
    vmem = pl.BlockSpec(memory_space=pltpu.VMEM)
    anym = pl.BlockSpec(memory_space=pl.ANY)
    dma = pltpu.SemaphoreType.DMA
    return pl.pallas_call(
        functools.partial(main_kernel, (n, qrows, krows, tok, krows ** -0.5)),
        out_shape=(jax.ShapeDtypeStruct((tok, model), BF), jax.ShapeDtypeStruct((tok, model), BF),
                   jax.ShapeDtypeStruct((wq.shape[0], mcol), F32), jax.ShapeDtypeStruct((wk.shape[0], mcol), F32),
                   jax.ShapeDtypeStruct((wv.shape[0], mcol), F32), jax.ShapeDtypeStruct((wo.shape[0], mcol), F32)),
        in_specs=[anym, anym, vmem, anym, anym, anym, anym],
        out_specs=(anym,) * 6,
        scratch_shapes=[
            pltpu.VMEM((8, tok), jnp.int32), pltpu.VMEM((n, 8, tok), jnp.int32), pltpu.VMEM((n, 8, tok), jnp.int32),
            pltpu.VMEM((total, 2 * krows), BF),
            pltpu.VMEM((2, n, tok, width), F32),
            pltpu.VMEM((2, 2 * krows, width), BF), pltpu.VMEM((2, 2 * krows, width), BF),
            pltpu.VMEM((2, 24, width), F32),
            pltpu.VMEM((krows, width), F32), pltpu.VMEM((krows, width), F32),
            pltpu.VMEM((n, krows, tok), F32), pltpu.VMEM((n, krows, tok), F32),
            pltpu.VMEM((n, n, rows, tok), BF),
            pltpu.VMEM((total, mcol), BF), pltpu.VMEM((total, mcol), BF),
            pltpu.VMEM((2, 2, tok, mcol), BF),
            pltpu.VMEM((2, qrows, model), BF), pltpu.VMEM((2, qrows, model), BF), pltpu.VMEM((2, 2 * krows, model), BF),
            dma((4, 2)), dma((4, 2)),
            dma((2, 2, n)), dma((2, 2, n)), dma((4, 2, n)), dma((8, 2, n)),
            dma((2, n)), dma((2, n)), dma((2, 2)), dma((2, 2)), dma((6,)), dma((2, n)),
            dma((n,)), dma((n,)), dma((2,)), dma((2,)), dma((n,)), dma((n,)),
            pltpu.SemaphoreType.REGULAR, pltpu.SemaphoreType.REGULAR, pltpu.SemaphoreType.REGULAR,
        ],
        compiler_params=pltpu.CompilerParams(collective_id=0, has_side_effects=True, vmem_limit_bytes=VMEM_MAX),
        name='attention_layer',
    )(x_act, dy_act, seg, wq, wk, wv, wo)


def copy_out(arrays):
    pieces = 4
    count = len(arrays)

    def kernel(*refs):
        src, dst, buf = refs[:count], refs[count:2 * count], refs[2 * count:3 * count]
        insem, outsem = refs[3 * count:]
        loads, stores = [], []
        for k, array in enumerate(arrays):
            size = array.shape[0] // pieces
            for p in range(pieces):
                rows = pl.ds(p * size, size)
                loads.append(pltpu.make_async_copy(src[k].at[rows], buf[k].at[rows], insem.at[k, p]))
                stores.append(pltpu.make_async_copy(buf[k].at[rows], dst[k].at[rows], outsem.at[k, p]))
        for copy in loads:
            copy.start()
        for copy, store in zip(loads, stores):
            copy.wait()
            store.start()
        for store in stores:
            store.wait()

    anym = pl.BlockSpec(memory_space=pl.ANY)
    return pl.pallas_call(
        kernel,
        out_shape=tuple(jax.ShapeDtypeStruct(a.shape, a.dtype) for a in arrays),
        in_specs=[anym] * count, out_specs=(anym,) * count,
        scratch_shapes=[pltpu.VMEM(a.shape, a.dtype) for a in arrays]
        + [pltpu.SemaphoreType.DMA((count, pieces)), pltpu.SemaphoreType.DMA((count, pieces))],
        compiler_params=pltpu.CompilerParams(vmem_limit_bytes=VMEM_MAX),
        name='copy_out',
    )(*arrays)


def solution(mesh):
    n = mesh.shape['cp']
    row_spec = P(('dp', 'cp'), None)
    tok_spec = P(('dp', 'cp'))
    weight_spec = P(None, None, None)
    grad_spec = P(('dp', 'cp'), None, None)

    def local_step(x_act, seg_ids, w_q, w_k, w_v, w_o, dy_act):
        model, q_heads, head_dim = w_q.shape
        kv_heads = w_k.shape[1]
        assert kv_heads == n and x_act.shape[0] % LANES == 0

        def flat(w):
            return w.transpose(1, 2, 0).reshape(w.shape[1] * head_dim, model)

        def unflat(g, heads):
            return g.reshape(heads, head_dim, g.shape[1]).transpose(2, 0, 1)

        wq, wk, wv, wo = flat(w_q), flat(w_k), flat(w_v), flat(w_o)
        y_out, dx_out, dwq, dwk, dwv, dwo = copy_out(attention_layer(n, x_act, dy_act, seg_ids, wq, wk, wv, wo))
        return (y_out, dx_out, unflat(dwq, q_heads), unflat(dwk, kv_heads), unflat(dwv, kv_heads), unflat(dwo, q_heads))

    return jax.shard_map(local_step, mesh=mesh,
                         in_specs=(row_spec, tok_spec, weight_spec, weight_spec, weight_spec, weight_spec, row_spec),
                         out_specs=(row_spec, row_spec, grad_spec, grad_spec, grad_spec, grad_spec),
                         check_vma=False)
```

```python
import functools

import jax
import jax.numpy as jnp
from jax import lax
from jax.experimental import pallas as pl
from jax.experimental.pallas import tpu as pltpu
from jax.sharding import PartitionSpec as P

BF = jnp.bfloat16
F32 = jnp.float32
LANES = 128
LOG2E = 1.4426950408889634
VMEM_MAX = 67043328


def rdma(src, dst, send_sem, recv_sem, peer):
    return pltpu.make_async_remote_copy(src_ref=src, dst_ref=dst, send_sem=send_sem, recv_sem=recv_sem,
                                        device_id={'cp': peer}, device_id_type=pl.DeviceIdType.MESH)


def dot_nt(left, right):
    return lax.dot_general(left, right, (((1,), (1,)), ((), ())), preferred_element_type=F32)


def dot_tn(left, right):
    return lax.dot_general(left, right, (((0,), (0,)), ((), ())), preferred_element_type=F32)


def dot_nn(left, right):
    return lax.dot_general(left, right, (((1,), (0,)), ((), ())), preferred_element_type=F32)


def pick(index, values):
    out = values[0]
    for k in range(1, len(values)):
        out = jnp.where(index == k, values[k], out)
    return out


def main_kernel(dims, x_ref, dy_ref, seg_ref, wq_ref, wk_ref, wv_ref, wo_ref,
                y_ref, dx_ref, dwq_ref, dwk_ref, dwv_ref, dwo_ref,
                seg_mine, seg_all, first_ref, kvn, pbuf, rhsq, rhsd, stats, oacc, dqacc, dkacc, dvacc,
                xall, qkv, gath, back, dyc, dyrel, dqrel, kvrel, frel, fpart, woa, wob,
                wsem, lsem, dyload, xsend, xrecv, xrelay, xpar, psend, precv, pfirst, psecond, gsend, grecv,
                ysend, yrecv, yfirst, ysecond, osem, relsem, parsem, rsem, dqsend, dqrecv, dqfirst, dqsecond,
                kvsend, kvrecv, kvfirst, kvsecond, fsend, frecv, ffirst, fsecond, outsem, free_far, free_par):
    n, qrows, krows, tok, scale = dims
    chips = n // 2
    heads = qrows // krows
    me = lax.axis_index('cp')
    chip, core = me // 2, me % 2
    sgn = 1 - 2 * core
    rows = 2 * qrows + 2 * krows
    width = rhsq.shape[2]
    group = width // tok
    pairs = heads // group
    prow = group * krows
    model = x_ref.shape[1]
    mcol = dyc.shape[1]
    half = tok // 2
    do0, kv0 = qrows, 2 * qrows
    remote = range(n - 1)

    def device(chip_off, flip):
        return ((chip + chip_off + chips) % chips) * 2 + (core + flip) % 2

    right, left, partner = device(1, 0), device(-1, 0), device(0, 1)
    dests = [device(2, 0), device(2, 1), device(-sgn, 0), device(-sgn, 1), device(sgn, 0), device(sgn, 1), partner]
    ahead = dests[4]
    relay_from = device(-sgn, 0)

    barrier = pltpu.get_barrier_semaphore()
    for peer in dests:
        pl.semaphore_signal(barrier, inc=1, device_id={'cp': peer}, device_id_type=pl.DeviceIdType.MESH)

    slot_table = (0, 4, 1, 2, 5, 6, 3, 7)
    off_table = (0, 0, chips - 1, 1, chips - 1, 1, 2, 2)
    flip_table = (0, 1, 0, 0, 1, 1, 0, 1)

    def source_of(order):
        return ((chip + pick(order, off_table)) % chips) * 2 + (core + pick(order, flip_table)) % 2

    def xhalf(ref, h):
        return ref.at[pl.ds(h * half, half)]

    def x_right(h):
        return rdma(xhalf(x_ref, h), xhalf(xall.at[me], h), xsend.at[0, h], xrecv.at[1, h], right)

    def x_left(h):
        return rdma(xhalf(x_ref, h), xhalf(xall.at[me], h), xsend.at[1, h], xrecv.at[2, h], left)

    def x_relay(h):
        tile, peer = (left, right) if h == 0 else (right, left)
        part = xhalf(xall.at[tile], h)
        return rdma(part, part, xrelay.at[h], xrecv.at[3, h], peer)

    def x_partner(slot):
        tile = (me, left, right, dests[0])[slot]
        src = x_ref if slot == 0 else xall.at[tile]
        return rdma(src, xall.at[tile], xpar.at[slot], xrecv.at[4 + slot, 0], partner)

    def do_tile(src):
        return qkv.at[src, pl.ds(do0, qrows)]

    def p_first(t):
        return rdma(gath.at[2, t], gath.at[6, t], psend.at[t], pfirst.at[t], ahead)

    def p_second(t):
        return rdma(gath.at[6, t], do_tile(relay_from), psecond.at[t], precv.at[relay_from], device(sgn, t))

    def p_direct(t):
        return rdma(gath.at[2, t], do_tile(me), psend.at[t], precv.at[me], dests[t])

    def do_arrived(src):
        rdma(gath.at[2, 0], do_tile(src), psend.at[0], precv.at[src], partner).wait_recv()

    def seg_copy(t):
        row = pl.ds(0, 1)
        return rdma(seg_mine.at[row], seg_all.at[me, row], gsend.at[t], grecv.at[t], dests[t])

    def columns(dst):
        return dy_ref.at[:, pl.ds(pl.multiple_of(dst * mcol, LANES), mcol)]

    def token_rows(src):
        return dyc.at[pl.ds(pl.multiple_of(src * tok, LANES), tok)]

    def y_first(t):
        return rdma(columns(dests[t]), dyrel.at[t], ysend.at[t], yfirst.at[t], ahead)

    def y_second(t):
        return rdma(dyrel.at[t], token_rows(relay_from), ysecond.at[t], yrecv.at[t], device(sgn, t))

    def y_direct(t):
        return rdma(columns(dests[t]), token_rows(me), ysend.at[t], yrecv.at[t], dests[t])

    def o_rows(pair, lo, size):
        return pl.ds(pl.multiple_of(pair * prow + lo, krows), size)

    def own_o(pair, j):
        return qkv.at[j, o_rows(pair, 0, prow)]

    def far_o(slot, pair, j, lo=0, size=None):
        return gath.at[slot - 1, j, o_rows(pair, lo, prow if size is None else size)]

    def own_right(pair, j):
        return rdma(own_o(pair, j), far_o(1, pair, j), osem.at[0, pair, j], rsem.at[1, pair, j], right)

    def own_left(pair, j):
        return rdma(own_o(pair, j), far_o(2, pair, j), osem.at[1, pair, j], rsem.at[2, pair, j], left)

    def relay_plus(pair, j):
        return rdma(far_o(1, pair, j, 0, krows), far_o(3, pair, j, 0, krows), relsem.at[0, pair, j], rsem.at[3, pair, j], right)

    def relay_minus(pair, j):
        return rdma(far_o(2, pair, j, krows, krows), far_o(3, pair, j, krows, krows), relsem.at[1, pair, j], rsem.at[0, pair, j], left)

    def to_partner(slot, pair, j):
        src = own_o(pair, j) if slot == 0 else far_o(slot, pair, j)
        return rdma(src, far_o(4 + slot, pair, j), parsem.at[slot, pair, j], rsem.at[4 + slot, pair, j], partner)

    def serve_near(pair, j):
        own_right(pair, j).wait_recv()
        relay_plus(pair, j).start()
        to_partner(1, pair, j).start()
        own_left(pair, j).wait_recv()
        relay_minus(pair, j).start()
        to_partner(2, pair, j).start()

    def serve_far(pair, j):
        relay_plus(pair, j).wait_recv()
        relay_minus(pair, j).wait_recv()
        to_partner(3, pair, j).start()

    def arrived(slot):
        for pair in range(pairs):
            for j in range(n):
                to_partner(slot - 4, pair, j).wait_recv()

    def dq_rows(pair):
        return pl.ds(pl.multiple_of(pair * prow, prow), prow)

    def dq_own(pair, j):
        return qkv.at[j, pl.ds(pl.multiple_of(do0 + pair * prow, prow), prow)]

    def dq_direct(pair, j):
        return rdma(dq_own(pair, j), back.at[me, dq_rows(pair)], dqsend.at[pair, j], dqrecv.at[pair, me], j)

    def dq_first(pair, j):
        return rdma(dq_own(pair, j), dqrel.at[pair, j % 2], dqsend.at[pair, j], dqfirst.at[pair, j % 2], ahead)

    def dq_second(pair, j):
        return rdma(dqrel.at[pair, j % 2], back.at[relay_from, dq_rows(pair)], dqsecond.at[pair, j % 2],
                    dqrecv.at[pair, relay_from], j)

    def send_dq(pair, j):
        owner_far = j // 2 == (chip + 2) % chips

        @pl.when(j == me)
        def _():
            back[me, dq_rows(pair)] = qkv[j, pl.ds(pl.multiple_of(do0 + pair * prow, prow), prow)]

        @pl.when(owner_far)
        def _():
            dq_first(pair, j).start()

        @pl.when((j != me) & jnp.logical_not(owner_far))
        def _():
            dq_direct(pair, j).start()

    def serve_dq(pair, j):
        @pl.when(j // 2 == (chip + sgn + chips) % chips)
        def _():
            dq_first(pair, j).wait_recv()
            dq_second(pair, j).start()

    def kv_own(src):
        return qkv.at[src, pl.ds(kv0, 2 * krows)]

    def kv_place(src):
        return back.at[src, pl.ds(qrows, 2 * krows)]

    def kv_first(t):
        return rdma(kv_own(dests[t]), kvrel.at[t], kvsend.at[t], kvfirst.at[t], ahead)

    def kv_second(t):
        return rdma(kvrel.at[t], kv_place(relay_from), kvsecond.at[t], kvrecv.at[t], device(sgn, t))

    def kv_direct(t):
        return rdma(kv_own(dests[t]), kv_place(me), kvsend.at[t], kvrecv.at[t], dests[t])

    def grad_places(part, owner):
        if part < pairs:
            return [(pl.ds(0, prow), dwq_ref.at[pl.ds(owner * qrows + part * prow, prow)], 0)]
        return [(pl.ds(0, krows), dwk_ref.at[pl.ds(owner * krows, krows)], 0),
                (pl.ds(krows, krows), dwv_ref.at[pl.ds(owner * krows, krows)], 1)]

    def block_ref(part, t):
        if part == 0:
            return fpart.at[t]
        return pbuf.at[1, 4 * (part - 1) + t // 3, pl.ds(0, prow), pl.ds(pl.multiple_of((t % 3) * mcol, LANES), mcol)]

    def f_first(part, t):
        return rdma(block_ref(part, t), frel.at[part, t], fsend.at[part, t, 0], ffirst.at[part, t], ahead)

    def f_second(part, t):
        return [rdma(frel.at[part, t, span], place, fsecond.at[part, t, k], frecv.at[part, t, k], device(sgn, t))
                for span, place, k in grad_places(part, relay_from)]

    def f_direct(part, t):
        return [rdma(block_ref(part, t).at[span], place, fsend.at[part, t, k], frecv.at[part, t, k], dests[t])
                for span, place, k in grad_places(part, me)]

    def f_own(part):
        return [pltpu.make_async_copy(block_ref(part, n - 1).at[span], place, outsem.at[part, k])
                for span, place, k in grad_places(part, me)]

    dest_off = (2, 2, -1, -1, 1, 1, 0, 0)
    dest_flip = (0, 1, 0, 1, 0, 1, 1, 0)

    def dest_of(t):
        return ((chip + sgn * pick(t, dest_off) + chips) % chips) * 2 + (core + pick(t, dest_flip)) % 2

    def weight_grads(part):
        lo = do0 + part * prow if part < pairs else kv0

        def block_step(t, carry):
            cols = pl.ds(pl.multiple_of(dest_of(t) * mcol, LANES), mcol)
            wide = jnp.concatenate([qkv[j, lo:lo + prow, :] for j in range(n)], axis=1)
            block_ref(part, t)[...] = dot_nn(wide, xall[:, :, cols].reshape(n * tok, mcol))
            for k in remote:
                @pl.when(t == k)
                def _():
                    for copy in [f_first(part, k)] if k < 2 else f_direct(part, k):
                        copy.start()

            @pl.when(t == n - 1)
            def _():
                for copy in f_own(part):
                    copy.start()
            return carry

        lax.fori_loop(0, n, block_step, 0)

    def relay_grads(part):
        for t in range(2):
            f_first(part, t).wait_recv()
            for copy in f_second(part, t):
                copy.start()

    def load(kind, order, buf):
        src = source_of(order)
        if kind == 0:
            return [pltpu.make_async_copy(wo_ref.at[pl.ds(src * qrows, qrows)], woa.at[buf], wsem.at[0, buf])]
        return [pltpu.make_async_copy(wq_ref.at[pl.ds(src * qrows, qrows)], wob.at[buf, pl.ds(0, qrows)], wsem.at[1, buf]),
                pltpu.make_async_copy(wk_ref.at[pl.ds(src * krows, krows)], wob.at[buf, pl.ds(qrows, krows)], wsem.at[2, buf]),
                pltpu.make_async_copy(wv_ref.at[pl.ds(src * krows, krows)], wob.at[buf, pl.ds(qrows + krows, krows)], wsem.at[3, buf])]

    parts = [(j, slice(j * width, min((j + 1) * width, model))) for j in range(-(-model // width))]

    def stage(buf):
        return pbuf.at[0, 6, pl.ds(0, qrows), pl.ds(pl.multiple_of(buf * mcol, LANES), mcol)]

    def save(order, buf):
        return pltpu.make_async_copy(stage(buf), dwo_ref.at[pl.ds(source_of(order) * qrows, qrows)], wsem.at[4, buf])

    def next_weights(kind, order):
        buf = order % 2
        for copy in load(kind, order, buf):
            copy.wait()

        @pl.when(order < n - 1)
        def _():
            for copy in load(kind, order + 1, 1 - buf):
                copy.start()

        return buf

    def close_o(order, own):
        buf = next_weights(0, order)
        slot = pick(order, slot_table)

        def tile_o(j):
            return qkv[j, 0:qrows, :] if own else gath[slot - 1, j]

        @pl.when(order >= 2)
        def _():
            save(order - 2, buf).wait()

        @pl.when(order >= 0)
        def _():
            stage(buf)[...] = dot_nn(jnp.concatenate([tile_o(j) for j in range(n)], axis=1), dyc[...])

        save(order, buf).start()
        for j, cols in parts:
            @pl.when(order >= 0)
            def _():
                pbuf[0, j, :, 0:cols.stop - cols.start] += dot_tn(tile_o(me), woa[buf, :, cols])

    def close_dx(order):
        buf = next_weights(1, order)
        for j, cols in parts:
            @pl.when(order >= 0)
            def _():
                pbuf[0, 3 + j, :, 0:cols.stop - cols.start] += dot_tn(back[source_of(order)], wob[buf, :, cols])

    def do_weights(t, buf):
        return pltpu.make_async_copy(wo_ref.at[pl.ds(dest_of(t) * qrows, qrows)], woa.at[buf], wsem.at[0, buf])

    dy_cols = [(c, c * tok, min(tok, model - c * tok)) for c in range(-(-model // tok))]
    dy_in = [pltpu.make_async_copy(dy_ref.at[:, pl.ds(lo, size)], back.at[c, :, pl.ds(0, size)], dyload.at[c])
             for c, lo, size in dy_cols]
    x_in = pltpu.make_async_copy(x_ref, xall.at[me], lsem.at[1])
    y_own = pltpu.make_async_copy(columns(me), token_rows(me), lsem.at[2])
    own_weights = [pltpu.make_async_copy(wq_ref.at[pl.ds(me * qrows, qrows)], wob.at[0, pl.ds(0, qrows)], lsem.at[3]),
                   pltpu.make_async_copy(wk_ref.at[pl.ds(me * krows, krows)], wob.at[0, pl.ds(qrows, krows)], lsem.at[4]),
                   pltpu.make_async_copy(wv_ref.at[pl.ds(me * krows, krows)], wob.at[0, pl.ds(qrows + krows, krows)], lsem.at[5])]
    for copy in dy_in:
        copy.start()
    do_weights(0, 0).start()
    for copy in [x_in, y_own] + own_weights:
        copy.start()
    seg_mine[...] = jnp.broadcast_to(seg_ref[...].reshape(1, tok), seg_mine.shape)
    pl.semaphore_wait(barrier, n - 1)
    for h in range(2):
        x_right(h).start()
        x_left(1 - h).start()
    x_partner(0).start()
    for t in remote:
        seg_copy(t).start()
    seg_all[me] = seg_mine[...]
    for copy in dy_in:
        copy.wait()

    def do_step(t, carry):
        buf = t % 2

        @pl.when(t < n - 1)
        def _():
            do_weights(t + 1, 1 - buf).start()

        do_weights(t, buf).wait()
        local = jnp.concatenate([back[c, :, 0:size] for c, lo, size in dy_cols], axis=1)
        block = dot_nt(woa[buf], local).astype(BF)

        @pl.when(t < n - 1)
        def _():
            gath[2, t] = block

        @pl.when(t == n - 1)
        def _():
            qkv[me, do0:kv0] = block
        return carry

    lax.fori_loop(0, n, do_step, 0)
    dkacc[...] = jnp.zeros_like(dkacc)
    dvacc[...] = jnp.zeros_like(dvacc)
    rhsq[...] = jnp.zeros_like(rhsq)
    rhsd[...] = jnp.zeros_like(rhsd)
    for copy in [x_in] + own_weights:
        copy.wait()

    def project_step(order, carry):
        @pl.when(order == 1)
        def _():
            x_partner(0).wait_recv()

        @pl.when(order == 2)
        def _():
            x_right(0).wait_recv()
            x_relay(0).start()
            x_left(1).wait_recv()
            x_relay(1).start()
            for t in remote:
                (p_first if t < 2 else p_direct)(t).start()
            x_right(1).wait_recv()
            x_partner(1).start()

        @pl.when(order == 3)
        def _():
            x_left(0).wait_recv()
            x_partner(2).start()

        @pl.when(order == 4)
        def _():
            x_partner(1).wait_recv()

        @pl.when(order == 5)
        def _():
            x_partner(2).wait_recv()

        @pl.when(order == 6)
        def _():
            for h in range(2):
                x_relay(h).wait_recv()
            x_partner(3).start()
            for t in range(2):
                p_first(t).wait_recv()
                p_second(t).start()

        @pl.when(order == 7)
        def _():
            x_partner(3).wait_recv()

        src = source_of(order)
        qkv[src, 0:qrows] = dot_nt(wob[0, 0:qrows], xall[src]).astype(BF)
        kv = dot_nt(wob[0, qrows:qrows + 2 * krows], xall[src]).astype(BF)
        qkv[src, kv0:rows] = kv
        kvn[pl.ds(pl.multiple_of(src * tok, LANES), tok), :] = kv.T
        return carry

    lax.fori_loop(0, n, project_step, 0)
    for t in remote:
        (y_first if t < 2 else y_direct)(t).start()

    for t in remote:
        seg_copy(t).wait_recv()
    row_id = lax.broadcasted_iota(jnp.int32, (n, tok), 0)
    lane_id = lax.broadcasted_iota(jnp.int32, (n, tok), 1)
    seg = jnp.zeros((n, tok), jnp.int32)
    for d in range(n):
        seg = jnp.where(row_id == d, seg_all[d, 0:1], seg)
    before = jnp.where(lane_id == 0, pltpu.roll(pltpu.roll(seg, 1, 1), 1, 0), pltpu.roll(seg, 1, 1))
    pos = row_id * tok + lane_id
    best = jnp.where((seg != before) & (pos > 0), pos, 0)
    shift = 1
    while shift < tok:
        best = jnp.maximum(best, jnp.where(lane_id >= shift, pltpu.roll(best, shift, 1), 0))
        shift *= 2
    end = jnp.broadcast_to(best[:, tok - 1:tok], (n, tok))
    carry_max = jnp.where(row_id >= 1, pltpu.roll(end, 1, 0), 0)
    shift = 1
    while shift < n:
        carry_max = jnp.maximum(carry_max, jnp.where(row_id >= shift, pltpu.roll(carry_max, shift, 0), 0))
        shift *= 2
    best = jnp.maximum(best, carry_max)
    for d in range(n):
        first_ref[d] = jnp.broadcast_to(best[d:d + 1], (8, tok))

    score_mul = scale * LOG2E
    grp = tok // 8
    lag = 2

    def keys(c):
        return kvn[pl.ds(pl.multiple_of(c * tok, LANES), tok), :]

    def q_rows(pair, g):
        return pl.ds(pl.multiple_of((pair * group + g) * krows, krows), krows)

    def do_rows(pair, g):
        return pl.ds(pl.multiple_of(do0 + (pair * group + g) * krows, krows), krows)

    def doc_starts(i):
        return jnp.concatenate([first_ref[i][0:1]] * group, axis=1)

    def score(i, par, c, top, diagonal):
        t = dot_nn(keys(c), rhsq[par]) * score_mul
        kpos = lax.broadcasted_iota(jnp.int32, (tok, width), 0)
        keep = kpos >= doc_starts(i) - c * tok
        if diagonal:
            qpos = lax.broadcasted_iota(jnp.int32, (1, tok), 1)
            keep = keep & (kpos <= jnp.concatenate([qpos] * group, axis=1))
        t = jnp.where(keep, t, -jnp.inf)
        pbuf[par, c] = t
        return jnp.maximum(top, jnp.max(t.reshape(grp, 8, width), axis=0))

    def value(par, c, top, total):
        p = jnp.exp2(pbuf[par, c] - top)
        oacc[...] += dot_nn(qkv[c, kv0 + krows:rows, :], p.astype(BF))
        return total + jnp.sum(p.reshape(grp, 8, width), axis=0)

    def grad(par, c):
        p = jnp.exp2(pbuf[par, c] - stats[par, 0:1])
        dp = dot_nn(keys(c), rhsd[par])
        ds = (p * (dp - stats[par, 8:9])).astype(BF)
        dqacc[...] += dot_nn(qkv[c, kv0:kv0 + krows, :], ds)
        pb = p.astype(BF)
        spans = [(slice(j * mcol, (j + 1) * mcol), slice(j * tok, (j + 1) * tok)) for j in range(width // mcol)]
        for qs, place in spans:
            woa[0, :, place] = ds[:, qs].T
            wob[0, 0:mcol, place] = pb[:, qs].T
        dkacc[c] += sum(dot_nn(rhsq[par, 0:krows, qs], woa[0, :, place]) for qs, place in spans)
        dvacc[c] += sum(dot_nn(rhsd[par, krows:2 * krows, qs], wob[0, 0:mcol, place]) for qs, place in spans)

    def tile_done(pair, j):
        dq = (dqacc[...] * scale).astype(BF)
        for g in range(group):
            qkv[j, do_rows(pair, g), :] = dq[:, g * tok:(g + 1) * tok]
        piece = pair * n + j

        @pl.when(piece == 0)
        def _():
            for t in remote:
                p_direct(t).wait_send()
            for t in range(2):
                p_second(t).wait_send()
            for peer in (right, left):
                pl.semaphore_signal(free_far, inc=1, device_id={'cp': peer}, device_id_type=pl.DeviceIdType.MESH)
            pl.semaphore_signal(free_par, inc=1, device_id={'cp': partner}, device_id_type=pl.DeviceIdType.MESH)

        own_right(pair, j).start()
        own_left(pair, j).start()
        to_partner(0, pair, j).start()
        send_dq(pair, j)

        @pl.when(piece == 1)
        def _():
            for t in range(2):
                y_first(t).wait_recv()
                y_second(t).start()

        @pl.when(piece == lag)
        def _():
            pl.semaphore_wait(free_far, 2)

        @pl.when(piece == n + 1)
        def _():
            relay_grads(0)

        @pl.when(piece >= lag)
        def _():
            old = piece - lag
            serve_near(old // n, old % n)
            serve_dq(old // n, old % n)

    def item_step(m, carry):
        pair, i = m // n, m % n
        par = i % 2
        last = 1 - par

        @pl.when((pair == 0) & (i != me))
        def _():
            do_arrived(i)

        for g in range(group):
            lanes = slice(g * tok, (g + 1) * tok)
            rhsq[par, 0:krows, lanes] = qkv[i, q_rows(pair, g), :]
            rhsd[par, krows:2 * krows, lanes] = qkv[i, do_rows(pair, g), :]
        dqacc[...] = jnp.zeros_like(dqacc)

        def both_step(c, top):
            grad(last, c)
            return score(i, par, c, top, False)

        top = lax.fori_loop(0, i, both_step, jnp.full((8, width), -jnp.inf, F32))
        top = score(i, par, i, top, True)

        @pl.when(i >= 1)
        def _():
            tile_done(pair, i - 1)

        top = jnp.max(top, axis=0, keepdims=True)
        oacc[...] = jnp.zeros_like(oacc)
        total = lax.fori_loop(0, i + 1, lambda c, acc: value(par, c, top, acc), jnp.zeros((8, width), F32))
        total = jnp.sum(total, axis=0, keepdims=True)
        o_blk = (oacc[...] * (1.0 / total)).astype(BF)
        stats[par, 0:8] = jnp.broadcast_to(top + jnp.log2(total), (8, width))
        delta = jnp.sum(rhsd[par, krows:2 * krows].astype(F32) * o_blk.astype(F32), axis=0, keepdims=True)
        stats[par, 8:16] = jnp.broadcast_to(delta, (8, width))
        for g in range(group):
            qkv[i, q_rows(pair, g), :] = o_blk[:, g * tok:(g + 1) * tok]

        @pl.when(i == n - 1)
        def _():
            dqacc[...] = jnp.zeros_like(dqacc)

            def last_step(c, inner):
                grad(par, c)
                return inner

            lax.fori_loop(0, n, last_step, 0)
            tile_done(pair, i)

        @pl.when(m == n - 1)
        def _():
            weight_grads(0)
        return carry

    lax.fori_loop(0, n * pairs, item_step, 0)

    for c in range(n):
        qkv[c, kv0:kv0 + krows, :] = (dkacc[c] * scale).astype(BF)
        qkv[c, kv0 + krows:rows, :] = dvacc[c].astype(BF)
    for t in remote:
        (kv_first if t < 2 else kv_direct)(t).start()
    back[me, qrows:qrows + 2 * krows] = qkv[me, kv0:rows]
    for kind in range(2):
        for copy in load(kind, 0, 0):
            copy.start()
    for part in range(1, pairs + 1):
        weight_grads(part)
    for old in range(n * pairs - lag, n * pairs):
        serve_near(old // n, old % n)
        serve_dq(old // n, old % n)
    for t in range(2):
        kv_first(t).wait_recv()
        kv_second(t).start()
    pbuf[0, 0:6] = jnp.zeros((6, tok, width), F32)
    y_own.wait()
    for t in remote:
        y_direct(t).wait_recv()

    def closing_step(r, carry):
        @pl.when(r == 1)
        def _():
            arrived(4)
            relay_grads(1)

        @pl.when(r == 2)
        def _():
            relay_grads(2)

        @pl.when(r == 4)
        def _():
            pl.semaphore_wait(free_par, 1)
            for pair in range(pairs):
                for j in range(n):
                    serve_far(pair, j)
            arrived(5)

        @pl.when(r == 5)
        def _():
            arrived(6)

        @pl.when(r == 7)
        def _():
            arrived(7)

        @pl.when(r == 0)
        def _():
            close_o(r, True)

        @pl.when((r >= 1) & (r < n))
        def _():
            close_o(r, False)

        @pl.when(r == n)
        def _():
            for t in remote:
                for pair in range(pairs):
                    rdma(dqrel.at[pair, 0], back.at[dests[t], dq_rows(pair)], dqsend.at[pair, 0],
                         dqrecv.at[pair, dests[t]], partner).wait_recv()
                kv_direct(t).wait_recv()

        @pl.when(r >= n)
        def _():
            close_dx(r - n)
        return carry

    lax.fori_loop(0, 2 * n, closing_step, 0)

    spare = tok - qrows

    def rounded(acc, buf, out, sem):
        for j, cols in parts:
            wide = pbuf[0, acc + j, :, 0:cols.stop - cols.start].astype(BF)
            buf[0, 0:qrows, cols] = wide[0:qrows]
            buf[1, 0:spare, cols] = wide[qrows:tok]
        return [pltpu.make_async_copy(buf.at[0, pl.ds(0, qrows)], out.at[pl.ds(0, qrows)], lsem.at[sem]),
                pltpu.make_async_copy(buf.at[1, pl.ds(0, spare)], out.at[pl.ds(qrows, spare)], lsem.at[sem + 1])]

    outs = rounded(0, woa, y_ref, 0) + rounded(3, wob, dx_ref, 2)
    for copy in outs:
        copy.start()

    for t in remote:
        seg_copy(t).wait_send()
        y_direct(t).wait_send()
        kv_direct(t).wait_send()
        for pair in range(pairs):
            rdma(dq_own(pair, 0), dqrel.at[pair, 0], dqsend.at[pair, dests[t]], dqfirst.at[pair, 0], partner).wait_send()
    for h in range(2):
        x_right(h).wait_send()
        x_left(h).wait_send()
        x_relay(h).wait_send()
    for slot in range(4):
        x_partner(slot).wait_send()
    for t in range(2):
        y_second(t).wait_send()
        kv_second(t).wait_send()
        for pair in range(pairs):
            dq_second(pair, t).wait_send()
    for pair in range(pairs):
        for j in range(n):
            own_right(pair, j).wait_send()
            own_left(pair, j).wait_send()
            relay_plus(pair, j).wait_send()
            relay_minus(pair, j).wait_send()
            for slot in range(4):
                to_partner(slot, pair, j).wait_send()
    for order in (n - 2, n - 1):
        save(order, order % 2).wait()
    for copy in outs:
        copy.wait()
    for part in range(pairs + 1):
        for copy in f_own(part):
            copy.wait()
        for t in remote:
            for copy in f_direct(part, t):
                copy.wait_recv()
        for t in range(2, n - 1):
            for copy in f_direct(part, t):
                copy.wait_send()
        for t in range(2):
            f_first(part, t).wait_send()
            for copy in f_second(part, t):
                copy.wait_send()


def attention_layer(n, x_act, dy_act, seg, wq, wk, wv, wo):
    tok, model = x_act.shape
    qrows, krows = wq.shape[0] // n, wk.shape[0] // n
    rows = 2 * qrows + 2 * krows
    total = n * tok
    mcol = model // n
    group = 2
    width = group * tok
    pairs = qrows // krows // group
    prow = group * krows
    vmem = pl.BlockSpec(memory_space=pltpu.VMEM)
    anym = pl.BlockSpec(memory_space=pl.ANY)
    dma = pltpu.SemaphoreType.DMA
    return pl.pallas_call(
        functools.partial(main_kernel, (n, qrows, krows, tok, krows ** -0.5)),
        out_shape=(jax.ShapeDtypeStruct((tok, model), BF), jax.ShapeDtypeStruct((tok, model), BF),
                   jax.ShapeDtypeStruct((wq.shape[0], mcol), F32), jax.ShapeDtypeStruct((wk.shape[0], mcol), F32),
                   jax.ShapeDtypeStruct((wv.shape[0], mcol), F32), jax.ShapeDtypeStruct((wo.shape[0], mcol), F32)),
        in_specs=[anym, anym, vmem, anym, anym, anym, anym],
        out_specs=(anym,) * 6,
        scratch_shapes=[
            pltpu.VMEM((8, tok), jnp.int32), pltpu.VMEM((n, 8, tok), jnp.int32), pltpu.VMEM((n, 8, tok), jnp.int32),
            pltpu.VMEM((total, 2 * krows), BF),
            pltpu.VMEM((2, n, tok, width), F32),
            pltpu.VMEM((2, 2 * krows, width), BF), pltpu.VMEM((2, 2 * krows, width), BF),
            pltpu.VMEM((2, 16, width), F32),
            pltpu.VMEM((krows, width), F32), pltpu.VMEM((krows, width), F32),
            pltpu.VMEM((n, krows, tok), F32), pltpu.VMEM((n, krows, tok), F32),
            pltpu.VMEM((n, tok, model), BF),
            pltpu.VMEM((n, rows, tok), BF),
            pltpu.VMEM((n - 1, n, qrows, tok), BF),
            pltpu.VMEM((n, qrows + 2 * krows, tok), BF),
            pltpu.VMEM((total, mcol), BF),
            pltpu.VMEM((2, tok, mcol), BF),
            pltpu.VMEM((pairs, 2, prow, tok), BF),
            pltpu.VMEM((2, 2 * krows, tok), BF),
            pltpu.VMEM((pairs + 1, 2, prow, mcol), F32),
            pltpu.VMEM((n, prow, mcol), F32),
            pltpu.VMEM((2, qrows, model), BF), pltpu.VMEM((2, qrows + 2 * krows, model), BF),
            dma((5, 2)), dma((6,)), dma((n,)),
            dma((2, 2)), dma((8, 2)), dma((2,)), dma((4,)),
            dma((n,)), dma((n,)), dma((2,)), dma((2,)), dma((n,)), dma((n,)),
            dma((n,)), dma((n,)), dma((2,)), dma((2,)),
            dma((2, pairs, n)), dma((2, pairs, n)), dma((4, pairs, n)), dma((8, pairs, n)),
            dma((pairs, n)), dma((pairs, n)), dma((pairs, 2)), dma((pairs, 2)),
            dma((n,)), dma((n,)), dma((2,)), dma((2,)),
            dma((pairs + 1, n, 2)), dma((pairs + 1, n, 2)), dma((pairs + 1, 2)), dma((pairs + 1, 2, 2)), dma((pairs + 1, 2)),
            pltpu.SemaphoreType.REGULAR, pltpu.SemaphoreType.REGULAR,
        ],
        compiler_params=pltpu.CompilerParams(collective_id=0, has_side_effects=True, vmem_limit_bytes=VMEM_MAX),
        name='attention_layer',
    )(x_act, dy_act, seg, wq, wk, wv, wo)


def copy_out(arrays):
    pieces = 4
    count = len(arrays)

    def kernel(*refs):
        src, dst, buf = refs[:count], refs[count:2 * count], refs[2 * count:3 * count]
        insem, outsem = refs[3 * count:]
        loads, stores = [], []
        for k, array in enumerate(arrays):
            size = array.shape[0] // pieces
            for p in range(pieces):
                rows = pl.ds(p * size, size)
                loads.append(pltpu.make_async_copy(src[k].at[rows], buf[k].at[rows], insem.at[k, p]))
                stores.append(pltpu.make_async_copy(buf[k].at[rows], dst[k].at[rows], outsem.at[k, p]))
        for copy in loads:
            copy.start()
        for copy, store in zip(loads, stores):
            copy.wait()
            store.start()
        for store in stores:
            store.wait()

    anym = pl.BlockSpec(memory_space=pl.ANY)
    return pl.pallas_call(
        kernel,
        out_shape=tuple(jax.ShapeDtypeStruct(a.shape, a.dtype) for a in arrays),
        in_specs=[anym] * count, out_specs=(anym,) * count,
        scratch_shapes=[pltpu.VMEM(a.shape, a.dtype) for a in arrays]
        + [pltpu.SemaphoreType.DMA((count, pieces)), pltpu.SemaphoreType.DMA((count, pieces))],
        compiler_params=pltpu.CompilerParams(vmem_limit_bytes=VMEM_MAX),
        name='copy_out',
    )(*arrays)


def solution(mesh):
    n = mesh.shape['cp']
    row_spec = P(('dp', 'cp'), None)
    tok_spec = P(('dp', 'cp'))
    weight_spec = P(None, None, None)
    grad_spec = P(('dp', 'cp'), None, None)

    def local_step(x_act, seg_ids, w_q, w_k, w_v, w_o, dy_act):
        model, q_heads, head_dim = w_q.shape
        kv_heads = w_k.shape[1]
        assert kv_heads == n and x_act.shape[0] % LANES == 0

        def flat(w):
            return w.transpose(1, 2, 0).reshape(w.shape[1] * head_dim, model)

        def unflat(g, heads):
            return g.reshape(heads, head_dim, g.shape[1]).transpose(2, 0, 1)

        wq, wk, wv, wo = flat(w_q), flat(w_k), flat(w_v), flat(w_o)
        y_out, dx_out, dwq, dwk, dwv, dwo = copy_out(attention_layer(n, x_act, dy_act, seg_ids, wq, wk, wv, wo))
        return (y_out, dx_out, unflat(dwq, q_heads), unflat(dwk, kv_heads), unflat(dwv, kv_heads), unflat(dwo, q_heads))

    return jax.shard_map(local_step, mesh=mesh,
                         in_specs=(row_spec, tok_spec, weight_spec, weight_spec, weight_spec, weight_spec, row_spec),
                         out_specs=(row_spec, row_spec, grad_spec, grad_spec, grad_spec, grad_spec),
                         check_vma=False)
```

```python
import functools

import jax
import jax.numpy as jnp
from jax import lax
from jax.experimental import pallas as pl
from jax.experimental.pallas import tpu as pltpu
from jax.sharding import PartitionSpec as P

BF = jnp.bfloat16
F32 = jnp.float32
LANES = 128
LOG2E = 1.4426950408889634
VMEM_MAX = 67043328


def rdma(src, dst, send_sem, recv_sem, peer):
    return pltpu.make_async_remote_copy(src_ref=src, dst_ref=dst, send_sem=send_sem, recv_sem=recv_sem,
                                        device_id={'cp': peer}, device_id_type=pl.DeviceIdType.MESH)


def dot_nt(left, right):
    return lax.dot_general(left, right, (((1,), (1,)), ((), ())), preferred_element_type=F32)


def dot_tn(left, right):
    return lax.dot_general(left, right, (((0,), (0,)), ((), ())), preferred_element_type=F32)


def dot_nn(left, right):
    return lax.dot_general(left, right, (((1,), (0,)), ((), ())), preferred_element_type=F32)


def pick(index, values):
    out = values[0]
    for k in range(1, len(values)):
        out = jnp.where(index == k, values[k], out)
    return out


def main_kernel(dims, x_ref, dy_ref, seg_ref, wq_ref, wk_ref, wv_ref, wo_ref,
                y_ref, dx_ref, dwq_ref, dwk_ref, dwv_ref, dwo_ref,
                seg_mine, seg_all, first_ref, kvn, pbuf, rhsq, rhsd, stats, oacc, dqacc, dkacc, dvacc,
                xall, qkv, gath, back, dyc, dyrel, dqrel, kvrel, frel, fpart, woa, wob,
                wsem, lsem, dyload, xsend, xrecv, xrelay, xpar, psend, precv, pfirst, psecond, gsend, grecv,
                ysend, yrecv, yfirst, ysecond, osem, relsem, parsem, rsem, dqsend, dqrecv, dqfirst, dqsecond,
                kvsend, kvrecv, kvfirst, kvsecond, fsend, frecv, ffirst, fsecond, outsem, free_far, free_par):
    n, qrows, krows, tok, scale = dims
    chips = n // 2
    heads = qrows // krows
    me = lax.axis_index('cp')
    chip, core = me // 2, me % 2
    sgn = 1 - 2 * core
    rows = 2 * qrows + 2 * krows
    width = rhsq.shape[2]
    group = width // tok
    pairs = heads // group
    prow = group * krows
    model = x_ref.shape[1]
    mcol = dyc.shape[1]
    half = tok // 2
    do0, kv0 = qrows, 2 * qrows
    remote = range(n - 1)

    def device(chip_off, flip):
        return ((chip + chip_off + chips) % chips) * 2 + (core + flip) % 2

    right, left, partner = device(1, 0), device(-1, 0), device(0, 1)
    dests = [device(2, 0), device(2, 1), device(-sgn, 0), device(-sgn, 1), device(sgn, 0), device(sgn, 1), partner]
    ahead = dests[4]
    relay_from = device(-sgn, 0)

    barrier = pltpu.get_barrier_semaphore()
    for peer in dests:
        pl.semaphore_signal(barrier, inc=1, device_id={'cp': peer}, device_id_type=pl.DeviceIdType.MESH)

    slot_table = (0, 4, 1, 2, 5, 6, 3, 7)
    off_table = (0, 0, chips - 1, 1, chips - 1, 1, 2, 2)
    flip_table = (0, 1, 0, 0, 1, 1, 0, 1)

    def source_of(order):
        return ((chip + pick(order, off_table)) % chips) * 2 + (core + pick(order, flip_table)) % 2

    def xhalf(ref, h):
        return ref.at[pl.ds(h * half, half)]

    def x_right(h):
        return rdma(xhalf(x_ref, h), xhalf(xall.at[me], h), xsend.at[0, h], xrecv.at[1, h], right)

    def x_left(h):
        return rdma(xhalf(x_ref, h), xhalf(xall.at[me], h), xsend.at[1, h], xrecv.at[2, h], left)

    def x_relay(h):
        tile, peer = (left, right) if h == 0 else (right, left)
        part = xhalf(xall.at[tile], h)
        return rdma(part, part, xrelay.at[h], xrecv.at[3, h], peer)

    def x_partner(slot):
        tile = (me, left, right, dests[0])[slot]
        src = x_ref if slot == 0 else xall.at[tile]
        return rdma(src, xall.at[tile], xpar.at[slot], xrecv.at[4 + slot, 0], partner)

    def do_tile(src):
        return qkv.at[src, pl.ds(do0, qrows)]

    def p_first(t):
        return rdma(gath.at[2, t], gath.at[6, t], psend.at[t], pfirst.at[t], ahead)

    def p_second(t):
        return rdma(gath.at[6, t], do_tile(relay_from), psecond.at[t], precv.at[relay_from], device(sgn, t))

    def p_direct(t):
        return rdma(gath.at[2, t], do_tile(me), psend.at[t], precv.at[me], dests[t])

    def do_arrived(src):
        rdma(gath.at[2, 0], do_tile(src), psend.at[0], precv.at[src], partner).wait_recv()

    def seg_copy(t):
        row = pl.ds(0, 1)
        return rdma(seg_mine.at[row], seg_all.at[me, row], gsend.at[t], grecv.at[t], dests[t])

    def columns(dst):
        return dy_ref.at[:, pl.ds(pl.multiple_of(dst * mcol, LANES), mcol)]

    def token_rows(src):
        return dyc.at[pl.ds(pl.multiple_of(src * tok, LANES), tok)]

    def y_first(t):
        return rdma(columns(dests[t]), dyrel.at[t], ysend.at[t], yfirst.at[t], ahead)

    def y_second(t):
        return rdma(dyrel.at[t], token_rows(relay_from), ysecond.at[t], yrecv.at[t], device(sgn, t))

    def y_direct(t):
        return rdma(columns(dests[t]), token_rows(me), ysend.at[t], yrecv.at[t], dests[t])

    def o_rows(pair, lo, size):
        return pl.ds(pl.multiple_of(pair * prow + lo, krows), size)

    def own_o(pair, j):
        return qkv.at[j, o_rows(pair, 0, prow)]

    def far_o(slot, pair, j, lo=0, size=None):
        return gath.at[slot - 1, j, o_rows(pair, lo, prow if size is None else size)]

    def own_right(pair, j):
        return rdma(own_o(pair, j), far_o(1, pair, j), osem.at[0, pair, j], rsem.at[1, pair, j], right)

    def own_left(pair, j):
        return rdma(own_o(pair, j), far_o(2, pair, j), osem.at[1, pair, j], rsem.at[2, pair, j], left)

    def relay_plus(pair, j):
        return rdma(far_o(1, pair, j, 0, krows), far_o(3, pair, j, 0, krows), relsem.at[0, pair, j], rsem.at[3, pair, j], right)

    def relay_minus(pair, j):
        return rdma(far_o(2, pair, j, krows, krows), far_o(3, pair, j, krows, krows), relsem.at[1, pair, j], rsem.at[0, pair, j], left)

    def to_partner(slot, pair, j):
        src = own_o(pair, j) if slot == 0 else far_o(slot, pair, j)
        return rdma(src, far_o(4 + slot, pair, j), parsem.at[slot, pair, j], rsem.at[4 + slot, pair, j], partner)

    def serve_near(pair, j):
        own_right(pair, j).wait_recv()
        relay_plus(pair, j).start()
        to_partner(1, pair, j).start()
        own_left(pair, j).wait_recv()
        relay_minus(pair, j).start()
        to_partner(2, pair, j).start()

    def serve_far(pair, j):
        relay_plus(pair, j).wait_recv()
        relay_minus(pair, j).wait_recv()
        to_partner(3, pair, j).start()

    def arrived(slot):
        for pair in range(pairs):
            for j in range(n):
                to_partner(slot - 4, pair, j).wait_recv()

    def dq_rows(pair):
        return pl.ds(pl.multiple_of(pair * prow, prow), prow)

    def dq_own(pair, j):
        return qkv.at[j, pl.ds(pl.multiple_of(do0 + pair * prow, prow), prow)]

    def dq_direct(pair, j):
        return rdma(dq_own(pair, j), back.at[me, dq_rows(pair)], dqsend.at[pair, j], dqrecv.at[pair, me], j)

    def dq_first(pair, j):
        return rdma(dq_own(pair, j), dqrel.at[pair, j % 2], dqsend.at[pair, j], dqfirst.at[pair, j % 2], ahead)

    def dq_second(pair, j):
        return rdma(dqrel.at[pair, j % 2], back.at[relay_from, dq_rows(pair)], dqsecond.at[pair, j % 2],
                    dqrecv.at[pair, relay_from], j)

    def send_dq(pair, j):
        owner_far = j // 2 == (chip + 2) % chips

        @pl.when(j == me)
        def _():
            back[me, dq_rows(pair)] = qkv[j, pl.ds(pl.multiple_of(do0 + pair * prow, prow), prow)]

        @pl.when(owner_far)
        def _():
            dq_first(pair, j).start()

        @pl.when((j != me) & jnp.logical_not(owner_far))
        def _():
            dq_direct(pair, j).start()

    def serve_dq(pair, j):
        @pl.when(j // 2 == (chip + sgn + chips) % chips)
        def _():
            dq_first(pair, j).wait_recv()
            dq_second(pair, j).start()

    def kv_own(src):
        return qkv.at[src, pl.ds(kv0, 2 * krows)]

    def kv_place(src):
        return back.at[src, pl.ds(qrows, 2 * krows)]

    def kv_first(t):
        return rdma(kv_own(dests[t]), kvrel.at[t], kvsend.at[t], kvfirst.at[t], ahead)

    def kv_second(t):
        return rdma(kvrel.at[t], kv_place(relay_from), kvsecond.at[t], kvrecv.at[t], device(sgn, t))

    def kv_direct(t):
        return rdma(kv_own(dests[t]), kv_place(me), kvsend.at[t], kvrecv.at[t], dests[t])

    def grad_places(part, owner):
        if part < pairs:
            return [(pl.ds(0, prow), dwq_ref.at[pl.ds(owner * qrows + part * prow, prow)], 0)]
        return [(pl.ds(0, krows), dwk_ref.at[pl.ds(owner * krows, krows)], 0),
                (pl.ds(krows, krows), dwv_ref.at[pl.ds(owner * krows, krows)], 1)]

    def block_ref(part, t):
        if part == 0:
            return fpart.at[t]
        return pbuf.at[1, 4 * (part - 1) + t // 3, pl.ds(0, prow), pl.ds(pl.multiple_of((t % 3) * mcol, LANES), mcol)]

    def f_first(part, t):
        return rdma(block_ref(part, t), frel.at[part, t], fsend.at[part, t, 0], ffirst.at[part, t], ahead)

    def f_second(part, t):
        return [rdma(frel.at[part, t, span], place, fsecond.at[part, t, k], frecv.at[part, t, k], device(sgn, t))
                for span, place, k in grad_places(part, relay_from)]

    def f_direct(part, t):
        return [rdma(block_ref(part, t).at[span], place, fsend.at[part, t, k], frecv.at[part, t, k], dests[t])
                for span, place, k in grad_places(part, me)]

    def f_own(part):
        return [pltpu.make_async_copy(block_ref(part, n - 1).at[span], place, outsem.at[part, k])
                for span, place, k in grad_places(part, me)]

    dest_off = (2, 2, -1, -1, 1, 1, 0, 0)
    dest_flip = (0, 1, 0, 1, 0, 1, 1, 0)

    def dest_of(t):
        return ((chip + sgn * pick(t, dest_off) + chips) % chips) * 2 + (core + pick(t, dest_flip)) % 2

    def weight_grads(part):
        lo = do0 + part * prow if part < pairs else kv0

        def block_step(t, carry):
            cols = pl.ds(pl.multiple_of(dest_of(t) * mcol, LANES), mcol)
            wide = jnp.concatenate([qkv[j, lo:lo + prow, :] for j in range(n)], axis=1)
            block_ref(part, t)[...] = dot_nn(wide, xall[:, :, cols].reshape(n * tok, mcol))
            for k in remote:
                @pl.when(t == k)
                def _():
                    for copy in [f_first(part, k)] if k < 2 else f_direct(part, k):
                        copy.start()

            @pl.when(t == n - 1)
            def _():
                for copy in f_own(part):
                    copy.start()
            return carry

        lax.fori_loop(0, n, block_step, 0)

    def relay_grads(part):
        for t in range(2):
            f_first(part, t).wait_recv()
            for copy in f_second(part, t):
                copy.start()

    def load(kind, order, buf):
        src = source_of(order)
        if kind == 0:
            return [pltpu.make_async_copy(wo_ref.at[pl.ds(src * qrows, qrows)], woa.at[buf], wsem.at[0, buf])]
        return [pltpu.make_async_copy(wq_ref.at[pl.ds(src * qrows, qrows)], wob.at[buf, pl.ds(0, qrows)], wsem.at[1, buf]),
                pltpu.make_async_copy(wk_ref.at[pl.ds(src * krows, krows)], wob.at[buf, pl.ds(qrows, krows)], wsem.at[2, buf]),
                pltpu.make_async_copy(wv_ref.at[pl.ds(src * krows, krows)], wob.at[buf, pl.ds(qrows + krows, krows)], wsem.at[3, buf])]

    parts = [(j, slice(j * width, min((j + 1) * width, model))) for j in range(-(-model // width))]

    def stage(buf):
        return pbuf.at[0, 6, pl.ds(0, qrows), pl.ds(pl.multiple_of(buf * mcol, LANES), mcol)]

    def save(order, buf):
        return pltpu.make_async_copy(stage(buf), dwo_ref.at[pl.ds(source_of(order) * qrows, qrows)], wsem.at[4, buf])

    def next_weights(kind, order):
        buf = order % 2
        for copy in load(kind, order, buf):
            copy.wait()

        @pl.when(order < n - 1)
        def _():
            for copy in load(kind, order + 1, 1 - buf):
                copy.start()

        return buf

    def close_o(order, own):
        buf = next_weights(0, order)
        slot = pick(order, slot_table)

        def tile_o(j):
            return qkv[j, 0:qrows, :] if own else gath[slot - 1, j]

        @pl.when(order >= 2)
        def _():
            save(order - 2, buf).wait()

        @pl.when(order >= 0)
        def _():
            stage(buf)[...] = dot_nn(jnp.concatenate([tile_o(j) for j in range(n)], axis=1), dyc[...])

        save(order, buf).start()
        for j, cols in parts:
            @pl.when(order >= 0)
            def _():
                pbuf[0, j, :, 0:cols.stop - cols.start] += dot_tn(tile_o(me), woa[buf, :, cols])

    def close_dx(order):
        buf = next_weights(1, order)
        for j, cols in parts:
            @pl.when(order >= 0)
            def _():
                pbuf[0, 3 + j, :, 0:cols.stop - cols.start] += dot_tn(back[source_of(order)], wob[buf, :, cols])

    def do_weights(t, buf):
        return pltpu.make_async_copy(wo_ref.at[pl.ds(dest_of(t) * qrows, qrows)], woa.at[buf], wsem.at[0, buf])

    dy_cols = [(c, c * tok, min(tok, model - c * tok)) for c in range(-(-model // tok))]
    dy_in = [pltpu.make_async_copy(dy_ref.at[:, pl.ds(lo, size)], back.at[c, :, pl.ds(0, size)], dyload.at[c])
             for c, lo, size in dy_cols]
    x_in = pltpu.make_async_copy(x_ref, xall.at[me], lsem.at[1])
    y_own = pltpu.make_async_copy(columns(me), token_rows(me), lsem.at[2])
    own_weights = [pltpu.make_async_copy(wq_ref.at[pl.ds(me * qrows, qrows)], wob.at[0, pl.ds(0, qrows)], lsem.at[3]),
                   pltpu.make_async_copy(wk_ref.at[pl.ds(me * krows, krows)], wob.at[0, pl.ds(qrows, krows)], lsem.at[4]),
                   pltpu.make_async_copy(wv_ref.at[pl.ds(me * krows, krows)], wob.at[0, pl.ds(qrows + krows, krows)], lsem.at[5])]
    for copy in dy_in:
        copy.start()
    do_weights(0, 0).start()
    for copy in [x_in, y_own] + own_weights:
        copy.start()
    seg_mine[...] = jnp.broadcast_to(seg_ref[...].reshape(1, tok), seg_mine.shape)
    pl.semaphore_wait(barrier, n - 1)
    for h in range(2):
        x_right(h).start()
        x_left(1 - h).start()
    x_partner(0).start()
    for t in remote:
        seg_copy(t).start()
    seg_all[me] = seg_mine[...]
    for copy in dy_in:
        copy.wait()

    def do_step(t, carry):
        buf = t % 2

        @pl.when(t < n - 1)
        def _():
            do_weights(t + 1, 1 - buf).start()

        do_weights(t, buf).wait()
        local = jnp.concatenate([back[c, :, 0:size] for c, lo, size in dy_cols], axis=1)
        block = dot_nt(woa[buf], local).astype(BF)

        @pl.when(t < n - 1)
        def _():
            gath[2, t] = block

        @pl.when(t == n - 1)
        def _():
            qkv[me, do0:kv0] = block
        return carry

    lax.fori_loop(0, n, do_step, 0)
    for t in remote:
        (p_first if t < 2 else p_direct)(t).start()
    dkacc[...] = jnp.zeros_like(dkacc)
    dvacc[...] = jnp.zeros_like(dvacc)
    rhsq[...] = jnp.zeros_like(rhsq)
    rhsd[...] = jnp.zeros_like(rhsd)
    for copy in [x_in] + own_weights:
        copy.wait()

    def project_step(order, carry):
        @pl.when(order == 1)
        def _():
            x_partner(0).wait_recv()

        @pl.when(order == 2)
        def _():
            x_right(0).wait_recv()
            x_relay(0).start()
            x_left(1).wait_recv()
            x_relay(1).start()
            x_right(1).wait_recv()
            x_partner(1).start()

        @pl.when(order == 3)
        def _():
            x_left(0).wait_recv()
            x_partner(2).start()

        @pl.when(order == 4)
        def _():
            x_partner(1).wait_recv()

        @pl.when(order == 5)
        def _():
            for t in range(2):
                p_first(t).wait_recv()
                p_second(t).start()
            x_partner(2).wait_recv()

        @pl.when(order == 6)
        def _():
            for h in range(2):
                x_relay(h).wait_recv()
            x_partner(3).start()

        @pl.when(order == 7)
        def _():
            x_partner(3).wait_recv()

        src = source_of(order)
        qkv[src, 0:qrows] = dot_nt(wob[0, 0:qrows], xall[src]).astype(BF)
        kv = dot_nt(wob[0, qrows:qrows + 2 * krows], xall[src]).astype(BF)
        qkv[src, kv0:rows] = kv
        kvn[pl.ds(pl.multiple_of(src * tok, LANES), tok), :] = kv.T
        return carry

    lax.fori_loop(0, n, project_step, 0)
    for t in remote:
        (y_first if t < 2 else y_direct)(t).start()

    for t in remote:
        seg_copy(t).wait_recv()
    row_id = lax.broadcasted_iota(jnp.int32, (n, tok), 0)
    lane_id = lax.broadcasted_iota(jnp.int32, (n, tok), 1)
    seg = jnp.zeros((n, tok), jnp.int32)
    for d in range(n):
        seg = jnp.where(row_id == d, seg_all[d, 0:1], seg)
    before = jnp.where(lane_id == 0, pltpu.roll(pltpu.roll(seg, 1, 1), 1, 0), pltpu.roll(seg, 1, 1))
    pos = row_id * tok + lane_id
    best = jnp.where((seg != before) & (pos > 0), pos, 0)
    shift = 1
    while shift < tok:
        best = jnp.maximum(best, jnp.where(lane_id >= shift, pltpu.roll(best, shift, 1), 0))
        shift *= 2
    end = jnp.broadcast_to(best[:, tok - 1:tok], (n, tok))
    carry_max = jnp.where(row_id >= 1, pltpu.roll(end, 1, 0), 0)
    shift = 1
    while shift < n:
        carry_max = jnp.maximum(carry_max, jnp.where(row_id >= shift, pltpu.roll(carry_max, shift, 0), 0))
        shift *= 2
    best = jnp.maximum(best, carry_max)
    for d in range(n):
        first_ref[d] = jnp.broadcast_to(best[d:d + 1], (8, tok))

    score_mul = scale * LOG2E
    grp = tok // 8
    lag = 5

    def keys(c):
        return kvn[pl.ds(pl.multiple_of(c * tok, LANES), tok), :]

    def q_rows(pair, g):
        return pl.ds(pl.multiple_of((pair * group + g) * krows, krows), krows)

    def do_rows(pair, g):
        return pl.ds(pl.multiple_of(do0 + (pair * group + g) * krows, krows), krows)

    def doc_starts(i):
        return jnp.concatenate([first_ref[i][0:1]] * group, axis=1)

    def score(i, par, c, top, diagonal):
        t = dot_nn(keys(c), rhsq[par]) * score_mul
        kpos = lax.broadcasted_iota(jnp.int32, (tok, width), 0)
        keep = kpos >= doc_starts(i) - c * tok
        if diagonal:
            qpos = lax.broadcasted_iota(jnp.int32, (1, tok), 1)
            keep = keep & (kpos <= jnp.concatenate([qpos] * group, axis=1))
        t = jnp.where(keep, t, -jnp.inf)
        pbuf[par, c] = t
        return jnp.maximum(top, jnp.max(t.reshape(grp, 8, width), axis=0))

    def value(par, c, top, total):
        p = jnp.exp2(pbuf[par, c] - top)
        oacc[...] += dot_nn(qkv[c, kv0 + krows:rows, :], p.astype(BF))
        return total + jnp.sum(p.reshape(grp, 8, width), axis=0)

    def grad(par, c):
        p = jnp.exp2(pbuf[par, c] - stats[par, 0:1])
        dp = dot_nn(keys(c), rhsd[par])
        ds = (p * (dp - stats[par, 8:9])).astype(BF)
        dqacc[...] += dot_nn(qkv[c, kv0:kv0 + krows, :], ds)
        pb = p.astype(BF)
        spans = [(slice(j * mcol, (j + 1) * mcol), slice(j * tok, (j + 1) * tok)) for j in range(width // mcol)]
        for qs, place in spans:
            woa[0, :, place] = ds[:, qs].T
            wob[0, 0:mcol, place] = pb[:, qs].T
        dkacc[c] += sum(dot_nn(rhsq[par, 0:krows, qs], woa[0, :, place]) for qs, place in spans)
        dvacc[c] += sum(dot_nn(rhsd[par, krows:2 * krows, qs], wob[0, 0:mcol, place]) for qs, place in spans)

    def tile_done(pair, j):
        dq = (dqacc[...] * scale).astype(BF)
        for g in range(group):
            qkv[j, do_rows(pair, g), :] = dq[:, g * tok:(g + 1) * tok]
        piece = pair * n + j

        @pl.when(piece == 0)
        def _():
            for t in remote:
                p_direct(t).wait_send()
            for t in range(2):
                p_second(t).wait_send()
            for peer in (right, left):
                pl.semaphore_signal(free_far, inc=1, device_id={'cp': peer}, device_id_type=pl.DeviceIdType.MESH)
            pl.semaphore_signal(free_par, inc=1, device_id={'cp': partner}, device_id_type=pl.DeviceIdType.MESH)

        own_right(pair, j).start()
        own_left(pair, j).start()
        to_partner(0, pair, j).start()
        send_dq(pair, j)

        @pl.when(piece == lag)
        def _():
            for t in range(2):
                y_first(t).wait_recv()
                y_second(t).start()

        @pl.when(piece == lag)
        def _():
            pl.semaphore_wait(free_far, 2)

        @pl.when(piece == n + lag + 1)
        def _():
            relay_grads(0)

        @pl.when(piece >= lag)
        def _():
            old = piece - lag
            serve_near(old // n, old % n)
            serve_dq(old // n, old % n)

    def item_step(m, carry):
        pair, i = m // n, m % n
        par = i % 2
        last = 1 - par

        @pl.when((pair == 0) & (i != me))
        def _():
            do_arrived(i)

        for g in range(group):
            lanes = slice(g * tok, (g + 1) * tok)
            rhsq[par, 0:krows, lanes] = qkv[i, q_rows(pair, g), :]
            rhsd[par, krows:2 * krows, lanes] = qkv[i, do_rows(pair, g), :]
        dqacc[...] = jnp.zeros_like(dqacc)

        def both_step(c, top):
            grad(last, c)
            return score(i, par, c, top, False)

        top = lax.fori_loop(0, i, both_step, jnp.full((8, width), -jnp.inf, F32))
        top = score(i, par, i, top, True)

        @pl.when(i >= 1)
        def _():
            tile_done(pair, i - 1)

        top = jnp.max(top, axis=0, keepdims=True)
        oacc[...] = jnp.zeros_like(oacc)
        total = lax.fori_loop(0, i + 1, lambda c, acc: value(par, c, top, acc), jnp.zeros((8, width), F32))
        total = jnp.sum(total, axis=0, keepdims=True)
        o_blk = (oacc[...] * (1.0 / total)).astype(BF)
        stats[par, 0:8] = jnp.broadcast_to(top + jnp.log2(total), (8, width))
        delta = jnp.sum(rhsd[par, krows:2 * krows].astype(F32) * o_blk.astype(F32), axis=0, keepdims=True)
        stats[par, 8:16] = jnp.broadcast_to(delta, (8, width))
        for g in range(group):
            qkv[i, q_rows(pair, g), :] = o_blk[:, g * tok:(g + 1) * tok]

        @pl.when(i == n - 1)
        def _():
            dqacc[...] = jnp.zeros_like(dqacc)

            def last_step(c, inner):
                grad(par, c)
                return inner

            lax.fori_loop(0, n, last_step, 0)
            tile_done(pair, i)

        @pl.when(m == n - 1)
        def _():
            weight_grads(0)
        return carry

    lax.fori_loop(0, n * pairs, item_step, 0)

    for c in range(n):
        qkv[c, kv0:kv0 + krows, :] = (dkacc[c] * scale).astype(BF)
        qkv[c, kv0 + krows:rows, :] = dvacc[c].astype(BF)
    for t in remote:
        (kv_first if t < 2 else kv_direct)(t).start()
    back[me, qrows:qrows + 2 * krows] = qkv[me, kv0:rows]
    for kind in range(2):
        for copy in load(kind, 0, 0):
            copy.start()
    for part in range(1, pairs + 1):
        weight_grads(part)
    for old in range(n * pairs - lag, n * pairs):
        serve_near(old // n, old % n)
        serve_dq(old // n, old % n)
    for t in range(2):
        kv_first(t).wait_recv()
        kv_second(t).start()
    pbuf[0, 0:6] = jnp.zeros((6, tok, width), F32)
    y_own.wait()
    for t in remote:
        y_direct(t).wait_recv()

    def closing_step(r, carry):
        @pl.when(r == 1)
        def _():
            arrived(4)
            relay_grads(1)

        @pl.when(r == 2)
        def _():
            relay_grads(2)

        @pl.when(r == 4)
        def _():
            pl.semaphore_wait(free_par, 1)
            for pair in range(pairs):
                for j in range(n):
                    serve_far(pair, j)
            arrived(5)

        @pl.when(r == 5)
        def _():
            arrived(6)

        @pl.when(r == 7)
        def _():
            arrived(7)

        @pl.when(r == 0)
        def _():
            close_o(r, True)

        @pl.when((r >= 1) & (r < n))
        def _():
            close_o(r, False)

        @pl.when(r == n)
        def _():
            for t in remote:
                for pair in range(pairs):
                    rdma(dqrel.at[pair, 0], back.at[dests[t], dq_rows(pair)], dqsend.at[pair, 0],
                         dqrecv.at[pair, dests[t]], partner).wait_recv()
                kv_direct(t).wait_recv()

        @pl.when(r >= n)
        def _():
            close_dx(r - n)
        return carry

    lax.fori_loop(0, 2 * n, closing_step, 0)

    spare = tok - qrows

    def rounded(acc, buf, out, sem):
        for j, cols in parts:
            wide = pbuf[0, acc + j, :, 0:cols.stop - cols.start].astype(BF)
            buf[0, 0:qrows, cols] = wide[0:qrows]
            buf[1, 0:spare, cols] = wide[qrows:tok]
        return [pltpu.make_async_copy(buf.at[0, pl.ds(0, qrows)], out.at[pl.ds(0, qrows)], lsem.at[sem]),
                pltpu.make_async_copy(buf.at[1, pl.ds(0, spare)], out.at[pl.ds(qrows, spare)], lsem.at[sem + 1])]

    outs = rounded(0, woa, y_ref, 0) + rounded(3, wob, dx_ref, 2)
    for copy in outs:
        copy.start()

    for t in remote:
        seg_copy(t).wait_send()
        y_direct(t).wait_send()
        kv_direct(t).wait_send()
        for pair in range(pairs):
            rdma(dq_own(pair, 0), dqrel.at[pair, 0], dqsend.at[pair, dests[t]], dqfirst.at[pair, 0], partner).wait_send()
    for h in range(2):
        x_right(h).wait_send()
        x_left(h).wait_send()
        x_relay(h).wait_send()
    for slot in range(4):
        x_partner(slot).wait_send()
    for t in range(2):
        y_second(t).wait_send()
        kv_second(t).wait_send()
        for pair in range(pairs):
            dq_second(pair, t).wait_send()
    for pair in range(pairs):
        for j in range(n):
            own_right(pair, j).wait_send()
            own_left(pair, j).wait_send()
            relay_plus(pair, j).wait_send()
            relay_minus(pair, j).wait_send()
            for slot in range(4):
                to_partner(slot, pair, j).wait_send()
    for order in (n - 2, n - 1):
        save(order, order % 2).wait()
    for copy in outs:
        copy.wait()
    for part in range(pairs + 1):
        for copy in f_own(part):
            copy.wait()
        for t in remote:
            for copy in f_direct(part, t):
                copy.wait_recv()
        for t in range(2, n - 1):
            for copy in f_direct(part, t):
                copy.wait_send()
        for t in range(2):
            f_first(part, t).wait_send()
            for copy in f_second(part, t):
                copy.wait_send()


def attention_layer(n, x_act, dy_act, seg, wq, wk, wv, wo):
    tok, model = x_act.shape
    qrows, krows = wq.shape[0] // n, wk.shape[0] // n
    rows = 2 * qrows + 2 * krows
    total = n * tok
    mcol = model // n
    group = 2
    width = group * tok
    pairs = qrows // krows // group
    prow = group * krows
    vmem = pl.BlockSpec(memory_space=pltpu.VMEM)
    anym = pl.BlockSpec(memory_space=pl.ANY)
    dma = pltpu.SemaphoreType.DMA
    return pl.pallas_call(
        functools.partial(main_kernel, (n, qrows, krows, tok, krows ** -0.5)),
        out_shape=(jax.ShapeDtypeStruct((tok, model), BF), jax.ShapeDtypeStruct((tok, model), BF),
                   jax.ShapeDtypeStruct((wq.shape[0], mcol), F32), jax.ShapeDtypeStruct((wk.shape[0], mcol), F32),
                   jax.ShapeDtypeStruct((wv.shape[0], mcol), F32), jax.ShapeDtypeStruct((wo.shape[0], mcol), F32)),
        in_specs=[anym, anym, vmem, anym, anym, anym, anym],
        out_specs=(anym,) * 6,
        scratch_shapes=[
            pltpu.VMEM((8, tok), jnp.int32), pltpu.VMEM((n, 8, tok), jnp.int32), pltpu.VMEM((n, 8, tok), jnp.int32),
            pltpu.VMEM((total, 2 * krows), BF),
            pltpu.VMEM((2, n, tok, width), F32),
            pltpu.VMEM((2, 2 * krows, width), BF), pltpu.VMEM((2, 2 * krows, width), BF),
            pltpu.VMEM((2, 16, width), F32),
            pltpu.VMEM((krows, width), F32), pltpu.VMEM((krows, width), F32),
            pltpu.VMEM((n, krows, tok), F32), pltpu.VMEM((n, krows, tok), F32),
            pltpu.VMEM((n, tok, model), BF),
            pltpu.VMEM((n, rows, tok), BF),
            pltpu.VMEM((n - 1, n, qrows, tok), BF),
            pltpu.VMEM((n, qrows + 2 * krows, tok), BF),
            pltpu.VMEM((total, mcol), BF),
            pltpu.VMEM((2, tok, mcol), BF),
            pltpu.VMEM((pairs, 2, prow, tok), BF),
            pltpu.VMEM((2, 2 * krows, tok), BF),
            pltpu.VMEM((pairs + 1, 2, prow, mcol), F32),
            pltpu.VMEM((n, prow, mcol), F32),
            pltpu.VMEM((2, qrows, model), BF), pltpu.VMEM((2, qrows + 2 * krows, model), BF),
            dma((5, 2)), dma((6,)), dma((n,)),
            dma((2, 2)), dma((8, 2)), dma((2,)), dma((4,)),
            dma((n,)), dma((n,)), dma((2,)), dma((2,)), dma((n,)), dma((n,)),
            dma((n,)), dma((n,)), dma((2,)), dma((2,)),
            dma((2, pairs, n)), dma((2, pairs, n)), dma((4, pairs, n)), dma((8, pairs, n)),
            dma((pairs, n)), dma((pairs, n)), dma((pairs, 2)), dma((pairs, 2)),
            dma((n,)), dma((n,)), dma((2,)), dma((2,)),
            dma((pairs + 1, n, 2)), dma((pairs + 1, n, 2)), dma((pairs + 1, 2)), dma((pairs + 1, 2, 2)), dma((pairs + 1, 2)),
            pltpu.SemaphoreType.REGULAR, pltpu.SemaphoreType.REGULAR,
        ],
        compiler_params=pltpu.CompilerParams(collective_id=0, has_side_effects=True, vmem_limit_bytes=VMEM_MAX),
        name='attention_layer',
    )(x_act, dy_act, seg, wq, wk, wv, wo)


def copy_out(arrays):
    pieces = 4
    count = len(arrays)

    def kernel(*refs):
        src, dst, buf = refs[:count], refs[count:2 * count], refs[2 * count:3 * count]
        insem, outsem = refs[3 * count:]
        loads, stores = [], []
        for k, array in enumerate(arrays):
            size = array.shape[0] // pieces
            for p in range(pieces):
                rows = pl.ds(p * size, size)
                loads.append(pltpu.make_async_copy(src[k].at[rows], buf[k].at[rows], insem.at[k, p]))
                stores.append(pltpu.make_async_copy(buf[k].at[rows], dst[k].at[rows], outsem.at[k, p]))
        for copy in loads:
            copy.start()
        for copy, store in zip(loads, stores):
            copy.wait()
            store.start()
        for store in stores:
            store.wait()

    anym = pl.BlockSpec(memory_space=pl.ANY)
    return pl.pallas_call(
        kernel,
        out_shape=tuple(jax.ShapeDtypeStruct(a.shape, a.dtype) for a in arrays),
        in_specs=[anym] * count, out_specs=(anym,) * count,
        scratch_shapes=[pltpu.VMEM(a.shape, a.dtype) for a in arrays]
        + [pltpu.SemaphoreType.DMA((count, pieces)), pltpu.SemaphoreType.DMA((count, pieces))],
        compiler_params=pltpu.CompilerParams(vmem_limit_bytes=VMEM_MAX),
        name='copy_out',
    )(*arrays)


def solution(mesh):
    n = mesh.shape['cp']
    row_spec = P(('dp', 'cp'), None)
    tok_spec = P(('dp', 'cp'))
    weight_spec = P(None, None, None)
    grad_spec = P(('dp', 'cp'), None, None)

    def local_step(x_act, seg_ids, w_q, w_k, w_v, w_o, dy_act):
        model, q_heads, head_dim = w_q.shape
        kv_heads = w_k.shape[1]
        assert kv_heads == n and x_act.shape[0] % LANES == 0

        def flat(w):
            return w.transpose(1, 2, 0).reshape(w.shape[1] * head_dim, model)

        def unflat(g, heads):
            return g.reshape(heads, head_dim, g.shape[1]).transpose(2, 0, 1)

        wq, wk, wv, wo = flat(w_q), flat(w_k), flat(w_v), flat(w_o)
        y_out, dx_out, dwq, dwk, dwv, dwo = copy_out(attention_layer(n, x_act, dy_act, seg_ids, wq, wk, wv, wo))
        return (y_out, dx_out, unflat(dwq, q_heads), unflat(dwk, kv_heads), unflat(dwv, kv_heads), unflat(dwo, q_heads))

    return jax.shard_map(local_step, mesh=mesh,
                         in_specs=(row_spec, tok_spec, weight_spec, weight_spec, weight_spec, weight_spec, row_spec),
                         out_specs=(row_spec, row_spec, grad_spec, grad_spec, grad_spec, grad_spec),
                         check_vma=False)
```

```python
import functools

import jax
import jax.numpy as jnp
from jax import lax
from jax.experimental import pallas as pl
from jax.experimental.pallas import tpu as pltpu
from jax.sharding import PartitionSpec as P

BF = jnp.bfloat16
F32 = jnp.float32
LANES = 128
LOG2E = 1.4426950408889634
VMEM_MAX = 67043328


def rdma(src, dst, send_sem, recv_sem, peer):
    return pltpu.make_async_remote_copy(src_ref=src, dst_ref=dst, send_sem=send_sem, recv_sem=recv_sem,
                                        device_id={'cp': peer}, device_id_type=pl.DeviceIdType.MESH)


def dot_nt(left, right):
    return lax.dot_general(left, right, (((1,), (1,)), ((), ())), preferred_element_type=F32)


def dot_tn(left, right):
    return lax.dot_general(left, right, (((0,), (0,)), ((), ())), preferred_element_type=F32)


def dot_nn(left, right):
    return lax.dot_general(left, right, (((1,), (0,)), ((), ())), preferred_element_type=F32)


def pick(index, values):
    out = values[0]
    for k in range(1, len(values)):
        out = jnp.where(index == k, values[k], out)
    return out


def main_kernel(dims, x_ref, dy_ref, seg_ref, wq_ref, wk_ref, wv_ref, wo_ref,
                y_ref, dx_ref, dwq_ref, dwk_ref, dwv_ref, dwo_ref,
                seg_mine, seg_all, first_ref, kvn, pbuf, rhsq, rhsd, stats, oacc, dqacc, dkacc, dvacc, gall, xc, dyc, xrel,
                woa, wob, woc, wsem, outsem, osem, relsem, parsem, rsem, xsend, xrecv, xfirst, xsecond, lsem, dxsem, xload,
                psend, precv, pfirst, psecond, gsend, grecv, free_near, free_far, free_par):
    n, qrows, krows, tok, scale = dims
    chips = n // 2
    heads = qrows // krows
    width = rhsq.shape[2]
    group = width // tok
    me = lax.axis_index('cp')
    chip, core = me // 2, me % 2
    sgn = 1 - 2 * core
    rows = 2 * qrows + 2 * krows
    model = x_ref.shape[1]
    mcol = xc.shape[1]
    do0, kv0 = qrows, 2 * qrows

    def device(chip_off, flip):
        return ((chip + chip_off + chips) % chips) * 2 + (core + flip) % 2

    right, left, partner = device(1, 0), device(-1, 0), device(0, 1)
    dests = [device(2, 0), device(2, 1), device(-sgn, 0), device(-sgn, 1), device(sgn, 0), device(sgn, 1), partner]
    ahead = dests[4]
    relay_from = device(-sgn, 0)

    barrier = pltpu.get_barrier_semaphore()
    for peer in dests:
        pl.semaphore_signal(barrier, inc=1, device_id={'cp': peer}, device_id_type=pl.DeviceIdType.MESH)

    sides = ((x_ref, xc), (dy_ref, dyc))

    def columns(ref, dst):
        return ref.at[:, pl.ds(pl.multiple_of(dst * mcol, LANES), mcol)]

    def token_rows(ref, src):
        return ref.at[pl.ds(pl.multiple_of(src * tok, LANES), tok)]

    def x_first(a, t):
        return rdma(columns(sides[a][0], dests[t]), xrel.at[a, t], xsend.at[a, t], xfirst.at[a, t], ahead)

    def x_second(a, t):
        return rdma(xrel.at[a, t], token_rows(sides[a][1], relay_from), xsecond.at[a, t], xrecv.at[a, t], device(sgn, t))

    def x_direct(a, t):
        return rdma(columns(sides[a][0], dests[t]), token_rows(sides[a][1], me), xsend.at[a, t], xrecv.at[a, t], dests[t])

    def x_own(a):
        return pltpu.make_async_copy(columns(sides[a][0], me), token_rows(sides[a][1], me), lsem.at[a])

    def view(slot, part, j):
        if part == 0:
            return gall.at[slot, j, pl.ds(0, kv0)]
        return gall.at[slot, pl.ds(j * (n // 2), n // 2), pl.ds(kv0, 2 * krows)]

    def own_right(part, j):
        return rdma(view(0, part, j), view(1, part, j), osem.at[0, part, j], rsem.at[1, part, j], right)

    def own_left(part, j):
        return rdma(view(0, part, j), view(2, part, j), osem.at[1, part, j], rsem.at[2, part, j], left)

    def relay_plus(part, j):
        src, dst = view(1, part, j), view(3, part, j)
        if part == 0:
            src, dst = src.at[pl.ds(0, do0)], dst.at[pl.ds(0, do0)]
        return rdma(src, dst, relsem.at[0, part, j], rsem.at[3, part, j], right)

    def relay_minus(part, j):
        src, dst = view(2, part, j), view(3, part, j)
        if part == 0:
            src, dst = src.at[pl.ds(do0, do0)], dst.at[pl.ds(do0, do0)]
        return rdma(src, dst, relsem.at[1, part, j], rsem.at[0, part, j], left)

    def to_partner(slot, part, j):
        return rdma(view(slot, part, j), view(4 + slot, part, j), parsem.at[slot, part, j], rsem.at[4 + slot, part, j], partner)

    def send_own(part, j):
        own_right(part, j).start()
        own_left(part, j).start()
        to_partner(0, part, j).start()

    def serve_near(j):
        own_right(0, j).wait_recv()
        relay_plus(0, j).start()
        to_partner(1, 0, j).start()
        own_left(0, j).wait_recv()
        relay_minus(0, j).start()
        to_partner(2, 0, j).start()

    def serve_near_kv():
        own_right(1, 0).wait_recv()
        relay_plus(1, 0).start()
        own_left(1, 1).wait_recv()
        relay_minus(1, 1).start()
        to_partner(1, 1, 0).start()
        to_partner(2, 1, 1).start()
        own_right(1, 1).wait_recv()
        to_partner(1, 1, 1).start()
        own_left(1, 0).wait_recv()
        to_partner(2, 1, 0).start()

    def serve_far(j):
        relay_plus(0, j).wait_recv()
        relay_minus(0, j).wait_recv()
        to_partner(3, 0, j).start()

    def serve_far_kv():
        relay_plus(1, 0).wait_recv()
        to_partner(3, 1, 0).start()
        relay_minus(1, 1).wait_recv()
        to_partner(3, 1, 1).start()

    def arrived_tiles(slot):
        for j in range(n):
            to_partner(slot - 4, 0, j).wait_recv()

    def arrived_kv(slot):
        for j in range(2):
            to_partner(slot - 4, 1, j).wait_recv()

    slot_table = (0, 4, 1, 2, 5, 6, 3, 7)
    off_table = (0, 0, chips - 1, 1, chips - 1, 1, 2, 2)
    flip_table = (0, 1, 0, 0, 1, 1, 0, 1)

    def source_of(order):
        return ((chip + pick(order, off_table)) % chips) * 2 + (core + pick(order, flip_table)) % 2

    def load(kind, order, buf):
        src = source_of(order)
        if kind == 0:
            return [pltpu.make_async_copy(wo_ref.at[pl.ds(src * qrows, qrows)], woa.at[buf], wsem.at[0, buf])]
        if kind == 1:
            return [pltpu.make_async_copy(wq_ref.at[pl.ds(src * qrows, qrows)], wob.at[buf], wsem.at[1, buf])]
        return [pltpu.make_async_copy(wk_ref.at[pl.ds(src * krows, krows)], woc.at[buf, pl.ds(0, krows)], wsem.at[2, buf]),
                pltpu.make_async_copy(wv_ref.at[pl.ds(src * krows, krows)], woc.at[buf, pl.ds(krows, krows)], wsem.at[3, buf])]

    def stage(kind, buf):
        if kind < 2:
            return pbuf.at[0, 6 + kind, pl.ds(0, qrows), pl.ds(pl.multiple_of(buf * mcol, LANES), mcol)]
        return pbuf.at[0, 6, pl.ds(pl.multiple_of(buf * 2 * krows, 8), 2 * krows), pl.ds(2 * mcol, mcol)]

    def save(kind, order, buf):
        src = source_of(order)
        if kind == 0:
            return [pltpu.make_async_copy(stage(0, buf), dwo_ref.at[pl.ds(src * qrows, qrows)], outsem.at[0, buf])]
        if kind == 1:
            return [pltpu.make_async_copy(stage(1, buf), dwq_ref.at[pl.ds(src * qrows, qrows)], outsem.at[1, buf])]
        both = stage(2, buf)
        return [pltpu.make_async_copy(both.at[pl.ds(0, krows)], dwk_ref.at[pl.ds(src * krows, krows)], outsem.at[2, buf]),
                pltpu.make_async_copy(both.at[pl.ds(krows, krows)], dwv_ref.at[pl.ds(src * krows, krows)], outsem.at[3, buf])]

    parts = [(j, slice(j * width, min((j + 1) * width, model))) for j in range(-(-model // width))]
    kinds = ((0, do0, woa, dyc, 0), (do0, kv0, wob, xc, 3), (kv0, rows, woc, xc, 3))

    def closing_part(kind, order):
        row0, row1, wbuf, other, acc = kinds[kind]
        buf = order % 2
        slot = pick(order, slot_table)
        for copy in load(kind, order, buf):
            copy.wait()

        @pl.when(order < n - 1)
        def _():
            for copy in load(kind, order + 1, 1 - buf):
                copy.start()

        @pl.when(order >= 2)
        def _():
            for copy in save(kind, order - 2, buf):
                copy.wait()

        @pl.when(order >= 0)
        def _():
            wide = jnp.concatenate([gall[slot, j, row0:row1, :] for j in range(n)], axis=1)
            stage(kind, buf)[...] = dot_nn(wide, other[...])

        for copy in save(kind, order, buf):
            copy.start()
        for j, cols in parts:
            @pl.when(order >= 0)
            def _():
                pbuf[0, acc + j, :, 0:cols.stop - cols.start] += dot_tn(gall[slot, me, row0:row1, :], wbuf[buf, :, cols])

    def block_copies(step, buf):
        pair, flip = step // 2, (step + step // 6) % 2
        off = 2 - 3 * pair + 5 * (pair // 2) + 2 * (pair // 3)
        dst = ((chip + sgn * off + chips) % chips) * 2 + (core + flip) % 2
        return [
            pltpu.make_async_copy(wo_ref.at[pl.ds(dst * qrows, qrows)], woa.at[buf], wsem.at[0, buf]),
            pltpu.make_async_copy(wq_ref.at[pl.ds(dst * qrows, qrows)], wob.at[buf], wsem.at[1, buf]),
            pltpu.make_async_copy(wk_ref.at[pl.ds(dst * krows, krows)], woc.at[buf, pl.ds(0, krows)], wsem.at[2, buf]),
            pltpu.make_async_copy(wv_ref.at[pl.ds(dst * krows, krows)], woc.at[buf, pl.ds(krows, krows)], wsem.at[3, buf]),
        ]

    def p_first(t):
        return rdma(gall.at[3, t], gall.at[7, t], psend.at[t], pfirst.at[t], ahead)

    def p_second(t):
        return rdma(gall.at[7, t], gall.at[0, relay_from], psecond.at[t], precv.at[t], device(sgn, t))

    def p_direct(t):
        return rdma(gall.at[3, t], gall.at[0, me], psend.at[t], precv.at[t], dests[t])

    def seg_copy(t):
        row = pl.ds(0, 1)
        return rdma(seg_mine.at[row], seg_all.at[me, row], gsend.at[t], grecv.at[t], dests[t])

    xcols = [(c, c * tok, min(tok, model - c * tok)) for c in range(-(-model // tok))]

    def x_loads(a):
        return [pltpu.make_async_copy(sides[a][0].at[:, pl.ds(lo, size)], gall.at[1 + a, c, pl.ds(0, tok), pl.ds(0, size)],
                                      xload.at[a, c]) for c, lo, size in xcols]

    def x_whole(a):
        return jnp.concatenate([gall[1 + a, c, 0:tok, 0:size] for c, lo, size in xcols], axis=1)

    for copy in x_loads(0):
        copy.start()
    for copy in block_copies(0, 0):
        copy.start()
    for copy in x_loads(1):
        copy.start()
    for a in range(2):
        x_own(a).start()
    seg_mine[...] = jnp.broadcast_to(seg_ref[...].reshape(1, tok), seg_mine.shape)
    pl.semaphore_wait(barrier, n - 1)
    for a in range(2):
        x_direct(a, 2).start()
    for t in range(n - 1):
        seg_copy(t).start()
    seg_all[me] = seg_mine[...]
    for copy in x_loads(0) + x_loads(1):
        copy.wait()

    def project_step(step, carry):
        buf = step % 2

        @pl.when(step < n - 1)
        def _():
            for copy in block_copies(step + 1, 1 - buf):
                copy.start()

        for copy in block_copies(step, buf):
            copy.wait()
        slot = 3 - 3 * (step // (n - 1))
        place = step + (me - step) * (step // (n - 1))
        gall[slot, place, 0:qrows] = dot_nt(wob[buf], x_whole(0)).astype(BF)
        gall[slot, place, kv0:rows] = dot_nt(woc[buf], x_whole(0)).astype(BF)
        gall[slot, place, do0:kv0] = dot_nt(woa[buf], x_whole(1)).astype(BF)
        for t in range(n - 1):
            @pl.when(step == t)
            def _():
                (p_first if t < 2 else p_direct)(t).start()
        return carry

    lax.fori_loop(0, n, project_step, 0)
    for peer in (right, left):
        pl.semaphore_signal(free_near, inc=1, device_id={'cp': peer}, device_id_type=pl.DeviceIdType.MESH)
    for t in range(2):
        p_first(t).wait_recv()
        p_second(t).start()
    for t in range(n - 1):
        for a in range(2):
            if t != 2:
                (x_first if t < 2 else x_direct)(a, t).start()

    for t in range(n - 1):
        seg_copy(t).wait_recv()
    row_id = lax.broadcasted_iota(jnp.int32, (n, tok), 0)
    lane_id = lax.broadcasted_iota(jnp.int32, (n, tok), 1)
    seg = jnp.zeros((n, tok), jnp.int32)
    for d in range(n):
        seg = jnp.where(row_id == d, seg_all[d, 0:1], seg)
    before = jnp.where(lane_id == 0, pltpu.roll(pltpu.roll(seg, 1, 1), 1, 0), pltpu.roll(seg, 1, 1))
    pos = row_id * tok + lane_id
    best = jnp.where((seg != before) & (pos > 0), pos, 0)
    shift = 1
    while shift < tok:
        best = jnp.maximum(best, jnp.where(lane_id >= shift, pltpu.roll(best, shift, 1), 0))
        shift *= 2
    end = jnp.broadcast_to(best[:, tok - 1:tok], (n, tok))
    carry_max = jnp.where(row_id >= 1, pltpu.roll(end, 1, 0), 0)
    shift = 1
    while shift < n:
        carry_max = jnp.maximum(carry_max, jnp.where(row_id >= shift, pltpu.roll(carry_max, shift, 0), 0))
        shift *= 2
    best = jnp.maximum(best, carry_max)
    for d in range(n):
        first_ref[d] = jnp.broadcast_to(best[d:d + 1], (8, tok))
    dkacc[...] = jnp.zeros_like(dkacc)
    dvacc[...] = jnp.zeros_like(dvacc)
    rhsq[...] = jnp.zeros_like(rhsq)
    rhsd[...] = jnp.zeros_like(rhsd)
    for t in range(n - 1):
        p_direct(t).wait_recv()

    def transpose_tile(c, carry):
        kvn[pl.ds(pl.multiple_of(c * tok, LANES), tok), :] = gall[0, c, kv0:rows, :].T
        return carry

    lax.fori_loop(0, n, transpose_tile, 0)
    score_mul = scale * LOG2E
    grp = tok // 8
    lag = 2

    def keys(c):
        return kvn[pl.ds(pl.multiple_of(c * tok, LANES), tok), :]

    def q_rows(pair, g):
        return pl.ds(pl.multiple_of((pair * group + g) * krows, krows), krows)

    def do_rows(pair, g):
        return pl.ds(pl.multiple_of(do0 + (pair * group + g) * krows, krows), krows)

    def doc_starts(i):
        return jnp.concatenate([first_ref[i][0:1]] * group, axis=1)

    def score(i, pair, c, top, diagonal):
        t = dot_nn(keys(c), rhsq[pair]) * score_mul
        kpos = lax.broadcasted_iota(jnp.int32, (tok, width), 0)
        keep = kpos >= doc_starts(i) - c * tok
        if diagonal:
            qpos = lax.broadcasted_iota(jnp.int32, (1, tok), 1)
            keep = keep & (kpos <= jnp.concatenate([qpos] * group, axis=1))
        t = jnp.where(keep, t, -jnp.inf)
        pbuf[pair, c] = t
        return jnp.maximum(top, jnp.max(t.reshape(grp, 8, width), axis=0))

    def value(pair, c, top, total):
        p = jnp.exp2(pbuf[pair, c] - top)
        oacc[...] += dot_nn(gall[0, c, kv0 + krows:rows, :], p.astype(BF))
        return total + jnp.sum(p.reshape(grp, 8, width), axis=0)

    def grad(pair, c):
        p = jnp.exp2(pbuf[pair, c] - stats[pair, 0:1])
        dp = dot_nn(keys(c), rhsd[pair])
        ds = (p * (dp - stats[pair, 8:9])).astype(BF)
        dqacc[...] += dot_nn(gall[0, c, kv0:kv0 + krows, :], ds)
        pb = p.astype(BF)
        spans = [(slice(j * mcol, (j + 1) * mcol), slice(j * tok, (j + 1) * tok)) for j in range(width // mcol)]
        for qs, place in spans:
            woa[0, :, place] = ds[:, qs].T
            wob[0, :, place] = pb[:, qs].T
        dkacc[c] += sum(dot_nn(rhsq[pair, 0:krows, qs], woa[0, :, place]) for qs, place in spans)
        dvacc[c] += sum(dot_nn(rhsd[pair, krows:2 * krows, qs], wob[0, :, place]) for qs, place in spans)

    def finish_dq(i, pair):
        dq = (dqacc[...] * scale).astype(BF)
        for g in range(group):
            gall[0, i, do_rows(pair, g), :] = dq[:, g * tok:(g + 1) * tok]

    def tile_done(i):
        @pl.when(i == 0)
        def _():
            for t in range(n - 1):
                p_direct(t).wait_send()
            for t in range(2):
                p_second(t).wait_send()
            for peer in (right, left):
                pl.semaphore_signal(free_far, inc=1, device_id={'cp': peer}, device_id_type=pl.DeviceIdType.MESH)
            pl.semaphore_signal(free_par, inc=1, device_id={'cp': partner}, device_id_type=pl.DeviceIdType.MESH)
            pl.semaphore_wait(free_near, 2)

        send_own(0, i)

        @pl.when(i == 1)
        def _():
            for t in range(2):
                for a in range(2):
                    x_first(a, t).wait_recv()
                    x_second(a, t).start()

        @pl.when(i == lag)
        def _():
            pl.semaphore_wait(free_far, 2)

        @pl.when(i >= lag)
        def _():
            serve_near(i - lag)

    def item_step(m, carry):
        i, pair = m // 2, m % 2
        last = 1 - pair
        top0 = jnp.full((8, width), -jnp.inf, F32)

        for g in range(group):
            lanes = slice(g * tok, (g + 1) * tok)
            rhsq[pair, 0:krows, lanes] = gall[0, i, q_rows(pair, g), :]
            rhsd[pair, krows:2 * krows, lanes] = gall[0, i, do_rows(pair, g), :]
        dqacc[...] = jnp.zeros_like(dqacc)

        def both_step(c, top):
            grad(last, c)
            return score(i, pair, c, top, False)

        top = lax.fori_loop(0, i, both_step, top0)
        stats[pair, 16:24] = top

        @pl.when(pair == 1)
        def _():
            grad(last, i)
            stats[pair, 16:24] = score(i, pair, i, stats[pair, 16:24], True)

        @pl.when(pair == 0)
        def _():
            stats[pair, 16:24] = score(i, pair, i, stats[pair, 16:24], True)

        @pl.when(m >= 1)
        def _():
            finish_dq((m - 1) // 2, last)

        top = jnp.max(stats[pair, 16:24], axis=0, keepdims=True)
        oacc[...] = jnp.zeros_like(oacc)
        total = lax.fori_loop(0, i + 1, lambda c, acc: value(pair, c, top, acc), jnp.zeros((8, width), F32))
        total = jnp.sum(total, axis=0, keepdims=True)
        o_blk = (oacc[...] * (1.0 / total)).astype(BF)
        stats[pair, 0:8] = jnp.broadcast_to(top + jnp.log2(total), (8, width))
        delta = jnp.sum(rhsd[pair, krows:2 * krows].astype(F32) * o_blk.astype(F32), axis=0, keepdims=True)
        stats[pair, 8:16] = jnp.broadcast_to(delta, (8, width))
        for g in range(group):
            gall[0, i, q_rows(pair, g), :] = o_blk[:, g * tok:(g + 1) * tok]

        @pl.when((pair == 0) & (i >= 1))
        def _():
            tile_done(i - 1)
        return carry

    lax.fori_loop(0, n * heads // group, item_step, 0)
    dqacc[...] = jnp.zeros_like(dqacc)

    def last_step(c, carry):
        grad(1, c)
        return carry

    lax.fori_loop(0, n, last_step, 0)
    finish_dq(n - 1, 1)
    tile_done(n - 1)
    for c in range(n):
        gall[0, c, kv0:kv0 + krows, :] = (dkacc[c] * scale).astype(BF)
        gall[0, c, kv0 + krows:rows, :] = dvacc[c].astype(BF)
    for j in range(2):
        send_own(1, j)
    for kind in range(3):
        for copy in load(kind, 0, 0):
            copy.start()
    pbuf[0, 0:6] = jnp.zeros((6, tok, width), F32)

    for a in range(2):
        x_own(a).wait()
        for t in range(n - 1):
            x_direct(a, t).wait_recv()

    near = n - 2
    spare = tok - qrows

    def rounded(acc, buf, out, sem):
        for j, cols in parts:
            wide = pbuf[0, acc + j, :, 0:cols.stop - cols.start].astype(BF)
            buf[0, :, cols] = wide[0:qrows]
            buf[1, 0:spare, cols] = wide[qrows:tok]
        return [pltpu.make_async_copy(buf.at[0], out.at[pl.ds(0, qrows)], lsem.at[sem]),
                pltpu.make_async_copy(buf.at[1, pl.ds(0, spare)], out.at[pl.ds(qrows, spare)], lsem.at[sem + 1])]

    def closing_step(r, carry):
        @pl.when(r == 1)
        def _():
            arrived_tiles(4)

        @pl.when(r == 2)
        def _():
            for j in range(n - lag, n):
                serve_near(j)

        @pl.when(r == 4)
        def _():
            pl.semaphore_wait(free_par, 1)
            for j in range(n - 2 * lag):
                serve_far(j)
            arrived_tiles(5)

        @pl.when(r == 5)
        def _():
            arrived_tiles(6)

        @pl.when(r == near)
        def _():
            serve_near_kv()

        @pl.when(r == near + 1)
        def _():
            arrived_kv(4)

        @pl.when(r == near + 4)
        def _():
            arrived_kv(5)
            arrived_kv(6)

        @pl.when(r == 2 * near)
        def _():
            for a in range(2):
                for t in range(n - 1):
                    x_direct(a, t).wait_send()
                for t in range(2):
                    x_second(a, t).wait_send()
            for t in range(n - 1):
                seg_copy(t).wait_send()
            for j in range(n):
                own_right(0, j).wait_send()
                own_left(0, j).wait_send()
                for slot in range(3):
                    to_partner(slot, 0, j).wait_send()
            for j in range(n - 2 * lag):
                relay_plus(0, j).wait_send()
                relay_minus(0, j).wait_send()
            for j in range(n - 2 * lag, n):
                serve_far(j)

        @pl.when(r == 2 * near + 1)
        def _():
            arrived_tiles(7)

        @pl.when((r < near) | ((r >= 2 * near) & (r < 2 * near + 2)))
        def _():
            order = r - near * (r // (2 * near))
            closing_part(0, order)
            closing_part(1, order)

        @pl.when((r >= near) & (r < 2 * near))
        def _():
            closing_part(2, r - near)
        return carry

    lax.fori_loop(0, 2 * near + 2, closing_step, 0)

    def kv_rows(slot):
        return jnp.concatenate([gall[slot, j, kv0:rows, :] for j in range(n)], axis=1)

    out_y = rounded(0, woa, y_ref, 2)
    for copy in out_y + load(2, n - 1, 1):
        copy.start()
    for copy in load(2, n - 2, 0) + load(2, n - 1, 1) + save(2, n - 4, 0) + save(2, n - 3, 1):
        copy.wait()
    serve_far_kv()
    stage(2, 0)[...] = dot_nn(kv_rows(3), xc[...])
    for copy in save(2, n - 2, 0):
        copy.start()
    arrived_kv(7)
    out_dx = []
    for j, cols in parts:
        far = jnp.concatenate([gall[slot, me, kv0:rows, :] for slot in (3, 7)], axis=0)
        size = cols.stop - cols.start
        total = pbuf[0, 3 + j, :, 0:size] + dot_tn(far, woc[:, :, cols].reshape(4 * krows, size))
        wide = total.astype(BF)
        wob[0, :, cols] = wide[0:qrows]
        wob[1, 0:spare, cols] = wide[qrows:tok]
        where = pl.ds(cols.start, size)
        out_dx += [pltpu.make_async_copy(wob.at[0, :, where], dx_ref.at[pl.ds(0, qrows), where], dxsem.at[j, 0]),
                   pltpu.make_async_copy(wob.at[1, pl.ds(0, spare), where], dx_ref.at[pl.ds(qrows, spare), where], dxsem.at[j, 1])]
        for copy in out_dx[-2:]:
            copy.start()
    stage(2, 1)[...] = dot_nn(kv_rows(7), xc[...])
    for copy in save(2, n - 1, 1):
        copy.start()
    for kind in range(3):
        for order in (n - 2, n - 1):
            for copy in save(kind, order, order % 2):
                copy.wait()
    for copy in out_y + out_dx:
        copy.wait()
    for j in range(n):
        to_partner(3, 0, j).wait_send()
    for j in range(n - 2 * lag, n):
        relay_plus(0, j).wait_send()
        relay_minus(0, j).wait_send()
    for j in range(2):
        for slot in range(4):
            to_partner(slot, 1, j).wait_send()
        own_right(1, j).wait_send()
        own_left(1, j).wait_send()
    relay_plus(1, 0).wait_send()
    relay_minus(1, 1).wait_send()


def attention_layer(n, x_act, dy_act, seg, wq, wk, wv, wo):
    tok, model = x_act.shape
    qrows, krows = wq.shape[0] // n, wk.shape[0] // n
    rows = 2 * qrows + 2 * krows
    total = n * tok
    mcol = model // n
    group = 2
    width = group * tok
    vmem = pl.BlockSpec(memory_space=pltpu.VMEM)
    anym = pl.BlockSpec(memory_space=pl.ANY)
    dma = pltpu.SemaphoreType.DMA
    return pl.pallas_call(
        functools.partial(main_kernel, (n, qrows, krows, tok, krows ** -0.5)),
        out_shape=(jax.ShapeDtypeStruct((tok, model), BF), jax.ShapeDtypeStruct((tok, model), BF),
                   jax.ShapeDtypeStruct((wq.shape[0], mcol), F32), jax.ShapeDtypeStruct((wk.shape[0], mcol), F32),
                   jax.ShapeDtypeStruct((wv.shape[0], mcol), F32), jax.ShapeDtypeStruct((wo.shape[0], mcol), F32)),
        in_specs=[anym, anym, vmem, anym, anym, anym, anym],
        out_specs=(anym,) * 6,
        scratch_shapes=[
            pltpu.VMEM((8, tok), jnp.int32), pltpu.VMEM((n, 8, tok), jnp.int32), pltpu.VMEM((n, 8, tok), jnp.int32),
            pltpu.VMEM((total, 2 * krows), BF),
            pltpu.VMEM((2, n, tok, width), F32),
            pltpu.VMEM((2, 2 * krows, width), BF), pltpu.VMEM((2, 2 * krows, width), BF),
            pltpu.VMEM((2, 24, width), F32),
            pltpu.VMEM((krows, width), F32), pltpu.VMEM((krows, width), F32),
            pltpu.VMEM((n, krows, tok), F32), pltpu.VMEM((n, krows, tok), F32),
            pltpu.VMEM((n, n, rows, tok), BF),
            pltpu.VMEM((total, mcol), BF), pltpu.VMEM((total, mcol), BF),
            pltpu.VMEM((2, 2, tok, mcol), BF),
            pltpu.VMEM((2, qrows, model), BF), pltpu.VMEM((2, qrows, model), BF), pltpu.VMEM((2, 2 * krows, model), BF),
            dma((4, 2)), dma((4, 2)),
            dma((2, 2, n)), dma((2, 2, n)), dma((4, 2, n)), dma((8, 2, n)),
            dma((2, n)), dma((2, n)), dma((2, 2)), dma((2, 2)), dma((6,)), dma((3, 2)), dma((2, n)),
            dma((n,)), dma((n,)), dma((2,)), dma((2,)), dma((n,)), dma((n,)),
            pltpu.SemaphoreType.REGULAR, pltpu.SemaphoreType.REGULAR, pltpu.SemaphoreType.REGULAR,
        ],
        compiler_params=pltpu.CompilerParams(collective_id=0, has_side_effects=True, vmem_limit_bytes=VMEM_MAX),
        name='attention_layer',
    )(x_act, dy_act, seg, wq, wk, wv, wo)


def copy_out(arrays):
    pieces = 4
    count = len(arrays)

    def kernel(*refs):
        src, dst, buf = refs[:count], refs[count:2 * count], refs[2 * count:3 * count]
        insem, outsem = refs[3 * count:]
        loads, stores = [], []
        for k, array in enumerate(arrays):
            size = array.shape[0] // pieces
            for p in range(pieces):
                rows = pl.ds(p * size, size)
                loads.append(pltpu.make_async_copy(src[k].at[rows], buf[k].at[rows], insem.at[k, p]))
                stores.append(pltpu.make_async_copy(buf[k].at[rows], dst[k].at[rows], outsem.at[k, p]))
        for copy in loads:
            copy.start()
        for copy, store in zip(loads, stores):
            copy.wait()
            store.start()
        for store in stores:
            store.wait()

    anym = pl.BlockSpec(memory_space=pl.ANY)
    return pl.pallas_call(
        kernel,
        out_shape=tuple(jax.ShapeDtypeStruct(a.shape, a.dtype) for a in arrays),
        in_specs=[anym] * count, out_specs=(anym,) * count,
        scratch_shapes=[pltpu.VMEM(a.shape, a.dtype) for a in arrays]
        + [pltpu.SemaphoreType.DMA((count, pieces)), pltpu.SemaphoreType.DMA((count, pieces))],
        compiler_params=pltpu.CompilerParams(vmem_limit_bytes=VMEM_MAX),
        name='copy_out',
    )(*arrays)


def solution(mesh):
    n = mesh.shape['cp']
    row_spec = P(('dp', 'cp'), None)
    tok_spec = P(('dp', 'cp'))
    weight_spec = P(None, None, None)
    grad_spec = P(('dp', 'cp'), None, None)

    def local_step(x_act, seg_ids, w_q, w_k, w_v, w_o, dy_act):
        model, q_heads, head_dim = w_q.shape
        kv_heads = w_k.shape[1]
        assert kv_heads == n and x_act.shape[0] % LANES == 0

        def flat(w):
            return w.transpose(1, 2, 0).reshape(w.shape[1] * head_dim, model)

        def unflat(g, heads):
            return g.reshape(heads, head_dim, g.shape[1]).transpose(2, 0, 1)

        wq, wk, wv, wo = flat(w_q), flat(w_k), flat(w_v), flat(w_o)
        y_out, dx_out, dwq, dwk, dwv, dwo = copy_out(attention_layer(n, x_act, dy_act, seg_ids, wq, wk, wv, wo))
        return (y_out, dx_out, unflat(dwq, q_heads), unflat(dwk, kv_heads), unflat(dwv, kv_heads), unflat(dwo, q_heads))

    return jax.shard_map(local_step, mesh=mesh,
                         in_specs=(row_spec, tok_spec, weight_spec, weight_spec, weight_spec, weight_spec, row_spec),
                         out_specs=(row_spec, row_spec, grad_spec, grad_spec, grad_spec, grad_spec),
                         check_vma=False)
```

```python
import functools

import jax
import jax.numpy as jnp
from jax import lax
from jax.experimental import pallas as pl
from jax.experimental.pallas import tpu as pltpu
from jax.sharding import PartitionSpec as P

BF = jnp.bfloat16
F32 = jnp.float32
LANES = 128
LOG2E = 1.4426950408889634
VMEM_MAX = 67043328


def rdma(src, dst, send_sem, recv_sem, peer):
    return pltpu.make_async_remote_copy(src_ref=src, dst_ref=dst, send_sem=send_sem, recv_sem=recv_sem,
                                        device_id={'cp': peer}, device_id_type=pl.DeviceIdType.MESH)


def dot_nt(left, right):
    return lax.dot_general(left, right, (((1,), (1,)), ((), ())), preferred_element_type=F32)


def dot_tn(left, right):
    return lax.dot_general(left, right, (((0,), (0,)), ((), ())), preferred_element_type=F32)


def dot_nn(left, right):
    return lax.dot_general(left, right, (((1,), (0,)), ((), ())), preferred_element_type=F32)


def pick(index, values):
    out = values[0]
    for k in range(1, len(values)):
        out = jnp.where(index == k, values[k], out)
    return out


def main_kernel(dims, x_ref, dy_ref, seg_ref, wq_ref, wk_ref, wv_ref, wo_ref,
                y_ref, dx_ref, dwq_ref, dwk_ref, dwv_ref, dwo_ref,
                seg_mine, seg_all, first_ref, kvn, pbuf, rhsq, rhsd, stats, oacc, dqacc, dkacc, dvacc, gall, xc, dyc, xrel,
                woa, wob, woc, wsem, outsem, osem, relsem, parsem, rsem, xsend, xrecv, xfirst, xsecond, lsem, dxsem, xload,
                psend, precv, pfirst, psecond, gsend, grecv, free_near, free_far, free_par):
    n, qrows, krows, tok, scale = dims
    chips = n // 2
    heads = qrows // krows
    width = rhsq.shape[2]
    group = width // tok
    me = lax.axis_index('cp')
    chip, core = me // 2, me % 2
    sgn = 1 - 2 * core
    rows = 2 * qrows + 2 * krows
    model = x_ref.shape[1]
    mcol = xc.shape[1]
    do0, kv0 = qrows, 2 * qrows

    def device(chip_off, flip):
        return ((chip + chip_off + chips) % chips) * 2 + (core + flip) % 2

    right, left, partner = device(1, 0), device(-1, 0), device(0, 1)
    dests = [device(2, 0), device(2, 1), device(-sgn, 0), device(-sgn, 1), device(sgn, 0), device(sgn, 1), partner]
    ahead = dests[4]
    relay_from = device(-sgn, 0)

    barrier = pltpu.get_barrier_semaphore()
    for peer in dests:
        pl.semaphore_signal(barrier, inc=1, device_id={'cp': peer}, device_id_type=pl.DeviceIdType.MESH)

    sides = ((x_ref, xc), (dy_ref, dyc))

    def columns(ref, dst):
        return ref.at[:, pl.ds(pl.multiple_of(dst * mcol, LANES), mcol)]

    def token_rows(ref, src):
        return ref.at[pl.ds(pl.multiple_of(src * tok, LANES), tok)]

    def x_first(a, t):
        return rdma(columns(sides[a][0], dests[t]), xrel.at[a, t], xsend.at[a, t], xfirst.at[a, t], ahead)

    def x_second(a, t):
        return rdma(xrel.at[a, t], token_rows(sides[a][1], relay_from), xsecond.at[a, t], xrecv.at[a, t], device(sgn, t))

    def x_direct(a, t):
        return rdma(columns(sides[a][0], dests[t]), token_rows(sides[a][1], me), xsend.at[a, t], xrecv.at[a, t], dests[t])

    def send_columns(a):
        for t in range(n - 1):
            if t != 2:
                (x_first if t < 2 else x_direct)(a, t).start()

    def relay_columns(a):
        for t in range(2):
            x_first(a, t).wait_recv()
            x_second(a, t).start()

    def x_own(a):
        return pltpu.make_async_copy(columns(sides[a][0], me), token_rows(sides[a][1], me), lsem.at[a])

    def view(slot, part, j):
        if part == 0:
            return gall.at[slot, j, pl.ds(0, kv0)]
        return gall.at[slot, pl.ds(j * (n // 2), n // 2), pl.ds(kv0, 2 * krows)]

    def own_right(part, j):
        return rdma(view(0, part, j), view(1, part, j), osem.at[0, part, j], rsem.at[1, part, j], right)

    def own_left(part, j):
        return rdma(view(0, part, j), view(2, part, j), osem.at[1, part, j], rsem.at[2, part, j], left)

    def relay_plus(part, j):
        src, dst = view(1, part, j), view(3, part, j)
        if part == 0:
            src, dst = src.at[pl.ds(0, do0)], dst.at[pl.ds(0, do0)]
        return rdma(src, dst, relsem.at[0, part, j], rsem.at[3, part, j], right)

    def relay_minus(part, j):
        src, dst = view(2, part, j), view(3, part, j)
        if part == 0:
            src, dst = src.at[pl.ds(do0, do0)], dst.at[pl.ds(do0, do0)]
        return rdma(src, dst, relsem.at[1, part, j], rsem.at[0, part, j], left)

    def to_partner(slot, part, j):
        return rdma(view(slot, part, j), view(4 + slot, part, j), parsem.at[slot, part, j], rsem.at[4 + slot, part, j], partner)

    def send_own(part, j):
        own_right(part, j).start()
        own_left(part, j).start()
        to_partner(0, part, j).start()

    def serve_near(j):
        own_right(0, j).wait_recv()
        relay_plus(0, j).start()
        to_partner(1, 0, j).start()
        own_left(0, j).wait_recv()
        relay_minus(0, j).start()
        to_partner(2, 0, j).start()

    def serve_near_kv():
        own_right(1, 0).wait_recv()
        relay_plus(1, 0).start()
        own_left(1, 1).wait_recv()
        relay_minus(1, 1).start()
        to_partner(1, 1, 0).start()
        to_partner(2, 1, 1).start()
        own_right(1, 1).wait_recv()
        to_partner(1, 1, 1).start()
        own_left(1, 0).wait_recv()
        to_partner(2, 1, 0).start()

    def serve_far(j):
        relay_plus(0, j).wait_recv()
        relay_minus(0, j).wait_recv()
        to_partner(3, 0, j).start()

    def serve_far_kv():
        relay_plus(1, 0).wait_recv()
        to_partner(3, 1, 0).start()
        relay_minus(1, 1).wait_recv()
        to_partner(3, 1, 1).start()

    def arrived_tiles(slot):
        for j in range(n):
            to_partner(slot - 4, 0, j).wait_recv()

    def arrived_kv(slot):
        for j in range(2):
            to_partner(slot - 4, 1, j).wait_recv()

    slot_table = (0, 4, 1, 2, 5, 6, 3, 7)
    off_table = (0, 0, chips - 1, 1, chips - 1, 1, 2, 2)
    flip_table = (0, 1, 0, 0, 1, 1, 0, 1)

    def source_of(order):
        return ((chip + pick(order, off_table)) % chips) * 2 + (core + pick(order, flip_table)) % 2

    def load(kind, order, buf):
        src = source_of(order)
        if kind == 0:
            return [pltpu.make_async_copy(wo_ref.at[pl.ds(src * qrows, qrows)], woa.at[buf], wsem.at[0, buf])]
        if kind == 1:
            return [pltpu.make_async_copy(wq_ref.at[pl.ds(src * qrows, qrows)], wob.at[buf], wsem.at[1, buf])]
        return [pltpu.make_async_copy(wk_ref.at[pl.ds(src * krows, krows)], woc.at[buf, pl.ds(0, krows)], wsem.at[2, buf]),
                pltpu.make_async_copy(wv_ref.at[pl.ds(src * krows, krows)], woc.at[buf, pl.ds(krows, krows)], wsem.at[3, buf])]

    def stage(kind, buf):
        if kind < 2:
            return pbuf.at[0, 6 + kind, pl.ds(0, qrows), pl.ds(pl.multiple_of(buf * mcol, LANES), mcol)]
        return pbuf.at[0, 6, pl.ds(pl.multiple_of(buf * 2 * krows, 8), 2 * krows), pl.ds(2 * mcol, mcol)]

    def save(kind, order, buf):
        src = source_of(order)
        if kind == 0:
            return [pltpu.make_async_copy(stage(0, buf), dwo_ref.at[pl.ds(src * qrows, qrows)], outsem.at[0, buf])]
        if kind == 1:
            return [pltpu.make_async_copy(stage(1, buf), dwq_ref.at[pl.ds(src * qrows, qrows)], outsem.at[1, buf])]
        both = stage(2, buf)
        return [pltpu.make_async_copy(both.at[pl.ds(0, krows)], dwk_ref.at[pl.ds(src * krows, krows)], outsem.at[2, buf]),
                pltpu.make_async_copy(both.at[pl.ds(krows, krows)], dwv_ref.at[pl.ds(src * krows, krows)], outsem.at[3, buf])]

    parts = [(j, slice(j * width, min((j + 1) * width, model))) for j in range(-(-model // width))]
    kinds = ((0, do0, woa, dyc, 0), (do0, kv0, wob, xc, 3), (kv0, rows, woc, xc, 3))

    def closing_part(kind, order):
        row0, row1, wbuf, other, acc = kinds[kind]
        buf = order % 2
        slot = pick(order, slot_table)
        for copy in load(kind, order, buf):
            copy.wait()

        @pl.when(order < n - 1)
        def _():
            for copy in load(kind, order + 1, 1 - buf):
                copy.start()

        @pl.when(order >= 2)
        def _():
            for copy in save(kind, order - 2, buf):
                copy.wait()

        @pl.when(order >= 0)
        def _():
            wide = jnp.concatenate([gall[slot, j, row0:row1, :] for j in range(n)], axis=1)
            stage(kind, buf)[...] = dot_nn(wide, other[...])

        for copy in save(kind, order, buf):
            copy.start()
        for j, cols in parts:
            @pl.when(order >= 0)
            def _():
                pbuf[0, acc + j, :, 0:cols.stop - cols.start] += dot_tn(gall[slot, me, row0:row1, :], wbuf[buf, :, cols])

    def block_copies(step, buf):
        pair, flip = step // 2, (step + step // 6) % 2
        off = 2 - 3 * pair + 5 * (pair // 2) + 2 * (pair // 3)
        dst = ((chip + sgn * off + chips) % chips) * 2 + (core + flip) % 2
        return [
            pltpu.make_async_copy(wo_ref.at[pl.ds(dst * qrows, qrows)], woa.at[buf], wsem.at[0, buf]),
            pltpu.make_async_copy(wq_ref.at[pl.ds(dst * qrows, qrows)], wob.at[buf], wsem.at[1, buf]),
            pltpu.make_async_copy(wk_ref.at[pl.ds(dst * krows, krows)], woc.at[buf, pl.ds(0, krows)], wsem.at[2, buf]),
            pltpu.make_async_copy(wv_ref.at[pl.ds(dst * krows, krows)], woc.at[buf, pl.ds(krows, krows)], wsem.at[3, buf]),
        ]

    def p_first(t):
        return rdma(gall.at[3, t], gall.at[7, t], psend.at[t], pfirst.at[t], ahead)

    def p_second(t):
        return rdma(gall.at[7, t], gall.at[0, relay_from], psecond.at[t], precv.at[t], device(sgn, t))

    def p_direct(t):
        return rdma(gall.at[3, t], gall.at[0, me], psend.at[t], precv.at[t], dests[t])

    def seg_copy(t):
        row = pl.ds(0, 1)
        return rdma(seg_mine.at[row], seg_all.at[me, row], gsend.at[t], grecv.at[t], dests[t])

    xcols = [(c, c * tok, min(tok, model - c * tok)) for c in range(-(-model // tok))]

    def x_loads(a):
        return [pltpu.make_async_copy(sides[a][0].at[:, pl.ds(lo, size)], gall.at[1 + a, c, pl.ds(0, tok), pl.ds(0, size)],
                                      xload.at[a, c]) for c, lo, size in xcols]

    def x_whole(a):
        return jnp.concatenate([gall[1 + a, c, 0:tok, 0:size] for c, lo, size in xcols], axis=1)

    for copy in x_loads(0):
        copy.start()
    for copy in block_copies(0, 0):
        copy.start()
    for copy in x_loads(1):
        copy.start()
    for a in range(2):
        x_own(a).start()
    seg_mine[...] = jnp.broadcast_to(seg_ref[...].reshape(1, tok), seg_mine.shape)
    pl.semaphore_wait(barrier, n - 1)
    for a in range(2):
        x_direct(a, 2).start()
    for t in range(n - 1):
        seg_copy(t).start()
    seg_all[me] = seg_mine[...]
    for copy in x_loads(0) + x_loads(1):
        copy.wait()

    def project_step(step, carry):
        buf = step % 2

        @pl.when(step < n - 1)
        def _():
            for copy in block_copies(step + 1, 1 - buf):
                copy.start()

        for copy in block_copies(step, buf):
            copy.wait()
        slot = 3 - 3 * (step // (n - 1))
        place = step + (me - step) * (step // (n - 1))
        gall[slot, place, 0:qrows] = dot_nt(wob[buf], x_whole(0)).astype(BF)
        gall[slot, place, kv0:rows] = dot_nt(woc[buf], x_whole(0)).astype(BF)
        gall[slot, place, do0:kv0] = dot_nt(woa[buf], x_whole(1)).astype(BF)
        for t in range(n - 1):
            @pl.when(step == t)
            def _():
                (p_first if t < 2 else p_direct)(t).start()
        return carry

    lax.fori_loop(0, n, project_step, 0)
    for peer in (right, left):
        pl.semaphore_signal(free_near, inc=1, device_id={'cp': peer}, device_id_type=pl.DeviceIdType.MESH)
    for t in range(2):
        p_first(t).wait_recv()
        p_second(t).start()
    send_columns(0)

    for t in range(n - 1):
        seg_copy(t).wait_recv()
    row_id = lax.broadcasted_iota(jnp.int32, (n, tok), 0)
    lane_id = lax.broadcasted_iota(jnp.int32, (n, tok), 1)
    seg = jnp.zeros((n, tok), jnp.int32)
    for d in range(n):
        seg = jnp.where(row_id == d, seg_all[d, 0:1], seg)
    before = jnp.where(lane_id == 0, pltpu.roll(pltpu.roll(seg, 1, 1), 1, 0), pltpu.roll(seg, 1, 1))
    pos = row_id * tok + lane_id
    best = jnp.where((seg != before) & (pos > 0), pos, 0)
    shift = 1
    while shift < tok:
        best = jnp.maximum(best, jnp.where(lane_id >= shift, pltpu.roll(best, shift, 1), 0))
        shift *= 2
    end = jnp.broadcast_to(best[:, tok - 1:tok], (n, tok))
    carry_max = jnp.where(row_id >= 1, pltpu.roll(end, 1, 0), 0)
    shift = 1
    while shift < n:
        carry_max = jnp.maximum(carry_max, jnp.where(row_id >= shift, pltpu.roll(carry_max, shift, 0), 0))
        shift *= 2
    best = jnp.maximum(best, carry_max)
    for d in range(n):
        first_ref[d] = jnp.broadcast_to(best[d:d + 1], (8, tok))
    dkacc[...] = jnp.zeros_like(dkacc)
    dvacc[...] = jnp.zeros_like(dvacc)
    rhsq[...] = jnp.zeros_like(rhsq)
    rhsd[...] = jnp.zeros_like(rhsd)
    for t in range(n - 1):
        p_direct(t).wait_recv()

    def transpose_tile(c, carry):
        kvn[pl.ds(pl.multiple_of(c * tok, LANES), tok), :] = gall[0, c, kv0:rows, :].T
        return carry

    lax.fori_loop(0, n, transpose_tile, 0)
    score_mul = scale * LOG2E
    grp = tok // 8
    lag = 2

    def keys(c):
        return kvn[pl.ds(pl.multiple_of(c * tok, LANES), tok), :]

    def q_rows(pair, g):
        return pl.ds(pl.multiple_of((pair * group + g) * krows, krows), krows)

    def do_rows(pair, g):
        return pl.ds(pl.multiple_of(do0 + (pair * group + g) * krows, krows), krows)

    def doc_starts(i):
        return jnp.concatenate([first_ref[i][0:1]] * group, axis=1)

    def score(i, pair, c, top, diagonal):
        t = dot_nn(keys(c), rhsq[pair]) * score_mul
        kpos = lax.broadcasted_iota(jnp.int32, (tok, width), 0)
        keep = kpos >= doc_starts(i) - c * tok
        if diagonal:
            qpos = lax.broadcasted_iota(jnp.int32, (1, tok), 1)
            keep = keep & (kpos <= jnp.concatenate([qpos] * group, axis=1))
        t = jnp.where(keep, t, -jnp.inf)
        pbuf[pair, c] = t
        return jnp.maximum(top, jnp.max(t.reshape(grp, 8, width), axis=0))

    def value(pair, c, top, total):
        p = jnp.exp2(pbuf[pair, c] - top)
        oacc[...] += dot_nn(gall[0, c, kv0 + krows:rows, :], p.astype(BF))
        return total + jnp.sum(p.reshape(grp, 8, width), axis=0)

    def grad(pair, c):
        p = jnp.exp2(pbuf[pair, c] - stats[pair, 0:1])
        dp = dot_nn(keys(c), rhsd[pair])
        ds = (p * (dp - stats[pair, 8:9])).astype(BF)
        dqacc[...] += dot_nn(gall[0, c, kv0:kv0 + krows, :], ds)
        pb = p.astype(BF)
        spans = [(slice(j * mcol, (j + 1) * mcol), slice(j * tok, (j + 1) * tok)) for j in range(width // mcol)]
        for qs, place in spans:
            woa[0, :, place] = ds[:, qs].T
            wob[0, :, place] = pb[:, qs].T
        dkacc[c] += sum(dot_nn(rhsq[pair, 0:krows, qs], woa[0, :, place]) for qs, place in spans)
        dvacc[c] += sum(dot_nn(rhsd[pair, krows:2 * krows, qs], wob[0, :, place]) for qs, place in spans)

    def finish_dq(i, pair):
        dq = (dqacc[...] * scale).astype(BF)
        for g in range(group):
            gall[0, i, do_rows(pair, g), :] = dq[:, g * tok:(g + 1) * tok]

    def tile_done(i):
        @pl.when(i == 0)
        def _():
            for t in range(n - 1):
                p_direct(t).wait_send()
            for t in range(2):
                p_second(t).wait_send()
            for peer in (right, left):
                pl.semaphore_signal(free_far, inc=1, device_id={'cp': peer}, device_id_type=pl.DeviceIdType.MESH)
            pl.semaphore_signal(free_par, inc=1, device_id={'cp': partner}, device_id_type=pl.DeviceIdType.MESH)
            pl.semaphore_wait(free_near, 2)

        send_own(0, i)

        @pl.when(i == 1)
        def _():
            relay_columns(0)

        @pl.when(i == 3)
        def _():
            send_columns(1)

        @pl.when(i == 5)
        def _():
            relay_columns(1)

        @pl.when(i == lag)
        def _():
            pl.semaphore_wait(free_far, 2)

        @pl.when(i >= lag)
        def _():
            serve_near(i - lag)

    def item_step(m, carry):
        i, pair = m // 2, m % 2
        last = 1 - pair
        top0 = jnp.full((8, width), -jnp.inf, F32)

        for g in range(group):
            lanes = slice(g * tok, (g + 1) * tok)
            rhsq[pair, 0:krows, lanes] = gall[0, i, q_rows(pair, g), :]
            rhsd[pair, krows:2 * krows, lanes] = gall[0, i, do_rows(pair, g), :]
        dqacc[...] = jnp.zeros_like(dqacc)

        def both_step(c, top):
            grad(last, c)
            return score(i, pair, c, top, False)

        top = lax.fori_loop(0, i, both_step, top0)
        stats[pair, 16:24] = top

        @pl.when(pair == 1)
        def _():
            grad(last, i)
            stats[pair, 16:24] = score(i, pair, i, stats[pair, 16:24], True)

        @pl.when(pair == 0)
        def _():
            stats[pair, 16:24] = score(i, pair, i, stats[pair, 16:24], True)

        @pl.when(m >= 1)
        def _():
            finish_dq((m - 1) // 2, last)

        top = jnp.max(stats[pair, 16:24], axis=0, keepdims=True)
        oacc[...] = jnp.zeros_like(oacc)
        total = lax.fori_loop(0, i + 1, lambda c, acc: value(pair, c, top, acc), jnp.zeros((8, width), F32))
        total = jnp.sum(total, axis=0, keepdims=True)
        o_blk = (oacc[...] * (1.0 / total)).astype(BF)
        stats[pair, 0:8] = jnp.broadcast_to(top + jnp.log2(total), (8, width))
        delta = jnp.sum(rhsd[pair, krows:2 * krows].astype(F32) * o_blk.astype(F32), axis=0, keepdims=True)
        stats[pair, 8:16] = jnp.broadcast_to(delta, (8, width))
        for g in range(group):
            gall[0, i, q_rows(pair, g), :] = o_blk[:, g * tok:(g + 1) * tok]

        @pl.when((pair == 0) & (i >= 1))
        def _():
            tile_done(i - 1)
        return carry

    lax.fori_loop(0, n * heads // group, item_step, 0)
    dqacc[...] = jnp.zeros_like(dqacc)

    def last_step(c, carry):
        grad(1, c)
        return carry

    lax.fori_loop(0, n, last_step, 0)
    finish_dq(n - 1, 1)
    tile_done(n - 1)
    for c in range(n):
        gall[0, c, kv0:kv0 + krows, :] = (dkacc[c] * scale).astype(BF)
        gall[0, c, kv0 + krows:rows, :] = dvacc[c].astype(BF)
    for j in range(2):
        send_own(1, j)
    for kind in range(3):
        for copy in load(kind, 0, 0):
            copy.start()
    pbuf[0, 0:6] = jnp.zeros((6, tok, width), F32)

    for a in range(2):
        x_own(a).wait()
        for t in range(n - 1):
            x_direct(a, t).wait_recv()

    near = n - 2
    spare = tok - qrows

    def rounded(acc, buf, out, sem):
        for j, cols in parts:
            wide = pbuf[0, acc + j, :, 0:cols.stop - cols.start].astype(BF)
            buf[0, :, cols] = wide[0:qrows]
            buf[1, 0:spare, cols] = wide[qrows:tok]
        return [pltpu.make_async_copy(buf.at[0], out.at[pl.ds(0, qrows)], lsem.at[sem]),
                pltpu.make_async_copy(buf.at[1, pl.ds(0, spare)], out.at[pl.ds(qrows, spare)], lsem.at[sem + 1])]

    def closing_step(r, carry):
        @pl.when(r == 1)
        def _():
            arrived_tiles(4)

        @pl.when(r == 2)
        def _():
            for j in range(n - lag, n):
                serve_near(j)

        @pl.when(r == 4)
        def _():
            pl.semaphore_wait(free_par, 1)
            for j in range(n - 2 * lag):
                serve_far(j)
            arrived_tiles(5)

        @pl.when(r == 5)
        def _():
            arrived_tiles(6)

        @pl.when(r == near)
        def _():
            serve_near_kv()

        @pl.when(r == near + 1)
        def _():
            arrived_kv(4)

        @pl.when(r == near + 4)
        def _():
            arrived_kv(5)
            arrived_kv(6)

        @pl.when(r == 2 * near)
        def _():
            for a in range(2):
                for t in range(n - 1):
                    x_direct(a, t).wait_send()
                for t in range(2):
                    x_second(a, t).wait_send()
            for t in range(n - 1):
                seg_copy(t).wait_send()
            for j in range(n):
                own_right(0, j).wait_send()
                own_left(0, j).wait_send()
                for slot in range(3):
                    to_partner(slot, 0, j).wait_send()
            for j in range(n - 2 * lag):
                relay_plus(0, j).wait_send()
                relay_minus(0, j).wait_send()
            for j in range(n - 2 * lag, n):
                serve_far(j)

        @pl.when(r == 2 * near + 1)
        def _():
            arrived_tiles(7)

        @pl.when((r < near) | ((r >= 2 * near) & (r < 2 * near + 2)))
        def _():
            order = r - near * (r // (2 * near))
            closing_part(0, order)
            closing_part(1, order)

        @pl.when((r >= near) & (r < 2 * near))
        def _():
            closing_part(2, r - near)
        return carry

    lax.fori_loop(0, 2 * near + 2, closing_step, 0)

    def kv_rows(slot):
        return jnp.concatenate([gall[slot, j, kv0:rows, :] for j in range(n)], axis=1)

    out_y = rounded(0, woa, y_ref, 2)
    for copy in out_y + load(2, n - 1, 1):
        copy.start()
    for copy in load(2, n - 2, 0) + load(2, n - 1, 1) + save(2, n - 4, 0) + save(2, n - 3, 1):
        copy.wait()
    serve_far_kv()
    stage(2, 0)[...] = dot_nn(kv_rows(3), xc[...])
    for copy in save(2, n - 2, 0):
        copy.start()
    arrived_kv(7)
    out_dx = []
    for j, cols in parts:
        far = jnp.concatenate([gall[slot, me, kv0:rows, :] for slot in (3, 7)], axis=0)
        size = cols.stop - cols.start
        total = pbuf[0, 3 + j, :, 0:size] + dot_tn(far, woc[:, :, cols].reshape(4 * krows, size))
        wide = total.astype(BF)
        wob[0, :, cols] = wide[0:qrows]
        wob[1, 0:spare, cols] = wide[qrows:tok]
        where = pl.ds(cols.start, size)
        out_dx += [pltpu.make_async_copy(wob.at[0, :, where], dx_ref.at[pl.ds(0, qrows), where], dxsem.at[j, 0]),
                   pltpu.make_async_copy(wob.at[1, pl.ds(0, spare), where], dx_ref.at[pl.ds(qrows, spare), where], dxsem.at[j, 1])]
        for copy in out_dx[-2:]:
            copy.start()
    stage(2, 1)[...] = dot_nn(kv_rows(7), xc[...])
    for copy in save(2, n - 1, 1):
        copy.start()
    for kind in range(3):
        for order in (n - 2, n - 1):
            for copy in save(kind, order, order % 2):
                copy.wait()
    for copy in out_y + out_dx:
        copy.wait()
    for j in range(n):
        to_partner(3, 0, j).wait_send()
    for j in range(n - 2 * lag, n):
        relay_plus(0, j).wait_send()
        relay_minus(0, j).wait_send()
    for j in range(2):
        for slot in range(4):
            to_partner(slot, 1, j).wait_send()
        own_right(1, j).wait_send()
        own_left(1, j).wait_send()
    relay_plus(1, 0).wait_send()
    relay_minus(1, 1).wait_send()


def attention_layer(n, x_act, dy_act, seg, wq, wk, wv, wo):
    tok, model = x_act.shape
    qrows, krows = wq.shape[0] // n, wk.shape[0] // n
    rows = 2 * qrows + 2 * krows
    total = n * tok
    mcol = model // n
    group = 2
    width = group * tok
    vmem = pl.BlockSpec(memory_space=pltpu.VMEM)
    anym = pl.BlockSpec(memory_space=pl.ANY)
    dma = pltpu.SemaphoreType.DMA
    return pl.pallas_call(
        functools.partial(main_kernel, (n, qrows, krows, tok, krows ** -0.5)),
        out_shape=(jax.ShapeDtypeStruct((tok, model), BF), jax.ShapeDtypeStruct((tok, model), BF),
                   jax.ShapeDtypeStruct((wq.shape[0], mcol), F32), jax.ShapeDtypeStruct((wk.shape[0], mcol), F32),
                   jax.ShapeDtypeStruct((wv.shape[0], mcol), F32), jax.ShapeDtypeStruct((wo.shape[0], mcol), F32)),
        in_specs=[anym, anym, vmem, anym, anym, anym, anym],
        out_specs=(anym,) * 6,
        scratch_shapes=[
            pltpu.VMEM((8, tok), jnp.int32), pltpu.VMEM((n, 8, tok), jnp.int32), pltpu.VMEM((n, 8, tok), jnp.int32),
            pltpu.VMEM((total, 2 * krows), BF),
            pltpu.VMEM((2, n, tok, width), F32),
            pltpu.VMEM((2, 2 * krows, width), BF), pltpu.VMEM((2, 2 * krows, width), BF),
            pltpu.VMEM((2, 24, width), F32),
            pltpu.VMEM((krows, width), F32), pltpu.VMEM((krows, width), F32),
            pltpu.VMEM((n, krows, tok), F32), pltpu.VMEM((n, krows, tok), F32),
            pltpu.VMEM((n, n, rows, tok), BF),
            pltpu.VMEM((total, mcol), BF), pltpu.VMEM((total, mcol), BF),
            pltpu.VMEM((2, 2, tok, mcol), BF),
            pltpu.VMEM((2, qrows, model), BF), pltpu.VMEM((2, qrows, model), BF), pltpu.VMEM((2, 2 * krows, model), BF),
            dma((4, 2)), dma((4, 2)),
            dma((2, 2, n)), dma((2, 2, n)), dma((4, 2, n)), dma((8, 2, n)),
            dma((2, n)), dma((2, n)), dma((2, 2)), dma((2, 2)), dma((6,)), dma((3, 2)), dma((2, n)),
            dma((n,)), dma((n,)), dma((2,)), dma((2,)), dma((n,)), dma((n,)),
            pltpu.SemaphoreType.REGULAR, pltpu.SemaphoreType.REGULAR, pltpu.SemaphoreType.REGULAR,
        ],
        compiler_params=pltpu.CompilerParams(collective_id=0, has_side_effects=True, vmem_limit_bytes=VMEM_MAX),
        name='attention_layer',
    )(x_act, dy_act, seg, wq, wk, wv, wo)


def copy_out(arrays):
    pieces = 4
    count = len(arrays)

    def kernel(*refs):
        src, dst, buf = refs[:count], refs[count:2 * count], refs[2 * count:3 * count]
        insem, outsem = refs[3 * count:]
        loads, stores = [], []
        for k, array in enumerate(arrays):
            size = array.shape[0] // pieces
            for p in range(pieces):
                rows = pl.ds(p * size, size)
                loads.append(pltpu.make_async_copy(src[k].at[rows], buf[k].at[rows], insem.at[k, p]))
                stores.append(pltpu.make_async_copy(buf[k].at[rows], dst[k].at[rows], outsem.at[k, p]))
        for copy in loads:
            copy.start()
        for copy, store in zip(loads, stores):
            copy.wait()
            store.start()
        for store in stores:
            store.wait()

    anym = pl.BlockSpec(memory_space=pl.ANY)
    return pl.pallas_call(
        kernel,
        out_shape=tuple(jax.ShapeDtypeStruct(a.shape, a.dtype) for a in arrays),
        in_specs=[anym] * count, out_specs=(anym,) * count,
        scratch_shapes=[pltpu.VMEM(a.shape, a.dtype) for a in arrays]
        + [pltpu.SemaphoreType.DMA((count, pieces)), pltpu.SemaphoreType.DMA((count, pieces))],
        compiler_params=pltpu.CompilerParams(vmem_limit_bytes=VMEM_MAX),
        name='copy_out',
    )(*arrays)


def solution(mesh):
    n = mesh.shape['cp']
    row_spec = P(('dp', 'cp'), None)
    tok_spec = P(('dp', 'cp'))
    weight_spec = P(None, None, None)
    grad_spec = P(('dp', 'cp'), None, None)

    def local_step(x_act, seg_ids, w_q, w_k, w_v, w_o, dy_act):
        model, q_heads, head_dim = w_q.shape
        kv_heads = w_k.shape[1]
        assert kv_heads == n and x_act.shape[0] % LANES == 0

        def flat(w):
            return w.transpose(1, 2, 0).reshape(w.shape[1] * head_dim, model)

        def unflat(g, heads):
            return g.reshape(heads, head_dim, g.shape[1]).transpose(2, 0, 1)

        wq, wk, wv, wo = flat(w_q), flat(w_k), flat(w_v), flat(w_o)
        y_out, dx_out, dwq, dwk, dwv, dwo = copy_out(attention_layer(n, x_act, dy_act, seg_ids, wq, wk, wv, wo))
        return (y_out, dx_out, unflat(dwq, q_heads), unflat(dwk, kv_heads), unflat(dwv, kv_heads), unflat(dwo, q_heads))

    return jax.shard_map(local_step, mesh=mesh,
                         in_specs=(row_spec, tok_spec, weight_spec, weight_spec, weight_spec, weight_spec, row_spec),
                         out_specs=(row_spec, row_spec, grad_spec, grad_spec, grad_spec, grad_spec),
                         check_vma=False)
```

```python
import functools

import jax
import jax.numpy as jnp
from jax import lax
from jax.experimental import pallas as pl
from jax.experimental.pallas import tpu as pltpu
from jax.sharding import PartitionSpec as P

BF = jnp.bfloat16
F32 = jnp.float32
LANES = 128
LOG2E = 1.4426950408889634
VMEM_MAX = 67043328


def rdma(src, dst, send_sem, recv_sem, peer):
    return pltpu.make_async_remote_copy(src_ref=src, dst_ref=dst, send_sem=send_sem, recv_sem=recv_sem,
                                        device_id={'cp': peer}, device_id_type=pl.DeviceIdType.MESH)


def dot_nt(left, right):
    return lax.dot_general(left, right, (((1,), (1,)), ((), ())), preferred_element_type=F32)


def dot_tn(left, right):
    return lax.dot_general(left, right, (((0,), (0,)), ((), ())), preferred_element_type=F32)


def dot_nn(left, right):
    return lax.dot_general(left, right, (((1,), (0,)), ((), ())), preferred_element_type=F32)


def pick(index, values):
    out = values[0]
    for k in range(1, len(values)):
        out = jnp.where(index == k, values[k], out)
    return out


def main_kernel(dims, x_ref, dy_ref, seg_ref, wq_ref, wk_ref, wv_ref, wo_ref,
                y_ref, dx_ref, dwq_ref, dwk_ref, dwv_ref, dwo_ref,
                seg_mine, seg_all, first_ref, kn, vn, pbuf, rhsq, rhsd, stats, oacc, dqacc, dkacc, dvacc, gall, xc, dyc, xrel,
                woa, wob, woc, wsem, outsem, osem, relsem, parsem, rsem, xsend, xrecv, xfirst, xsecond, lsem, dxsem, xload,
                psend, precv, pfirst, psecond, gsend, grecv, free_near, free_far, free_par):
    n, qrows, krows, tok, scale = dims
    chips = n // 2
    heads = qrows // krows
    width = rhsq.shape[2]
    group = width // tok
    me = lax.axis_index('cp')
    chip, core = me // 2, me % 2
    sgn = 1 - 2 * core
    rows = 2 * qrows + 2 * krows
    model = x_ref.shape[1]
    mcol = xc.shape[1]
    do0, kv0 = qrows, 2 * qrows

    def device(chip_off, flip):
        return ((chip + chip_off + chips) % chips) * 2 + (core + flip) % 2

    right, left, partner = device(1, 0), device(-1, 0), device(0, 1)
    dests = [device(2, 0), device(2, 1), device(-sgn, 0), device(-sgn, 1), device(sgn, 0), device(sgn, 1), partner]
    ahead = dests[4]
    relay_from = device(-sgn, 0)

    barrier = pltpu.get_barrier_semaphore()
    for peer in dests:
        pl.semaphore_signal(barrier, inc=1, device_id={'cp': peer}, device_id_type=pl.DeviceIdType.MESH)

    sides = ((x_ref, xc), (dy_ref, dyc))

    def columns(ref, dst):
        return ref.at[:, pl.ds(pl.multiple_of(dst * mcol, LANES), mcol)]

    def token_rows(ref, src):
        return ref.at[pl.ds(pl.multiple_of(src * tok, LANES), tok)]

    def x_first(a, t):
        return rdma(columns(sides[a][0], dests[t]), xrel.at[a, t], xsend.at[a, t], xfirst.at[a, t], ahead)

    def x_second(a, t):
        return rdma(xrel.at[a, t], token_rows(sides[a][1], relay_from), xsecond.at[a, t], xrecv.at[a, t], device(sgn, t))

    def x_direct(a, t):
        return rdma(columns(sides[a][0], dests[t]), token_rows(sides[a][1], me), xsend.at[a, t], xrecv.at[a, t], dests[t])

    def send_columns(a):
        for t in range(n - 1):
            if t != 2:
                (x_first if t < 2 else x_direct)(a, t).start()

    def relay_columns(a):
        for t in range(2):
            x_first(a, t).wait_recv()
            x_second(a, t).start()

    def x_own(a):
        return pltpu.make_async_copy(columns(sides[a][0], me), token_rows(sides[a][1], me), lsem.at[a])

    def view(slot, part, j):
        if part == 0:
            return gall.at[slot, j, pl.ds(0, kv0)]
        return gall.at[slot, pl.ds(j * (n // 2), n // 2), pl.ds(kv0, 2 * krows)]

    def own_right(part, j):
        return rdma(view(0, part, j), view(1, part, j), osem.at[0, part, j], rsem.at[1, part, j], right)

    def own_left(part, j):
        return rdma(view(0, part, j), view(2, part, j), osem.at[1, part, j], rsem.at[2, part, j], left)

    def relay_plus(part, j):
        src, dst = view(1, part, j), view(3, part, j)
        if part == 0:
            src, dst = src.at[pl.ds(0, do0)], dst.at[pl.ds(0, do0)]
        return rdma(src, dst, relsem.at[0, part, j], rsem.at[3, part, j], right)

    def relay_minus(part, j):
        src, dst = view(2, part, j), view(3, part, j)
        if part == 0:
            src, dst = src.at[pl.ds(do0, do0)], dst.at[pl.ds(do0, do0)]
        return rdma(src, dst, relsem.at[1, part, j], rsem.at[0, part, j], left)

    def to_partner(slot, part, j):
        return rdma(view(slot, part, j), view(4 + slot, part, j), parsem.at[slot, part, j], rsem.at[4 + slot, part, j], partner)

    def send_own(part, j):
        own_right(part, j).start()
        own_left(part, j).start()
        to_partner(0, part, j).start()

    def serve_near(j):
        own_right(0, j).wait_recv()
        relay_plus(0, j).start()
        to_partner(1, 0, j).start()
        own_left(0, j).wait_recv()
        relay_minus(0, j).start()
        to_partner(2, 0, j).start()

    def serve_near_kv():
        own_right(1, 0).wait_recv()
        relay_plus(1, 0).start()
        own_left(1, 1).wait_recv()
        relay_minus(1, 1).start()
        to_partner(1, 1, 0).start()
        to_partner(2, 1, 1).start()
        own_right(1, 1).wait_recv()
        to_partner(1, 1, 1).start()
        own_left(1, 0).wait_recv()
        to_partner(2, 1, 0).start()

    def serve_far(j):
        relay_plus(0, j).wait_recv()
        relay_minus(0, j).wait_recv()
        to_partner(3, 0, j).start()

    def serve_far_kv():
        relay_plus(1, 0).wait_recv()
        to_partner(3, 1, 0).start()
        relay_minus(1, 1).wait_recv()
        to_partner(3, 1, 1).start()

    def arrived_tiles(slot):
        for j in range(n):
            to_partner(slot - 4, 0, j).wait_recv()

    def arrived_kv(slot):
        for j in range(2):
            to_partner(slot - 4, 1, j).wait_recv()

    slot_table = (0, 4, 1, 2, 5, 6, 3, 7)
    off_table = (0, 0, chips - 1, 1, chips - 1, 1, 2, 2)
    flip_table = (0, 1, 0, 0, 1, 1, 0, 1)

    def source_of(order):
        return ((chip + pick(order, off_table)) % chips) * 2 + (core + pick(order, flip_table)) % 2

    def load(kind, order, buf):
        src = source_of(order)
        if kind == 0:
            return [pltpu.make_async_copy(wo_ref.at[pl.ds(src * qrows, qrows)], woa.at[buf], wsem.at[0, buf])]
        if kind == 1:
            return [pltpu.make_async_copy(wq_ref.at[pl.ds(src * qrows, qrows)], wob.at[buf], wsem.at[1, buf])]
        return [pltpu.make_async_copy(wk_ref.at[pl.ds(src * krows, krows)], woc.at[buf, pl.ds(0, krows)], wsem.at[2, buf]),
                pltpu.make_async_copy(wv_ref.at[pl.ds(src * krows, krows)], woc.at[buf, pl.ds(krows, krows)], wsem.at[3, buf])]

    def stage(kind, buf):
        if kind < 2:
            return pbuf.at[0, 6 + kind, pl.ds(0, qrows), pl.ds(pl.multiple_of(buf * mcol, LANES), mcol)]
        return pbuf.at[0, 6, pl.ds(pl.multiple_of(buf * 2 * krows, 8), 2 * krows), pl.ds(2 * mcol, mcol)]

    def save(kind, order, buf):
        src = source_of(order)
        if kind == 0:
            return [pltpu.make_async_copy(stage(0, buf), dwo_ref.at[pl.ds(src * qrows, qrows)], outsem.at[0, buf])]
        if kind == 1:
            return [pltpu.make_async_copy(stage(1, buf), dwq_ref.at[pl.ds(src * qrows, qrows)], outsem.at[1, buf])]
        both = stage(2, buf)
        return [pltpu.make_async_copy(both.at[pl.ds(0, krows)], dwk_ref.at[pl.ds(src * krows, krows)], outsem.at[2, buf]),
                pltpu.make_async_copy(both.at[pl.ds(krows, krows)], dwv_ref.at[pl.ds(src * krows, krows)], outsem.at[3, buf])]

    parts = [(j, slice(j * width, min((j + 1) * width, model))) for j in range(-(-model // width))]
    kinds = ((0, do0, woa, dyc, 0), (do0, kv0, wob, xc, 3), (kv0, rows, woc, xc, 3))

    def closing_part(kind, order):
        row0, row1, wbuf, other, acc = kinds[kind]
        buf = order % 2
        slot = pick(order, slot_table)
        for copy in load(kind, order, buf):
            copy.wait()

        @pl.when(order < n - 1)
        def _():
            for copy in load(kind, order + 1, 1 - buf):
                copy.start()

        @pl.when(order >= 2)
        def _():
            for copy in save(kind, order - 2, buf):
                copy.wait()

        @pl.when(order >= 0)
        def _():
            wide = jnp.concatenate([gall[slot, j, row0:row1, :] for j in range(n)], axis=1)
            stage(kind, buf)[...] = dot_nn(wide, other[...])

        for copy in save(kind, order, buf):
            copy.start()
        for j, cols in parts:
            @pl.when(order >= 0)
            def _():
                pbuf[0, acc + j, :, 0:cols.stop - cols.start] += dot_tn(gall[slot, me, row0:row1, :], wbuf[buf, :, cols])

    def block_copies(step, buf):
        pair, flip = step // 2, (step + step // 6) % 2
        off = 2 - 3 * pair + 5 * (pair // 2) + 2 * (pair // 3)
        dst = ((chip + sgn * off + chips) % chips) * 2 + (core + flip) % 2
        return [
            pltpu.make_async_copy(wo_ref.at[pl.ds(dst * qrows, qrows)], woa.at[buf], wsem.at[0, buf]),
            pltpu.make_async_copy(wq_ref.at[pl.ds(dst * qrows, qrows)], wob.at[buf], wsem.at[1, buf]),
            pltpu.make_async_copy(wk_ref.at[pl.ds(dst * krows, krows)], woc.at[buf, pl.ds(0, krows)], wsem.at[2, buf]),
            pltpu.make_async_copy(wv_ref.at[pl.ds(dst * krows, krows)], woc.at[buf, pl.ds(krows, krows)], wsem.at[3, buf]),
        ]

    def p_first(t):
        return rdma(gall.at[3, t], gall.at[7, t], psend.at[t], pfirst.at[t], ahead)

    def p_second(t):
        return rdma(gall.at[7, t], gall.at[0, relay_from], psecond.at[t], precv.at[t], device(sgn, t))

    def p_direct(t):
        return rdma(gall.at[3, t], gall.at[0, me], psend.at[t], precv.at[t], dests[t])

    def seg_copy(t):
        row = pl.ds(0, 1)
        return rdma(seg_mine.at[row], seg_all.at[me, row], gsend.at[t], grecv.at[t], dests[t])

    xcols = [(c, c * tok, min(tok, model - c * tok)) for c in range(-(-model // tok))]

    def x_loads(a):
        return [pltpu.make_async_copy(sides[a][0].at[:, pl.ds(lo, size)], gall.at[1 + a, c, pl.ds(0, tok), pl.ds(0, size)],
                                      xload.at[a, c]) for c, lo, size in xcols]

    def x_whole(a):
        return jnp.concatenate([gall[1 + a, c, 0:tok, 0:size] for c, lo, size in xcols], axis=1)

    for copy in x_loads(0):
        copy.start()
    for copy in block_copies(0, 0):
        copy.start()
    for copy in x_loads(1):
        copy.start()
    for a in range(2):
        x_own(a).start()
    seg_mine[...] = jnp.broadcast_to(seg_ref[...].reshape(1, tok), seg_mine.shape)
    pl.semaphore_wait(barrier, n - 1)
    for a in range(2):
        x_direct(a, 2).start()
    for t in range(n - 1):
        seg_copy(t).start()
    seg_all[me] = seg_mine[...]
    for copy in x_loads(0) + x_loads(1):
        copy.wait()

    def project_step(step, carry):
        buf = step % 2

        @pl.when(step < n - 1)
        def _():
            for copy in block_copies(step + 1, 1 - buf):
                copy.start()

        for copy in block_copies(step, buf):
            copy.wait()
        slot = 3 - 3 * (step // (n - 1))
        place = step + (me - step) * (step // (n - 1))
        gall[slot, place, 0:qrows] = dot_nt(wob[buf], x_whole(0)).astype(BF)
        gall[slot, place, kv0:rows] = dot_nt(woc[buf], x_whole(0)).astype(BF)
        gall[slot, place, do0:kv0] = dot_nt(woa[buf], x_whole(1)).astype(BF)
        for t in range(n - 1):
            @pl.when(step == t)
            def _():
                (p_first if t < 2 else p_direct)(t).start()
        return carry

    lax.fori_loop(0, n, project_step, 0)
    for peer in (right, left):
        pl.semaphore_signal(free_near, inc=1, device_id={'cp': peer}, device_id_type=pl.DeviceIdType.MESH)
    for t in range(2):
        p_first(t).wait_recv()
        p_second(t).start()
    send_columns(0)

    for t in range(n - 1):
        seg_copy(t).wait_recv()
    row_id = lax.broadcasted_iota(jnp.int32, (n, tok), 0)
    lane_id = lax.broadcasted_iota(jnp.int32, (n, tok), 1)
    seg = jnp.zeros((n, tok), jnp.int32)
    for d in range(n):
        seg = jnp.where(row_id == d, seg_all[d, 0:1], seg)
    before = jnp.where(lane_id == 0, pltpu.roll(pltpu.roll(seg, 1, 1), 1, 0), pltpu.roll(seg, 1, 1))
    pos = row_id * tok + lane_id
    best = jnp.where((seg != before) & (pos > 0), pos, 0)
    shift = 1
    while shift < tok:
        best = jnp.maximum(best, jnp.where(lane_id >= shift, pltpu.roll(best, shift, 1), 0))
        shift *= 2
    end = jnp.broadcast_to(best[:, tok - 1:tok], (n, tok))
    carry_max = jnp.where(row_id >= 1, pltpu.roll(end, 1, 0), 0)
    shift = 1
    while shift < n:
        carry_max = jnp.maximum(carry_max, jnp.where(row_id >= shift, pltpu.roll(carry_max, shift, 0), 0))
        shift *= 2
    best = jnp.maximum(best, carry_max)
    for d in range(n):
        first_ref[d] = jnp.broadcast_to(best[d:d + 1], (8, tok))
    dkacc[...] = jnp.zeros_like(dkacc)
    dvacc[...] = jnp.zeros_like(dvacc)
    for t in range(n - 1):
        p_direct(t).wait_recv()

    def transpose_tile(c, carry):
        here = pl.ds(pl.multiple_of(c * tok, LANES), tok)
        kn[here, :] = gall[0, c, kv0:kv0 + krows, :].T
        vn[here, :] = gall[0, c, kv0 + krows:rows, :].T
        return carry

    lax.fori_loop(0, n, transpose_tile, 0)
    score_mul = scale * LOG2E
    grp = tok // 8
    lag, late = 2, n // 2 + 1

    def keys(ref, c):
        return ref[pl.ds(pl.multiple_of(c * tok, LANES), tok), :]

    def q_rows(pair, g):
        return pl.ds(pl.multiple_of((pair * group + g) * krows, krows), krows)

    def do_rows(pair, g):
        return pl.ds(pl.multiple_of(do0 + (pair * group + g) * krows, krows), krows)

    def doc_starts(i):
        return jnp.concatenate([first_ref[i][0:1]] * group, axis=1)

    def score(i, pair, c, top, diagonal):
        t = dot_nn(keys(kn, c), rhsq[pair]) * score_mul
        kpos = lax.broadcasted_iota(jnp.int32, (tok, width), 0)
        keep = kpos >= doc_starts(i) - c * tok
        if diagonal:
            qpos = lax.broadcasted_iota(jnp.int32, (1, tok), 1)
            keep = keep & (kpos <= jnp.concatenate([qpos] * group, axis=1))
        t = jnp.where(keep, t, -jnp.inf)
        pbuf[pair, c] = t
        return jnp.maximum(top, jnp.max(t.reshape(grp, 8, width), axis=0))

    def value(pair, c, top, total):
        p = jnp.exp2(pbuf[pair, c] - top)
        oacc[...] += dot_nn(gall[0, c, kv0 + krows:rows, :], p.astype(BF))
        return total + jnp.sum(p.reshape(grp, 8, width), axis=0)

    def grad(pair, c):
        p = jnp.exp2(pbuf[pair, c] - stats[pair, 0:1])
        dp = dot_nn(keys(vn, c), rhsd[pair])
        ds = (p * (dp - stats[pair, 8:9])).astype(BF)
        dqacc[...] += dot_nn(gall[0, c, kv0:kv0 + krows, :], ds)
        pb = p.astype(BF)
        spans = [(slice(j * mcol, (j + 1) * mcol), slice(j * tok, (j + 1) * tok)) for j in range(width // mcol)]
        for qs, place in spans:
            woa[0, :, place] = ds[:, qs].T
            wob[0, :, place] = pb[:, qs].T
        dkacc[c] += sum(dot_nn(rhsq[pair, :, qs], woa[0, :, place]) for qs, place in spans)
        dvacc[c] += sum(dot_nn(rhsd[pair, :, qs], wob[0, :, place]) for qs, place in spans)

    def finish_dq(i, pair):
        dq = (dqacc[...] * scale).astype(BF)
        for g in range(group):
            gall[0, i, do_rows(pair, g), :] = dq[:, g * tok:(g + 1) * tok]

    def tile_done(i):
        @pl.when(i == 0)
        def _():
            for t in range(n - 1):
                p_direct(t).wait_send()
            for t in range(2):
                p_second(t).wait_send()
            for peer in (right, left):
                pl.semaphore_signal(free_far, inc=1, device_id={'cp': peer}, device_id_type=pl.DeviceIdType.MESH)
            pl.semaphore_signal(free_par, inc=1, device_id={'cp': partner}, device_id_type=pl.DeviceIdType.MESH)
            pl.semaphore_wait(free_near, 2)

        send_own(0, i)

        @pl.when(i == 1)
        def _():
            relay_columns(0)

        @pl.when(i == 3)
        def _():
            send_columns(1)

        @pl.when(i == 5)
        def _():
            relay_columns(1)

        @pl.when(i == lag)
        def _():
            pl.semaphore_wait(free_far, 2)

        @pl.when((i >= lag) & (i < late))
        def _():
            serve_near(i - lag)

        @pl.when(i == n - 1)
        def _():
            serve_near(i - 1)

    def item_step(m, carry):
        i, pair = m // 2, m % 2
        last = 1 - pair
        top0 = jnp.full((8, width), -jnp.inf, F32)

        for g in range(group):
            lanes = slice(g * tok, (g + 1) * tok)
            rhsq[pair, :, lanes] = gall[0, i, q_rows(pair, g), :]
            rhsd[pair, :, lanes] = gall[0, i, do_rows(pair, g), :]
        dqacc[...] = jnp.zeros_like(dqacc)

        def both_step(c, top):
            grad(last, c)
            return score(i, pair, c, top, False)

        top = lax.fori_loop(0, i, both_step, top0)
        stats[pair, 16:24] = top

        @pl.when(pair == 1)
        def _():
            grad(last, i)
            stats[pair, 16:24] = score(i, pair, i, stats[pair, 16:24], True)

        @pl.when(pair == 0)
        def _():
            stats[pair, 16:24] = score(i, pair, i, stats[pair, 16:24], True)

        @pl.when(m >= 1)
        def _():
            finish_dq((m - 1) // 2, last)

        top = jnp.max(stats[pair, 16:24], axis=0, keepdims=True)
        oacc[...] = jnp.zeros_like(oacc)
        def two_values(c, total):
            return value(pair, 2 * c + 1, top, value(pair, 2 * c, top, total))

        stats[pair, 16:24] = lax.fori_loop(0, (i + 1) // 2, two_values, jnp.zeros((8, width), F32))

        @pl.when(i % 2 == 0)
        def _():
            stats[pair, 16:24] = value(pair, i, top, stats[pair, 16:24])

        total = stats[pair, 16:24]
        total = jnp.sum(total, axis=0, keepdims=True)
        o_blk = (oacc[...] * (1.0 / total)).astype(BF)
        stats[pair, 0:8] = jnp.broadcast_to(top + jnp.log2(total), (8, width))
        delta = jnp.sum(rhsd[pair].astype(F32) * o_blk.astype(F32), axis=0, keepdims=True)
        stats[pair, 8:16] = jnp.broadcast_to(delta, (8, width))
        for g in range(group):
            gall[0, i, q_rows(pair, g), :] = o_blk[:, g * tok:(g + 1) * tok]

        @pl.when((pair == 0) & (i >= 1))
        def _():
            tile_done(i - 1)

        @pl.when((pair == 1) & (i >= late))
        def _():
            serve_near(i - lag)
        return carry

    lax.fori_loop(0, n * heads // group, item_step, 0)
    dqacc[...] = jnp.zeros_like(dqacc)

    def last_step(c, carry):
        grad(1, c)
        return carry

    lax.fori_loop(0, n, last_step, 0)
    finish_dq(n - 1, 1)
    tile_done(n - 1)
    for c in range(n):
        gall[0, c, kv0:kv0 + krows, :] = (dkacc[c] * scale).astype(BF)
        gall[0, c, kv0 + krows:rows, :] = dvacc[c].astype(BF)
    for j in range(2):
        send_own(1, j)
    for kind in range(3):
        for copy in load(kind, 0, 0):
            copy.start()
    pbuf[0, 0:6] = jnp.zeros((6, tok, width), F32)

    for a in range(2):
        x_own(a).wait()
        for t in range(n - 1):
            x_direct(a, t).wait_recv()

    near = n - 2
    spare = tok - qrows

    def rounded(acc, buf, out, sem):
        for j, cols in parts:
            wide = pbuf[0, acc + j, :, 0:cols.stop - cols.start].astype(BF)
            buf[0, :, cols] = wide[0:qrows]
            buf[1, 0:spare, cols] = wide[qrows:tok]
        return [pltpu.make_async_copy(buf.at[0], out.at[pl.ds(0, qrows)], lsem.at[sem]),
                pltpu.make_async_copy(buf.at[1, pl.ds(0, spare)], out.at[pl.ds(qrows, spare)], lsem.at[sem + 1])]

    def closing_step(r, carry):
        @pl.when(r == 1)
        def _():
            arrived_tiles(4)

        @pl.when(r == 2)
        def _():
            serve_near(n - 1)

        @pl.when(r == 4)
        def _():
            pl.semaphore_wait(free_par, 1)
            for j in range(n - 2 * lag):
                serve_far(j)
            arrived_tiles(5)

        @pl.when(r == 5)
        def _():
            arrived_tiles(6)

        @pl.when(r == near)
        def _():
            serve_near_kv()

        @pl.when(r == near + 1)
        def _():
            arrived_kv(4)

        @pl.when(r == near + 4)
        def _():
            arrived_kv(5)
            arrived_kv(6)

        @pl.when(r == 2 * near)
        def _():
            for a in range(2):
                for t in range(n - 1):
                    x_direct(a, t).wait_send()
                for t in range(2):
                    x_second(a, t).wait_send()
            for t in range(n - 1):
                seg_copy(t).wait_send()
            for j in range(n):
                own_right(0, j).wait_send()
                own_left(0, j).wait_send()
                for slot in range(3):
                    to_partner(slot, 0, j).wait_send()
            for j in range(n - 2 * lag):
                relay_plus(0, j).wait_send()
                relay_minus(0, j).wait_send()
            for j in range(n - 2 * lag, n):
                serve_far(j)

        @pl.when(r == 2 * near + 1)
        def _():
            arrived_tiles(7)

        @pl.when((r < near) | ((r >= 2 * near) & (r < 2 * near + 2)))
        def _():
            order = r - near * (r // (2 * near))
            closing_part(0, order)
            closing_part(1, order)

        @pl.when((r >= near) & (r < 2 * near))
        def _():
            closing_part(2, r - near)
        return carry

    lax.fori_loop(0, 2 * near + 2, closing_step, 0)

    def kv_rows(slot):
        return jnp.concatenate([gall[slot, j, kv0:rows, :] for j in range(n)], axis=1)

    out_y = rounded(0, woa, y_ref, 2)
    for copy in out_y + load(2, n - 1, 1):
        copy.start()
    for copy in load(2, n - 2, 0) + load(2, n - 1, 1) + save(2, n - 4, 0) + save(2, n - 3, 1):
        copy.wait()
    serve_far_kv()
    stage(2, 0)[...] = dot_nn(kv_rows(3), xc[...])
    for copy in save(2, n - 2, 0):
        copy.start()
    arrived_kv(7)
    out_dx = []
    for j, cols in parts:
        far = jnp.concatenate([gall[slot, me, kv0:rows, :] for slot in (3, 7)], axis=0)
        size = cols.stop - cols.start
        total = pbuf[0, 3 + j, :, 0:size] + dot_tn(far, woc[:, :, cols].reshape(4 * krows, size))
        wide = total.astype(BF)
        wob[0, :, cols] = wide[0:qrows]
        wob[1, 0:spare, cols] = wide[qrows:tok]
        where = pl.ds(cols.start, size)
        out_dx += [pltpu.make_async_copy(wob.at[0, :, where], dx_ref.at[pl.ds(0, qrows), where], dxsem.at[j, 0]),
                   pltpu.make_async_copy(wob.at[1, pl.ds(0, spare), where], dx_ref.at[pl.ds(qrows, spare), where], dxsem.at[j, 1])]
        for copy in out_dx[-2:]:
            copy.start()
    stage(2, 1)[...] = dot_nn(kv_rows(7), xc[...])
    for copy in save(2, n - 1, 1):
        copy.start()
    for kind in range(3):
        for order in (n - 2, n - 1):
            for copy in save(kind, order, order % 2):
                copy.wait()
    for copy in out_y + out_dx:
        copy.wait()
    for j in range(n):
        to_partner(3, 0, j).wait_send()
    for j in range(n - 2 * lag, n):
        relay_plus(0, j).wait_send()
        relay_minus(0, j).wait_send()
    for j in range(2):
        for slot in range(4):
            to_partner(slot, 1, j).wait_send()
        own_right(1, j).wait_send()
        own_left(1, j).wait_send()
    relay_plus(1, 0).wait_send()
    relay_minus(1, 1).wait_send()


def attention_layer(n, x_act, dy_act, seg, wq, wk, wv, wo):
    tok, model = x_act.shape
    qrows, krows = wq.shape[0] // n, wk.shape[0] // n
    rows = 2 * qrows + 2 * krows
    total = n * tok
    mcol = model // n
    group = 2
    width = group * tok
    vmem = pl.BlockSpec(memory_space=pltpu.VMEM)
    anym = pl.BlockSpec(memory_space=pl.ANY)
    dma = pltpu.SemaphoreType.DMA
    return pl.pallas_call(
        functools.partial(main_kernel, (n, qrows, krows, tok, krows ** -0.5)),
        out_shape=(jax.ShapeDtypeStruct((tok, model), BF), jax.ShapeDtypeStruct((tok, model), BF),
                   jax.ShapeDtypeStruct((wq.shape[0], mcol), F32), jax.ShapeDtypeStruct((wk.shape[0], mcol), F32),
                   jax.ShapeDtypeStruct((wv.shape[0], mcol), F32), jax.ShapeDtypeStruct((wo.shape[0], mcol), F32)),
        in_specs=[anym, anym, vmem, anym, anym, anym, anym],
        out_specs=(anym,) * 6,
        scratch_shapes=[
            pltpu.VMEM((8, tok), jnp.int32), pltpu.VMEM((n, 8, tok), jnp.int32), pltpu.VMEM((n, 8, tok), jnp.int32),
            pltpu.VMEM((total, krows), BF), pltpu.VMEM((total, krows), BF),
            pltpu.VMEM((2, n, tok, width), F32),
            pltpu.VMEM((2, krows, width), BF), pltpu.VMEM((2, krows, width), BF),
            pltpu.VMEM((2, 24, width), F32),
            pltpu.VMEM((krows, width), F32), pltpu.VMEM((krows, width), F32),
            pltpu.VMEM((n, krows, tok), F32), pltpu.VMEM((n, krows, tok), F32),
            pltpu.VMEM((n, n, rows, tok), BF),
            pltpu.VMEM((total, mcol), BF), pltpu.VMEM((total, mcol), BF),
            pltpu.VMEM((2, 2, tok, mcol), BF),
            pltpu.VMEM((2, qrows, model), BF), pltpu.VMEM((2, qrows, model), BF), pltpu.VMEM((2, 2 * krows, model), BF),
            dma((4, 2)), dma((4, 2)),
            dma((2, 2, n)), dma((2, 2, n)), dma((4, 2, n)), dma((8, 2, n)),
            dma((2, n)), dma((2, n)), dma((2, 2)), dma((2, 2)), dma((6,)), dma((3, 2)), dma((2, n)),
            dma((n,)), dma((n,)), dma((2,)), dma((2,)), dma((n,)), dma((n,)),
            pltpu.SemaphoreType.REGULAR, pltpu.SemaphoreType.REGULAR, pltpu.SemaphoreType.REGULAR,
        ],
        compiler_params=pltpu.CompilerParams(collective_id=0, has_side_effects=True, vmem_limit_bytes=VMEM_MAX),
        name='attention_layer',
    )(x_act, dy_act, seg, wq, wk, wv, wo)


def copy_out(arrays):
    pieces = 4
    count = len(arrays)

    def kernel(*refs):
        src, dst, buf = refs[:count], refs[count:2 * count], refs[2 * count:3 * count]
        insem, outsem = refs[3 * count:]
        loads, stores = [], []
        for k, array in enumerate(arrays):
            size = array.shape[0] // pieces
            for p in range(pieces):
                rows = pl.ds(p * size, size)
                loads.append(pltpu.make_async_copy(src[k].at[rows], buf[k].at[rows], insem.at[k, p]))
                stores.append(pltpu.make_async_copy(buf[k].at[rows], dst[k].at[rows], outsem.at[k, p]))
        for copy in loads:
            copy.start()
        for copy, store in zip(loads, stores):
            copy.wait()
            store.start()
        for store in stores:
            store.wait()

    anym = pl.BlockSpec(memory_space=pl.ANY)
    return pl.pallas_call(
        kernel,
        out_shape=tuple(jax.ShapeDtypeStruct(a.shape, a.dtype) for a in arrays),
        in_specs=[anym] * count, out_specs=(anym,) * count,
        scratch_shapes=[pltpu.VMEM(a.shape, a.dtype) for a in arrays]
        + [pltpu.SemaphoreType.DMA((count, pieces)), pltpu.SemaphoreType.DMA((count, pieces))],
        compiler_params=pltpu.CompilerParams(vmem_limit_bytes=VMEM_MAX),
        name='copy_out',
    )(*arrays)


def solution(mesh):
    n = mesh.shape['cp']
    row_spec = P(('dp', 'cp'), None)
    tok_spec = P(('dp', 'cp'))
    weight_spec = P(None, None, None)
    grad_spec = P(('dp', 'cp'), None, None)

    def local_step(x_act, seg_ids, w_q, w_k, w_v, w_o, dy_act):
        model, q_heads, head_dim = w_q.shape
        kv_heads = w_k.shape[1]
        assert kv_heads == n and x_act.shape[0] % LANES == 0

        def flat(w):
            return w.transpose(1, 2, 0).reshape(w.shape[1] * head_dim, model)

        def unflat(g, heads):
            return g.reshape(heads, head_dim, g.shape[1]).transpose(2, 0, 1)

        wq, wk, wv, wo = flat(w_q), flat(w_k), flat(w_v), flat(w_o)
        y_out, dx_out, dwq, dwk, dwv, dwo = copy_out(attention_layer(n, x_act, dy_act, seg_ids, wq, wk, wv, wo))
        return (y_out, dx_out, unflat(dwq, q_heads), unflat(dwk, kv_heads), unflat(dwv, kv_heads), unflat(dwo, q_heads))

    return jax.shard_map(local_step, mesh=mesh,
                         in_specs=(row_spec, tok_spec, weight_spec, weight_spec, weight_spec, weight_spec, row_spec),
                         out_specs=(row_spec, row_spec, grad_spec, grad_spec, grad_spec, grad_spec),
                         check_vma=False)
```

```python
import functools

import jax
import jax.numpy as jnp
from jax import lax
from jax.experimental import pallas as pl
from jax.experimental.pallas import tpu as pltpu
from jax.sharding import PartitionSpec as P

BF = jnp.bfloat16
F32 = jnp.float32
LANES = 128
LOG2E = 1.4426950408889634
VMEM_MAX = 67043328


def rdma(src, dst, send_sem, recv_sem, peer):
    return pltpu.make_async_remote_copy(src_ref=src, dst_ref=dst, send_sem=send_sem, recv_sem=recv_sem,
                                        device_id={'cp': peer}, device_id_type=pl.DeviceIdType.MESH)


def dot_nt(left, right):
    return lax.dot_general(left, right, (((1,), (1,)), ((), ())), preferred_element_type=F32)


def dot_tn(left, right):
    return lax.dot_general(left, right, (((0,), (0,)), ((), ())), preferred_element_type=F32)


def dot_nn(left, right):
    return lax.dot_general(left, right, (((1,), (0,)), ((), ())), preferred_element_type=F32)


def pick(index, values):
    out = values[0]
    for k in range(1, len(values)):
        out = jnp.where(index == k, values[k], out)
    return out


def main_kernel(dims, x_ref, dy_ref, seg_ref, wq_ref, wk_ref, wv_ref, wo_ref,
                y_ref, dx_ref, dwq_ref, dwk_ref, dwv_ref, dwo_ref,
                seg_mine, seg_all, first_ref, kvn, pbuf, rhsq, rhsd, stats, oacc, dqacc, dkacc, dvacc, gall, xc, dyc, xrel,
                woa, wob, woc, wsem, outsem, osem, relsem, parsem, rsem, xsend, xrecv, xfirst, xsecond, lsem, dxsem, xload,
                psend, precv, pfirst, psecond, gsend, grecv, free_near, free_far, free_par):
    n, qrows, krows, tok, scale = dims
    chips = n // 2
    heads = qrows // krows
    width = rhsq.shape[2]
    group = width // tok
    me = lax.axis_index('cp')
    chip, core = me // 2, me % 2
    sgn = 1 - 2 * core
    rows = 2 * qrows + 2 * krows
    model = x_ref.shape[1]
    mcol = xc.shape[1]
    do0, kv0 = qrows, 2 * qrows

    def device(chip_off, flip):
        return ((chip + chip_off + chips) % chips) * 2 + (core + flip) % 2

    right, left, partner = device(1, 0), device(-1, 0), device(0, 1)
    dests = [device(2, 0), device(2, 1), device(-sgn, 0), device(-sgn, 1), device(sgn, 0), device(sgn, 1), partner]
    ahead = dests[4]
    relay_from = device(-sgn, 0)

    barrier = pltpu.get_barrier_semaphore()
    for peer in dests:
        pl.semaphore_signal(barrier, inc=1, device_id={'cp': peer}, device_id_type=pl.DeviceIdType.MESH)

    sides = ((x_ref, xc), (dy_ref, dyc))

    def columns(ref, dst):
        return ref.at[:, pl.ds(pl.multiple_of(dst * mcol, LANES), mcol)]

    def token_rows(ref, src):
        return ref.at[pl.ds(pl.multiple_of(src * tok, LANES), tok)]

    def x_first(a, t):
        return rdma(columns(sides[a][0], dests[t]), xrel.at[a, t], xsend.at[a, t], xfirst.at[a, t], ahead)

    def x_second(a, t):
        return rdma(xrel.at[a, t], token_rows(sides[a][1], relay_from), xsecond.at[a, t], xrecv.at[a, t], device(sgn, t))

    def x_direct(a, t):
        return rdma(columns(sides[a][0], dests[t]), token_rows(sides[a][1], me), xsend.at[a, t], xrecv.at[a, t], dests[t])

    def send_columns(a):
        for t in range(n - 1):
            if t != 2:
                (x_first if t < 2 else x_direct)(a, t).start()

    def relay_columns(a):
        for t in range(2):
            x_first(a, t).wait_recv()
            x_second(a, t).start()

    def x_own(a):
        return pltpu.make_async_copy(columns(sides[a][0], me), token_rows(sides[a][1], me), lsem.at[a])

    def view(slot, part, j):
        if part == 0:
            return gall.at[slot, j, pl.ds(0, kv0)]
        return gall.at[slot, pl.ds(j * (n // 2), n // 2), pl.ds(kv0, 2 * krows)]

    def own_right(part, j):
        return rdma(view(0, part, j), view(1, part, j), osem.at[0, part, j], rsem.at[1, part, j], right)

    def own_left(part, j):
        return rdma(view(0, part, j), view(2, part, j), osem.at[1, part, j], rsem.at[2, part, j], left)

    def relay_plus(part, j):
        src, dst = view(1, part, j), view(3, part, j)
        if part == 0:
            src, dst = src.at[pl.ds(0, do0)], dst.at[pl.ds(0, do0)]
        return rdma(src, dst, relsem.at[0, part, j], rsem.at[3, part, j], right)

    def relay_minus(part, j):
        src, dst = view(2, part, j), view(3, part, j)
        if part == 0:
            src, dst = src.at[pl.ds(do0, do0)], dst.at[pl.ds(do0, do0)]
        return rdma(src, dst, relsem.at[1, part, j], rsem.at[0, part, j], left)

    def to_partner(slot, part, j):
        return rdma(view(slot, part, j), view(4 + slot, part, j), parsem.at[slot, part, j], rsem.at[4 + slot, part, j], partner)

    def send_own(part, j):
        own_right(part, j).start()
        own_left(part, j).start()
        to_partner(0, part, j).start()

    def serve_near(j):
        own_right(0, j).wait_recv()
        relay_plus(0, j).start()
        to_partner(1, 0, j).start()
        own_left(0, j).wait_recv()
        relay_minus(0, j).start()
        to_partner(2, 0, j).start()

    def serve_near_kv():
        own_right(1, 0).wait_recv()
        relay_plus(1, 0).start()
        own_left(1, 1).wait_recv()
        relay_minus(1, 1).start()
        to_partner(1, 1, 0).start()
        to_partner(2, 1, 1).start()
        own_right(1, 1).wait_recv()
        to_partner(1, 1, 1).start()
        own_left(1, 0).wait_recv()
        to_partner(2, 1, 0).start()

    def serve_far(j):
        relay_plus(0, j).wait_recv()
        relay_minus(0, j).wait_recv()
        to_partner(3, 0, j).start()

    def serve_far_kv():
        relay_plus(1, 0).wait_recv()
        to_partner(3, 1, 0).start()
        relay_minus(1, 1).wait_recv()
        to_partner(3, 1, 1).start()

    def arrived_tiles(slot):
        for j in range(n):
            to_partner(slot - 4, 0, j).wait_recv()

    def arrived_kv(slot):
        for j in range(2):
            to_partner(slot - 4, 1, j).wait_recv()

    slot_table = (0, 4, 1, 2, 5, 6, 3, 7)
    off_table = (0, 0, chips - 1, 1, chips - 1, 1, 2, 2)
    flip_table = (0, 1, 0, 0, 1, 1, 0, 1)

    def source_of(order):
        return ((chip + pick(order, off_table)) % chips) * 2 + (core + pick(order, flip_table)) % 2

    def load(kind, order, buf):
        src = source_of(order)
        if kind == 0:
            return [pltpu.make_async_copy(wo_ref.at[pl.ds(src * qrows, qrows)], woa.at[buf], wsem.at[0, buf])]
        if kind == 1:
            return [pltpu.make_async_copy(wq_ref.at[pl.ds(src * qrows, qrows)], wob.at[buf], wsem.at[1, buf])]
        return [pltpu.make_async_copy(wk_ref.at[pl.ds(src * krows, krows)], woc.at[buf, pl.ds(0, krows)], wsem.at[2, buf]),
                pltpu.make_async_copy(wv_ref.at[pl.ds(src * krows, krows)], woc.at[buf, pl.ds(krows, krows)], wsem.at[3, buf])]

    def stage(kind, buf):
        if kind < 2:
            return pbuf.at[0, 6 + kind, pl.ds(0, qrows), pl.ds(pl.multiple_of(buf * mcol, LANES), mcol)]
        return pbuf.at[0, 6, pl.ds(pl.multiple_of(buf * 2 * krows, 8), 2 * krows), pl.ds(2 * mcol, mcol)]

    def save(kind, order, buf):
        src = source_of(order)
        if kind == 0:
            return [pltpu.make_async_copy(stage(0, buf), dwo_ref.at[pl.ds(src * qrows, qrows)], outsem.at[0, buf])]
        if kind == 1:
            return [pltpu.make_async_copy(stage(1, buf), dwq_ref.at[pl.ds(src * qrows, qrows)], outsem.at[1, buf])]
        both = stage(2, buf)
        return [pltpu.make_async_copy(both.at[pl.ds(0, krows)], dwk_ref.at[pl.ds(src * krows, krows)], outsem.at[2, buf]),
                pltpu.make_async_copy(both.at[pl.ds(krows, krows)], dwv_ref.at[pl.ds(src * krows, krows)], outsem.at[3, buf])]

    parts = [(j, slice(j * width, min((j + 1) * width, model))) for j in range(-(-model // width))]
    kinds = ((0, do0, woa, dyc, 0), (do0, kv0, wob, xc, 3), (kv0, rows, woc, xc, 3))

    def closing_part(kind, order):
        row0, row1, wbuf, other, acc = kinds[kind]
        buf = order % 2
        slot = pick(order, slot_table)
        for copy in load(kind, order, buf):
            copy.wait()

        @pl.when(order < n - 1)
        def _():
            for copy in load(kind, order + 1, 1 - buf):
                copy.start()

        @pl.when(order >= 2)
        def _():
            for copy in save(kind, order - 2, buf):
                copy.wait()

        @pl.when(order >= 0)
        def _():
            wide = jnp.concatenate([gall[slot, j, row0:row1, :] for j in range(n)], axis=1)
            stage(kind, buf)[...] = dot_nn(wide, other[...])

        for copy in save(kind, order, buf):
            copy.start()
        for j, cols in parts:
            @pl.when(order >= 0)
            def _():
                pbuf[0, acc + j, :, 0:cols.stop - cols.start] += dot_tn(gall[slot, me, row0:row1, :], wbuf[buf, :, cols])

    def block_copies(step, buf):
        pair, flip = step // 2, (step + step // 6) % 2
        off = 2 - 3 * pair + 5 * (pair // 2) + 2 * (pair // 3)
        dst = ((chip + sgn * off + chips) % chips) * 2 + (core + flip) % 2
        return [
            pltpu.make_async_copy(wo_ref.at[pl.ds(dst * qrows, qrows)], woa.at[buf], wsem.at[0, buf]),
            pltpu.make_async_copy(wq_ref.at[pl.ds(dst * qrows, qrows)], wob.at[buf], wsem.at[1, buf]),
            pltpu.make_async_copy(wk_ref.at[pl.ds(dst * krows, krows)], woc.at[buf, pl.ds(0, krows)], wsem.at[2, buf]),
            pltpu.make_async_copy(wv_ref.at[pl.ds(dst * krows, krows)], woc.at[buf, pl.ds(krows, krows)], wsem.at[3, buf]),
        ]

    def p_first(t):
        return rdma(gall.at[3, t], gall.at[7, t], psend.at[t], pfirst.at[t], ahead)

    def p_second(t):
        return rdma(gall.at[7, t], gall.at[0, relay_from], psecond.at[t], precv.at[t], device(sgn, t))

    def p_direct(t):
        return rdma(gall.at[3, t], gall.at[0, me], psend.at[t], precv.at[t], dests[t])

    def seg_copy(t):
        row = pl.ds(0, 1)
        return rdma(seg_mine.at[row], seg_all.at[me, row], gsend.at[t], grecv.at[t], dests[t])

    xcols = [(c, c * tok, min(tok, model - c * tok)) for c in range(-(-model // tok))]

    def x_loads(a):
        return [pltpu.make_async_copy(sides[a][0].at[:, pl.ds(lo, size)], gall.at[1 + a, c, pl.ds(0, tok), pl.ds(0, size)],
                                      xload.at[a, c]) for c, lo, size in xcols]

    def x_whole(a):
        return jnp.concatenate([gall[1 + a, c, 0:tok, 0:size] for c, lo, size in xcols], axis=1)

    for copy in x_loads(0):
        copy.start()
    for copy in block_copies(0, 0):
        copy.start()
    for copy in x_loads(1):
        copy.start()
    for a in range(2):
        x_own(a).start()
    seg_mine[...] = jnp.broadcast_to(seg_ref[...].reshape(1, tok), seg_mine.shape)
    pl.semaphore_wait(barrier, n - 1)
    for a in range(2):
        x_direct(a, 2).start()
    for t in range(n - 1):
        seg_copy(t).start()
    seg_all[me] = seg_mine[...]
    for copy in x_loads(0) + x_loads(1):
        copy.wait()

    def project_step(step, carry):
        buf = step % 2

        @pl.when(step < n - 1)
        def _():
            for copy in block_copies(step + 1, 1 - buf):
                copy.start()

        for copy in block_copies(step, buf):
            copy.wait()
        slot = 3 - 3 * (step // (n - 1))
        place = step + (me - step) * (step // (n - 1))
        gall[slot, place, 0:qrows] = dot_nt(wob[buf], x_whole(0)).astype(BF)
        gall[slot, place, kv0:rows] = dot_nt(woc[buf], x_whole(0)).astype(BF)
        gall[slot, place, do0:kv0] = dot_nt(woa[buf], x_whole(1)).astype(BF)
        for t in range(n - 1):
            @pl.when(step == t)
            def _():
                (p_first if t < 2 else p_direct)(t).start()
        return carry

    lax.fori_loop(0, n, project_step, 0)
    for peer in (right, left):
        pl.semaphore_signal(free_near, inc=1, device_id={'cp': peer}, device_id_type=pl.DeviceIdType.MESH)
    for t in range(2):
        p_first(t).wait_recv()
        p_second(t).start()
    send_columns(0)

    for t in range(n - 1):
        seg_copy(t).wait_recv()
    row_id = lax.broadcasted_iota(jnp.int32, (n, tok), 0)
    lane_id = lax.broadcasted_iota(jnp.int32, (n, tok), 1)
    seg = jnp.zeros((n, tok), jnp.int32)
    for d in range(n):
        seg = jnp.where(row_id == d, seg_all[d, 0:1], seg)
    before = jnp.where(lane_id == 0, pltpu.roll(pltpu.roll(seg, 1, 1), 1, 0), pltpu.roll(seg, 1, 1))
    pos = row_id * tok + lane_id
    best = jnp.where((seg != before) & (pos > 0), pos, 0)
    shift = 1
    while shift < tok:
        best = jnp.maximum(best, jnp.where(lane_id >= shift, pltpu.roll(best, shift, 1), 0))
        shift *= 2
    end = jnp.broadcast_to(best[:, tok - 1:tok], (n, tok))
    carry_max = jnp.where(row_id >= 1, pltpu.roll(end, 1, 0), 0)
    shift = 1
    while shift < n:
        carry_max = jnp.maximum(carry_max, jnp.where(row_id >= shift, pltpu.roll(carry_max, shift, 0), 0))
        shift *= 2
    best = jnp.maximum(best, carry_max)
    for d in range(n):
        first_ref[d] = jnp.broadcast_to(best[d:d + 1], (8, tok))
    dkacc[...] = jnp.zeros_like(dkacc)
    dvacc[...] = jnp.zeros_like(dvacc)
    rhsq[...] = jnp.zeros_like(rhsq)
    rhsd[...] = jnp.zeros_like(rhsd)
    for t in range(n - 1):
        p_direct(t).wait_recv()

    def transpose_tile(c, carry):
        kvn[pl.ds(pl.multiple_of(c * tok, LANES), tok), :] = gall[0, c, kv0:rows, :].T
        return carry

    lax.fori_loop(0, n, transpose_tile, 0)
    score_mul = scale * LOG2E
    grp = tok // 8
    lag = 2

    def keys(c):
        return kvn[pl.ds(pl.multiple_of(c * tok, LANES), tok), :]

    def q_rows(pair, g):
        return pl.ds(pl.multiple_of((pair * group + g) * krows, krows), krows)

    def do_rows(pair, g):
        return pl.ds(pl.multiple_of(do0 + (pair * group + g) * krows, krows), krows)

    def doc_starts(i):
        return jnp.concatenate([first_ref[i][0:1]] * group, axis=1)

    def score(i, pair, c, top, diagonal):
        t = dot_nn(keys(c), rhsq[pair]) * score_mul
        kpos = lax.broadcasted_iota(jnp.int32, (tok, width), 0)
        keep = kpos >= doc_starts(i) - c * tok
        if diagonal:
            qpos = lax.broadcasted_iota(jnp.int32, (1, tok), 1)
            keep = keep & (kpos <= jnp.concatenate([qpos] * group, axis=1))
        t = jnp.where(keep, t, -jnp.inf)
        pbuf[pair, c] = t
        return jnp.maximum(top, jnp.max(t.reshape(grp, 8, width), axis=0))

    def value(pair, c, top, total):
        p = jnp.exp2(pbuf[pair, c] - top)
        oacc[...] += dot_nn(gall[0, c, kv0 + krows:rows, :], p.astype(BF))
        return total + jnp.sum(p.reshape(grp, 8, width), axis=0)

    def grad(pair, c):
        p = jnp.exp2(pbuf[pair, c] - stats[pair, 0:1])
        dp = dot_nn(keys(c), rhsd[pair])
        ds = (p * (dp - stats[pair, 8:9])).astype(BF)
        dqacc[...] += dot_nn(gall[0, c, kv0:kv0 + krows, :], ds)
        pb = p.astype(BF)
        spans = [(slice(j * mcol, (j + 1) * mcol), slice(j * tok, (j + 1) * tok)) for j in range(width // mcol)]
        for qs, place in spans:
            woa[0, :, place] = ds[:, qs].T
            wob[0, :, place] = pb[:, qs].T
        dkacc[c] += sum(dot_nn(rhsq[pair, 0:krows, qs], woa[0, :, place]) for qs, place in spans)
        dvacc[c] += sum(dot_nn(rhsd[pair, krows:2 * krows, qs], wob[0, :, place]) for qs, place in spans)

    def finish_dq(i, pair):
        dq = (dqacc[...] * scale).astype(BF)
        for g in range(group):
            gall[0, i, do_rows(pair, g), :] = dq[:, g * tok:(g + 1) * tok]

    def tile_done(i):
        @pl.when(i == 0)
        def _():
            for t in range(n - 1):
                p_direct(t).wait_send()
            for t in range(2):
                p_second(t).wait_send()
            for peer in (right, left):
                pl.semaphore_signal(free_far, inc=1, device_id={'cp': peer}, device_id_type=pl.DeviceIdType.MESH)
            pl.semaphore_signal(free_par, inc=1, device_id={'cp': partner}, device_id_type=pl.DeviceIdType.MESH)
            pl.semaphore_wait(free_near, 2)

        send_own(0, i)

        @pl.when(i == 1)
        def _():
            relay_columns(0)

        @pl.when(i == 3)
        def _():
            send_columns(1)

        @pl.when(i == 5)
        def _():
            relay_columns(1)

        @pl.when(i == lag)
        def _():
            pl.semaphore_wait(free_far, 2)

        @pl.when(i >= lag)
        def _():
            serve_near(i - lag)

    def item_step(m, carry):
        i, pair = m // 2, m % 2
        last = 1 - pair
        top0 = jnp.full((8, width), -jnp.inf, F32)

        for g in range(group):
            lanes = slice(g * tok, (g + 1) * tok)
            rhsq[pair, 0:krows, lanes] = gall[0, i, q_rows(pair, g), :]
            rhsd[pair, krows:2 * krows, lanes] = gall[0, i, do_rows(pair, g), :]
        dqacc[...] = jnp.zeros_like(dqacc)

        def both_step(c, top):
            grad(last, c)
            return score(i, pair, c, top, False)

        top = lax.fori_loop(0, i, both_step, top0)
        stats[pair, 16:24] = top

        @pl.when(pair == 1)
        def _():
            grad(last, i)
            stats[pair, 16:24] = score(i, pair, i, stats[pair, 16:24], True)

        @pl.when(pair == 0)
        def _():
            stats[pair, 16:24] = score(i, pair, i, stats[pair, 16:24], True)

        @pl.when(m >= 1)
        def _():
            finish_dq((m - 1) // 2, last)

        top = jnp.max(stats[pair, 16:24], axis=0, keepdims=True)
        oacc[...] = jnp.zeros_like(oacc)
        total = lax.fori_loop(0, i + 1, lambda c, acc: value(pair, c, top, acc), jnp.zeros((8, width), F32))
        total = jnp.sum(total, axis=0, keepdims=True)
        o_blk = (oacc[...] * (1.0 / total)).astype(BF)
        stats[pair, 0:8] = jnp.broadcast_to(top + jnp.log2(total), (8, width))
        delta = jnp.sum(rhsd[pair, krows:2 * krows].astype(F32) * o_blk.astype(F32), axis=0, keepdims=True)
        stats[pair, 8:16] = jnp.broadcast_to(delta, (8, width))
        for g in range(group):
            gall[0, i, q_rows(pair, g), :] = o_blk[:, g * tok:(g + 1) * tok]

        @pl.when((pair == 0) & (i >= 1))
        def _():
            tile_done(i - 1)
        return carry

    lax.fori_loop(0, n * heads // group, item_step, 0)
    dqacc[...] = jnp.zeros_like(dqacc)

    def last_step(c, carry):
        grad(1, c)
        return carry

    lax.fori_loop(0, n, last_step, 0)
    finish_dq(n - 1, 1)
    tile_done(n - 1)
    for c in range(n):
        gall[0, c, kv0:kv0 + krows, :] = (dkacc[c] * scale).astype(BF)
        gall[0, c, kv0 + krows:rows, :] = dvacc[c].astype(BF)
    for j in range(2):
        send_own(1, j)
    for kind in range(3):
        for copy in load(kind, 0, 0):
            copy.start()
    pbuf[0, 0:6] = jnp.zeros((6, tok, width), F32)

    for a in range(2):
        x_own(a).wait()
        for t in range(n - 1):
            x_direct(a, t).wait_recv()

    near = n - 2
    spare = tok - qrows

    def rounded(acc, buf, out, sem):
        for j, cols in parts:
            wide = pbuf[0, acc + j, :, 0:cols.stop - cols.start].astype(BF)
            buf[0, :, cols] = wide[0:qrows]
            buf[1, 0:spare, cols] = wide[qrows:tok]
        return [pltpu.make_async_copy(buf.at[0], out.at[pl.ds(0, qrows)], lsem.at[sem]),
                pltpu.make_async_copy(buf.at[1, pl.ds(0, spare)], out.at[pl.ds(qrows, spare)], lsem.at[sem + 1])]

    def closing_step(r, carry):
        @pl.when(r == 1)
        def _():
            arrived_tiles(4)

        @pl.when(r == 2)
        def _():
            for j in range(n - lag, n):
                serve_near(j)

        @pl.when(r == 4)
        def _():
            pl.semaphore_wait(free_par, 1)
            for j in range(n - 2 * lag):
                serve_far(j)
            arrived_tiles(5)

        @pl.when(r == 5)
        def _():
            arrived_tiles(6)

        @pl.when(r == near)
        def _():
            serve_near_kv()

        @pl.when(r == near + 1)
        def _():
            arrived_kv(4)

        @pl.when(r == near + 4)
        def _():
            arrived_kv(5)
            arrived_kv(6)

        @pl.when(r == 2 * near)
        def _():
            for a in range(2):
                for t in range(n - 1):
                    x_direct(a, t).wait_send()
                for t in range(2):
                    x_second(a, t).wait_send()
            for t in range(n - 1):
                seg_copy(t).wait_send()
            for j in range(n):
                own_right(0, j).wait_send()
                own_left(0, j).wait_send()
                for slot in range(3):
                    to_partner(slot, 0, j).wait_send()
            for j in range(n - 2 * lag):
                relay_plus(0, j).wait_send()
                relay_minus(0, j).wait_send()
            for j in range(n - 2 * lag, n):
                serve_far(j)

        @pl.when(r == 2 * near + 1)
        def _():
            arrived_tiles(7)

        @pl.when((r < near) | ((r >= 2 * near) & (r < 2 * near + 2)))
        def _():
            order = r - near * (r // (2 * near))
            closing_part(0, order)
            closing_part(1, order)

        @pl.when((r >= near) & (r < 2 * near))
        def _():
            closing_part(2, r - near)
        return carry

    lax.fori_loop(0, 2 * near + 2, closing_step, 0)

    def kv_rows(slot):
        return jnp.concatenate([gall[slot, j, kv0:rows, :] for j in range(n)], axis=1)

    out_y = rounded(0, woa, y_ref, 2)
    for copy in out_y + load(2, n - 1, 1):
        copy.start()
    for copy in load(2, n - 2, 0) + load(2, n - 1, 1) + save(2, n - 4, 0) + save(2, n - 3, 1):
        copy.wait()
    serve_far_kv()
    stage(2, 0)[...] = dot_nn(kv_rows(3), xc[...])
    for copy in save(2, n - 2, 0):
        copy.start()
    arrived_kv(7)
    out_dx = []
    for j, cols in parts:
        far = jnp.concatenate([gall[slot, me, kv0:rows, :] for slot in (3, 7)], axis=0)
        size = cols.stop - cols.start
        total = pbuf[0, 3 + j, :, 0:size] + dot_tn(far, woc[:, :, cols].reshape(4 * krows, size))
        wide = total.astype(BF)
        wob[0, :, cols] = wide[0:qrows]
        wob[1, 0:spare, cols] = wide[qrows:tok]
        where = pl.ds(cols.start, size)
        out_dx += [pltpu.make_async_copy(wob.at[0, :, where], dx_ref.at[pl.ds(0, qrows), where], dxsem.at[j, 0]),
                   pltpu.make_async_copy(wob.at[1, pl.ds(0, spare), where], dx_ref.at[pl.ds(qrows, spare), where], dxsem.at[j, 1])]
        for copy in out_dx[-2:]:
            copy.start()
    stage(2, 1)[...] = dot_nn(kv_rows(7), xc[...])
    for copy in save(2, n - 1, 1):
        copy.start()
    for j in range(n):
        to_partner(3, 0, j).wait_send()
    for j in range(n - 2 * lag, n):
        relay_plus(0, j).wait_send()
        relay_minus(0, j).wait_send()
    for j in range(2):
        for slot in range(4):
            to_partner(slot, 1, j).wait_send()
        own_right(1, j).wait_send()
        own_left(1, j).wait_send()
    relay_plus(1, 0).wait_send()
    relay_minus(1, 1).wait_send()
    for kind in range(3):
        for order in (n - 2, n - 1):
            for copy in save(kind, order, order % 2):
                copy.wait()
    for copy in out_y + out_dx:
        copy.wait()


def attention_layer(n, x_act, dy_act, seg, wq, wk, wv, wo):
    tok, model = x_act.shape
    qrows, krows = wq.shape[0] // n, wk.shape[0] // n
    rows = 2 * qrows + 2 * krows
    total = n * tok
    mcol = model // n
    group = 2
    width = group * tok
    vmem = pl.BlockSpec(memory_space=pltpu.VMEM)
    anym = pl.BlockSpec(memory_space=pl.ANY)
    dma = pltpu.SemaphoreType.DMA
    return pl.pallas_call(
        functools.partial(main_kernel, (n, qrows, krows, tok, krows ** -0.5)),
        out_shape=(jax.ShapeDtypeStruct((tok, model), BF), jax.ShapeDtypeStruct((tok, model), BF),
                   jax.ShapeDtypeStruct((wq.shape[0], mcol), F32), jax.ShapeDtypeStruct((wk.shape[0], mcol), F32),
                   jax.ShapeDtypeStruct((wv.shape[0], mcol), F32), jax.ShapeDtypeStruct((wo.shape[0], mcol), F32)),
        in_specs=[anym, anym, vmem, anym, anym, anym, anym],
        out_specs=(anym,) * 6,
        scratch_shapes=[
            pltpu.VMEM((8, tok), jnp.int32), pltpu.VMEM((n, 8, tok), jnp.int32), pltpu.VMEM((n, 8, tok), jnp.int32),
            pltpu.VMEM((total, 2 * krows), BF),
            pltpu.VMEM((2, n, tok, width), F32),
            pltpu.VMEM((2, 2 * krows, width), BF), pltpu.VMEM((2, 2 * krows, width), BF),
            pltpu.VMEM((2, 24, width), F32),
            pltpu.VMEM((krows, width), F32), pltpu.VMEM((krows, width), F32),
            pltpu.VMEM((n, krows, tok), F32), pltpu.VMEM((n, krows, tok), F32),
            pltpu.VMEM((n, n, rows, tok), BF),
            pltpu.VMEM((total, mcol), BF), pltpu.VMEM((total, mcol), BF),
            pltpu.VMEM((2, 2, tok, mcol), BF),
            pltpu.VMEM((2, qrows, model), BF), pltpu.VMEM((2, qrows, model), BF), pltpu.VMEM((2, 2 * krows, model), BF),
            dma((4, 2)), dma((4, 2)),
            dma((2, 2, n)), dma((2, 2, n)), dma((4, 2, n)), dma((8, 2, n)),
            dma((2, n)), dma((2, n)), dma((2, 2)), dma((2, 2)), dma((6,)), dma((3, 2)), dma((2, n)),
            dma((n,)), dma((n,)), dma((2,)), dma((2,)), dma((n,)), dma((n,)),
            pltpu.SemaphoreType.REGULAR, pltpu.SemaphoreType.REGULAR, pltpu.SemaphoreType.REGULAR,
        ],
        compiler_params=pltpu.CompilerParams(collective_id=0, has_side_effects=True, vmem_limit_bytes=VMEM_MAX),
        name='attention_layer',
    )(x_act, dy_act, seg, wq, wk, wv, wo)


def copy_out(arrays):
    pieces = 4
    count = len(arrays)

    def kernel(*refs):
        src, dst, buf = refs[:count], refs[count:2 * count], refs[2 * count:3 * count]
        insem, outsem = refs[3 * count:]
        loads, stores = [], []
        for k, array in enumerate(arrays):
            size = array.shape[0] // pieces
            for p in range(pieces):
                rows = pl.ds(p * size, size)
                loads.append(pltpu.make_async_copy(src[k].at[rows], buf[k].at[rows], insem.at[k, p]))
                stores.append(pltpu.make_async_copy(buf[k].at[rows], dst[k].at[rows], outsem.at[k, p]))
        for copy in loads:
            copy.start()
        for copy, store in zip(loads, stores):
            copy.wait()
            store.start()
        for store in stores:
            store.wait()

    anym = pl.BlockSpec(memory_space=pl.ANY)
    return pl.pallas_call(
        kernel,
        out_shape=tuple(jax.ShapeDtypeStruct(a.shape, a.dtype) for a in arrays),
        in_specs=[anym] * count, out_specs=(anym,) * count,
        scratch_shapes=[pltpu.VMEM(a.shape, a.dtype) for a in arrays]
        + [pltpu.SemaphoreType.DMA((count, pieces)), pltpu.SemaphoreType.DMA((count, pieces))],
        compiler_params=pltpu.CompilerParams(vmem_limit_bytes=VMEM_MAX),
        name='copy_out',
    )(*arrays)


def solution(mesh):
    n = mesh.shape['cp']
    row_spec = P(('dp', 'cp'), None)
    tok_spec = P(('dp', 'cp'))
    weight_spec = P(None, None, None)
    grad_spec = P(('dp', 'cp'), None, None)

    def local_step(x_act, seg_ids, w_q, w_k, w_v, w_o, dy_act):
        model, q_heads, head_dim = w_q.shape
        kv_heads = w_k.shape[1]
        assert kv_heads == n and x_act.shape[0] % LANES == 0

        def flat(w):
            return w.transpose(1, 2, 0).reshape(w.shape[1] * head_dim, model)

        def unflat(g, heads):
            return g.reshape(heads, head_dim, g.shape[1]).transpose(2, 0, 1)

        wq, wk, wv, wo = flat(w_q), flat(w_k), flat(w_v), flat(w_o)
        y_out, dx_out, dwq, dwk, dwv, dwo = copy_out(attention_layer(n, x_act, dy_act, seg_ids, wq, wk, wv, wo))
        return (y_out, dx_out, unflat(dwq, q_heads), unflat(dwk, kv_heads), unflat(dwv, kv_heads), unflat(dwo, q_heads))

    return jax.shard_map(local_step, mesh=mesh,
                         in_specs=(row_spec, tok_spec, weight_spec, weight_spec, weight_spec, weight_spec, row_spec),
                         out_specs=(row_spec, row_spec, grad_spec, grad_spec, grad_spec, grad_spec),
                         check_vma=False)
```
